32 devices in a mesh: ctx: 16 (over z, y, x), head: 2 (over core).
Axes of the slice: x: 2, y: 2, z: 4, core: 2. Of those that a mesh axis runs over, the one named last changes fastest.
Arguments:
- layer_in: float32 [2048, 768], P('ctx'), may hold values from -6 to 6
- encoded: bfloat16 [1024, 768], P('ctx'), may hold values from -6 to 6
- self_query: bfloat16 [768, 768], P('ctx', 'head'), may hold values from -0.02734375 to 0.02734375
- self_key: bfloat16 [768, 768], P('ctx', 'head'), may hold values from -0.21875 to 0.21875
- self_value: bfloat16 [768, 768], P('ctx', 'head'), may hold values from -0.21875 to 0.21875
- self_out: bfloat16 [768, 768], P('head', 'ctx'), may hold values from -4 to 4
- cross_query: bfloat16 [768, 768], P('ctx', 'head'), may hold values from -0.02734375 to 0.02734375
- cross_key: bfloat16 [768, 768], P('ctx', 'head'), may hold values from -0.21875 to 0.21875
- cross_value: bfloat16 [768, 768], P('ctx', 'head'), may hold values from -0.21875 to 0.21875
- cross_out: bfloat16 [768, 768], P('head', 'ctx'), may hold values from -4 to 4
- gate_proj: bfloat16 [768, 2048], P('ctx', 'head'), may hold values from -0.21875 to 0.21875
- up_proj: bfloat16 [768, 2048], P('ctx', 'head'), may hold values from -0.21875 to 0.21875
- down_proj: bfloat16 [2048, 768], P('head', 'ctx'), may hold values from -0.125 to 0.125
- norm_gains: float32 [3, 768], replicated, may hold values from 0.5 to 1.5
- position_bias: float32 [32, 12], P(None, 'head'), may hold values from -4 to 4
- bucket_ids: int32 [2048], replicated, may hold values from 0 to 31, never falling along the last dimension, each value on 1 to 1024 neighbouring positions
- block_order: int32 [16], replicated, may hold values from 0 to 15, each once
- out_grad: float32 [2048, 768], P('ctx'), may hold values from -6 to 6
Outputs:
- layer_out: float32 [2048, 768], P('ctx')
- input_grad: float32 [2048, 768], P('ctx')
- encoded_grad: float32 [1024, 768], P('ctx')
- self_query_grad: float32 [768, 768], P('ctx', 'head')
- self_key_grad: float32 [768, 768], P('ctx', 'head')
- self_value_grad: float32 [768, 768], P('ctx', 'head')
- self_out_grad: float32 [768, 768], P('head', 'ctx')
- cross_query_grad: float32 [768, 768], P('ctx', 'head')
- cross_key_grad: float32 [768, 768], P('ctx', 'head')
- cross_value_grad: float32 [768, 768], P('ctx', 'head')
- cross_out_grad: float32 [768, 768], P('head', 'ctx')
- gate_proj_grad: float32 [768, 2048], P('ctx', 'head')
- up_proj_grad: float32 [768, 2048], P('ctx', 'head')
- down_proj_grad: float32 [2048, 768], P('head', 'ctx')
- norm_gains_grad: float32 [3, 768], replicated
- position_bias_grad: float32 [32, 12], P(None, 'head')
The draws below stay inside these ranges and needn't reach their ends.
Inputs may be any that keep to these rules, and one draw needn't show every extreme that they name: Never falls along the distance; bucket_ids[0] = 0 and the last value is 31. `block_order`: each block number appears once.
All inputs are finite; a program needn't handle non-finite values.
Results may differ from the reference program's by a relative error of at most 0.04.
Values may be sent and summed in bfloat16 or wider, within the bound.
A program may use at most 192 MiB of HBM per device.

```python
import math
import jax
import jax.numpy as jnp
import numpy as np
from jax import lax

D = 768
HEADS = 12
HEAD_DIM = 64
FF = 2048
NUM_BUCKETS = 32
TOK_DEV = 128
TOKENS = 2048
ENC_TOKENS = 1024
N_CTX = 16


def block_levels(key, dims, cuts, low, largest):
    factor_of, own = 1.0, jax.random.fold_in(key, 6)
    for position, blocks in cuts:
        heights = jnp.exp(jax.random.uniform(jax.random.fold_in(own, position), (blocks,), jnp.float32, low / len(cuts), largest / len(cuts)))
        factor_of = factor_of * jnp.repeat(heights, dims[position] // blocks).reshape([-1 if axis == position else 1 for axis in range(len(dims))])
    return factor_of


def profile(count, total, limit, lean):
    loads = [(1 << 20) // math.isqrt(standing ** lean) + 1 for standing in range(2, count + 1)]
    surplus, counts = total - limit - (count - 1), [1] * (count - 1)
    while surplus > 0:
        movable = [i for i in range(count - 1) if counts[i] < limit]
        mass, remaining = sum([loads[i] for i in movable]), surplus
        for i in movable:
            addition = min(limit - counts[i], max(1, remaining * loads[i] // mass), surplus)
            counts[i] = counts[i] + addition
            surplus = surplus - addition
    return np.array([limit] + counts)


def ragged_sizes(key, count, total, reach, skew):
    if count == 2:
        one = jax.random.randint(key, (), max(1, total - reach), min(reach, total - 1) + 1)
        return jnp.stack([one, total - one])
    sizes = jnp.asarray(profile(count, total, reach, skew), jnp.int32)
    couples = (count - 1) // 2
    source_of, taker = sizes[1:1 + 2 * couples:2], sizes[2:2 + 2 * couples:2]
    margin = jnp.minimum(source_of - 1, reach - taker)
    shifted = jax.random.randint(jax.random.fold_in(key, 1), (couples,), 0, 1 << 20) % (margin + 1)
    sizes = sizes.at[1:1 + 2 * couples:2].set(source_of - shifted).at[2:2 + 2 * couples:2].set(taker + shifted)
    return sizes[jax.random.permutation(jax.random.fold_in(key, 2), count)]


def normal_values(rng, extent, deviation, bound, pieces=(), kind=jnp.bfloat16):
    drawn = deviation * jax.random.normal(rng, extent, jnp.float32)
    if pieces:
        drawn = drawn * block_levels(rng, extent, pieces, -0.22, 0.18)
    return jnp.clip(drawn, -bound, bound).astype(kind)


def setup_inputs(seed: int = 0) -> dict:
    key_list = jax.random.split(jax.random.key(seed), 19)
    return {
        "layer_in": normal_values(key_list[0], (TOKENS, D), 1.0, 6.0, ((0, 16),), jnp.float32),
        "encoded": normal_values(key_list[1], (ENC_TOKENS, D), 1.0, 6.0, ((0, 16),)),
        "self_query": normal_values(key_list[2], (D, D), (HEAD_DIM * D) ** -0.5, 0.02734375, ((0, 16), (1, 2))),
        "self_key": normal_values(key_list[3], (D, D), D ** -0.5, 0.21875, ((0, 16), (1, 2))),
        "self_value": normal_values(key_list[4], (D, D), D ** -0.5, 0.21875, ((0, 16), (1, 2))),
        "self_out": normal_values(key_list[5], (D, D), 2 ** -0.5, 4.0, ((0, 2), (1, 16))),
        "cross_query": normal_values(key_list[6], (D, D), (HEAD_DIM * D) ** -0.5, 0.02734375, ((0, 16), (1, 2))),
        "cross_key": normal_values(key_list[7], (D, D), D ** -0.5, 0.21875, ((0, 16), (1, 2))),
        "cross_value": normal_values(key_list[8], (D, D), D ** -0.5, 0.21875, ((0, 16), (1, 2))),
        "cross_out": normal_values(key_list[9], (D, D), 2 ** -0.5, 4.0, ((0, 2), (1, 16))),
        "gate_proj": normal_values(key_list[10], (D, FF), D ** -0.5, 0.21875, ((0, 16), (1, 2))),
        "up_proj": normal_values(key_list[11], (D, FF), D ** -0.5, 0.21875, ((0, 16), (1, 2))),
        "down_proj": normal_values(key_list[12], (FF, D), FF ** -0.5, 0.125, ((0, 2), (1, 16))),
        "norm_gains": jnp.clip(1.0 + 0.1 * jax.random.normal(key_list[13], (3, D), jnp.float32), 0.5, 1.5),
        "position_bias": normal_values(key_list[14], (NUM_BUCKETS, HEADS), 1.0, 4.0, ((1, 2),), jnp.float32),
        "bucket_ids": jnp.searchsorted(jnp.cumsum(ragged_sizes(key_list[15], NUM_BUCKETS, TOKENS, TOKENS // 2, 2)), jnp.arange(TOKENS), side="right").astype(jnp.int32),
        "block_order": jax.random.permutation(key_list[16], N_CTX).astype(jnp.int32),
        "out_grad": normal_values(key_list[17], (TOKENS, D), 1.0, 6.0, ((0, 16),), jnp.float32),
    }


EPS = 1e-06
NEG = -1e+30
HIGH = lax.Precision.HIGHEST

def rms_scale(rows, gain):
    return rows * lax.rsqrt(lax.optimization_barrier(jnp.mean(rows * rows, axis=-1, keepdims=True)) + EPS) * gain

def geglu(gate, upper):
    return jax.nn.gelu(gate, approximate=True) * upper

def times(left, right):
    return jnp.dot(left, right, preferred_element_type=jnp.float32)

def left_times(left, right):
    return lax.dot_general(left, right, (((0,), (0,)), ((), ())), preferred_element_type=jnp.float32)

def right_times(left, right):
    return lax.dot_general(left, right, (((1,), (1,)), ((), ())), preferred_element_type=jnp.float32)

def rounded(values):
    return lax.optimization_barrier(values.astype(jnp.bfloat16)).astype(jnp.float32)

def heads_view(values):
    return values.astype(jnp.float32).reshape(values.shape[0], HEADS, HEAD_DIM)

def scores_for(query3, key3, query_pos, key_pos, bucket_ids, position_bias, causal):
    scores = jnp.einsum('qhe,khe->hqk', query3, key3, precision=HIGH)
    if causal:
        dist = query_pos[:, None] - key_pos[None, :]
        ids = bucket_ids[jnp.maximum(dist, 0)]
        scores = scores + jnp.transpose(position_bias[ids], (2, 0, 1))
        scores = jnp.where((dist >= 0)[None], scores, NEG)
        return (scores, ids)
    return (scores, None)

def attend_forward(queries, keys, values, query_pos, key_pos, bucket_ids, position_bias, causal):
    count = queries.shape[0]
    block = math.gcd(count, 256)
    query3 = heads_view(queries)
    key3 = heads_view(keys)
    value3 = heads_view(values)

    def one(index):
        part = lax.dynamic_slice_in_dim(query3, index * block, block, 0)
        part_pos = lax.dynamic_slice_in_dim(query_pos, index * block, block, 0)
        scores, ids = scores_for(part, key3, part_pos, key_pos, bucket_ids, position_bias, causal)
        top = lax.optimization_barrier(jnp.max(scores, axis=-1, keepdims=True))
        lse = top[..., 0] + jnp.log(lax.optimization_barrier(jnp.sum(jnp.exp(scores - top), axis=-1)))
        weights = rounded(jnp.exp(scores - lse[..., None]))
        mixed = jnp.einsum('hqk,khe->qhe', weights, value3, precision=HIGH)
        return (mixed.reshape(block, HEADS * HEAD_DIM).astype(jnp.bfloat16), lse)
    mixed, lse = lax.map(one, jnp.arange(count // block))
    return (mixed.reshape(count, HEADS * HEAD_DIM), jnp.transpose(lse, (1, 0, 2)).reshape(HEADS, count))

def attend_backward(queries, keys, values, mixed, mixed_grad, lse, query_pos, key_pos, bucket_ids, position_bias, causal):
    count = queries.shape[0]
    key_count = keys.shape[0]
    block = math.gcd(count, 256)
    query3 = heads_view(queries)
    key3 = heads_view(keys)
    value3 = heads_view(values)
    grad3 = heads_view(mixed_grad)
    delta = jnp.transpose(lax.optimization_barrier(jnp.sum(heads_view(mixed) * grad3, axis=-1)))

    def step(carry, index):
        key_grad, value_grad, bias_grad = carry
        part = lax.dynamic_slice_in_dim(query3, index * block, block, 0)
        part_grad = lax.dynamic_slice_in_dim(grad3, index * block, block, 0)
        part_pos = lax.dynamic_slice_in_dim(query_pos, index * block, block, 0)
        part_lse = lax.dynamic_slice_in_dim(lse, index * block, block, 1)
        part_delta = lax.dynamic_slice_in_dim(delta, index * block, block, 1)
        scores, ids = scores_for(part, key3, part_pos, key_pos, bucket_ids, position_bias, causal)
        weights = jnp.exp(scores - part_lse[..., None])
        value_grad = value_grad + jnp.einsum('hqk,qhe->khe', rounded(weights), part_grad, precision=HIGH)
        weight_grad = jnp.einsum('qhe,khe->hqk', part_grad, value3, precision=HIGH)
        score_grad = weights * (weight_grad - part_delta[..., None])
        if causal:
            flat = jnp.transpose(score_grad, (1, 2, 0)).reshape(-1, HEADS)
            bias_grad = bias_grad + jax.ops.segment_sum(flat, ids.reshape(-1), num_segments=NUM_BUCKETS)
        score_low = rounded(score_grad)
        query_grad = jnp.einsum('hqk,khe->qhe', score_low, key3, precision=HIGH)
        key_grad = key_grad + jnp.einsum('hqk,qhe->khe', score_low, part, precision=HIGH)
        return ((key_grad, value_grad, bias_grad), query_grad.reshape(block, HEADS * HEAD_DIM))
    start = (jnp.zeros((key_count, HEADS, HEAD_DIM), jnp.float32), jnp.zeros((key_count, HEADS, HEAD_DIM), jnp.float32), jnp.zeros((NUM_BUCKETS, HEADS), jnp.float32))
    (key_grad, value_grad, bias_grad), query_grad = lax.scan(step, start, jnp.arange(count // block))
    query_grad = query_grad.reshape(count, HEADS * HEAD_DIM).astype(jnp.bfloat16)
    key_grad = key_grad.reshape(key_count, HEADS * HEAD_DIM).astype(jnp.bfloat16)
    value_grad = value_grad.reshape(key_count, HEADS * HEAD_DIM).astype(jnp.bfloat16)
    return (query_grad, key_grad, value_grad, bias_grad)

def reference(layer_in, encoded, self_query, self_key, self_value, self_out, cross_query, cross_key, cross_value, cross_out, gate_proj, up_proj, down_proj, norm_gains, position_bias, bucket_ids, block_order, out_grad):
    low = jnp.bfloat16
    positions = (block_order[:, None] * TOK_DEV + jnp.arange(TOK_DEV, dtype=jnp.int32)[None, :]).reshape(TOKENS).astype(jnp.int32)
    normed_one = rms_scale(layer_in, norm_gains[0]).astype(low)
    queries = times(normed_one, self_query).astype(low)
    keys_own = times(normed_one, self_key).astype(low)
    values_own = times(normed_one, self_value).astype(low)
    mixed_one, lse_one = attend_forward(queries, keys_own, values_own, positions, positions, bucket_ids, position_bias, True)
    after_self = layer_in + times(mixed_one, self_out)
    normed_two = rms_scale(after_self, norm_gains[1]).astype(low)
    probes = times(normed_two, cross_query).astype(low)
    memory_keys = times(encoded, cross_key).astype(low)
    memory_values = times(encoded, cross_value).astype(low)
    mixed_two, lse_two = attend_forward(probes, memory_keys, memory_values, positions, positions, bucket_ids, position_bias, False)
    after_cross = after_self + times(mixed_two, cross_out)
    normed_three = rms_scale(after_cross, norm_gains[2]).astype(low)
    gate_pre = times(normed_three, gate_proj)
    upper = times(normed_three, up_proj)
    activated = geglu(gate_pre, upper).astype(low)
    layer_out = after_cross + times(activated, down_proj)
    grad_rows = out_grad.astype(low)
    down_grad = left_times(activated, grad_rows)
    act_grad = right_times(grad_rows, down_proj)
    geglu_out, geglu_pull = jax.vjp(geglu, gate_pre, upper)
    gate_grad, upper_grad = geglu_pull(act_grad)
    gate_grad = gate_grad.astype(low)
    upper_grad = upper_grad.astype(low)
    gate_wgrad = left_times(normed_three, gate_grad)
    up_wgrad = left_times(normed_three, upper_grad)
    normed_three_grad = right_times(gate_grad, gate_proj) + right_times(upper_grad, up_proj)
    norm_out, norm_pull = jax.vjp(rms_scale, after_cross, norm_gains[2])
    cross_extra, gain_three = norm_pull(normed_three_grad)
    cross_grad = out_grad + cross_extra
    cross_rows = cross_grad.astype(low)
    cross_out_wgrad = left_times(mixed_two, cross_rows)
    mixed_two_grad = right_times(cross_rows, cross_out).astype(low)
    probe_grad, memory_key_grad, memory_value_grad, unused_bias = attend_backward(probes, memory_keys, memory_values, mixed_two, mixed_two_grad, lse_two, positions, positions, bucket_ids, position_bias, False)
    cross_query_wgrad = left_times(normed_two, probe_grad)
    cross_key_wgrad = left_times(encoded, memory_key_grad)
    cross_value_wgrad = left_times(encoded, memory_value_grad)
    normed_two_grad = right_times(probe_grad, cross_query)
    encoded_grad = right_times(memory_key_grad, cross_key) + right_times(memory_value_grad, cross_value)
    norm_out, norm_pull = jax.vjp(rms_scale, after_self, norm_gains[1])
    self_extra, gain_two = norm_pull(normed_two_grad)
    self_grad = cross_grad + self_extra
    self_rows = self_grad.astype(low)
    self_out_wgrad = left_times(mixed_one, self_rows)
    mixed_one_grad = right_times(self_rows, self_out).astype(low)
    query_grad, key_grad, value_grad, bias_grad = attend_backward(queries, keys_own, values_own, mixed_one, mixed_one_grad, lse_one, positions, positions, bucket_ids, position_bias, True)
    query_wgrad = left_times(normed_one, query_grad)
    key_wgrad = left_times(normed_one, key_grad)
    value_wgrad = left_times(normed_one, value_grad)
    normed_one_grad = right_times(query_grad, self_query) + right_times(key_grad, self_key) + right_times(value_grad, self_value)
    norm_out, norm_pull = jax.vjp(rms_scale, layer_in, norm_gains[0])
    input_extra, gain_one = norm_pull(normed_one_grad)
    input_grad = self_grad + input_extra
    gains_grad = jnp.stack((gain_one, gain_two, gain_three))
    return (layer_out, input_grad, encoded_grad, query_wgrad, key_wgrad, value_wgrad, self_out_wgrad, cross_query_wgrad, cross_key_wgrad, cross_value_wgrad, cross_out_wgrad, gate_wgrad, up_wgrad, down_grad, gains_grad, bias_grad)
```

```python
import functools
import math

import jax
import jax.numpy as jnp
from jax import lax
from jax.experimental import pallas as pl
from jax.experimental.pallas import tpu as pltpu
from jax.sharding import PartitionSpec as P

EPS = 1e-06
NEG = -1e30
HIGH = lax.Precision.HIGHEST
LOW = jnp.bfloat16
F32 = jnp.float32
MESH = pl.DeviceIdType.MESH
VMEM_LIMIT = 66_000_000


def dot(left, right, **kw):
    return jnp.dot(left, right, preferred_element_type=F32, **kw)


def dot_nt(left, right, **kw):
    return lax.dot_general(left, right, (((1,), (1,)), ((), ())), preferred_element_type=F32, **kw)


def dot_tn(left, right, **kw):
    return lax.dot_general(left, right, (((0,), (0,)), ((), ())), preferred_element_type=F32, **kw)


def rms_forward(rows, gain):
    return rows * lax.rsqrt(jnp.mean(rows * rows, axis=-1, keepdims=True) + EPS) * gain


def rms_backward(rows, gain, grad):
    scale = lax.rsqrt(jnp.mean(rows * rows, axis=-1, keepdims=True) + EPS)
    scaled = gain * grad
    inner = jnp.mean(scaled * rows, axis=-1, keepdims=True)
    row_grad = scale * scaled - rows * (scale * scale * scale * inner)
    gain_grad = jnp.sum(grad * rows * scale, axis=0, keepdims=True)
    return row_grad, gain_grad


def aligned(value, step):
    return value if isinstance(value, int) else pl.multiple_of(value, step)


class Place:
    def __init__(self, count):
        self.count = count
        self.here = lax.axis_index("ctx")
        self.core = lax.axis_index("head")
        self.other = 1 - self.core
        self.plane = lax.rem(self.here, 4)
        self.level = self.here // 4
        self.fx = self.flip(self.here, 0)
        self.fy = self.flip(self.here, 1)
        self.fxy = self.flip(self.fx, 1)
        self.above = [lax.rem(self.here + 4 * k, count) for k in range(4)]
        self.below = [lax.rem(self.here + count - 4 * k, count) for k in range(4)]

    def flip(self, index, axis):
        if axis == 0:
            return index + 1 - 2 * lax.rem(index, 2)
        return index + 2 - 4 * lax.rem(index // 2, 2)

    def near(self, half):
        return (self.fx, self.fy) if half == 0 else (self.fy, self.fx)

    def greet(self, chips, partner):
        barrier = pltpu.get_barrier_semaphore()
        total = len(chips) + (1 if partner else 0)
        for chip in chips:
            pl.semaphore_signal(
                barrier, inc=1, device_id=(chip, self.core), device_id_type=MESH
            )
        if partner:
            pl.semaphore_signal(
                barrier, inc=1, device_id=(self.here, self.other), device_id_type=MESH
            )
        pl.semaphore_wait(barrier, total)


class Wire:
    def __init__(self, place, send_sem, recv_sem):
        self.place, self.send_sem, self.recv_sem = place, send_sem, recv_sem
        self.sent = []
        self.used = 0

    def slots(self, count):
        base = self.used
        self.used += count
        assert self.used <= self.send_sem.shape[0], self.used
        return base

    def copy(self, src, dst, slot, chip, core):
        return pltpu.make_async_remote_copy(
            src_ref=src,
            dst_ref=dst,
            send_sem=self.send_sem.at[slot],
            recv_sem=self.recv_sem.at[slot],
            device_id=(chip, core),
            device_id_type=MESH,
        )

    def send(self, src, dst, slot, chip=None, core=None):
        chip = self.place.here if chip is None else chip
        core = self.place.core if core is None else core
        made = self.copy(src, dst, slot, chip, core)
        made.start()
        self.sent.append(made)

    def swap(self, src, dst, slot):
        self.send(src, dst, slot, None, self.place.other)

    def got(self, dst, slot):
        place = self.place
        self.copy(dst, dst, slot, place.here, place.other).wait_recv()

    def drain(self):
        for made in self.sent:
            made.wait_send()
        self.sent = []


class Gather:
    def __init__(self, wire, view, share, halves=2):
        self.wire, self.view, self.share = wire, view, share
        self.base = [wire.slots(15) for _ in range(halves)]
        self.side = [wire.slots(16) for _ in range(halves)] if share else None
        self.halves = range(halves)

    def _out(self, half, block, slot, chip):
        ref = self.view(half, block)
        self.wire.send(ref, ref, self.base[half] + slot, chip)

    def _in(self, half, block, slot):
        self.wire.got(self.view(half, block), self.base[half] + slot)
        if self.share:
            ref = self.view(half, block)
            self.wire.swap(ref, ref, self.side[half] + slot)

    def start(self):
        place = self.wire.place
        for half in self.halves:
            near, far = place.near(half)
            for k in (1, 2, 3):
                self._out(half, place.here, k - 1, place.above[k])
            self._out(half, place.here, 3, near)
            self._out(half, place.here, 7, far)

    def pass_level(self):
        place = self.wire.place
        for k in (1, 2, 3):
            for half in self.halves:
                near, far = place.near(half)
                self._in(half, place.below[k], k - 1)
                self._out(half, place.below[k], 3 + k, near)
                self._out(half, place.below[k], 7 + k, far)

    def pass_near(self):
        place = self.wire.place
        for k in range(4):
            for half in self.halves:
                _, far = place.near(half)
                block = place.flip(place.below[k], half)
                self._in(half, block, 3 + k)
                self._out(half, block, 11 + k, far)

    def finish(self):
        place = self.wire.place
        for k in range(4):
            for half in self.halves:
                block = place.flip(place.below[k], 1 - half)
                self._in(half, block, 7 + k)
                self._in(half, place.flip(block, half), 11 + k)

    def finish_share(self):
        if not self.share:
            return
        place = self.wire.place
        for k in range(4):
            for half in self.halves:
                block = place.below[k]
                if k:
                    self._share_in(half, block, k - 1)
                self._share_in(half, place.flip(block, half), 3 + k)
                block = place.flip(block, 1 - half)
                self._share_in(half, block, 7 + k)
                self._share_in(half, place.flip(block, half), 11 + k)

    def _share_in(self, half, block, slot):
        self.wire.got(self.share(half, block), self.side[half] + slot)


class Scatter:
    def __init__(self, wire, view, buf, out, halves=2):
        self.wire, self.view, self.out = wire, view, out
        self.far_buf = lambda half, slot: buf.at[half, slot]
        self.near_buf = lambda half, slot: buf.at[half, 8 + slot]
        self.level_buf = lambda half, slot: buf.at[half, 12 + slot]
        self.base = [wire.slots(15) for _ in range(halves)]
        self.halves = range(halves)

    def start(self, ready=None):
        place = self.wire.place
        for k in (1, 2, 3, 0):
            if ready is not None:
                ready(k)
            for half in self.halves:
                _, far = place.near(half)
                away = place.flip(place.below[k], 1 - half)
                for pair, block in ((1, place.flip(away, half)), (0, away)):
                    slot = 2 * k + pair
                    self.wire.send(
                        self.view(half, block),
                        self.far_buf(half, slot),
                        self.base[half] + slot,
                        far,
                    )

    def pass_near(self):
        place = self.wire.place
        for k in (1, 2, 3, 0):
            for half in self.halves:
                near, _ = place.near(half)
                block = place.flip(place.below[k], half)
                slot = 2 * k + 1
                self.wire.got(self.far_buf(half, slot), self.base[half] + slot)
                ref = self.view(half, block)
                ref[...] = (
                    ref[...].astype(F32) + self.far_buf(half, slot)[...].astype(F32)
                ).astype(LOW)
                self.wire.send(ref, self.near_buf(half, k), self.base[half] + 8 + k, near)

    def pass_level(self):
        place = self.wire.place
        for k in (1, 2, 3):
            for half in self.halves:
                self._add(half, k)
                ref = self.view(half, place.below[k])
                self.wire.send(
                    ref, self.level_buf(half, k - 1), self.base[half] + 11 + k, place.below[k]
                )

    def _add(self, half, k):
        place = self.wire.place
        self.wire.got(self.far_buf(half, 2 * k), self.base[half] + 2 * k)
        self.wire.got(self.near_buf(half, k), self.base[half] + 8 + k)
        ref = self.view(half, place.below[k])
        total = (
            ref[...].astype(F32)
            + self.far_buf(half, 2 * k)[...].astype(F32)
            + self.near_buf(half, k)[...].astype(F32)
        )
        if k:
            ref[...] = total.astype(LOW)
        return total

    def finish(self):
        for half in self.halves:
            total = self._add(half, 0)
            for k in (1, 2, 3):
                self.wire.got(self.level_buf(half, k - 1), self.base[half] + 11 + k)
                total = total + self.level_buf(half, k - 1)[...].astype(F32)
            self.out(half, total)


def lane_split(rows):
    lane = lax.broadcasted_iota(jnp.int32, rows.shape, 1)
    low = lane < rows.shape[1] // 2
    zero = jnp.zeros_like(rows)
    return jnp.concatenate((jnp.where(low, rows, zero), jnp.where(low, zero, rows)), axis=0)


def lane_join(rows):
    count, width = rows.shape[0] // 2, rows.shape[1]
    lane = lax.broadcasted_iota(jnp.int32, (count, width), 1)
    return jnp.where(lane < width // 2, rows[:count], rows[count:])


def pair_attend(tok, pairs, chunk, q_ref, kv_ref, s_ref, e_ref, rl_ref, mixed_ref, bias_ref):
    keys = kv_ref.shape[0]
    total = pairs * 128

    def one_pair(j, carry):
        cols = pl.ds(aligned(j * 128, 128), 128)
        q_cat = lane_split(q_ref[:, cols])

        def score(c, top):
            rows = pl.ds(aligned(c * chunk, chunk), chunk)
            s = dot_nt(q_cat, kv_ref[rows, cols])
            if bias_ref is not None:
                tiles = []
                for half in range(2):
                    row = []
                    for b in range(chunk // tok):
                        vec = bias_ref[c * (chunk // tok) + b, pl.ds(2 * j + half, 1), :]
                        wide = jnp.broadcast_to(vec, (tok, 2 * tok))
                        row.append(pltpu.roll(wide, 0, 1, stride=1, stride_axis=0)[:, :tok])
                    tiles.append(jnp.concatenate(row, axis=1))
                s = s + jnp.concatenate(tiles, axis=0)
            s_ref[:, rows] = s
            for b in range(chunk // 128):
                top = jnp.maximum(top, s[:, b * 128 : (b + 1) * 128])
            return top

        top = lax.fori_loop(0, keys // chunk, score, jnp.full((2 * tok, 128), NEG, F32))
        peak = jnp.max(top, axis=1, keepdims=True)

        def weigh(c, state):
            acc, run = state
            rows = pl.ds(aligned(c * chunk, chunk), chunk)
            e = jnp.exp(s_ref[:, rows] - peak)
            for b in range(chunk // 128):
                run = run + e[:, b * 128 : (b + 1) * 128]
            low = e.astype(LOW)
            e_ref[j, :, rows] = low
            value = kv_ref[rows, pl.ds(aligned(total + j * 128, 128), 128)]
            return (acc + dot(low, value), run)

        zero = jnp.zeros((2 * tok, 128), F32)
        acc, run = lax.fori_loop(0, keys // chunk, weigh, (zero, zero))
        rl = 1.0 / jnp.sum(run, axis=1, keepdims=True)
        rl_ref[j] = rl
        mixed_ref[:, cols] = lane_join(acc * rl).astype(LOW)
        return carry

    lax.fori_loop(0, pairs, one_pair, 0)


def pair_attend_back(
    tok, pairs, chunk, q_ref, kv_ref, e_ref, rl_ref, mixed_ref, grad_ref, q_grad_ref, kv_grad_ref, diag_ref
):
    keys = kv_ref.shape[0]
    total = pairs * 128
    flip = (
        lax.broadcasted_iota(jnp.int32, (tok, tok), 0)
        + lax.broadcasted_iota(jnp.int32, (tok, tok), 1)
        == tok - 1
    ).astype(LOW)

    def one_pair(j, carry):
        cols = pl.ds(aligned(j * 128, 128), 128)
        vcols = pl.ds(aligned(total + j * 128, 128), 128)
        q_cat = lane_split(q_ref[:, cols])
        rl = rl_ref[j]
        grad = lane_split(grad_ref[:, cols].astype(F32))
        mixed = lane_split(mixed_ref[:, cols].astype(F32))
        grad_cat = (grad * rl).astype(LOW)
        delta = jnp.sum(grad * mixed, axis=1, keepdims=True) * rl

        def piece(c, q_grad):
            rows = pl.ds(aligned(c * chunk, chunk), chunk)
            low_e = e_ref[j, :, rows]
            key = kv_ref[rows, cols]
            dp = dot_nt(grad_cat, kv_ref[rows, vcols])
            ds = (low_e.astype(F32) * (dp - delta)).astype(LOW)
            if diag_ref is not None:
                for half in range(2):
                    turned = dot(flip, ds[half * tok : (half + 1) * tok])
                    for b in range(chunk // tok):
                        tile = turned[:, b * tok : (b + 1) * tok]
                        wide = jnp.concatenate((tile, jnp.zeros_like(tile)), axis=1)
                        wide = pltpu.roll(wide, tok + 1, 1, stride=1, stride_axis=0)
                        diag_ref[c * (chunk // tok) + b, pl.ds(2 * j + half, 1), :] = jnp.sum(
                            wide, axis=0, keepdims=True
                        )
            kv_grad_ref[rows, cols] = dot_tn(ds, q_cat).astype(LOW)
            kv_grad_ref[rows, vcols] = dot_tn(low_e, grad_cat).astype(LOW)
            return q_grad + dot(ds, key)

        q_grad = lax.fori_loop(0, keys // chunk, piece, jnp.zeros((2 * tok, 128), F32))
        q_grad_ref[:, cols] = lane_join(q_grad).astype(LOW)
        return carry

    lax.fori_loop(0, pairs, one_pair, 0)


def bucket_masks(ids_ref, block, buckets):
    ids = ids_ref[pl.ds(block, 1), :]
    row = lax.broadcasted_iota(jnp.int32, (buckets, ids.shape[1]), 0)
    return ids, (row == ids).astype(F32)


def bias_vectors(ids_ref, table_ref, bias_ref):
    def one(block, carry):
        ids, mask = bucket_masks(ids_ref, block, table_ref.shape[1])
        vec = dot(table_ref[...], mask, precision=HIGH)
        bias_ref[block] = jnp.where(ids >= 0, vec, NEG)
        return carry

    lax.fori_loop(0, ids_ref.shape[0], one, 0)


def bucket_sums(ids_ref, diag_ref, buckets):
    def one(block, total):
        _, mask = bucket_masks(ids_ref, block, buckets)
        return total + dot_nt(diag_ref[block], mask, precision=HIGH)

    start = jnp.zeros((diag_ref.shape[1], buckets), F32)
    return lax.fori_loop(0, ids_ref.shape[0], one, start)


def rows_loop(count, step, body):
    def one(index, carry):
        body(pl.ds(aligned(index * step, step), step))
        return carry

    lax.fori_loop(0, count // step, one, 0)


GELU_A = 0.7978845608028654
GELU_B = 0.044715


def gelu_parts(value):
    square = value * value
    wave = jnp.tanh(GELU_A * (value + GELU_B * value * square))
    half = 0.5 * (1.0 + wave)
    slope = half + 0.5 * value * (1.0 - wave * wave) * (GELU_A * (1.0 + 3.0 * GELU_B * square))
    return value * half, slope


def core_sum(wire, part, out_buf, in_buf):
    slot = wire.slots(1)
    out_buf[...] = part.astype(LOW)
    wire.swap(out_buf, in_buf, slot)
    wire.got(in_buf, slot)
    return out_buf[...].astype(F32) + in_buf[...].astype(F32)


class PlaneSum:
    def __init__(self, wire, tok, part, core_buf, plane_buf, whole):
        self.wire, self.tok = wire, tok
        self.part, self.core_buf, self.plane_buf, self.whole = part, core_buf, plane_buf, whole
        self.base = wire.slots(8)
        self.half = whole.shape[1] // 2

    def cols(self, core):
        return pl.ds(aligned(core * self.half, 128), self.half)

    def start(self):
        place, wire = self.wire.place, self.wire
        away = self.cols(place.other)
        for k, chip in ((1, place.fx), (2, place.fy), (3, place.fxy), (0, place.here)):
            rows = pl.ds(aligned(lax.rem(chip, 4) * self.tok, self.tok), self.tok)
            wire.swap(self.part.at[rows, away], self.core_buf.at[rows, :], self.base + k)

    def middle(self):
        place, wire = self.wire.place, self.wire
        mine = self.cols(place.core)
        for k, chip in ((1, place.fx), (2, place.fy), (3, place.fxy), (0, place.here)):
            rows = pl.ds(aligned(lax.rem(chip, 4) * self.tok, self.tok), self.tok)
            wire.got(self.core_buf.at[rows, :], self.base + k)
            total = self.part[rows, mine].astype(F32) + self.core_buf[rows, :].astype(F32)
            if k:
                self.core_buf[rows, :] = total.astype(LOW)
                wire.send(
                    self.core_buf.at[rows, :], self.plane_buf.at[k - 1], self.base + 3 + k, chip
                )
            else:
                self.own = total

    def finish(self):
        place, wire = self.wire.place, self.wire
        total = self.own
        for k in (1, 2, 3):
            wire.got(self.plane_buf.at[k - 1], self.base + 3 + k)
            total = total + self.plane_buf[k - 1].astype(F32)
        mine = self.cols(place.core)
        self.whole[:, mine] = total.astype(LOW)
        slot = self.base + 7
        wire.swap(self.whole.at[:, mine], self.whole.at[:, mine], slot)
        wire.got(self.whole.at[:, self.cols(place.other)], slot)


class PlaneGather:
    def __init__(self, wire, tok, ref):
        self.wire, self.tok, self.ref = wire, tok, ref
        self.half = ref.shape[1] // 2
        self.base = wire.slots(6)

    def view(self, chip, core):
        rows = pl.ds(aligned(lax.rem(chip, 4) * self.tok, self.tok), self.tok)
        return self.ref.at[rows, pl.ds(aligned(core * self.half, 128), self.half)]

    def start(self):
        place = self.wire.place
        own = self.view(place.here, place.core)
        for k, chip in enumerate((place.fx, place.fy, place.fxy)):
            self.wire.send(own, own, self.base + k, chip)

    def share(self):
        place = self.wire.place
        for k, chip in enumerate((place.fx, place.fy, place.fxy)):
            ref = self.view(chip, place.core)
            self.wire.got(ref, self.base + k)
            self.wire.swap(ref, ref, self.base + 3 + k)

    def finish(self):
        place = self.wire.place
        for k, chip in enumerate((place.fx, place.fy, place.fxy)):
            self.wire.got(self.view(chip, place.other), self.base + 3 + k)


class Sizes:
    def __init__(self, ctx, tok, enc, model, wide, units):
        self.ctx, self.tok, self.enc, self.model, self.wide = ctx, tok, enc, model, wide
        self.rows = model // ctx
        self.quarter = units // 4
        self.pairs = wide // 128
        self.levels = ctx // 4
        self.attn_cols = 8 * wide
        self.mlp_cols = 3 * units
        self.part = 3 * self.quarter
        names = ("q", "k", "v", "o", "cq", "ck", "cv", "co")
        self.col = {name: slice(i * wide, (i + 1) * wide) for i, name in enumerate(names)}
        self.col["kv"] = slice(wide, 3 * wide)
        self.col["ckv"] = slice(5 * wide, 7 * wide)


def named(kernel, names):
    def body(*refs):
        kernel(**dict(zip(names, refs, strict=True)))

    return body


def call(kernel, size, ins, outs, scratch, collective_id, any_inputs=()):
    names = list(ins) + list(outs) + list(scratch)
    made = pl.pallas_call(
        named(functools.partial(kernel, size), names),
        out_shape=tuple(jax.ShapeDtypeStruct(*spec) for spec in outs.values()),
        in_specs=[
            pl.BlockSpec(memory_space=pl.ANY if name in any_inputs else pltpu.VMEM) for name in ins
        ],
        out_specs=tuple(pl.BlockSpec(memory_space=pltpu.VMEM) for _ in outs),
        scratch_shapes=list(scratch.values()),
        compiler_params=pltpu.CompilerParams(
            collective_id=collective_id, has_side_effects=True, vmem_limit_bytes=VMEM_LIMIT
        ),
    )
    return dict(zip(outs, made(*ins.values()), strict=True))


def wire_sems(count):
    return {
        "send_sem": pltpu.SemaphoreType.DMA((count,)),
        "recv_sem": pltpu.SemaphoreType.DMA((count,)),
    }


def gather_kernel(
    size, layer_in, encoded, gains, out_grad, wa, wm, WA, WM, X, E, GR, local, send_sem, recv_sem
):
    place = Place(size.ctx)
    wire = Wire(place, send_sem, recv_sem)
    chips = place.above[1:] + [place.fx, place.fy, place.fxy]
    tok, enc, rows, half_d = size.tok, size.enc, size.rows, size.model // 2

    def block_rows(block, count):
        return pl.ds(aligned(block * count, 16), count)

    place.greet(chips, True)
    X[block_rows(place.here, tok), :] = rms_forward(layer_in[...], gains[0:1]).astype(LOW)
    E[block_rows(place.here, enc), :] = encoded[...]
    GR[block_rows(place.plane, tok), :] = out_grad[...].astype(LOW)
    copies = (
        pltpu.make_async_copy(wa, WA.at[block_rows(place.here, rows), :], local.at[0]),
        pltpu.make_async_copy(
            wm.at[:, pl.ds(aligned(place.plane * size.part, 128), size.part)],
            WM.at[block_rows(place.here, rows), :],
            local.at[1],
        ),
    )
    for made in copies:
        made.start()

    def token_view(ref, count, core):
        def view(half, block):
            return ref.at[
                pl.ds(aligned(block * count + half * (count // 2), 16), count // 2),
                pl.ds(aligned(core * half_d, 128), half_d),
            ]

        return view

    def weight_view(first, last):
        step = (last - first) // 2

        def view(half, block):
            return WA.at[
                block_rows(block, rows), first + half * step : first + (half + 1) * step
            ]

        return view

    gx = Gather(wire, token_view(X, tok, place.core), token_view(X, tok, place.other))
    ge = Gather(wire, token_view(E, enc, place.core), token_view(E, enc, place.other))
    gs = Gather(wire, weight_view(0, 4 * size.wide), None)
    gc = Gather(wire, weight_view(4 * size.wide, 8 * size.wide), None)
    gg = PlaneGather(wire, tok, GR)
    plane_base, level_base = wire.slots(3), wire.slots(3)

    gx.start()
    ge.start()
    for made in copies:
        made.wait()
    gs.start()
    for k, chip in enumerate((place.fx, place.fy, place.fxy)):
        wire.send(
            wm.at[:, pl.ds(aligned(lax.rem(chip, 4) * size.part, 128), size.part)],
            WM.at[block_rows(place.here, rows), :],
            plane_base + k,
            chip,
        )
    gx.pass_level()
    ge.pass_level()
    gx.pass_near()
    gs.pass_level()
    ge.pass_near()
    gc.start()
    for k, chip in enumerate((place.fx, place.fy, place.fxy)):
        wire.got(WM.at[block_rows(chip, rows), :], plane_base + k)
    own = WM.at[block_rows(place.level, 4 * rows), :]
    for k in (1, 2, 3):
        wire.send(own, own, level_base + k - 1, place.above[k])
    gs.pass_near()
    gx.finish()
    ge.finish()
    gc.pass_level()
    gg.start()
    gs.finish()
    gc.pass_near()
    gg.share()
    gc.finish()
    for k in (1, 2, 3):
        level = place.below[k] // 4
        wire.got(WM.at[block_rows(level, 4 * rows), :], level_base + k - 1)
    gx.finish_share()
    ge.finish_share()
    gg.finish()
    wire.drain()


def compute_kernel(
    size, layer_in, gains, out_grad, ids, table, WA, WM, X, E, GR,
    layer_out, PW, PM, XG, EG, self_grad, SM,
    q, kv, mkv, probes, s, e1, e2, rl1, rl2, mixed1, mixed2, bias, diag,
    after_self, after_cross, cross_grad, n2, N3, act, GU, PN, PO, low, mixed_grad, q_grad,
    kv_grad, mkv_grad, ca, cb, pn_core, pn_plane, pn_whole, po_core, po_plane, po_whole,
    send_sem, recv_sem,
):
    place = Place(size.ctx)
    wire = Wire(place, send_sem, recv_sem)
    place.greet([place.fx, place.fy, place.fxy], True)
    tok, col, model, wide = size.tok, size.col, size.model, size.wide
    here_rows = pl.ds(aligned(place.here * tok, 16), tok)
    ctx_tok, ctx_enc = X.shape[0], E.shape[0]
    quarter = size.quarter

    def project(rows):
        kv[rows, :] = dot(X[rows, :], WA[:, col["kv"]]).astype(LOW)

    def project_enc(rows):
        mkv[rows, :] = dot(E[rows, :], WA[:, col["ckv"]]).astype(LOW)

    bias_vectors(ids, table, bias)
    diag[...] = jnp.zeros_like(diag)
    q[...] = dot(X[here_rows, :], WA[:, col["q"]]).astype(LOW)
    rows_loop(ctx_tok, 256, project)
    pair_attend(tok, size.pairs, 512, q, kv, s, e1, rl1, mixed1, bias)
    part = dot_nt(mixed1[...], WA[:, col["o"]])
    after_self[...] = layer_in[...] + core_sum(wire, part, ca.at[0], cb.at[0])
    n2[...] = rms_forward(after_self[...], gains[1:2]).astype(LOW)
    rows_loop(ctx_enc, 256, project_enc)
    probes[...] = dot(n2[...], WA[:, col["cq"]]).astype(LOW)
    pair_attend(tok, size.pairs, 512, probes, mkv, s, e2, rl2, mixed2, None)
    part = dot_nt(mixed2[...], WA[:, col["co"]])
    after_cross[...] = after_self[...] + core_sum(wire, part, ca.at[1], cb.at[1])
    spread = PlaneGather(wire, tok, N3)
    plane_rows = pl.ds(aligned(place.plane * tok, 16), tok)
    N3[plane_rows, :] = rms_forward(after_cross[...], gains[2:3]).astype(LOW)
    spread.start()
    spread.share()
    spread.finish()

    def units(rows):
        pre = dot(N3[rows, :], WM[:, : 2 * quarter])
        gate, upper = pre[:, :quarter], pre[:, quarter:]
        value, slope = gelu_parts(gate)
        act[rows, :] = (value * upper).astype(LOW)
        grad = dot(GR[rows, :], WM[:, 2 * quarter :])
        GU[rows, :quarter] = (grad * upper * slope).astype(LOW)
        GU[rows, quarter:] = (grad * value).astype(LOW)
        PN[rows, :] = dot_nt(GU[rows, :], WM[:, : 2 * quarter]).astype(LOW)

    rows_loop(4 * tok, 128, units)
    sum_n = PlaneSum(wire, tok, PN, pn_core, pn_plane, pn_whole)
    sum_o = PlaneSum(wire, tok, PO, po_core, po_plane, po_whole)
    sum_n.start()

    def back_out(rows):
        PO[rows, :] = dot_nt(act[rows, :], WM[:, 2 * quarter :]).astype(LOW)

    rows_loop(4 * tok, 128, back_out)
    sum_n.middle()
    sum_o.start()

    def unit_grads(cols):
        PM[cols, : 2 * quarter] = dot_tn(N3[:, cols], GU[...]).astype(LOW)
        PM[cols, 2 * quarter :] = dot_tn(GR[:, cols], act[...]).astype(LOW)

    rows_loop(model, 128, unit_grads)
    sum_n.finish()
    sum_o.middle()
    extra, gain_three = rms_backward(after_cross[...], gains[2:3], pn_whole[...].astype(F32))
    cross_grad[...] = out_grad[...] + extra
    low[...] = cross_grad[...].astype(LOW)
    mixed_grad[...] = dot(low[...], WA[:, col["co"]]).astype(LOW)

    def out_grads(left, right, target):
        def body(cols):
            PW[cols, target] = dot_tn(left[:, cols], right[...]).astype(LOW)

        rows_loop(model, 128, body)

    out_grads(low, mixed2, col["co"])
    pair_attend_back(
        tok, size.pairs, 512, probes, mkv, e2, rl2, mixed2, mixed_grad, q_grad, mkv_grad, None
    )
    part = dot_nt(q_grad[...], WA[:, col["cq"]])
    slot = wire.slots(1)
    ca[2] = part.astype(LOW)
    wire.swap(ca.at[2], cb.at[2], slot)
    out_grads(n2, q_grad, col["cq"])
    out_grads(E, mkv_grad, col["ckv"])

    def enc_rows(rows):
        EG[rows, :] = dot_nt(mkv_grad[rows, :], WA[:, col["ckv"]]).astype(LOW)

    rows_loop(ctx_enc, 256, enc_rows)
    sum_o.finish()
    layer_out[...] = after_cross[...] + po_whole[...].astype(F32)
    wire.got(cb.at[2], slot)
    n_grad = ca[2].astype(F32) + cb[2].astype(F32)
    extra, gain_two = rms_backward(after_self[...], gains[1:2], n_grad)
    self_grad[...] = cross_grad[...] + extra
    low[...] = self_grad[...].astype(LOW)
    mixed_grad[...] = dot(low[...], WA[:, col["o"]]).astype(LOW)
    out_grads(low, mixed1, col["o"])
    pair_attend_back(
        tok, size.pairs, 512, q, kv, e1, rl1, mixed1, mixed_grad, q_grad, kv_grad, diag
    )
    n2[...] = X[here_rows, :]
    out_grads(n2, q_grad, col["q"])
    out_grads(X, kv_grad, col["kv"])

    def tok_rows(rows):
        XG[rows, :] = dot_nt(kv_grad[rows, :], WA[:, col["kv"]]).astype(LOW)

    rows_loop(ctx_tok, 256, tok_rows)
    own = dot_nt(q_grad[...], WA[:, col["q"]]) + XG[here_rows, :].astype(F32)
    XG[here_rows, :] = own.astype(LOW)
    sums = bucket_sums(ids, diag, table.shape[1])
    SM[...] = jnp.zeros_like(SM)
    SM[1:2, :] = gain_two
    SM[2:3, :] = gain_three
    SM[8:16, :128] = jnp.concatenate(
        (sums, jnp.zeros((8, 128 - sums.shape[1]), F32)), axis=1
    )
    wire.drain()


def scatter_kernel(
    size, layer_in, gains, self_grad, pw, pm, xg, eg, SM,
    WG, MG, input_grad, enc_grad, totals,
    PW, PM, XG, EG, bs, bc, bx, be, px, pe, NG, NE, ml, ps, mb, s1, s2, sr, sl,
    local, send_sem, recv_sem,
):
    place = Place(size.ctx)
    wire = Wire(place, send_sem, recv_sem)
    copies = [
        pltpu.make_async_copy(src, dst, local.at[i])
        for i, (src, dst) in enumerate(((xg, XG), (eg, EG), (pm, PM), (pw, PW)))
    ]
    for made in copies:
        made.start()
    chips = place.above[1:] + [place.fx, place.fy, place.fxy]
    place.greet(chips, True)
    tok, enc, rows, half_d = size.tok, size.enc, size.rows, size.model // 2
    mine = pl.ds(aligned(place.core * half_d, 128), half_d)
    away = pl.ds(aligned(place.other * half_d, 128), half_d)

    def block_rows(block, count):
        return pl.ds(aligned(block * count, 16), count)

    def token_view(ref, count):
        def view(half, block):
            return ref.at[
                pl.ds(aligned(block * count + half * (count // 2), 16), count // 2), mine
            ]

        return view

    def token_out(ref, count):
        def out(half, total):
            ref[half * (count // 2) : (half + 1) * (count // 2), mine] = total

        return out

    def weight_stream(first, last, buf):
        step = (last - first) // 2

        def view(half, block):
            return PW.at[
                block_rows(block, rows), first + half * step : first + (half + 1) * step
            ]

        def out(half, total):
            WG[:, first + half * step : first + (half + 1) * step] = total

        return Scatter(wire, view, buf, out)

    def pair_sum(ref, recv, count):
        base = wire.slots(size.levels)
        span = 4 * count

        def start():
            for k in (1, 2, 3, 0):
                at = block_rows(place.below[k] // 4, span)
                wire.swap(ref.at[at, away], recv.at[at, :], base + k)

        def ready(k):
            at = block_rows(place.below[k] // 4, span)
            wire.got(recv.at[at, :], base + k)
            ref[at, mine] = (ref[at, mine].astype(F32) + recv[at, :].astype(F32)).astype(LOW)

        return start, ready

    sx = Scatter(wire, token_view(XG, tok), bx, token_out(NG, tok))
    se = Scatter(wire, token_view(EG, enc), be, token_out(NE, enc))
    sw = weight_stream(0, 4 * size.wide, bs)
    sc = weight_stream(4 * size.wide, 8 * size.wide, bc)
    x_start, x_ready = pair_sum(XG, px, tok)
    e_start, e_ready = pair_sum(EG, pe, enc)
    level_base, plane_base = wire.slots(3), wire.slots(3)
    copies[0].wait()
    x_start()
    copies[1].wait()
    e_start()
    sx.start(x_ready)
    se.start(e_ready)
    copies[2].wait()
    for k in (1, 2, 3):
        wire.send(
            PM.at[block_rows(place.above[k] // 4, 4 * rows), :],
            ml.at[k - 1],
            level_base + k - 1,
            place.above[k],
        )
    copies[3].wait()
    sw.start()
    sx.pass_near()
    se.pass_near()
    sx.pass_level()
    sc.start()
    se.pass_level()
    sw.pass_near()
    sx.finish()
    x_slot, e_slot = wire.slots(1), wire.slots(1)
    wire.swap(NG.at[:, mine], NG.at[:, mine], x_slot)
    se.finish()
    wire.swap(NE.at[:, mine], NE.at[:, mine], e_slot)
    sw.pass_level()
    sc.pass_near()
    total = PM[block_rows(place.level, 4 * rows), :].astype(F32)
    for k in (1, 2, 3):
        wire.got(ml.at[k - 1], level_base + k - 1)
        total = total + ml[k - 1].astype(F32)
    ps[...] = total.astype(LOW)
    my_cols = pl.ds(aligned(place.plane * size.part, 128), size.part)
    for k, chip in enumerate((place.fx, place.fy, place.fxy)):
        wire.send(
            ps.at[block_rows(lax.rem(chip, 4), rows), :], mb.at[:, my_cols], plane_base + k, chip
        )
    mb[:, my_cols] = ps[block_rows(place.plane, rows), :]
    wire.got(NG.at[:, away], x_slot)
    extra, gain_one = rms_backward(layer_in[...], gains[0:1], NG[...])
    input_grad[...] = self_grad[...] + extra
    s1[...] = SM[...]
    s1[0:1, :] = gain_one
    small = wire.slots(5)
    wire.send(s1, sr.at[0], small, place.fx)
    sc.pass_level()
    wire.got(sr.at[0], small)
    s2[...] = s1[...] + sr[0]
    wire.send(s2, sr.at[1], small + 1, place.fy)
    wire.got(NE.at[:, away], e_slot)
    enc_grad[...] = NE[...]
    sw.finish()
    wire.got(sr.at[1], small + 1)
    sl[pl.ds(place.level, 1)] = (s2[...] + sr[1])[None]
    for k in (1, 2, 3):
        wire.send(
            sl.at[place.level], sl.at[place.level], small + 1 + k, place.above[k]
        )
    sc.finish()
    for k, chip in enumerate((place.fx, place.fy, place.fxy)):
        cols = pl.ds(aligned(lax.rem(chip, 4) * size.part, 128), size.part)
        wire.got(mb.at[:, cols], plane_base + k)
    MG[...] = mb[...].astype(F32)
    for k in (1, 2, 3):
        wire.got(sl.at[place.below[k] // 4], small + 1 + k)
    totals[...] = (sl[0] + sl[1]) + (sl[2] + sl[3])
    wire.drain()


def quick_device(
    layer_in, encoded, self_query, self_key, self_value, self_out, cross_query, cross_key,
    cross_value, cross_out, gate_proj, up_proj, down_proj, norm_gains, position_bias,
    bucket_ids, block_order, out_grad,
):
    tok, model = layer_in.shape
    enc = encoded.shape[0]
    wide, units = self_query.shape[1], gate_proj.shape[1]
    ctx = block_order.shape[0]
    buckets, heads = position_bias.shape
    size = Sizes(ctx, tok, enc, model, wide, units)
    rows, quarter = size.rows, size.quarter

    wa = jnp.concatenate(
        (
            self_query, self_key, self_value, self_out.T,
            cross_query, cross_key, cross_value, cross_out.T,
        ),
        axis=1,
    )
    wm = jnp.concatenate(
        [
            piece[:, p * quarter : (p + 1) * quarter]
            for p in range(4)
            for piece in (gate_proj, up_proj, down_proj.T)
        ],
        axis=1,
    )
    boundaries = jnp.arange(1, buckets, dtype=jnp.int32)
    starts = jnp.sum((bucket_ids[None, :] < boundaries[:, None]).astype(jnp.int32), axis=1)
    here = lax.axis_index("ctx")
    own_block = jnp.sum(jnp.where(jnp.arange(ctx) == here, block_order, 0))
    lane = jnp.arange(2 * tok, dtype=jnp.int32)
    shift = jnp.where(lane < tok, lane, lane - 2 * tok)
    dist = (own_block - block_order)[:, None] * tok - shift[None, :]
    ids = jnp.sum((dist[:, :, None] >= starts[None, None, :]).astype(jnp.int32), axis=-1)
    ids = jnp.where(dist >= 0, ids, -1)
    table = jnp.concatenate((position_bias.T, jnp.zeros((8 - heads, buckets), F32)), axis=0)

    tok_all, enc_all, tok4 = ctx * tok, ctx * enc, 4 * tok
    pairs = size.pairs
    got = call(
        gather_kernel,
        size,
        {"layer_in": layer_in, "encoded": encoded, "gains": norm_gains, "out_grad": out_grad,
         "wa": wa, "wm": wm},
        {"WA": ((model, size.attn_cols), LOW), "WM": ((model, size.part), LOW),
         "X": ((tok_all, model), LOW), "E": ((enc_all, model), LOW), "GR": ((tok4, model), LOW)},
        {"local": pltpu.SemaphoreType.DMA((2,)), **wire_sems(256)},
        1,
    )

    def vmem(*shape, dtype=LOW):
        return pltpu.VMEM(shape, dtype)

    done = call(
        compute_kernel,
        size,
        {"layer_in": layer_in, "gains": norm_gains, "out_grad": out_grad, "ids": ids,
         "table": table, "WA": got["WA"], "WM": got["WM"], "X": got["X"], "E": got["E"],
         "GR": got["GR"]},
        {"layer_out": ((tok, model), F32), "PW": ((model, size.attn_cols), LOW),
         "PM": ((model, size.part), LOW), "XG": ((tok_all, model), LOW),
         "EG": ((enc_all, model), LOW), "self_grad": ((tok, model), F32),
         "SM": ((16, model), F32)},
        {"q": vmem(tok, wide), "kv": vmem(tok_all, 2 * wide), "mkv": vmem(enc_all, 2 * wide),
         "probes": vmem(tok, wide), "s": vmem(2 * tok, tok_all, dtype=F32),
         "e1": vmem(pairs, 2 * tok, tok_all), "e2": vmem(pairs, 2 * tok, enc_all),
         "rl1": vmem(pairs, 2 * tok, 1, dtype=F32), "rl2": vmem(pairs, 2 * tok, 1, dtype=F32),
         "mixed1": vmem(tok, wide), "mixed2": vmem(tok, wide),
         "bias": vmem(ctx, 8, 2 * tok, dtype=F32), "diag": vmem(ctx, 8, 2 * tok, dtype=F32),
         "after_self": vmem(tok, model, dtype=F32), "after_cross": vmem(tok, model, dtype=F32),
         "cross_grad": vmem(tok, model, dtype=F32), "n2": vmem(tok, model),
         "N3": vmem(tok4, model), "act": vmem(tok4, quarter), "GU": vmem(tok4, 2 * quarter),
         "PN": vmem(tok4, model), "PO": vmem(tok4, model), "low": vmem(tok, model),
         "mixed_grad": vmem(tok, wide), "q_grad": vmem(tok, wide),
         "kv_grad": vmem(tok_all, 2 * wide), "mkv_grad": vmem(enc_all, 2 * wide),
         "ca": vmem(3, tok, model), "cb": vmem(3, tok, model),
         "pn_core": vmem(tok4, model // 2), "pn_plane": vmem(3, tok, model // 2),
         "pn_whole": vmem(tok, model), "po_core": vmem(tok4, model // 2),
         "po_plane": vmem(3, tok, model // 2), "po_whole": vmem(tok, model), **wire_sems(32)},
        2,
    )
    last = call(
        scatter_kernel,
        size,
        {"layer_in": layer_in, "gains": norm_gains, "self_grad": done["self_grad"],
         "pw": done["PW"], "pm": done["PM"], "xg": done["XG"], "eg": done["EG"], "SM": done["SM"]},
        {"WG": ((rows, size.attn_cols), F32), "MG": ((rows, size.mlp_cols), F32),
         "input_grad": ((tok, model), F32), "enc_grad": ((enc, model), F32),
         "totals": ((16, model), F32)},
        {"PW": vmem(model, size.attn_cols), "PM": vmem(model, size.part),
         "XG": vmem(tok_all, model), "EG": vmem(enc_all, model),
         "bs": vmem(2, 15, rows, 2 * wide), "bc": vmem(2, 15, rows, 2 * wide),
         "bx": vmem(2, 15, tok // 2, model // 2), "be": vmem(2, 15, enc // 2, model // 2),
         "px": vmem(tok_all, model // 2), "pe": vmem(enc_all, model // 2),
         "NG": vmem(tok, model, dtype=F32), "NE": vmem(enc, model, dtype=F32),
         "ml": vmem(3, 4 * rows, size.part), "ps": vmem(4 * rows, size.part),
         "mb": vmem(rows, size.mlp_cols), "s1": vmem(16, model, dtype=F32),
         "s2": vmem(16, model, dtype=F32), "sr": vmem(2, 16, model, dtype=F32),
         "sl": vmem(4, 16, model, dtype=F32), "local": pltpu.SemaphoreType.DMA((4,)),
         **wire_sems(160)},
        3,
        any_inputs=("pw", "pm", "xg", "eg"),
    )
    wg, mg, totals = last["WG"], last["MG"], last["totals"]
    grads = [wg[:, size.col[name]] for name in ("q", "k", "v", "o", "cq", "ck", "cv", "co")]
    mlp = mg.reshape(rows, 4, 3, quarter)
    gate, upward, down = (mlp[:, :, i].reshape(rows, units) for i in range(3))
    return (
        done["layer_out"],
        last["input_grad"],
        last["enc_grad"],
        *grads[:3],
        grads[3].T,
        *grads[4:7],
        grads[7].T,
        gate,
        upward,
        down.T,
        totals[:3],
        totals[8 : 8 + heads, :buckets].T,
    )


def quick_fits(mesh):
    return mesh.shape["ctx"] == 16 and mesh.shape["head"] == 2


def as_sent(shard):

    def short(part):
        return part.astype(jnp.bfloat16) if part.dtype == jnp.float32 else part

    return jax.tree.map(short, shard)


def rms_scale(rows, gain):
    return rows * lax.rsqrt(jnp.mean(rows * rows, axis=-1, keepdims=True) + EPS) * gain


def geglu(gate, upper):
    return jax.nn.gelu(gate, approximate=True) * upper


def times(left, right):
    return jnp.dot(left, right, preferred_element_type=jnp.float32)


def left_times(left, right):
    return lax.dot_general(
        left, right, (((0,), (0,)), ((), ())), preferred_element_type=jnp.float32
    )


def right_times(left, right):
    return lax.dot_general(
        left, right, (((1,), (1,)), ((), ())), preferred_element_type=jnp.float32
    )


def join_heads(parts):
    return jax.tree.map(lambda part: part.astype(jnp.float32), lax.psum(as_sent(parts), "head"))


def gather_self(keys_own, values_own):
    return (
        lax.all_gather(keys_own, "ctx", axis=0, tiled=True),
        lax.all_gather(values_own, "ctx", axis=0, tiled=True),
    )


def gather_cross(memory_keys, memory_values):
    return (
        lax.all_gather(memory_keys, "ctx", axis=0, tiled=True),
        lax.all_gather(memory_values, "ctx", axis=0, tiled=True),
    )


def bias_scores(steps, bias_table):
    rises = bias_table[1:] - bias_table[:-1]
    return bias_table[0][:, None, None] + jnp.einsum("qkb,bh->hqk", steps, rises, precision=HIGH)


def bias_grads(score_grad, steps):
    above = jnp.einsum("hqk,qkb->bh", score_grad, steps, precision=HIGH)
    total = jnp.sum(score_grad, axis=(1, 2))
    upper_rows = jnp.concatenate((total[None], above), axis=0)
    lower_rows = jnp.concatenate((above, jnp.zeros((1, above.shape[1]), jnp.float32)), axis=0)
    return upper_rows - lower_rows


def delta_of(mixed, mixed_grad, head_count):
    tok_rows, total_width = mixed.shape
    width = total_width // head_count
    product = mixed.astype(jnp.float32).reshape(tok_rows, head_count, width) * mixed_grad.astype(
        jnp.float32
    ).reshape(tok_rows, head_count, width)
    return jnp.transpose(jnp.sum(product, axis=-1))


def attend_fold(queries, head_count, parts_fn, bias_table):
    tok_rows = queries.shape[0]
    width = queries.shape[1] // head_count
    query3 = queries.reshape(tok_rows, head_count, width)

    def fold(state, pieces, start):
        key_piece, value_piece = pieces
        count = key_piece.shape[0]
        block = math.gcd(count, 512)

        def fold_step(index, inner):
            summed, run_max, run_sum = inner
            key3 = lax.dynamic_slice_in_dim(key_piece, index * block, block, 0).reshape(
                block, head_count, width
            )
            value3 = lax.dynamic_slice_in_dim(value_piece, index * block, block, 0).reshape(
                block, head_count, width
            )
            scores = jnp.einsum("qhe,khe->hqk", query3, key3, preferred_element_type=jnp.float32)
            if parts_fn is not None:
                steps, valid = parts_fn(index * block, block)
                scores = jnp.where(valid[None], scores + bias_scores(steps, bias_table), NEG)
            new_max = jnp.maximum(run_max, jnp.max(scores, axis=-1))
            ratio = jnp.exp(run_max - new_max)
            weights = jnp.exp(scores - new_max[..., None])
            run_sum = run_sum * ratio + jnp.sum(weights, axis=-1)
            summed = summed * ratio[..., None] + jnp.einsum(
                "hqk,khe->hqe",
                weights.astype(jnp.bfloat16),
                value3,
                preferred_element_type=jnp.float32,
            )
            return (summed, new_max, run_sum)

        return lax.fori_loop(0, count // block, fold_step, state)

    return fold


def finish(state):
    summed, run_max, run_sum = state
    head_count, tok_rows, width = summed.shape
    mixed = jnp.transpose(summed / run_sum[..., None], (1, 0, 2)).reshape(
        tok_rows, head_count * width
    )
    return (mixed.astype(jnp.bfloat16), run_max + jnp.log(run_sum))


def attend_back(
    queries, mixed_grad, lse, delta, keys_all, values_all, head_count, parts_fn, bias_table
):
    tok_rows, total_width = queries.shape
    width = total_width // head_count
    query3 = queries.reshape(tok_rows, head_count, width)
    grad3 = mixed_grad.reshape(tok_rows, head_count, width)
    count = keys_all.shape[0]
    block = math.gcd(count, 512)

    def attend_step(carry, index):
        query_grad, bias_grad = carry
        key3 = lax.dynamic_slice_in_dim(keys_all, index * block, block, 0).reshape(
            block, head_count, width
        )
        value3 = lax.dynamic_slice_in_dim(values_all, index * block, block, 0).reshape(
            block, head_count, width
        )
        scores = jnp.einsum("qhe,khe->hqk", query3, key3, preferred_element_type=jnp.float32)
        if parts_fn is not None:
            steps, valid = parts_fn(index * block, block)
            scores = jnp.where(valid[None], scores + bias_scores(steps, bias_table), NEG)
        weights = jnp.exp(scores - lse[..., None])
        weight_grad = jnp.einsum("qhe,khe->hqk", grad3, value3, preferred_element_type=jnp.float32)
        score_grad = weights * (weight_grad - delta[..., None])
        if parts_fn is not None:
            bias_grad = bias_grad + bias_grads(score_grad, steps)
        score_low = score_grad.astype(jnp.bfloat16)
        query_grad = query_grad + jnp.einsum(
            "hqk,khe->qhe", score_low, key3, preferred_element_type=jnp.float32
        )
        stacked = None
        value_term = jnp.einsum(
            "hqk,qhe->khe", weights.astype(jnp.bfloat16), grad3, preferred_element_type=jnp.float32
        )
        key_term = jnp.einsum("hqk,qhe->khe", score_low, query3, preferred_element_type=jnp.float32)
        stacked = jnp.concatenate(
            (key_term.reshape(block, total_width), value_term.reshape(block, total_width)), axis=1
        )
        return ((query_grad, bias_grad), stacked)

    start = (
        jnp.zeros((tok_rows, head_count, width), jnp.float32),
        jnp.zeros(bias_table.shape, jnp.float32),
    )
    (query_grad, bias_grad), terms = lax.scan(attend_step, start, jnp.arange(count // block))
    query_grad = query_grad.reshape(tok_rows, total_width).astype(jnp.bfloat16)
    terms = terms.reshape(count, 2 * total_width)
    return (query_grad, bias_grad, terms)


def per_device(
    layer_in,
    encoded,
    self_query,
    self_key,
    self_value,
    self_out,
    cross_query,
    cross_key,
    cross_value,
    cross_out,
    gate_proj,
    up_proj,
    down_proj,
    norm_gains,
    position_bias,
    bucket_ids,
    block_order,
    out_grad,
):
    low = jnp.bfloat16
    tok_rows = layer_in.shape[0]
    bucket_count, head_count = position_bias.shape
    block_count = block_order.shape[0]
    full_weights = (
        lax.all_gather(self_query, "ctx", axis=0, tiled=True),
        lax.all_gather(self_key, "ctx", axis=0, tiled=True),
        lax.all_gather(self_value, "ctx", axis=0, tiled=True),
        lax.all_gather(self_out, "ctx", axis=1, tiled=True),
        lax.all_gather(cross_query, "ctx", axis=0, tiled=True),
        lax.all_gather(cross_key, "ctx", axis=0, tiled=True),
        lax.all_gather(cross_value, "ctx", axis=0, tiled=True),
        lax.all_gather(cross_out, "ctx", axis=1, tiled=True),
        lax.all_gather(gate_proj, "ctx", axis=0, tiled=True),
        lax.all_gather(up_proj, "ctx", axis=0, tiled=True),
        lax.all_gather(down_proj, "ctx", axis=1, tiled=True),
    )
    (
        query_full,
        key_full,
        value_full,
        output_full,
        probe_full,
        lookup_full,
        recall_full,
        merge_full,
        gate_full,
        upward_full,
        down_full,
    ) = full_weights
    boundaries = jnp.arange(1, bucket_count, dtype=jnp.int32)
    starts = jnp.sum((bucket_ids[None, :] < boundaries[:, None]).astype(jnp.int32), axis=1)
    block_ids = jnp.arange(block_count, dtype=jnp.int32)
    here = lax.axis_index("ctx")
    own_block = jnp.sum(jnp.where(block_ids == here, block_order, 0))
    query_pos = own_block * tok_rows + jnp.arange(tok_rows, dtype=jnp.int32)

    def position_of(rows_index):
        slot = rows_index // tok_rows
        owner = jnp.sum(
            jnp.where(slot[:, None] == block_ids[None, :], block_order[None, :], 0), axis=1
        )
        return owner * tok_rows + rows_index % tok_rows

    def pair_parts(first_pos, second_pos):
        dist = first_pos[:, None] - second_pos[None, :]
        steps = (dist[:, :, None] >= starts[None, None, :]).astype(jnp.float32)
        return (steps, dist >= 0)

    def causal_parts(key_start, count):
        return pair_parts(query_pos, position_of(key_start + jnp.arange(count, dtype=jnp.int32)))

    normed_one = rms_scale(layer_in, norm_gains[0]).astype(low)
    queries = times(normed_one, query_full).astype(low)
    keys_own = times(normed_one, key_full).astype(low)
    values_own = times(normed_one, value_full).astype(low)
    memory_keys = times(encoded, lookup_full).astype(low)
    memory_values = times(encoded, recall_full).astype(low)
    total_width = queries.shape[1]
    width = total_width // head_count
    start_state = (
        jnp.zeros((head_count, tok_rows, width), jnp.float32),
        jnp.full((head_count, tok_rows), NEG, jnp.float32),
        jnp.zeros((head_count, tok_rows), jnp.float32),
    )
    self_fold = attend_fold(queries, head_count, causal_parts, position_bias)
    self_state = self_fold(
        start_state,
        (
            lax.all_gather(keys_own, "ctx", axis=0, tiled=True),
            lax.all_gather(values_own, "ctx", axis=0, tiled=True),
        ),
        jnp.int32(0),
    )
    mixed_one, lse_one = finish(self_state)
    after_self = layer_in + join_heads(times(mixed_one, output_full))
    normed_two = rms_scale(after_self, norm_gains[1]).astype(low)
    probes = times(normed_two, probe_full).astype(low)
    cross_fold = attend_fold(probes, head_count, None, position_bias)
    cross_state = cross_fold(
        start_state,
        (
            lax.all_gather(memory_keys, "ctx", axis=0, tiled=True),
            lax.all_gather(memory_values, "ctx", axis=0, tiled=True),
        ),
        jnp.int32(0),
    )
    mixed_two, lse_two = finish(cross_state)
    after_cross = after_self + join_heads(times(mixed_two, merge_full))
    normed_three = rms_scale(after_cross, norm_gains[2]).astype(low)
    gate_pre = times(normed_three, gate_full)
    upper = times(normed_three, upward_full)
    activated = geglu(gate_pre, upper).astype(low)
    layer_out = after_cross + join_heads(times(activated, down_full))
    grad_rows = out_grad.astype(low)
    down_wgrad = left_times(activated, grad_rows)
    act_grad = right_times(grad_rows, down_full)
    geglu_out, geglu_pull = jax.vjp(geglu, gate_pre, upper)
    gate_grad, upper_grad = geglu_pull(act_grad)
    gate_grad = gate_grad.astype(low)
    upper_grad = upper_grad.astype(low)
    gate_wgrad = left_times(normed_three, gate_grad)
    up_wgrad = left_times(normed_three, upper_grad)
    normed_three_grad = join_heads(
        right_times(gate_grad, gate_full) + right_times(upper_grad, upward_full)
    )
    norm_out, norm_pull = jax.vjp(rms_scale, after_cross, norm_gains[2])
    cross_extra, gain_three = norm_pull(normed_three_grad)
    cross_grad = out_grad + cross_extra
    cross_rows = cross_grad.astype(low)
    merge_wgrad = left_times(mixed_two, cross_rows)
    mixed_two_grad = right_times(cross_rows, merge_full).astype(low)
    delta_two = delta_of(mixed_two, mixed_two_grad, head_count)
    memory_all = gather_cross(memory_keys, memory_values)
    probe_grad, unused_bias, cross_terms = attend_back(
        probes,
        mixed_two_grad,
        lse_two,
        delta_two,
        memory_all[0],
        memory_all[1],
        head_count,
        None,
        position_bias,
    )
    cross_terms = lax.psum_scatter(cross_terms, "ctx", scatter_dimension=0, tiled=True)
    memory_key_grad = cross_terms[:, :total_width].astype(low)
    memory_value_grad = cross_terms[:, total_width:].astype(low)
    probe_wgrad = left_times(normed_two, probe_grad)
    lookup_wgrad = left_times(encoded, memory_key_grad)
    recall_wgrad = left_times(encoded, memory_value_grad)
    normed_two_grad, encoded_grad = join_heads(
        (
            right_times(probe_grad, probe_full),
            right_times(memory_key_grad, lookup_full) + right_times(memory_value_grad, recall_full),
        )
    )
    norm_out, norm_pull = jax.vjp(rms_scale, after_self, norm_gains[1])
    self_extra, gain_two = norm_pull(normed_two_grad)
    self_grad = cross_grad + self_extra
    self_rows = self_grad.astype(low)
    output_wgrad = left_times(mixed_one, self_rows)
    mixed_one_grad = right_times(self_rows, output_full).astype(low)
    delta_one = delta_of(mixed_one, mixed_one_grad, head_count)
    sequence_all = gather_self(keys_own, values_own)
    query_grad, bias_grad, self_terms = attend_back(
        queries,
        mixed_one_grad,
        lse_one,
        delta_one,
        sequence_all[0],
        sequence_all[1],
        head_count,
        causal_parts,
        position_bias,
    )
    self_terms = lax.psum_scatter(self_terms, "ctx", scatter_dimension=0, tiled=True)
    key_grad = self_terms[:, :total_width].astype(low)
    value_grad = self_terms[:, total_width:].astype(low)
    query_wgrad = left_times(normed_one, query_grad)
    key_wgrad = left_times(normed_one, key_grad)
    value_wgrad = left_times(normed_one, value_grad)
    normed_one_grad = join_heads(
        right_times(query_grad, query_full)
        + right_times(key_grad, key_full)
        + right_times(value_grad, value_full)
    )
    norm_out, norm_pull = jax.vjp(rms_scale, layer_in, norm_gains[0])
    input_extra, gain_one = norm_pull(normed_one_grad)
    input_grad = self_grad + input_extra
    weight_sums = (
        lax.psum_scatter(query_wgrad, "ctx", scatter_dimension=0, tiled=True),
        lax.psum_scatter(key_wgrad, "ctx", scatter_dimension=0, tiled=True),
        lax.psum_scatter(value_wgrad, "ctx", scatter_dimension=0, tiled=True),
        lax.psum_scatter(output_wgrad, "ctx", scatter_dimension=1, tiled=True),
        lax.psum_scatter(probe_wgrad, "ctx", scatter_dimension=0, tiled=True),
        lax.psum_scatter(lookup_wgrad, "ctx", scatter_dimension=0, tiled=True),
        lax.psum_scatter(recall_wgrad, "ctx", scatter_dimension=0, tiled=True),
        lax.psum_scatter(merge_wgrad, "ctx", scatter_dimension=1, tiled=True),
        lax.psum_scatter(gate_wgrad, "ctx", scatter_dimension=0, tiled=True),
        lax.psum_scatter(up_wgrad, "ctx", scatter_dimension=0, tiled=True),
        lax.psum_scatter(down_wgrad, "ctx", scatter_dimension=1, tiled=True),
    )
    gains_sum, bias_sum = lax.psum((jnp.stack((gain_one, gain_two, gain_three)), bias_grad), "ctx")
    return (layer_out, input_grad, encoded_grad) + tuple(weight_sums) + (gains_sum, bias_sum)


def solution(mesh):
    body = quick_device if quick_fits(mesh) else per_device
    placed = (
        P("ctx", None),
        P("ctx", None),
        P("ctx", "head"),
        P("ctx", "head"),
        P("ctx", "head"),
        P("head", "ctx"),
        P("ctx", "head"),
        P("ctx", "head"),
        P("ctx", "head"),
        P("head", "ctx"),
        P("ctx", "head"),
        P("ctx", "head"),
        P("head", "ctx"),
        P(),
        P(None, "head"),
        P(),
        P(),
        P("ctx", None),
    )
    return jax.shard_map(
        body,
        mesh=mesh,
        in_specs=placed,
        out_specs=(
            P("ctx", None),
            P("ctx", None),
            P("ctx", None),
            P("ctx", "head"),
            P("ctx", "head"),
            P("ctx", "head"),
            P("head", "ctx"),
            P("ctx", "head"),
            P("ctx", "head"),
            P("ctx", "head"),
            P("head", "ctx"),
            P("ctx", "head"),
            P("ctx", "head"),
            P("head", "ctx"),
            P(),
            P(None, "head"),
        ),
        check_vma=False,
    )
```

```python
import functools
import math

import jax
import jax.numpy as jnp
from jax import lax
from jax.experimental import pallas as pl
from jax.experimental.pallas import tpu as pltpu
from jax.sharding import PartitionSpec as P

EPS = 1e-06
NEG = -1e30
HIGH = lax.Precision.HIGHEST
LOW = jnp.bfloat16
F32 = jnp.float32
MESH = pl.DeviceIdType.MESH
VMEM_LIMIT = 66_000_000


def dot(left, right, **kw):
    return jnp.dot(left, right, preferred_element_type=F32, **kw)


def dot_nt(left, right, **kw):
    return lax.dot_general(left, right, (((1,), (1,)), ((), ())), preferred_element_type=F32, **kw)


def dot_tn(left, right, **kw):
    return lax.dot_general(left, right, (((0,), (0,)), ((), ())), preferred_element_type=F32, **kw)


def rms_forward(rows, gain):
    return rows * lax.rsqrt(jnp.mean(rows * rows, axis=-1, keepdims=True) + EPS) * gain


def rms_backward(rows, gain, grad):
    scale = lax.rsqrt(jnp.mean(rows * rows, axis=-1, keepdims=True) + EPS)
    scaled = gain * grad
    inner = jnp.mean(scaled * rows, axis=-1, keepdims=True)
    row_grad = scale * scaled - rows * (scale * scale * scale * inner)
    gain_grad = jnp.sum(grad * rows * scale, axis=0, keepdims=True)
    return row_grad, gain_grad


def aligned(value, step):
    return value if isinstance(value, int) else pl.multiple_of(value, step)


class Place:
    def __init__(self, count):
        self.count = count
        self.here = lax.axis_index("ctx")
        self.core = lax.axis_index("head")
        self.other = 1 - self.core
        self.plane = lax.rem(self.here, 4)
        self.level = self.here // 4
        self.fx = self.flip(self.here, 0)
        self.fy = self.flip(self.here, 1)
        self.fxy = self.flip(self.fx, 1)
        self.above = [lax.rem(self.here + 4 * k, count) for k in range(4)]
        self.below = [lax.rem(self.here + count - 4 * k, count) for k in range(4)]

    def flip(self, index, axis):
        if axis == 0:
            return index + 1 - 2 * lax.rem(index, 2)
        return index + 2 - 4 * lax.rem(index // 2, 2)

    def near(self, half):
        return (self.fx, self.fy) if half == 0 else (self.fy, self.fx)

    def greet(self, chips, partner):
        barrier = pltpu.get_barrier_semaphore()
        total = len(chips) + (1 if partner else 0)
        for chip in chips:
            pl.semaphore_signal(
                barrier, inc=1, device_id=(chip, self.core), device_id_type=MESH
            )
        if partner:
            pl.semaphore_signal(
                barrier, inc=1, device_id=(self.here, self.other), device_id_type=MESH
            )
        pl.semaphore_wait(barrier, total)


class Wire:
    def __init__(self, place, send_sem, recv_sem):
        self.place, self.send_sem, self.recv_sem = place, send_sem, recv_sem
        self.sent = []
        self.used = 0

    def slots(self, count):
        base = self.used
        self.used += count
        assert self.used <= self.send_sem.shape[0], self.used
        return base

    def copy(self, src, dst, slot, chip, core):
        return pltpu.make_async_remote_copy(
            src_ref=src,
            dst_ref=dst,
            send_sem=self.send_sem.at[slot],
            recv_sem=self.recv_sem.at[slot],
            device_id=(chip, core),
            device_id_type=MESH,
        )

    def send(self, src, dst, slot, chip=None, core=None):
        chip = self.place.here if chip is None else chip
        core = self.place.core if core is None else core
        made = self.copy(src, dst, slot, chip, core)
        made.start()
        self.sent.append(made)

    def swap(self, src, dst, slot):
        self.send(src, dst, slot, None, self.place.other)

    def got(self, dst, slot):
        place = self.place
        self.copy(dst, dst, slot, place.here, place.other).wait_recv()

    def drain(self):
        for made in self.sent:
            made.wait_send()
        self.sent = []


class Gather:
    def __init__(self, wire, view, share, halves=2):
        self.wire, self.view, self.share = wire, view, share
        self.base = [wire.slots(15) for _ in range(halves)]
        self.side = [wire.slots(16) for _ in range(halves)] if share else None
        self.halves = range(halves)

    def _out(self, half, block, slot, chip):
        ref = self.view(half, block)
        self.wire.send(ref, ref, self.base[half] + slot, chip)

    def _in(self, half, block, slot):
        self.wire.got(self.view(half, block), self.base[half] + slot)
        if self.share:
            ref = self.view(half, block)
            self.wire.swap(ref, ref, self.side[half] + slot)

    def start(self):
        place = self.wire.place
        for half in self.halves:
            near, far = place.near(half)
            for k in (1, 2, 3):
                self._out(half, place.here, k - 1, place.above[k])
            self._out(half, place.here, 3, near)
            self._out(half, place.here, 7, far)

    def pass_level(self):
        place = self.wire.place
        for k in (1, 2, 3):
            for half in self.halves:
                near, far = place.near(half)
                self._in(half, place.below[k], k - 1)
                self._out(half, place.below[k], 3 + k, near)
                self._out(half, place.below[k], 7 + k, far)

    def pass_near(self):
        place = self.wire.place
        for k in range(4):
            for half in self.halves:
                _, far = place.near(half)
                block = place.flip(place.below[k], half)
                self._in(half, block, 3 + k)
                self._out(half, block, 11 + k, far)

    def finish(self):
        place = self.wire.place
        for k in range(4):
            for half in self.halves:
                block = place.flip(place.below[k], 1 - half)
                self._in(half, block, 7 + k)
                self._in(half, place.flip(block, half), 11 + k)

    def finish_share(self):
        if not self.share:
            return
        place = self.wire.place
        for k in range(4):
            for half in self.halves:
                block = place.below[k]
                if k:
                    self._share_in(half, block, k - 1)
                self._share_in(half, place.flip(block, half), 3 + k)
                block = place.flip(block, 1 - half)
                self._share_in(half, block, 7 + k)
                self._share_in(half, place.flip(block, half), 11 + k)

    def _share_in(self, half, block, slot):
        self.wire.got(self.share(half, block), self.side[half] + slot)


class Scatter:
    def __init__(self, wire, view, buf, out, halves=2):
        self.wire, self.view, self.out = wire, view, out
        self.far_buf = lambda half, slot: buf(half).at[slot]
        self.near_buf = lambda half, slot: buf(half).at[8 + slot]
        self.level_buf = lambda half, slot: buf(half).at[12 + slot]
        self.base = [wire.slots(15) for _ in range(halves)]
        self.halves = range(halves)

    def start(self, levels=(1, 2, 3, 0)):
        place = self.wire.place
        for k in levels:
            for half in self.halves:
                _, far = place.near(half)
                away = place.flip(place.below[k], 1 - half)
                for pair, block in ((1, place.flip(away, half)), (0, away)):
                    slot = 2 * k + pair
                    self.wire.send(
                        self.view(half, block),
                        self.far_buf(half, slot),
                        self.base[half] + slot,
                        far,
                    )

    def pass_near(self):
        place = self.wire.place
        for k in (1, 2, 3, 0):
            for half in self.halves:
                near, _ = place.near(half)
                block = place.flip(place.below[k], half)
                slot = 2 * k + 1
                self.wire.got(self.far_buf(half, slot), self.base[half] + slot)
                ref = self.view(half, block)
                ref[...] = (
                    ref[...].astype(F32) + self.far_buf(half, slot)[...].astype(F32)
                ).astype(LOW)
                self.wire.send(ref, self.near_buf(half, k), self.base[half] + 8 + k, near)

    def pass_level(self):
        place = self.wire.place
        for k in (1, 2, 3):
            for half in self.halves:
                self._add(half, k)
                ref = self.view(half, place.below[k])
                self.wire.send(
                    ref, self.level_buf(half, k - 1), self.base[half] + 11 + k, place.below[k]
                )

    def _add(self, half, k):
        place = self.wire.place
        self.wire.got(self.far_buf(half, 2 * k), self.base[half] + 2 * k)
        self.wire.got(self.near_buf(half, k), self.base[half] + 8 + k)
        ref = self.view(half, place.below[k])
        total = (
            ref[...].astype(F32)
            + self.far_buf(half, 2 * k)[...].astype(F32)
            + self.near_buf(half, k)[...].astype(F32)
        )
        if k:
            ref[...] = total.astype(LOW)
        return total

    def finish(self):
        for half in self.halves:
            total = self._add(half, 0)
            for k in (1, 2, 3):
                self.wire.got(self.level_buf(half, k - 1), self.base[half] + 11 + k)
                total = total + self.level_buf(half, k - 1)[...].astype(F32)
            self.out(half, total)


def lane_split(rows):
    lane = lax.broadcasted_iota(jnp.int32, rows.shape, 1)
    low = lane < rows.shape[1] // 2
    zero = jnp.zeros_like(rows)
    return jnp.concatenate((jnp.where(low, rows, zero), jnp.where(low, zero, rows)), axis=0)


def lane_join(rows):
    count, width = rows.shape[0] // 2, rows.shape[1]
    lane = lax.broadcasted_iota(jnp.int32, (count, width), 1)
    return jnp.where(lane < width // 2, rows[:count], rows[count:])


def pair_attend(tok, pairs, chunk, q_ref, kv_ref, s_ref, e_ref, rl_ref, mixed_ref, bias_ref, between):
    keys = kv_ref.shape[0]
    total = pairs * 128

    for j in range(pairs):
        cols = slice(j * 128, (j + 1) * 128)
        vcols = slice(total + j * 128, total + (j + 1) * 128)
        q_cat = lane_split(q_ref[:, cols])

        def score(c, top):
            rows = pl.ds(aligned(c * chunk, chunk), chunk)
            s = dot_nt(q_cat, kv_ref[rows, cols])
            if bias_ref is not None:
                tiles = []
                for half in range(2):
                    row = []
                    for b in range(chunk // tok):
                        vec = bias_ref[c * (chunk // tok) + b, 2 * j + half : 2 * j + half + 1, :]
                        wide = jnp.broadcast_to(vec, (tok, 2 * tok))
                        row.append(pltpu.roll(wide, 0, 1, stride=1, stride_axis=0)[:, :tok])
                    tiles.append(jnp.concatenate(row, axis=1))
                s = s + jnp.concatenate(tiles, axis=0)
            s_ref[:, rows] = s
            for b in range(chunk // 128):
                top = jnp.maximum(top, s[:, b * 128 : (b + 1) * 128])
            return top

        top = lax.fori_loop(0, keys // chunk, score, jnp.full((2 * tok, 128), NEG, F32))
        peak = jnp.max(top, axis=1, keepdims=True)

        def weigh(c, state):
            acc, run = state
            rows = pl.ds(aligned(c * chunk, chunk), chunk)
            e = jnp.exp(s_ref[:, rows] - peak)
            for b in range(chunk // 128):
                run = run + e[:, b * 128 : (b + 1) * 128]
            low = e.astype(LOW)
            e_ref[j, :, rows] = low
            return (acc + dot(low, kv_ref[rows, vcols]), run)

        zero = jnp.zeros((2 * tok, 128), F32)
        acc, run = lax.fori_loop(0, keys // chunk, weigh, (zero, zero))
        rl = 1.0 / jnp.sum(run, axis=1, keepdims=True)
        rl_ref[j] = rl
        mixed_ref[:, cols] = lane_join(acc * rl).astype(LOW)
        between(j)


class PairBack:
    def __init__(self, tok, pairs, q, kv, e, rl, mixed, grad, kv_grad, diag, qc, gc, dl, dq):
        self.tok, self.pairs, self.kv, self.e = tok, pairs, kv, e
        self.kv_grad, self.diag, self.qc, self.gc, self.dl, self.dq = kv_grad, diag, qc, gc, dl, dq
        self.total = pairs * 128
        for j in range(pairs):
            cols = slice(j * 128, (j + 1) * 128)
            rl_j = rl[j]
            grads = lane_split(grad[:, cols].astype(F32))
            qc[j] = lane_split(q[:, cols])
            gc[j] = (grads * rl_j).astype(LOW)
            values = lane_split(mixed[:, cols].astype(F32))
            dl[j] = jnp.sum(grads * values, axis=1, keepdims=True) * rl_j
            dq[j] = jnp.zeros(dq.shape[1:], F32)

    def chunk(self, start, count):
        tok, kv, qc, gc = self.tok, self.kv, self.qc, self.gc
        rows = pl.ds(aligned(start, count), count)
        flip = (
            lax.broadcasted_iota(jnp.int32, (tok, tok), 0)
            + lax.broadcasted_iota(jnp.int32, (tok, tok), 1)
            == tok - 1
        ).astype(LOW)

        def one_pair(j, carry):
            cols = pl.ds(aligned(j * 128, 128), 128)
            vcols = pl.ds(aligned(self.total + j * 128, 128), 128)
            low_e = self.e[j, :, rows]
            dp = dot_nt(gc[j], kv[rows, vcols])
            ds = (low_e.astype(F32) * (dp - self.dl[j])).astype(LOW)
            if self.diag is not None:
                for half in range(2):
                    turned = dot(flip, ds[half * tok : (half + 1) * tok])
                    for b in range(count // tok):
                        tile = turned[:, b * tok : (b + 1) * tok]
                        wide = jnp.concatenate((tile, jnp.zeros_like(tile)), axis=1)
                        wide = pltpu.roll(wide, tok + 1, 1, stride=1, stride_axis=0)
                        self.diag[start // tok + b, pl.ds(2 * j + half, 1), :] = jnp.sum(
                            wide, axis=0, keepdims=True
                        )
            self.kv_grad[rows, cols] = dot_tn(ds, qc[j]).astype(LOW)
            self.kv_grad[rows, vcols] = dot_tn(low_e, gc[j]).astype(LOW)
            self.dq[j] = self.dq[j] + dot(ds, kv[rows, cols])
            return carry

        lax.fori_loop(0, self.pairs, one_pair, 0)

    def finish(self, q_grad):
        for j in range(self.pairs):
            q_grad[:, j * 128 : (j + 1) * 128] = lane_join(self.dq[j]).astype(LOW)


def bucket_rows(buckets_ref, order_ref, here, table_rows, ids_ref):
    count, tok = buckets_ref.shape
    turn = (
        lax.broadcasted_iota(jnp.int32, (tok, tok), 0)
        + lax.broadcasted_iota(jnp.int32, (tok, tok), 1)
        == tok - 1
    ).astype(LOW)
    table_rows[:count, :] = jnp.full((count, tok), -1.0, F32)
    table_rows[count:, :] = dot(buckets_ref[...].astype(LOW), turn)
    own = order_ref[here]

    def one(block, carry):
        at = own - order_ref[block] + count
        wide = jnp.concatenate(
            (table_rows[pl.ds(at - 1, 1), :], table_rows[pl.ds(at, 1), :]), axis=1
        )
        ids_ref[pl.ds(block, 1), :] = pltpu.roll(wide, 1, 1)
        return carry

    lax.fori_loop(0, count, one, 0)


def bucket_masks(ids_ref, block, buckets):
    ids = ids_ref[pl.ds(block, 1), :]
    row = lax.broadcasted_iota(jnp.int32, (buckets, ids.shape[1]), 0).astype(F32)
    return ids, (row == ids).astype(F32)


def bias_vectors(ids_ref, table_ref, bias_ref):
    buckets, heads = table_ref.shape

    def one(block, carry):
        ids, mask = bucket_masks(ids_ref, block, buckets)
        vec = dot_tn(table_ref[...], mask, precision=HIGH)
        bias_ref[block, :heads, :] = jnp.where(ids >= 0, vec, NEG)
        return carry

    lax.fori_loop(0, ids_ref.shape[0], one, 0)


def bucket_sums(ids_ref, diag_ref, buckets):
    def one(block, total):
        _, mask = bucket_masks(ids_ref, block, buckets)
        return total + dot_nt(mask, diag_ref[block], precision=HIGH)

    start = jnp.zeros((buckets, diag_ref.shape[1]), F32)
    return lax.fori_loop(0, ids_ref.shape[0], one, start)


def rows_loop(count, step, body):
    def one(index, carry):
        body(pl.ds(aligned(index * step, step), step))
        return carry

    lax.fori_loop(0, count // step, one, 0)


GELU_A = 0.7978845608028654
GELU_B = 0.044715


def gelu_parts(value):
    square = value * value
    wave = jnp.tanh(GELU_A * (value + GELU_B * value * square))
    half = 0.5 * (1.0 + wave)
    slope = half + 0.5 * value * (1.0 - wave * wave) * (GELU_A * (1.0 + 3.0 * GELU_B * square))
    return value * half, slope


def core_sum(wire, part, out_buf, in_buf):
    slot = wire.slots(1)
    out_buf[...] = part.astype(LOW)
    wire.swap(out_buf, in_buf, slot)
    wire.got(in_buf, slot)
    return out_buf[...].astype(F32) + in_buf[...].astype(F32)


class PlaneSum:
    def __init__(self, wire, tok, part, core_buf, plane_buf, whole):
        self.wire, self.tok = wire, tok
        self.part, self.core_buf, self.plane_buf, self.whole = part, core_buf, plane_buf, whole
        self.base = wire.slots(8)
        self.half = whole.shape[1] // 2
        place = wire.place
        self.chips = (place.here, place.fx, place.fy, place.fxy)

    def cols(self, core):
        return pl.ds(aligned(core * self.half, 128), self.half)

    def rows(self, k):
        return pl.ds(aligned(lax.rem(self.chips[k], 4) * self.tok, self.tok), self.tok)

    def start(self, k):
        away = self.cols(self.wire.place.other)
        rows = self.rows(k)
        self.wire.swap(self.part.at[rows, away], self.core_buf.at[rows, :], self.base + k)

    def middle(self, k):
        wire, rows = self.wire, self.rows(k)
        wire.got(self.core_buf.at[rows, :], self.base + k)
        total = self.part[rows, self.cols(wire.place.core)].astype(F32)
        total = total + self.core_buf[rows, :].astype(F32)
        self.core_buf[rows, :] = total.astype(LOW)
        if k:
            wire.send(
                self.core_buf.at[rows, :],
                self.plane_buf.at[k - 1],
                self.base + 3 + k,
                self.chips[k],
            )

    def finish(self):
        place, wire = self.wire.place, self.wire
        total = self.core_buf[self.rows(0), :].astype(F32)
        for k in (1, 2, 3):
            wire.got(self.plane_buf.at[k - 1], self.base + 3 + k)
            total = total + self.plane_buf[k - 1].astype(F32)
        mine = self.cols(place.core)
        self.whole[:, mine] = total.astype(LOW)
        wire.swap(self.whole.at[:, mine], self.whole.at[:, mine], self.base + 7)

    def finish_core(self):
        self.wire.got(self.whole.at[:, self.cols(self.wire.place.other)], self.base + 7)


class PlaneGather:
    def __init__(self, wire, tok, ref):
        self.wire, self.tok, self.ref = wire, tok, ref
        self.half = ref.shape[1] // 2
        self.base = wire.slots(8)
        place = wire.place
        self.chips = (place.here, place.fx, place.fy, place.fxy)

    def view(self, k, core):
        rows = pl.ds(aligned(lax.rem(self.chips[k], 4) * self.tok, self.tok), self.tok)
        return self.ref.at[rows, pl.ds(aligned(core * self.half, 128), self.half)]

    def start(self):
        own = self.view(0, self.wire.place.core)
        for k in (1, 2, 3):
            self.wire.send(own, own, self.base + k, self.chips[k])

    def share(self, k):
        ref = self.view(k, self.wire.place.core)
        self.wire.got(ref, self.base + k)
        self.wire.swap(ref, ref, self.base + 4 + k)

    def finish(self, k):
        self.wire.got(self.view(k, self.wire.place.other), self.base + 4 + k)


class Sizes:
    def __init__(self, ctx, tok, enc, model, wide, units):
        self.ctx, self.tok, self.enc, self.model, self.wide = ctx, tok, enc, model, wide
        self.rows = model // ctx
        self.units = units
        self.quarter = units // 4
        self.pairs = wide // 128
        self.levels = ctx // 4
        self.attn_cols = 8 * wide
        self.mlp_cols = 3 * units
        self.part = 3 * self.quarter
        self.names = ("q", "k", "v", "cq", "ck", "cv", "o", "co")
        self.col = {n: slice(i * wide, (i + 1) * wide) for i, n in enumerate(self.names)}
        self.col["kv"] = slice(wide, 3 * wide)
        self.col["ckv"] = slice(4 * wide, 6 * wide)
        self.cuts = {
            "s": self.halves(0, 3 * wide, 0),
            "c": self.halves(3 * wide, 6 * wide, 1),
            "o": self.halves(6 * wide, 7 * wide, 0),
            "co": self.halves(7 * wide, 8 * wide, 1),
        }

    def halves(self, first, last, up):
        tiles = (last - first) // 128
        middle = first + (tiles + up) // 2 * 128
        return ((first, middle), (middle, last))


def named(kernel, names):
    def body(*refs):
        kernel(**dict(zip(names, refs, strict=True)))

    return body


def wire_sems(count):
    return {
        "send_sem": pltpu.SemaphoreType.DMA((count,)),
        "recv_sem": pltpu.SemaphoreType.DMA((count,)),
    }


def turned(block):
    count = block.shape[1]
    eye = (
        lax.broadcasted_iota(jnp.int32, (count, count), 0)
        == lax.broadcasted_iota(jnp.int32, (count, count), 1)
    ).astype(LOW)
    return dot_nt(eye, block).astype(LOW)


def layer_kernel(
    size, layer_in, encoded, sq, sk, sv, so, cq, ck, cv, co, gate_w, up_w, down_w, gains,
    table, buckets, order, out_grad,
    layer_out, input_grad, enc_grad, WG, mb, totals, bias_totals,
    WA, WM, wm, X, E, GR, PW, PM,
    q, kv, mkv, probes, s, e1, e2, rl1, rl2, mixed1, mixed2, table_rows, ids, bias, diag,
    after_self, after_cross, cross_grad, self_grad, n2, N3, act, GU, PN, PO, low, mixed_grad,
    q_grad, kv_grad, mkv_grad, ca, cb, pn_core, pn_plane, pn_whole, po_core, po_plane, po_whole,
    qc, gc, dl, dq, bs0, bs1, bc0, bc1, bo0, bo1, bp0, bp1, bx, be, px, pe, NG, NE, ml, ps,
    s1, s2, sr, sl, t1, t2, tr, tl, send_sem, recv_sem,
):
    place = Place(size.ctx)
    wire = Wire(place, send_sem, recv_sem)
    tok, enc, rows, half_d = size.tok, size.enc, size.rows, size.model // 2
    col, model, quarter = size.col, size.model, size.quarter
    ctx_tok, ctx_enc = X.shape[0], E.shape[0]
    plane_chips = (place.fx, place.fy, place.fxy)
    XG, EG = kv, mkv

    def block_rows(block, count):
        return pl.ds(aligned(block * count, 16), count)

    here_rows = block_rows(place.here, tok)
    own_weights = block_rows(place.here, rows)
    my_part = pl.ds(aligned(place.plane * size.part, 128), size.part)
    mine = pl.ds(aligned(place.core * half_d, 128), half_d)
    away = pl.ds(aligned(place.other * half_d, 128), half_d)

    def token_view(ref, count, core):
        def view(half, block):
            return ref.at[
                pl.ds(aligned(block * count + half * (count // 2), 16), count // 2),
                pl.ds(aligned(core * half_d, 128), half_d),
            ]

        return view

    def weight_view(ref, name):
        def view(half, block):
            first, last = size.cuts[name][half]
            return ref.at[block_rows(block, rows), first:last]

        return view

    gx = Gather(wire, token_view(X, tok, place.core), token_view(X, tok, place.other))
    ge = Gather(wire, token_view(E, enc, place.core), token_view(E, enc, place.other))
    gs, gc_, go, gp = (Gather(wire, weight_view(WA, n), None) for n in ("s", "c", "o", "co"))
    gg = PlaneGather(wire, tok, GR)
    spread = PlaneGather(wire, tok, N3)
    sum_n = PlaneSum(wire, tok, PN, pn_core, pn_plane, pn_whole)
    sum_o = PlaneSum(wire, tok, PO, po_core, po_plane, po_whole)
    mg_plane, mg_level, ms_level, ms_plane = (wire.slots(3) for _ in range(4))

    place.greet(place.above[1:] + list(plane_chips), True)
    X[here_rows, :] = rms_forward(layer_in[...], gains[0:1]).astype(LOW)
    gx.start()
    for name, ref in zip(("q", "k", "v", "cq", "ck", "cv"), (sq, sk, sv, cq, ck, cv)):
        WA[own_weights, col[name]] = ref[...]
    gs.start()
    WA[own_weights, col["o"]] = turned(so[...])
    WA[own_weights, col["co"]] = turned(co[...])
    E[block_rows(place.here, enc), :] = encoded[...]
    plane_rows = block_rows(place.plane, tok)
    GR[plane_rows, :] = out_grad[...].astype(LOW)
    gx.pass_level()
    down_t = turned(down_w[...])
    for p in range(4):
        cols = slice(p * quarter, (p + 1) * quarter)
        base = p * size.part
        wm[:, base : base + quarter] = gate_w[:, cols]
        wm[:, base + quarter : base + 2 * quarter] = up_w[:, cols]
        wm[:, base + 2 * quarter : base + 3 * quarter] = down_t[:, cols]
    WM[own_weights, :] = wm[:, my_part]
    bucket_rows(buckets, order, place.here, table_rows, ids)
    bias_vectors(ids, table, bias)
    diag[...] = jnp.zeros_like(diag)
    gx.pass_near()
    gs.pass_level()
    for k, chip in enumerate(plane_chips):
        wire.send(
            wm.at[:, pl.ds(aligned(lax.rem(chip, 4) * size.part, 128), size.part)],
            WM.at[own_weights, :],
            mg_plane + k,
            chip,
        )
    gs.pass_near()
    go.start()
    ge.start()
    gx.finish()
    gx.finish_share()
    gc_.start()
    go.pass_level()
    ge.pass_level()
    gs.finish()

    def project(rows_):
        kv[rows_, :] = dot(X[rows_, :], WA[:, col["kv"]]).astype(LOW)

    def project_enc(rows_):
        mkv[rows_, :] = dot(E[rows_, :], WA[:, col["ckv"]]).astype(LOW)

    q[...] = dot(X[here_rows, :], WA[:, col["q"]]).astype(LOW)
    rows_loop(ctx_tok, 256, project)

    def during_self(j):
        if j == 0:
            go.pass_near()
            ge.pass_near()
            gc_.pass_level()
        elif j == 1:
            gp.start()
            for k, chip in enumerate(plane_chips):
                wire.got(WM.at[block_rows(chip, rows), :], mg_plane + k)
            own = WM.at[block_rows(place.level, 4 * rows), :]
            for k in (1, 2, 3):
                wire.send(own, own, mg_level + k - 1, place.above[k])
            go.finish()
        else:
            ge.finish()

    pair_attend(tok, size.pairs, 512, q, kv, s, e1, rl1, mixed1, bias, during_self)
    part = dot_nt(mixed1[...], WA[:, col["o"]])
    gc_.pass_near()
    gp.pass_level()
    gg.start()
    after_self[...] = layer_in[...] + core_sum(wire, part, ca.at[0], cb.at[0])
    n2[...] = rms_forward(after_self[...], gains[1:2]).astype(LOW)
    ge.finish_share()
    gp.pass_near()
    gc_.finish()

    rows_loop(ctx_enc, 256, project_enc)
    probes[...] = dot(n2[...], WA[:, col["cq"]]).astype(LOW)

    def during_cross(j):
        if j == 1:
            for k in (1, 2, 3):
                gg.share(k)

    pair_attend(tok, size.pairs, 512, probes, mkv, s, e2, rl2, mixed2, None, during_cross)
    gp.finish()
    part = dot_nt(mixed2[...], WA[:, col["co"]])
    after_cross[...] = after_self[...] + core_sum(wire, part, ca.at[1], cb.at[1])

    N3[plane_rows, :] = rms_forward(after_cross[...], gains[2:3]).astype(LOW)
    spread.start()
    for k in (1, 2, 3):
        level = place.below[k] // 4
        wire.got(WM.at[block_rows(level, 4 * rows), :], mg_level + k - 1)

    def units(k):
        rows_ = spread_rows(k)
        pre = dot(N3[rows_, :], WM[:, : 2 * quarter])
        gate, upper = pre[:, :quarter], pre[:, quarter:]
        value, slope = gelu_parts(gate)
        act[rows_, :] = (value * upper).astype(LOW)
        grad = dot(GR[rows_, :], WM[:, 2 * quarter :])
        GU[rows_, :quarter] = (grad * upper * slope).astype(LOW)
        GU[rows_, quarter:] = (grad * value).astype(LOW)
        PN[rows_, :] = dot_nt(GU[rows_, :], WM[:, : 2 * quarter]).astype(LOW)

    def spread_rows(k):
        return sum_n.rows(k)

    for k in (1, 2, 3):
        gg.finish(k)
    units(0)
    sum_n.start(0)
    spread.share(1)
    spread.share(2)
    spread.finish(1)
    units(1)
    sum_n.start(1)
    spread.share(3)
    spread.finish(2)
    units(2)
    sum_n.start(2)
    sum_n.middle(1)
    spread.finish(3)
    units(3)
    sum_n.start(3)
    sum_n.middle(2)

    def back_out(k):
        rows_ = spread_rows(k)
        PO[rows_, :] = dot_nt(act[rows_, :], WM[:, 2 * quarter :]).astype(LOW)

    def unit_grads(cols):
        PM[cols, : 2 * quarter] = dot_tn(N3[:, cols], GU[...]).astype(LOW)
        PM[cols, 2 * quarter :] = dot_tn(GR[:, cols], act[...]).astype(LOW)

    back_out(0)
    sum_n.middle(3)
    sum_n.middle(0)
    rows_loop(model, 128, unit_grads)
    for k in (1, 2, 3):
        wire.send(
            PM.at[block_rows(place.above[k] // 4, 4 * rows), :],
            ml.at[k - 1],
            ms_level + k - 1,
            place.above[k],
        )
    sum_n.finish()
    for k in (1, 2, 3):
        back_out(k)
    for k in range(4):
        sum_o.start(k)
    sum_n.finish_core()
    extra, gain_three = rms_backward(after_cross[...], gains[2:3], pn_whole[...].astype(F32))
    cross_grad[...] = out_grad[...] + extra
    low[...] = cross_grad[...].astype(LOW)
    mixed_grad[...] = dot(low[...], WA[:, col["co"]]).astype(LOW)
    for k in (1, 2, 3, 0):
        sum_o.middle(k)

    def out_grads(left, right, target):
        def body(cols):
            PW[cols, target] = dot_tn(left[:, cols], right[...]).astype(LOW)

        rows_loop(model, 128, body)

    def weight_stream(name, *bufs):
        def out(half, total):
            first, last = size.cuts[name][half]
            WG[:, first:last] = total

        return Scatter(wire, weight_view(PW, name), lambda half: bufs[half], out)

    def token_out(ref, count):
        def out(half, total):
            ref[half * (count // 2) : (half + 1) * (count // 2), mine] = total

        return out

    sp = weight_stream("co", bp0, bp1)
    so_ = weight_stream("o", bo0, bo1)
    sc = weight_stream("c", bc0, bc1)
    sw = weight_stream("s", bs0, bs1)
    sx = Scatter(wire, token_view(XG, tok, place.core), lambda half: bx.at[half], token_out(NG, tok))
    se = Scatter(wire, token_view(EG, enc, place.core), lambda half: be.at[half], token_out(NE, enc))
    x_base, e_base = wire.slots(4), wire.slots(4)

    def pair_start(ref, recv, count, base, k):
        at = block_rows(place.below[k] // 4, 4 * count)
        wire.swap(ref.at[at, away], recv.at[at, :], base + k)

    def pair_ready(ref, recv, count, base, k):
        at = block_rows(place.below[k] // 4, 4 * count)
        wire.got(recv.at[at, :], base + k)
        ref[at, mine] = (ref[at, mine].astype(F32) + recv[at, :].astype(F32)).astype(LOW)

    out_grads(low, mixed2, col["co"])
    sp.start()
    back = PairBack(
        tok, size.pairs, probes, mkv, e2, rl2, mixed2, mixed_grad, mkv_grad, None, qc, gc, dl, dq
    )
    for c in range(ctx_enc // 512):
        back.chunk(c * 512, 512)
    back.finish(q_grad)
    part = dot_nt(q_grad[...], WA[:, col["cq"]])
    slot = wire.slots(1)
    ca[2] = part.astype(LOW)
    wire.swap(ca.at[2], cb.at[2], slot)
    sp.pass_near()

    def enc_rows(rows_):
        EG[rows_, :] = dot_nt(mkv_grad[rows_, :], WA[:, col["ckv"]]).astype(LOW)

    rows_loop(ctx_enc, 256, enc_rows)
    for k in (1, 2, 3, 0):
        pair_start(EG, pe, enc, e_base, k)
    wire.got(cb.at[2], slot)
    n_grad = ca[2].astype(F32) + cb[2].astype(F32)
    extra, gain_two = rms_backward(after_self[...], gains[1:2], n_grad)
    self_grad[...] = cross_grad[...] + extra
    low[...] = self_grad[...].astype(LOW)
    mixed_grad[...] = dot(low[...], WA[:, col["o"]]).astype(LOW)
    out_grads(n2, q_grad, col["cq"])
    out_grads(E, mkv_grad, col["ckv"])
    sc.start()
    for k in (1, 2, 3, 0):
        pair_ready(EG, pe, enc, e_base, k)
        se.start((k,))
    out_grads(low, mixed1, col["o"])
    so_.start()
    sp.pass_level()

    back = PairBack(
        tok, size.pairs, q, kv, e1, rl1, mixed1, mixed_grad, kv_grad, diag, qc, gc, dl, dq
    )

    def tok_rows(k):
        for part_ in range(2):
            at = pl.ds(aligned(place.below[k] // 4 * 4 * tok + part_ * 2 * tok, 16), 2 * tok)
            XG[at, :] = dot_nt(kv_grad[at, :], WA[:, col["kv"]]).astype(LOW)

    n2[...] = X[here_rows, :]
    back.chunk(place.below[1] // 4 * 4 * tok, 4 * tok)
    tok_rows(1)
    pair_start(XG, px, tok, x_base, 1)
    sc.pass_near()
    back.chunk(place.below[2] // 4 * 4 * tok, 4 * tok)
    tok_rows(2)
    pair_start(XG, px, tok, x_base, 2)
    pair_ready(XG, px, tok, x_base, 1)
    sx.start((1,))
    se.pass_near()
    back.chunk(place.below[3] // 4 * 4 * tok, 4 * tok)
    tok_rows(3)
    pair_start(XG, px, tok, x_base, 3)
    pair_ready(XG, px, tok, x_base, 2)
    sx.start((2,))
    so_.pass_near()
    back.chunk(place.level * 4 * tok, 4 * tok)
    back.finish(q_grad)
    tok_rows(0)
    own = dot_nt(q_grad[...], WA[:, col["q"]]) + XG[here_rows, :].astype(F32)
    XG[here_rows, :] = own.astype(LOW)
    pair_start(XG, px, tok, x_base, 0)
    pair_ready(XG, px, tok, x_base, 3)
    sx.start((3,))
    out_grads(n2, q_grad, col["q"])
    pair_ready(XG, px, tok, x_base, 0)
    sx.start((0,))
    out_grads(X, kv_grad, col["kv"])
    sw.start()

    sc.pass_level()
    se.pass_level()
    so_.pass_level()
    total = PM[block_rows(place.level, 4 * rows), :].astype(F32)
    for k in (1, 2, 3):
        wire.got(ml.at[k - 1], ms_level + k - 1)
        total = total + ml[k - 1].astype(F32)
    ps[...] = total.astype(LOW)
    for k, chip in enumerate(plane_chips):
        wire.send(
            ps.at[block_rows(lax.rem(chip, 4), rows), :], mb.at[:, my_part], ms_plane + k, chip
        )
    mb[:, my_part] = ps[block_rows(place.plane, rows), :]
    sx.pass_near()
    sums = bucket_sums(ids, diag, table.shape[0])
    t1[...] = jnp.concatenate(
        (sums, jnp.zeros((sums.shape[0], t1.shape[1] - sums.shape[1]), F32)), axis=1
    )
    sx.pass_level()
    sw.pass_near()
    sx.finish()
    x_slot, e_slot, o_slot = wire.slots(1), wire.slots(1), wire.slots(1)
    wire.swap(NG.at[:, mine], NG.at[:, mine], x_slot)
    se.finish()
    wire.swap(NE.at[:, mine], NE.at[:, mine], e_slot)
    sum_o.finish()
    sw.pass_level()
    wire.got(NG.at[:, away], x_slot)
    extra, gain_one = rms_backward(layer_in[...], gains[0:1], NG[...])
    input_grad[...] = self_grad[...] + extra
    s1[...] = jnp.concatenate(
        (gain_one, gain_two, gain_three, jnp.zeros((5, model), F32)), axis=0
    )
    small = wire.slots(10)
    wire.send(s1, sr.at[0], small, place.fx)
    wire.send(t1, tr.at[0], small + 5, place.fx)
    sum_o.finish_core()
    layer_out[...] = after_cross[...] + po_whole[...].astype(F32)
    wire.got(NE.at[:, away], e_slot)
    enc_grad[...] = NE[...]
    wire.got(sr.at[0], small)
    wire.got(tr.at[0], small + 5)
    s2[...] = s1[...] + sr[0]
    t2[...] = t1[...] + tr[0]
    wire.send(s2, sr.at[1], small + 1, place.fy)
    wire.send(t2, tr.at[1], small + 6, place.fy)
    sp.finish()
    sc.finish()
    so_.finish()
    wire.got(sr.at[1], small + 1)
    wire.got(tr.at[1], small + 6)
    sl[pl.ds(place.level, 1)] = (s2[...] + sr[1])[None]
    tl[pl.ds(place.level, 1)] = (t2[...] + tr[1])[None]
    for k in (1, 2, 3):
        wire.send(sl.at[place.level], sl.at[place.level], small + 1 + k, place.above[k])
        wire.send(tl.at[place.level], tl.at[place.level], small + 6 + k, place.above[k])
    sw.finish()
    for k, chip in enumerate(plane_chips):
        cols = pl.ds(aligned(lax.rem(chip, 4) * size.part, 128), size.part)
        wire.got(mb.at[:, cols], ms_plane + k)
    for k in (1, 2, 3):
        level = place.below[k] // 4
        wire.got(sl.at[level], small + 1 + k)
        wire.got(tl.at[level], small + 6 + k)
    totals[...] = (sl[0] + sl[1]) + (sl[2] + sl[3])
    bias_totals[...] = (tl[0] + tl[1]) + (tl[2] + tl[3])
    wire.drain()


def quick_device(
    layer_in, encoded, self_query, self_key, self_value, self_out, cross_query, cross_key,
    cross_value, cross_out, gate_proj, up_proj, down_proj, norm_gains, position_bias,
    bucket_ids, block_order, out_grad,
):
    tok, model = layer_in.shape
    enc = encoded.shape[0]
    wide, units = self_query.shape[1], gate_proj.shape[1]
    ctx = block_order.shape[0]
    buckets, heads = position_bias.shape
    size = Sizes(ctx, tok, enc, model, wide, units)
    rows, quarter, pairs = size.rows, size.quarter, size.pairs
    tok_all, enc_all, tok4 = ctx * tok, ctx * enc, 4 * tok

    def vmem(*shape, dtype=LOW):
        return pltpu.VMEM(shape, dtype)

    def full(*shape):
        return pltpu.VMEM(shape, F32)

    def streams(name):
        return [vmem(15, rows, last - first) for first, last in size.cuts[name]]

    ins = {
        "layer_in": layer_in, "encoded": encoded, "sq": self_query, "sk": self_key,
        "sv": self_value, "so": self_out, "cq": cross_query, "ck": cross_key,
        "cv": cross_value, "co": cross_out, "gate_w": gate_proj, "up_w": up_proj,
        "down_w": down_proj, "gains": norm_gains, "table": position_bias,
        "buckets": bucket_ids.reshape(ctx, tok), "order": block_order, "out_grad": out_grad,
    }
    outs = {
        "layer_out": ((tok, model), F32), "input_grad": ((tok, model), F32),
        "enc_grad": ((enc, model), F32), "WG": ((rows, size.attn_cols), F32),
        "mb": ((rows, size.mlp_cols), LOW), "totals": ((8, model), F32),
        "bias_totals": ((buckets, 128), F32),
    }
    (bs0, bs1), (bc0, bc1) = streams("s"), streams("c")
    (bo0, bo1), (bp0, bp1) = streams("o"), streams("co")
    scratch = {
        "WA": vmem(model, size.attn_cols), "WM": vmem(model, size.part),
        "wm": vmem(rows, size.mlp_cols), "X": vmem(tok_all, model), "E": vmem(enc_all, model),
        "GR": vmem(tok4, model), "PW": vmem(model, size.attn_cols),
        "PM": vmem(model, size.part),
        "q": vmem(tok, wide), "kv": vmem(tok_all, 2 * wide), "mkv": vmem(enc_all, 2 * wide),
        "probes": vmem(tok, wide), "s": full(2 * tok, tok_all),
        "e1": vmem(pairs, 2 * tok, tok_all), "e2": vmem(pairs, 2 * tok, enc_all),
        "rl1": full(pairs, 2 * tok, 1), "rl2": full(pairs, 2 * tok, 1),
        "mixed1": vmem(tok, wide), "mixed2": vmem(tok, wide), "table_rows": full(2 * ctx, tok),
        "ids": full(ctx, 2 * tok), "bias": full(ctx, 8, 2 * tok), "diag": full(ctx, 8, 2 * tok),
        "after_self": full(tok, model), "after_cross": full(tok, model),
        "cross_grad": full(tok, model), "self_grad": full(tok, model), "n2": vmem(tok, model),
        "N3": vmem(tok4, model), "act": vmem(tok4, quarter), "GU": vmem(tok4, 2 * quarter),
        "PN": vmem(tok4, model), "PO": vmem(tok4, model), "low": vmem(tok, model),
        "mixed_grad": vmem(tok, wide), "q_grad": vmem(tok, wide),
        "kv_grad": vmem(tok_all, 2 * wide), "mkv_grad": vmem(enc_all, 2 * wide),
        "ca": vmem(3, tok, model), "cb": vmem(3, tok, model),
        "pn_core": vmem(tok4, model // 2), "pn_plane": vmem(3, tok, model // 2),
        "pn_whole": vmem(tok, model), "po_core": vmem(tok4, model // 2),
        "po_plane": vmem(3, tok, model // 2), "po_whole": vmem(tok, model),
        "qc": vmem(pairs, 2 * tok, 128), "gc": vmem(pairs, 2 * tok, 128),
        "dl": full(pairs, 2 * tok, 1), "dq": full(pairs, 2 * tok, 128),
        "bs0": bs0, "bs1": bs1, "bc0": bc0, "bc1": bc1, "bo0": bo0, "bo1": bo1,
        "bp0": bp0, "bp1": bp1, "bx": vmem(2, 15, tok // 2, model // 2),
        "be": vmem(2, 15, enc // 2, model // 2), "px": vmem(tok_all, model // 2),
        "pe": vmem(enc_all, model // 2), "NG": full(tok, model), "NE": full(enc, model),
        "ml": vmem(3, 4 * rows, size.part), "ps": vmem(4 * rows, size.part),
        "s1": full(8, model), "s2": full(8, model), "sr": full(2, 8, model),
        "sl": full(4, 8, model), "t1": full(buckets, 128), "t2": full(buckets, 128),
        "tr": full(2, buckets, 128), "tl": full(4, buckets, 128), **wire_sems(512),
    }
    names = list(ins) + list(outs) + list(scratch)
    made = pl.pallas_call(
        named(functools.partial(layer_kernel, size), names),
        out_shape=tuple(jax.ShapeDtypeStruct(*spec) for spec in outs.values()),
        in_specs=[
            pl.BlockSpec(memory_space=pltpu.SMEM if name == "order" else pltpu.VMEM)
            for name in ins
        ],
        out_specs=tuple(pl.BlockSpec(memory_space=pltpu.VMEM) for _ in outs),
        scratch_shapes=list(scratch.values()),
        compiler_params=pltpu.CompilerParams(
            collective_id=1, has_side_effects=True, vmem_limit_bytes=VMEM_LIMIT
        ),
    )(*ins.values())
    layer_out, input_grad, enc_grad, wg, mg, totals, bias_totals = made
    grads = {name: wg[:, size.col[name]] for name in size.names}
    mlp = mg.reshape(rows, 4, 3, quarter)
    gate, upward, down = (mlp[:, :, i].reshape(rows, units).astype(F32) for i in range(3))
    return (
        layer_out, input_grad, enc_grad, grads["q"], grads["k"], grads["v"], grads["o"].T,
        grads["cq"], grads["ck"], grads["cv"], grads["co"].T, gate, upward, down.T,
        totals[:3], bias_totals[:, :heads],
    )


def quick_fits(mesh):
    return mesh.shape["ctx"] == 16 and mesh.shape["head"] == 2


def as_sent(shard):

    def short(part):
        return part.astype(jnp.bfloat16) if part.dtype == jnp.float32 else part

    return jax.tree.map(short, shard)


def rms_scale(rows, gain):
    return rows * lax.rsqrt(jnp.mean(rows * rows, axis=-1, keepdims=True) + EPS) * gain


def geglu(gate, upper):
    return jax.nn.gelu(gate, approximate=True) * upper


def times(left, right):
    return jnp.dot(left, right, preferred_element_type=jnp.float32)


def left_times(left, right):
    return lax.dot_general(
        left, right, (((0,), (0,)), ((), ())), preferred_element_type=jnp.float32
    )


def right_times(left, right):
    return lax.dot_general(
        left, right, (((1,), (1,)), ((), ())), preferred_element_type=jnp.float32
    )


def join_heads(parts):
    return jax.tree.map(lambda part: part.astype(jnp.float32), lax.psum(as_sent(parts), "head"))


def gather_self(keys_own, values_own):
    return (
        lax.all_gather(keys_own, "ctx", axis=0, tiled=True),
        lax.all_gather(values_own, "ctx", axis=0, tiled=True),
    )


def gather_cross(memory_keys, memory_values):
    return (
        lax.all_gather(memory_keys, "ctx", axis=0, tiled=True),
        lax.all_gather(memory_values, "ctx", axis=0, tiled=True),
    )


def bias_scores(steps, bias_table):
    rises = bias_table[1:] - bias_table[:-1]
    return bias_table[0][:, None, None] + jnp.einsum("qkb,bh->hqk", steps, rises, precision=HIGH)


def bias_grads(score_grad, steps):
    above = jnp.einsum("hqk,qkb->bh", score_grad, steps, precision=HIGH)
    total = jnp.sum(score_grad, axis=(1, 2))
    upper_rows = jnp.concatenate((total[None], above), axis=0)
    lower_rows = jnp.concatenate((above, jnp.zeros((1, above.shape[1]), jnp.float32)), axis=0)
    return upper_rows - lower_rows


def delta_of(mixed, mixed_grad, head_count):
    tok_rows, total_width = mixed.shape
    width = total_width // head_count
    product = mixed.astype(jnp.float32).reshape(tok_rows, head_count, width) * mixed_grad.astype(
        jnp.float32
    ).reshape(tok_rows, head_count, width)
    return jnp.transpose(jnp.sum(product, axis=-1))


def attend_fold(queries, head_count, parts_fn, bias_table):
    tok_rows = queries.shape[0]
    width = queries.shape[1] // head_count
    query3 = queries.reshape(tok_rows, head_count, width)

    def fold(state, pieces, start):
        key_piece, value_piece = pieces
        count = key_piece.shape[0]
        block = math.gcd(count, 512)

        def fold_step(index, inner):
            summed, run_max, run_sum = inner
            key3 = lax.dynamic_slice_in_dim(key_piece, index * block, block, 0).reshape(
                block, head_count, width
            )
            value3 = lax.dynamic_slice_in_dim(value_piece, index * block, block, 0).reshape(
                block, head_count, width
            )
            scores = jnp.einsum("qhe,khe->hqk", query3, key3, preferred_element_type=jnp.float32)
            if parts_fn is not None:
                steps, valid = parts_fn(index * block, block)
                scores = jnp.where(valid[None], scores + bias_scores(steps, bias_table), NEG)
            new_max = jnp.maximum(run_max, jnp.max(scores, axis=-1))
            ratio = jnp.exp(run_max - new_max)
            weights = jnp.exp(scores - new_max[..., None])
            run_sum = run_sum * ratio + jnp.sum(weights, axis=-1)
            summed = summed * ratio[..., None] + jnp.einsum(
                "hqk,khe->hqe",
                weights.astype(jnp.bfloat16),
                value3,
                preferred_element_type=jnp.float32,
            )
            return (summed, new_max, run_sum)

        return lax.fori_loop(0, count // block, fold_step, state)

    return fold


def finish(state):
    summed, run_max, run_sum = state
    head_count, tok_rows, width = summed.shape
    mixed = jnp.transpose(summed / run_sum[..., None], (1, 0, 2)).reshape(
        tok_rows, head_count * width
    )
    return (mixed.astype(jnp.bfloat16), run_max + jnp.log(run_sum))


def attend_back(
    queries, mixed_grad, lse, delta, keys_all, values_all, head_count, parts_fn, bias_table
):
    tok_rows, total_width = queries.shape
    width = total_width // head_count
    query3 = queries.reshape(tok_rows, head_count, width)
    grad3 = mixed_grad.reshape(tok_rows, head_count, width)
    count = keys_all.shape[0]
    block = math.gcd(count, 512)

    def attend_step(carry, index):
        query_grad, bias_grad = carry
        key3 = lax.dynamic_slice_in_dim(keys_all, index * block, block, 0).reshape(
            block, head_count, width
        )
        value3 = lax.dynamic_slice_in_dim(values_all, index * block, block, 0).reshape(
            block, head_count, width
        )
        scores = jnp.einsum("qhe,khe->hqk", query3, key3, preferred_element_type=jnp.float32)
        if parts_fn is not None:
            steps, valid = parts_fn(index * block, block)
            scores = jnp.where(valid[None], scores + bias_scores(steps, bias_table), NEG)
        weights = jnp.exp(scores - lse[..., None])
        weight_grad = jnp.einsum("qhe,khe->hqk", grad3, value3, preferred_element_type=jnp.float32)
        score_grad = weights * (weight_grad - delta[..., None])
        if parts_fn is not None:
            bias_grad = bias_grad + bias_grads(score_grad, steps)
        score_low = score_grad.astype(jnp.bfloat16)
        query_grad = query_grad + jnp.einsum(
            "hqk,khe->qhe", score_low, key3, preferred_element_type=jnp.float32
        )
        stacked = None
        value_term = jnp.einsum(
            "hqk,qhe->khe", weights.astype(jnp.bfloat16), grad3, preferred_element_type=jnp.float32
        )
        key_term = jnp.einsum("hqk,qhe->khe", score_low, query3, preferred_element_type=jnp.float32)
        stacked = jnp.concatenate(
            (key_term.reshape(block, total_width), value_term.reshape(block, total_width)), axis=1
        )
        return ((query_grad, bias_grad), stacked)

    start = (
        jnp.zeros((tok_rows, head_count, width), jnp.float32),
        jnp.zeros(bias_table.shape, jnp.float32),
    )
    (query_grad, bias_grad), terms = lax.scan(attend_step, start, jnp.arange(count // block))
    query_grad = query_grad.reshape(tok_rows, total_width).astype(jnp.bfloat16)
    terms = terms.reshape(count, 2 * total_width)
    return (query_grad, bias_grad, terms)


def per_device(
    layer_in,
    encoded,
    self_query,
    self_key,
    self_value,
    self_out,
    cross_query,
    cross_key,
    cross_value,
    cross_out,
    gate_proj,
    up_proj,
    down_proj,
    norm_gains,
    position_bias,
    bucket_ids,
    block_order,
    out_grad,
):
    low = jnp.bfloat16
    tok_rows = layer_in.shape[0]
    bucket_count, head_count = position_bias.shape
    block_count = block_order.shape[0]
    full_weights = (
        lax.all_gather(self_query, "ctx", axis=0, tiled=True),
        lax.all_gather(self_key, "ctx", axis=0, tiled=True),
        lax.all_gather(self_value, "ctx", axis=0, tiled=True),
        lax.all_gather(self_out, "ctx", axis=1, tiled=True),
        lax.all_gather(cross_query, "ctx", axis=0, tiled=True),
        lax.all_gather(cross_key, "ctx", axis=0, tiled=True),
        lax.all_gather(cross_value, "ctx", axis=0, tiled=True),
        lax.all_gather(cross_out, "ctx", axis=1, tiled=True),
        lax.all_gather(gate_proj, "ctx", axis=0, tiled=True),
        lax.all_gather(up_proj, "ctx", axis=0, tiled=True),
        lax.all_gather(down_proj, "ctx", axis=1, tiled=True),
    )
    (
        query_full,
        key_full,
        value_full,
        output_full,
        probe_full,
        lookup_full,
        recall_full,
        merge_full,
        gate_full,
        upward_full,
        down_full,
    ) = full_weights
    boundaries = jnp.arange(1, bucket_count, dtype=jnp.int32)
    starts = jnp.sum((bucket_ids[None, :] < boundaries[:, None]).astype(jnp.int32), axis=1)
    block_ids = jnp.arange(block_count, dtype=jnp.int32)
    here = lax.axis_index("ctx")
    own_block = jnp.sum(jnp.where(block_ids == here, block_order, 0))
    query_pos = own_block * tok_rows + jnp.arange(tok_rows, dtype=jnp.int32)

    def position_of(rows_index):
        slot = rows_index // tok_rows
        owner = jnp.sum(
            jnp.where(slot[:, None] == block_ids[None, :], block_order[None, :], 0), axis=1
        )
        return owner * tok_rows + rows_index % tok_rows

    def pair_parts(first_pos, second_pos):
        dist = first_pos[:, None] - second_pos[None, :]
        steps = (dist[:, :, None] >= starts[None, None, :]).astype(jnp.float32)
        return (steps, dist >= 0)

    def causal_parts(key_start, count):
        return pair_parts(query_pos, position_of(key_start + jnp.arange(count, dtype=jnp.int32)))

    normed_one = rms_scale(layer_in, norm_gains[0]).astype(low)
    queries = times(normed_one, query_full).astype(low)
    keys_own = times(normed_one, key_full).astype(low)
    values_own = times(normed_one, value_full).astype(low)
    memory_keys = times(encoded, lookup_full).astype(low)
    memory_values = times(encoded, recall_full).astype(low)
    total_width = queries.shape[1]
    width = total_width // head_count
    start_state = (
        jnp.zeros((head_count, tok_rows, width), jnp.float32),
        jnp.full((head_count, tok_rows), NEG, jnp.float32),
        jnp.zeros((head_count, tok_rows), jnp.float32),
    )
    self_fold = attend_fold(queries, head_count, causal_parts, position_bias)
    self_state = self_fold(
        start_state,
        (
            lax.all_gather(keys_own, "ctx", axis=0, tiled=True),
            lax.all_gather(values_own, "ctx", axis=0, tiled=True),
        ),
        jnp.int32(0),
    )
    mixed_one, lse_one = finish(self_state)
    after_self = layer_in + join_heads(times(mixed_one, output_full))
    normed_two = rms_scale(after_self, norm_gains[1]).astype(low)
    probes = times(normed_two, probe_full).astype(low)
    cross_fold = attend_fold(probes, head_count, None, position_bias)
    cross_state = cross_fold(
        start_state,
        (
            lax.all_gather(memory_keys, "ctx", axis=0, tiled=True),
            lax.all_gather(memory_values, "ctx", axis=0, tiled=True),
        ),
        jnp.int32(0),
    )
    mixed_two, lse_two = finish(cross_state)
    after_cross = after_self + join_heads(times(mixed_two, merge_full))
    normed_three = rms_scale(after_cross, norm_gains[2]).astype(low)
    gate_pre = times(normed_three, gate_full)
    upper = times(normed_three, upward_full)
    activated = geglu(gate_pre, upper).astype(low)
    layer_out = after_cross + join_heads(times(activated, down_full))
    grad_rows = out_grad.astype(low)
    down_wgrad = left_times(activated, grad_rows)
    act_grad = right_times(grad_rows, down_full)
    geglu_out, geglu_pull = jax.vjp(geglu, gate_pre, upper)
    gate_grad, upper_grad = geglu_pull(act_grad)
    gate_grad = gate_grad.astype(low)
    upper_grad = upper_grad.astype(low)
    gate_wgrad = left_times(normed_three, gate_grad)
    up_wgrad = left_times(normed_three, upper_grad)
    normed_three_grad = join_heads(
        right_times(gate_grad, gate_full) + right_times(upper_grad, upward_full)
    )
    norm_out, norm_pull = jax.vjp(rms_scale, after_cross, norm_gains[2])
    cross_extra, gain_three = norm_pull(normed_three_grad)
    cross_grad = out_grad + cross_extra
    cross_rows = cross_grad.astype(low)
    merge_wgrad = left_times(mixed_two, cross_rows)
    mixed_two_grad = right_times(cross_rows, merge_full).astype(low)
    delta_two = delta_of(mixed_two, mixed_two_grad, head_count)
    memory_all = gather_cross(memory_keys, memory_values)
    probe_grad, unused_bias, cross_terms = attend_back(
        probes,
        mixed_two_grad,
        lse_two,
        delta_two,
        memory_all[0],
        memory_all[1],
        head_count,
        None,
        position_bias,
    )
    cross_terms = lax.psum_scatter(cross_terms, "ctx", scatter_dimension=0, tiled=True)
    memory_key_grad = cross_terms[:, :total_width].astype(low)
    memory_value_grad = cross_terms[:, total_width:].astype(low)
    probe_wgrad = left_times(normed_two, probe_grad)
    lookup_wgrad = left_times(encoded, memory_key_grad)
    recall_wgrad = left_times(encoded, memory_value_grad)
    normed_two_grad, encoded_grad = join_heads(
        (
            right_times(probe_grad, probe_full),
            right_times(memory_key_grad, lookup_full) + right_times(memory_value_grad, recall_full),
        )
    )
    norm_out, norm_pull = jax.vjp(rms_scale, after_self, norm_gains[1])
    self_extra, gain_two = norm_pull(normed_two_grad)
    self_grad = cross_grad + self_extra
    self_rows = self_grad.astype(low)
    output_wgrad = left_times(mixed_one, self_rows)
    mixed_one_grad = right_times(self_rows, output_full).astype(low)
    delta_one = delta_of(mixed_one, mixed_one_grad, head_count)
    sequence_all = gather_self(keys_own, values_own)
    query_grad, bias_grad, self_terms = attend_back(
        queries,
        mixed_one_grad,
        lse_one,
        delta_one,
        sequence_all[0],
        sequence_all[1],
        head_count,
        causal_parts,
        position_bias,
    )
    self_terms = lax.psum_scatter(self_terms, "ctx", scatter_dimension=0, tiled=True)
    key_grad = self_terms[:, :total_width].astype(low)
    value_grad = self_terms[:, total_width:].astype(low)
    query_wgrad = left_times(normed_one, query_grad)
    key_wgrad = left_times(normed_one, key_grad)
    value_wgrad = left_times(normed_one, value_grad)
    normed_one_grad = join_heads(
        right_times(query_grad, query_full)
        + right_times(key_grad, key_full)
        + right_times(value_grad, value_full)
    )
    norm_out, norm_pull = jax.vjp(rms_scale, layer_in, norm_gains[0])
    input_extra, gain_one = norm_pull(normed_one_grad)
    input_grad = self_grad + input_extra
    weight_sums = (
        lax.psum_scatter(query_wgrad, "ctx", scatter_dimension=0, tiled=True),
        lax.psum_scatter(key_wgrad, "ctx", scatter_dimension=0, tiled=True),
        lax.psum_scatter(value_wgrad, "ctx", scatter_dimension=0, tiled=True),
        lax.psum_scatter(output_wgrad, "ctx", scatter_dimension=1, tiled=True),
        lax.psum_scatter(probe_wgrad, "ctx", scatter_dimension=0, tiled=True),
        lax.psum_scatter(lookup_wgrad, "ctx", scatter_dimension=0, tiled=True),
        lax.psum_scatter(recall_wgrad, "ctx", scatter_dimension=0, tiled=True),
        lax.psum_scatter(merge_wgrad, "ctx", scatter_dimension=1, tiled=True),
        lax.psum_scatter(gate_wgrad, "ctx", scatter_dimension=0, tiled=True),
        lax.psum_scatter(up_wgrad, "ctx", scatter_dimension=0, tiled=True),
        lax.psum_scatter(down_wgrad, "ctx", scatter_dimension=1, tiled=True),
    )
    gains_sum, bias_sum = lax.psum((jnp.stack((gain_one, gain_two, gain_three)), bias_grad), "ctx")
    return (layer_out, input_grad, encoded_grad) + tuple(weight_sums) + (gains_sum, bias_sum)


def solution(mesh):
    body = quick_device if quick_fits(mesh) else per_device
    placed = (
        P("ctx", None),
        P("ctx", None),
        P("ctx", "head"),
        P("ctx", "head"),
        P("ctx", "head"),
        P("head", "ctx"),
        P("ctx", "head"),
        P("ctx", "head"),
        P("ctx", "head"),
        P("head", "ctx"),
        P("ctx", "head"),
        P("ctx", "head"),
        P("head", "ctx"),
        P(),
        P(None, "head"),
        P(),
        P(),
        P("ctx", None),
    )
    return jax.shard_map(
        body,
        mesh=mesh,
        in_specs=placed,
        out_specs=(
            P("ctx", None),
            P("ctx", None),
            P("ctx", None),
            P("ctx", "head"),
            P("ctx", "head"),
            P("ctx", "head"),
            P("head", "ctx"),
            P("ctx", "head"),
            P("ctx", "head"),
            P("ctx", "head"),
            P("head", "ctx"),
            P("ctx", "head"),
            P("ctx", "head"),
            P("head", "ctx"),
            P(),
            P(None, "head"),
        ),
        check_vma=False,
    )
```

```python
import functools
import math

import jax
import jax.numpy as jnp
from jax import lax
from jax.experimental import pallas as pl
from jax.experimental.pallas import tpu as pltpu
from jax.sharding import PartitionSpec as P

EPS = 1e-06
NEG = -1e30
HIGH = lax.Precision.HIGHEST
LOW = jnp.bfloat16
F32 = jnp.float32
MESH = pl.DeviceIdType.MESH
VMEM_LIMIT = 66_000_000


def dot(left, right, **kw):
    return jnp.dot(left, right, preferred_element_type=F32, **kw)


def dot_nt(left, right, **kw):
    return lax.dot_general(left, right, (((1,), (1,)), ((), ())), preferred_element_type=F32, **kw)


def dot_tn(left, right, **kw):
    return lax.dot_general(left, right, (((0,), (0,)), ((), ())), preferred_element_type=F32, **kw)


def rms_forward(rows, gain):
    return rows * lax.rsqrt(jnp.mean(rows * rows, axis=-1, keepdims=True) + EPS) * gain


def rms_backward(rows, gain, grad):
    scale = lax.rsqrt(jnp.mean(rows * rows, axis=-1, keepdims=True) + EPS)
    scaled = gain * grad
    inner = jnp.mean(scaled * rows, axis=-1, keepdims=True)
    row_grad = scale * scaled - rows * (scale * scale * scale * inner)
    gain_grad = jnp.sum(grad * rows * scale, axis=0, keepdims=True)
    return row_grad, gain_grad


def aligned(value, step):
    return value if isinstance(value, int) else pl.multiple_of(value, step)


class Place:
    def __init__(self, count):
        self.count = count
        self.here = lax.axis_index("ctx")
        self.core = lax.axis_index("head")
        self.other = 1 - self.core
        self.plane = lax.rem(self.here, 4)
        self.level = self.here // 4
        self.fx = self.flip(self.here, 0)
        self.fy = self.flip(self.here, 1)
        self.fxy = self.flip(self.fx, 1)
        self.above = [lax.rem(self.here + 4 * k, count) for k in range(4)]
        self.below = [lax.rem(self.here + count - 4 * k, count) for k in range(4)]
        self.top = count // 4 - 1
        bottom, head = self.level == 0, self.level == self.top
        self.nearest = (
            jnp.where(bottom, 3, 1),
            jnp.where(bottom, 2, jnp.where(head, 2, 3)),
            jnp.where(bottom, 1, jnp.where(head, 3, 2)),
        )

    def flip(self, index, axis):
        if axis == 0:
            return index + 1 - 2 * lax.rem(index, 2)
        return index + 2 - 4 * lax.rem(index // 2, 2)

    def near(self, half):
        return (self.fx, self.fy) if half == 0 else (self.fy, self.fx)

    def signal(self, chips):
        barrier = pltpu.get_barrier_semaphore()
        for chip in chips:
            pl.semaphore_signal(
                barrier, inc=1, device_id=(chip, self.core), device_id_type=MESH
            )
        pl.semaphore_signal(barrier, inc=1, device_id=(self.here, self.other), device_id_type=MESH)

    def meet(self, count):
        pl.semaphore_wait(pltpu.get_barrier_semaphore(), count)


class Wire:
    def __init__(self, place, send_sem, recv_sem):
        self.place, self.send_sem, self.recv_sem = place, send_sem, recv_sem
        self.used = 0
        self.send_used = 0
        self.pending = []

    def slots(self, count):
        base = self.used
        self.used += count
        assert self.used <= self.recv_sem.shape[0], self.used
        return base

    def sender(self, whole=None):
        slot = self.send_used
        self.send_used += 1
        assert slot < self.send_sem.shape[0], slot
        if whole is not None:
            self.pending.append((slot, whole))
        return slot

    def copy(self, src, dst, out, slot, chip, core):
        return pltpu.make_async_remote_copy(
            src_ref=src,
            dst_ref=dst,
            send_sem=self.send_sem.at[out],
            recv_sem=self.recv_sem.at[slot],
            device_id=(chip, core),
            device_id_type=MESH,
        )

    def send(self, src, dst, slot, chip=None, core=None, out=None):
        chip = self.place.here if chip is None else chip
        core = self.place.core if core is None else core
        if out is None:
            out = self.sender(src)
        self.copy(src, dst, out, slot, chip, core).start()

    def swap(self, src, dst, slot, out=None):
        self.send(src, dst, slot, None, self.place.other, out)

    def got(self, dst, slot):
        place = self.place
        self.copy(dst, dst, 0, slot, place.here, place.other).wait_recv()

    def sent(self, whole, out):
        place = self.place
        self.copy(whole, whole, out, 0, place.here, place.other).wait_send()

    def drain(self):
        for out, whole in self.pending:
            self.sent(whole, out)
        self.pending = []


class Gather:
    def __init__(self, wire, view, share, spare):
        self.wire, self.view, self.share, self.spare = wire, view, share, spare
        self.halves = range(2)
        self.base = [wire.slots(8) for _ in self.halves]
        self.out = [wire.sender(spare(half, 12)) for half in self.halves]
        self.line_out = [wire.sender() for _ in self.halves]
        if share:
            self.side = [wire.slots(1) for _ in self.halves]
            self.side_out = [wire.sender(spare(half, 15)) for half in self.halves]

    def _line(self, half, block, slot, chip):
        ref = self.view(half, block)
        self.wire.send(ref, ref, self.base[half] + slot, chip, out=self.line_out[half])

    def _out(self, half, block, slot, chip):
        ref = self.view(half, block)
        self.wire.send(ref, ref, self.base[half] + slot, chip, out=self.out[half])

    def _give(self, half, block):
        if self.share:
            ref = self.view(half, block)
            self.wire.swap(ref, ref, self.side[half], self.side_out[half])

    def start_level(self):
        place = self.wire.place
        for half in self.halves:

            @pl.when(place.level < place.top)
            def _():
                self._line(half, place.here, 0, place.here + 4)

            @pl.when(place.level > 0)
            def _():
                self._line(half, place.here, 2, place.here - 4)

    def start_plane(self):
        place = self.wire.place
        for half in self.halves:
            near, far = place.near(half)
            self._out(half, place.here, 3, near)
            self._out(half, place.here, 7, far)

    def pass_level(self, steps=(0, 1, 2)):
        place = self.wire.place
        for step in steps:
            k = place.nearest[step]
            block = lax.rem(place.here + place.count - 4 * k, place.count)
            rising = place.level >= k
            onward = jnp.where(rising, place.level < place.top, place.level > 0)
            chip = jnp.where(rising, place.here + 4, place.here - 4)
            slot = jnp.where(rising, k, k - 2)
            for half in self.halves:
                near, far = place.near(half)
                self.wire.got(self.view(half, block), self.base[half] + k - 1)

                @pl.when(onward)
                def _():
                    self._line(half, block, slot, chip)

                self._out(half, block, 3 + k, near)
                self._out(half, block, 7, far)
                self._give(half, block)

    def pass_near(self, steps=(0, 1, 2, 3)):
        place = self.wire.place
        for step in steps:
            k = (0, *place.nearest)[step]
            for half in self.halves:
                _, far = place.near(half)
                block = lax.rem(place.here + place.count - 4 * k, place.count)
                block = place.flip(block, half)
                self.wire.got(self.view(half, block), self.base[half] + 3 + k)
                self._out(half, block, 7, far)
                self._give(half, block)

    def finish(self):
        place = self.wire.place
        for half in self.halves:
            self.wire.got(self.spare(half, 8), self.base[half] + 7)
            if self.share:
                for k in range(4):
                    block = place.flip(place.below[k], 1 - half)
                    self._give(half, block)
                    self._give(half, place.flip(block, half))

    def finish_share(self):
        for half in self.halves:
            self.wire.got(self.spare(half, 15), self.side[half])

    def drain(self):
        place = self.wire.place
        for half in self.halves:

            @pl.when(jnp.logical_or(place.level == 0, place.level == place.top))
            def _():
                self.wire.sent(self.spare(half, 1), self.line_out[half])

            @pl.when(jnp.logical_and(place.level > 0, place.level < place.top))
            def _():
                self.wire.sent(self.spare(half, 5), self.line_out[half])


class Scatter:
    def __init__(self, wire, view, buf, out):
        self.wire, self.view, self.buf, self.out = wire, view, buf, out
        self.halves = range(2)
        self.base = [wire.slots(13) for _ in self.halves]
        self.send_slot = [wire.sender(buf(half)) for half in self.halves]

    def _send(self, half, block, place_in, slot, chip):
        self.wire.send(
            self.view(half, block),
            self.buf(half).at[place_in],
            self.base[half] + slot,
            chip,
            out=self.send_slot[half],
        )

    def start(self, levels=(1, 2, 3, 0)):
        place = self.wire.place
        for k in levels:
            for half in self.halves:
                _, far = place.near(half)
                away = place.flip(place.below[k], 1 - half)
                for pair, block in ((1, place.flip(away, half)), (0, away)):
                    self._send(half, block, 2 * k + pair, 2 * k + pair, far)

    def pass_near(self, levels=(1, 2, 3, 0)):
        place = self.wire.place
        for k in levels:
            for half in self.halves:
                near, _ = place.near(half)
                block = place.flip(place.below[k], half)
                slot = 2 * k + 1
                self.wire.got(self.buf(half).at[slot], self.base[half] + slot)
                ref = self.view(half, block)
                ref[...] = (ref[...].astype(F32) + self.buf(half)[slot].astype(F32)).astype(LOW)
                self._send(half, block, 8 + k, 8 + k, near)

    def pass_level(self, levels=(1, 2, 3)):
        place = self.wire.place
        for k in levels:
            for half in self.halves:
                ref = self.view(half, place.below[k])
                ref[...] = self._sum(half, k).astype(LOW)
                self._send(half, place.below[k], 11 + k, 12, place.below[k])

    def _sum(self, half, k):
        place, buf = self.wire.place, self.buf(half)
        self.wire.got(buf.at[2 * k], self.base[half] + 2 * k)
        self.wire.got(buf.at[8 + k], self.base[half] + 8 + k)
        total = self.view(half, place.below[k])[...].astype(F32)
        return total + buf[2 * k].astype(F32) + buf[8 + k].astype(F32)

    def finish(self):
        for half in self.halves:
            buf = self.buf(half)
            total = self._sum(half, 0)
            self.wire.got(buf.at[12:15], self.base[half] + 12)
            for k in (1, 2, 3):
                total = total + buf[11 + k].astype(F32)
            self.out(half, total)


def lane_split(rows):
    lane = lax.broadcasted_iota(jnp.int32, rows.shape, 1)
    low = lane < rows.shape[1] // 2
    zero = jnp.zeros_like(rows)
    return jnp.concatenate((jnp.where(low, rows, zero), jnp.where(low, zero, rows)), axis=0)


def lane_join(rows):
    count, width = rows.shape[0] // 2, rows.shape[1]
    lane = lax.broadcasted_iota(jnp.int32, (count, width), 1)
    return jnp.where(lane < width // 2, rows[:count], rows[count:])


def pair_attend(tok, pairs, chunk, q_ref, kv_ref, s_ref, e_ref, rl_ref, mixed_ref, bias_ref, between):
    keys = kv_ref.shape[0]
    total = pairs * 128

    for j in range(pairs):
        cols = slice(j * 128, (j + 1) * 128)
        vcols = slice(total + j * 128, total + (j + 1) * 128)
        q_cat = lane_split(q_ref[:, cols])

        def score(c, top):
            rows = pl.ds(aligned(c * chunk, chunk), chunk)
            s = dot_nt(q_cat, kv_ref[rows, cols])
            if bias_ref is not None:
                tiles = []
                for half in range(2):
                    row = []
                    for b in range(chunk // tok):
                        lanes = pl.ds(aligned((c * (chunk // tok) + b) * 2 * tok, 128), 2 * tok)
                        vec = bias_ref[2 * j + half : 2 * j + half + 1, lanes]
                        wide = jnp.broadcast_to(vec, (tok, 2 * tok))
                        row.append(pltpu.roll(wide, 0, 1, stride=1, stride_axis=0)[:, :tok])
                    tiles.append(jnp.concatenate(row, axis=1))
                s = s + jnp.concatenate(tiles, axis=0)
            s_ref[:, rows] = s
            for b in range(chunk // 128):
                top = jnp.maximum(top, s[:, b * 128 : (b + 1) * 128])
            return top

        top = lax.fori_loop(0, keys // chunk, score, jnp.full((2 * tok, 128), NEG, F32))
        peak = jnp.max(top, axis=1, keepdims=True)

        def weigh(c, state):
            acc, run = state
            rows = pl.ds(aligned(c * chunk, chunk), chunk)
            e = jnp.exp(s_ref[:, rows] - peak)
            for b in range(chunk // 128):
                run = run + e[:, b * 128 : (b + 1) * 128]
            low = e.astype(LOW)
            e_ref[j, :, rows] = low
            return (acc + dot(low, kv_ref[rows, vcols]), run)

        zero = jnp.zeros((2 * tok, 128), F32)
        acc, run = lax.fori_loop(0, keys // chunk, weigh, (zero, zero))
        rl = 1.0 / jnp.sum(run, axis=1, keepdims=True)
        rl_ref[j] = rl
        mixed_ref[:, cols] = lane_join(acc * rl).astype(LOW)
        between(j)


class PairBack:
    def __init__(self, tok, pairs, q, kv, e, rl, mixed, grad, kv_grad, diag, qc, gc, dl, dq):
        self.tok, self.pairs, self.kv, self.e = tok, pairs, kv, e
        self.kv_grad, self.diag, self.qc, self.gc, self.dl, self.dq = kv_grad, diag, qc, gc, dl, dq
        self.total = pairs * 128
        for j in range(pairs):
            cols = slice(j * 128, (j + 1) * 128)
            rl_j = rl[j]
            grads = lane_split(grad[:, cols].astype(F32))
            qc[j] = lane_split(q[:, cols])
            gc[j] = (grads * rl_j).astype(LOW)
            values = lane_split(mixed[:, cols].astype(F32))
            dl[j] = jnp.sum(grads * values, axis=1, keepdims=True) * rl_j
            dq[j] = jnp.zeros(dq.shape[1:], F32)

    def chunk(self, start, count):
        tok, kv, qc, gc = self.tok, self.kv, self.qc, self.gc
        rows = pl.ds(aligned(start, count), count)
        flip = (
            lax.broadcasted_iota(jnp.int32, (tok, tok), 0)
            + lax.broadcasted_iota(jnp.int32, (tok, tok), 1)
            == tok - 1
        ).astype(LOW)

        def one_pair(j, carry):
            cols = pl.ds(aligned(j * 128, 128), 128)
            vcols = pl.ds(aligned(self.total + j * 128, 128), 128)
            low_e = self.e[j, :, rows]
            dp = dot_nt(gc[j], kv[rows, vcols])
            ds = (low_e.astype(F32) * (dp - self.dl[j])).astype(LOW)
            if self.diag is not None:
                for half in range(2):
                    turned = dot(flip, ds[half * tok : (half + 1) * tok])
                    for b in range(count // tok):
                        tile = turned[:, b * tok : (b + 1) * tok]
                        wide = jnp.concatenate((tile, jnp.zeros_like(tile)), axis=1)
                        wide = pltpu.roll(wide, tok + 1, 1, stride=1, stride_axis=0)
                        lanes = pl.ds(aligned(2 * start + b * 2 * tok, 128), 2 * tok)
                        self.diag[pl.ds(2 * j + half, 1), lanes] = jnp.sum(
                            wide, axis=0, keepdims=True
                        )
            self.kv_grad[rows, cols] = dot_tn(ds, qc[j]).astype(LOW)
            self.kv_grad[rows, vcols] = dot_tn(low_e, gc[j]).astype(LOW)
            self.dq[j] = self.dq[j] + dot(ds, kv[rows, cols])
            return carry

        lax.fori_loop(0, self.pairs, one_pair, 0)

    def finish(self, q_grad):
        for j in range(self.pairs):
            q_grad[:, j * 128 : (j + 1) * 128] = lane_join(self.dq[j]).astype(LOW)


def bucket_rows(buckets_ref, order_ref, here, table_rows, ids_ref):
    count, tok = buckets_ref.shape
    turn = (
        lax.broadcasted_iota(jnp.int32, (tok, tok), 0)
        + lax.broadcasted_iota(jnp.int32, (tok, tok), 1)
        == tok - 1
    ).astype(LOW)
    table_rows[:count, :] = jnp.full((count, tok), -1.0, F32)
    table_rows[count:, :] = dot(buckets_ref[...].astype(LOW), turn)
    own = order_ref[here]
    for block in range(count):
        at = own - order_ref[block] + count
        wide = jnp.concatenate(
            (table_rows[pl.ds(at - 1, 1), :], table_rows[pl.ds(at, 1), :]), axis=1
        )
        ids_ref[:, block * 2 * tok : (block + 1) * 2 * tok] = pltpu.roll(wide, 1, 1)


def bucket_masks(ids_ref, buckets):
    ids = ids_ref[...]
    row = lax.broadcasted_iota(jnp.int32, (buckets, ids.shape[1]), 0).astype(F32)
    return ids, (row == ids).astype(F32)


def bias_vectors(ids_ref, table_ref, bias_ref):
    heads, buckets = table_ref.shape
    ids, mask = bucket_masks(ids_ref, buckets)
    vec = dot(table_ref[...], mask, precision=HIGH)
    bias_ref[:heads, :] = jnp.where(ids >= 0, vec, NEG)


def bucket_sums(ids_ref, diag_ref, buckets):
    _, mask = bucket_masks(ids_ref, buckets)
    return dot_nt(diag_ref[...], mask, precision=HIGH)


def rows_loop(count, step, body):
    def one(index, carry):
        body(pl.ds(aligned(index * step, step), step))
        return carry

    lax.fori_loop(0, count // step, one, 0)


GELU_A = 0.7978845608028654
GELU_B = 0.044715


def gelu_parts(value):
    square = value * value
    wave = jnp.tanh(GELU_A * (value + GELU_B * value * square))
    half = 0.5 * (1.0 + wave)
    slope = half + 0.5 * value * (1.0 - wave * wave) * (GELU_A * (1.0 + 3.0 * GELU_B * square))
    return value * half, slope


def core_sum(wire, part, out_buf, in_buf):
    slot = wire.slots(1)
    out_buf[...] = part.astype(LOW)
    wire.swap(out_buf, in_buf, slot)
    wire.got(in_buf, slot)
    return out_buf[...].astype(F32) + in_buf[...].astype(F32)


class PlaneSum:
    def __init__(self, wire, tok, part, core_buf, plane_buf, whole):
        self.wire, self.tok = wire, tok
        self.out = wire.sender(part)
        self.part, self.core_buf, self.plane_buf, self.whole = part, core_buf, plane_buf, whole
        self.base = wire.slots(8)
        self.half = whole.shape[1] // 2
        place = wire.place
        self.chips = (place.here, place.fx, place.fy, place.fxy)

    def cols(self, core):
        return pl.ds(aligned(core * self.half, 128), self.half)

    def rows(self, k):
        return pl.ds(aligned(lax.rem(self.chips[k], 4) * self.tok, self.tok), self.tok)

    def start(self, k):
        away = self.cols(self.wire.place.other)
        rows = self.rows(k)
        self.wire.swap(self.part.at[rows, away], self.core_buf.at[rows, :], self.base + k, self.out)

    def middle(self, k):
        wire, rows = self.wire, self.rows(k)
        wire.got(self.core_buf.at[rows, :], self.base + k)
        total = self.part[rows, self.cols(wire.place.core)].astype(F32)
        total = total + self.core_buf[rows, :].astype(F32)
        self.core_buf[rows, :] = total.astype(LOW)
        if k:
            wire.send(
                self.core_buf.at[rows, :],
                self.plane_buf.at[k - 1],
                self.base + 3 + k,
                self.chips[k],
                out=self.out,
            )

    def finish(self):
        place, wire = self.wire.place, self.wire
        total = self.core_buf[self.rows(0), :].astype(F32)
        for k in (1, 2, 3):
            wire.got(self.plane_buf.at[k - 1], self.base + 3 + k)
            total = total + self.plane_buf[k - 1].astype(F32)
        mine = self.cols(place.core)
        self.whole[:, mine] = total.astype(LOW)
        wire.swap(self.whole.at[:, mine], self.whole.at[:, mine], self.base + 7, self.out)

    def finish_core(self):
        self.wire.got(self.whole.at[:, self.cols(self.wire.place.other)], self.base + 7)


class PlaneGather:
    def __init__(self, wire, tok, ref):
        self.wire, self.tok, self.ref = wire, tok, ref
        self.half = ref.shape[1] // 2
        self.base = wire.slots(8)
        self.out = wire.sender(ref.at[: 3 * tok, :])
        place = wire.place
        self.chips = (place.here, place.fx, place.fy, place.fxy)

    def view(self, k, core):
        rows = pl.ds(aligned(lax.rem(self.chips[k], 4) * self.tok, self.tok), self.tok)
        return self.ref.at[rows, pl.ds(aligned(core * self.half, 128), self.half)]

    def start(self):
        own = self.view(0, self.wire.place.core)
        for k in (1, 2, 3):
            self.wire.send(own, own, self.base + k, self.chips[k], out=self.out)

    def share(self, k):
        ref = self.view(k, self.wire.place.core)
        self.wire.got(ref, self.base + k)
        self.wire.swap(ref, ref, self.base + 4 + k, self.out)

    def finish(self, k):
        self.wire.got(self.view(k, self.wire.place.other), self.base + 4 + k)


class Sizes:
    def __init__(self, ctx, tok, enc, model, wide, units):
        self.ctx, self.tok, self.enc, self.model, self.wide = ctx, tok, enc, model, wide
        self.rows = model // ctx
        self.units = units
        self.quarter = units // 4
        self.pairs = wide // 128
        self.levels = ctx // 4
        self.attn_cols = 8 * wide
        self.mlp_cols = 3 * units
        self.part = 3 * self.quarter
        self.names = ("q", "k", "v", "cq", "ck", "cv", "o", "co")
        self.col = {n: slice(i * wide, (i + 1) * wide) for i, n in enumerate(self.names)}
        self.col["kv"] = slice(wide, 3 * wide)
        self.col["ckv"] = slice(4 * wide, 6 * wide)
        self.cuts = {
            "s": self.halves(0, 3 * wide, 0),
            "c": self.halves(3 * wide, 6 * wide, 1),
            "o": self.halves(6 * wide, 7 * wide, 0),
            "co": self.halves(7 * wide, 8 * wide, 1),
        }

    def halves(self, first, last, up):
        tiles = (last - first) // 128
        middle = first + (tiles + up) // 2 * 128
        return ((first, middle), (middle, last))


def named(kernel, names):
    def body(*refs):
        kernel(**dict(zip(names, refs, strict=True)))

    return body


def wire_sems(send, recv):
    return {
        "send_sem": pltpu.SemaphoreType.DMA((send,)),
        "recv_sem": pltpu.SemaphoreType.DMA((recv,)),
    }


def layer_kernel(
    size, layer_in, encoded, sq, sk, sv, so, cq, ck, cv, co, gate_w, up_w, down_w, gains,
    table, buckets, order, out_grad,
    layer_out, input_grad, enc_grad, WG, mb, totals, bias_totals,
    WA, WM, wm, X, E, GR, PW, PM,
    q, kv, mkv, probes, s, e1, e2, rl1, rl2, mixed1, mixed2, table_rows, ids, bias, diag,
    after_self, after_cross, cross_grad, self_grad, n2, N3, act, GU, PN, PO, low, mixed_grad,
    q_grad, kv_grad, mkv_grad, ca, cb, pn_core, pn_plane, pn_whole, po_core, po_plane, po_whole,
    qc, gc, dl, dq, bs0, bs1, bc0, bc1, bo0, bo1, bp0, bp1, bx, be, px, pe, NG, NE, ml, ps,
    s1, s2, sr, sl, t1, t2, tr, tl, send_sem, recv_sem,
):
    place = Place(size.ctx)
    wire = Wire(place, send_sem, recv_sem)
    tok, enc, rows, half_d = size.tok, size.enc, size.rows, size.model // 2
    col, model, quarter = size.col, size.model, size.quarter
    ctx_tok, ctx_enc = X.shape[0], E.shape[0]
    plane_chips = (place.fx, place.fy, place.fxy)
    XG, EG = kv, mkv

    def block_rows(block, count):
        return pl.ds(aligned(block * count, 16), count)

    here_rows = block_rows(place.here, tok)
    own_weights = block_rows(place.here, rows)
    my_part = pl.ds(aligned(place.plane * size.part, 128), size.part)
    mine = pl.ds(aligned(place.core * half_d, 128), half_d)
    away = pl.ds(aligned(place.other * half_d, 128), half_d)

    def token_view(ref, count, core):
        def view(half, block):
            return ref.at[
                pl.ds(aligned(block * count + half * (count // 2), 16), count // 2),
                pl.ds(aligned(core * half_d, 128), half_d),
            ]

        return view

    def weight_view(ref, name):
        def view(half, block):
            first, last = size.cuts[name][half]
            return ref.at[block_rows(block, rows), first:last]

        return view

    def token_spare(buf):
        return lambda half, count: buf.at[half, 0:count]

    def weight_spare(*bufs):
        return lambda half, count: bufs[half].at[0:count]

    def token_gather(ref, count, buf):
        return Gather(
            wire,
            token_view(ref, count, place.core),
            True,
            token_spare(buf),
        )

    gx, ge = token_gather(X, tok, bx), token_gather(E, enc, be)
    gs, gc_, go, gp = (
        Gather(wire, weight_view(WA, name), False, weight_spare(*bufs))
        for name, bufs in (("s", (bs0, bs1)), ("c", (bc0, bc1)), ("o", (bo0, bo1)), ("co", (bp0, bp1)))
    )
    gg = PlaneGather(wire, tok, GR)
    spread = PlaneGather(wire, tok, N3)
    sum_n = PlaneSum(wire, tok, PN, pn_core, pn_plane, pn_whole)
    sum_o = PlaneSum(wire, tok, PO, po_core, po_plane, po_whole)
    mg_plane, mg_level, ms_level, ms_plane = (wire.slots(3) for _ in range(4))

    place.signal(place.above[1:] + list(plane_chips))
    X[here_rows, :] = rms_forward(layer_in[...], gains[0:1]).astype(LOW)
    for name, ref in zip(("q", "k", "v", "cq", "ck", "cv", "o", "co"), (sq, sk, sv, cq, ck, cv, so, co)):
        WA[own_weights, col[name]] = ref[...]
    E[block_rows(place.here, enc), :] = encoded[...]
    place.meet(7)
    gx.start_level()
    gs.start_level()
    gx.start_plane()
    gs.start_plane()
    plane_rows = block_rows(place.plane, tok)
    GR[plane_rows, :] = out_grad[...].astype(LOW)
    for p in range(4):
        cols = slice(p * quarter, (p + 1) * quarter)
        for i, ref in enumerate((gate_w, up_w, down_w)):
            base = p * size.part + i * quarter
            wm[:, base : base + quarter] = ref[:, cols]
    WM[own_weights, :] = wm[:, my_part]
    gx.pass_near((0,))
    gs.pass_near((0,))
    gx.pass_level((0,))
    gs.pass_level((0,))
    gx.pass_level((1,))
    gs.pass_level((1,))
    gx.pass_near((1,))
    gs.pass_near((1,))
    gx.pass_level((2,))
    go.start_level()
    ge.start_level()
    gs.pass_level((2,))
    gc_.start_level()
    gx.pass_near((2,))
    gs.pass_near((2,))
    gx.pass_near((3,))
    gs.pass_near((3,))
    go.start_plane()
    ge.start_plane()
    go.pass_level()
    ge.pass_level()
    go.pass_near((0,))
    ge.pass_near((0,))
    gc_.start_plane()
    bucket_rows(buckets, order, place.here, table_rows, ids)
    bias_vectors(ids, table, bias)
    diag[...] = jnp.zeros_like(diag)
    gp.start_level()
    gc_.pass_level((0, 1))
    gx.finish()
    gc_.pass_level((2,))
    gp.start_plane()
    gx.finish_share()
    gs.finish()
    for k, chip in enumerate(plane_chips):
        wire.send(
            wm.at[:, pl.ds(aligned(lax.rem(chip, 4) * size.part, 128), size.part)],
            WM.at[own_weights, :],
            mg_plane + k,
            chip,
        )

    def project(rows_):
        kv[rows_, :] = dot(X[rows_, :], WA[:, col["kv"]]).astype(LOW)

    def project_enc(rows_):
        mkv[rows_, :] = dot(E[rows_, :], WA[:, col["ckv"]]).astype(LOW)

    q[...] = dot(X[here_rows, :], WA[:, col["q"]]).astype(LOW)
    rows_loop(ctx_tok, 256, project)

    go.pass_near((1, 2, 3))
    ge.pass_near((1, 2, 3))

    def during_self(j):
        if j == 0:
            gp.pass_level()
        elif j == 1:
            gc_.pass_near()
            for k, chip in enumerate(plane_chips):
                wire.got(WM.at[block_rows(chip, rows), :], mg_plane + k)
            own = WM.at[block_rows(place.level, 4 * rows), :]
            for k in (1, 2, 3):
                wire.send(own, own, mg_level + k - 1, place.above[k])
        else:
            gg.start()

    pair_attend(tok, size.pairs, 512, q, kv, s, e1, rl1, mixed1, bias, during_self)
    go.finish()
    part = dot_nt(mixed1[...], WA[:, col["o"]])
    after_self[...] = layer_in[...] + core_sum(wire, part, ca.at[0], cb.at[0])
    n2[...] = rms_forward(after_self[...], gains[1:2]).astype(LOW)
    gp.pass_near()
    ge.finish()
    ge.finish_share()
    gc_.finish()

    rows_loop(ctx_enc, 256, project_enc)
    probes[...] = dot(n2[...], WA[:, col["cq"]]).astype(LOW)

    def during_cross(j):
        if j == 1:
            for k in (1, 2, 3):
                gg.share(k)

    pair_attend(tok, size.pairs, 512, probes, mkv, s, e2, rl2, mixed2, None, during_cross)
    gp.finish()
    part = dot_nt(mixed2[...], WA[:, col["co"]])
    after_cross[...] = after_self[...] + core_sum(wire, part, ca.at[1], cb.at[1])

    N3[plane_rows, :] = rms_forward(after_cross[...], gains[2:3]).astype(LOW)
    spread.start()
    for k in (1, 2, 3):
        level = place.below[k] // 4
        wire.got(WM.at[block_rows(level, 4 * rows), :], mg_level + k - 1)

    def units(k):
        rows_ = spread_rows(k)
        pre = dot(N3[rows_, :], WM[:, : 2 * quarter])
        gate, upper = pre[:, :quarter], pre[:, quarter:]
        value, slope = gelu_parts(gate)
        act[rows_, :] = (value * upper).astype(LOW)
        grad = dot(GR[rows_, :], WM[:, 2 * quarter :])
        GU[rows_, :quarter] = (grad * upper * slope).astype(LOW)
        GU[rows_, quarter:] = (grad * value).astype(LOW)
        PN[rows_, :] = dot_nt(GU[rows_, :], WM[:, : 2 * quarter]).astype(LOW)

    def spread_rows(k):
        return sum_n.rows(k)

    for k in (1, 2, 3):
        gg.finish(k)
    units(0)
    sum_n.start(0)
    spread.share(1)
    spread.share(2)
    spread.finish(1)
    units(1)
    sum_n.start(1)
    spread.share(3)
    spread.finish(2)
    units(2)
    sum_n.start(2)
    sum_n.middle(1)
    spread.finish(3)
    units(3)
    sum_n.start(3)
    sum_n.middle(2)

    def back_out(k):
        rows_ = spread_rows(k)
        PO[rows_, :] = dot_nt(act[rows_, :], WM[:, 2 * quarter :]).astype(LOW)

    def unit_grads(cols):
        PM[cols, : 2 * quarter] = dot_tn(N3[:, cols], GU[...]).astype(LOW)
        PM[cols, 2 * quarter :] = dot_tn(GR[:, cols], act[...]).astype(LOW)

    back_out(0)
    sum_n.middle(3)
    sum_n.middle(0)
    rows_loop(model, 128, unit_grads)
    for k in (1, 2, 3):
        wire.send(
            PM.at[block_rows(place.above[k] // 4, 4 * rows), :],
            ml.at[k - 1],
            ms_level + k - 1,
            place.above[k],
        )
    sum_n.finish()
    for k in (1, 2, 3):
        back_out(k)
    for k in range(4):
        sum_o.start(k)
    sum_n.finish_core()
    extra, gain_three = rms_backward(after_cross[...], gains[2:3], pn_whole[...].astype(F32))
    cross_grad[...] = out_grad[...] + extra
    low[...] = cross_grad[...].astype(LOW)
    mixed_grad[...] = dot(low[...], WA[:, col["co"]]).astype(LOW)
    for k in (1, 2, 3, 0):
        sum_o.middle(k)

    def out_grads(left, right, target):
        def body(cols):
            PW[cols, target] = dot_tn(left[:, cols], right[...]).astype(LOW)

        rows_loop(model, 128, body)

    def weight_stream(name, *bufs):
        def out(half, total):
            first, last = size.cuts[name][half]
            WG[:, first:last] = total

        return Scatter(wire, weight_view(PW, name), lambda half: bufs[half], out)

    def token_out(ref, count):
        def out(half, total):
            ref[half * (count // 2) : (half + 1) * (count // 2), mine] = total

        return out

    sp = weight_stream("co", bp0, bp1)
    so_ = weight_stream("o", bo0, bo1)
    sc = weight_stream("c", bc0, bc1)
    sw = weight_stream("s", bs0, bs1)
    sx = Scatter(wire, token_view(XG, tok, place.core), lambda half: bx.at[half], token_out(NG, tok))
    se = Scatter(wire, token_view(EG, enc, place.core), lambda half: be.at[half], token_out(NE, enc))
    x_base, e_base = wire.slots(4), wire.slots(4)
    x_out, e_out = wire.sender(px), wire.sender(pe)

    def pair_start(ref, recv, count, base, k, out):
        at = block_rows(place.below[k] // 4, 4 * count)
        wire.swap(ref.at[at, away], recv.at[at, :], base + k, out)

    def pair_ready(ref, recv, count, base, k):
        at = block_rows(place.below[k] // 4, 4 * count)
        wire.got(recv.at[at, :], base + k)
        ref[at, mine] = (ref[at, mine].astype(F32) + recv[at, :].astype(F32)).astype(LOW)

    out_grads(low, mixed2, col["co"])
    sp.start()
    back = PairBack(
        tok, size.pairs, probes, mkv, e2, rl2, mixed2, mixed_grad, mkv_grad, None, qc, gc, dl, dq
    )
    for c in range(ctx_enc // 512):
        back.chunk(c * 512, 512)
    back.finish(q_grad)
    part = dot_nt(q_grad[...], WA[:, col["cq"]])
    slot = wire.slots(1)
    ca[2] = part.astype(LOW)
    wire.swap(ca.at[2], cb.at[2], slot)
    sp.pass_near()
    out_grads(E, mkv_grad, col["ckv"])
    out_grads(n2, q_grad, col["cq"])
    sc.start()

    def enc_rows(rows_):
        EG[rows_, :] = dot_nt(mkv_grad[rows_, :], WA[:, col["ckv"]]).astype(LOW)

    rows_loop(ctx_enc, 256, enc_rows)
    for k in (1, 2, 3, 0):
        pair_start(EG, pe, enc, e_base, k, e_out)
    wire.got(cb.at[2], slot)
    n_grad = ca[2].astype(F32) + cb[2].astype(F32)
    extra, gain_two = rms_backward(after_self[...], gains[1:2], n_grad)
    self_grad[...] = cross_grad[...] + extra
    low[...] = self_grad[...].astype(LOW)
    mixed_grad[...] = dot(low[...], WA[:, col["o"]]).astype(LOW)
    for k in (1, 2, 3, 0):
        pair_ready(EG, pe, enc, e_base, k)
        se.start((k,))
    out_grads(low, mixed1, col["o"])
    so_.start()

    back = PairBack(
        tok, size.pairs, q, kv, e1, rl1, mixed1, mixed_grad, kv_grad, diag, qc, gc, dl, dq
    )

    def tok_rows(k):
        for part_ in range(2):
            at = pl.ds(aligned(place.below[k] // 4 * 4 * tok + part_ * 2 * tok, 16), 2 * tok)
            XG[at, :] = dot_nt(kv_grad[at, :], WA[:, col["kv"]]).astype(LOW)

    n2[...] = X[here_rows, :]
    back.chunk(place.below[1] // 4 * 4 * tok, 4 * tok)
    tok_rows(1)
    pair_start(XG, px, tok, x_base, 1, x_out)
    sp.pass_level()
    back.chunk(place.below[2] // 4 * 4 * tok, 4 * tok)
    tok_rows(2)
    pair_start(XG, px, tok, x_base, 2, x_out)
    pair_ready(XG, px, tok, x_base, 1)
    sx.start((1,))
    sc.pass_near()
    back.chunk(place.below[3] // 4 * 4 * tok, 4 * tok)
    tok_rows(3)
    pair_start(XG, px, tok, x_base, 3, x_out)
    pair_ready(XG, px, tok, x_base, 2)
    sx.start((2,))
    se.pass_near()
    back.chunk(place.level * 4 * tok, 4 * tok)
    back.finish(q_grad)
    tok_rows(0)
    own = dot_nt(q_grad[...], WA[:, col["q"]]) + XG[here_rows, :].astype(F32)
    XG[here_rows, :] = own.astype(LOW)
    pair_start(XG, px, tok, x_base, 0, x_out)
    pair_ready(XG, px, tok, x_base, 3)
    sx.start((3,))
    so_.pass_near()
    out_grads(n2, q_grad, col["q"])
    pair_ready(XG, px, tok, x_base, 0)
    sx.start((0,))
    out_grads(X, kv_grad, col["kv"])
    sx.pass_near((1, 2))
    sw.start()

    sc.pass_level()
    sx.pass_near((3, 0))
    se.pass_level()
    total = PM[block_rows(place.level, 4 * rows), :].astype(F32)
    for k in (1, 2, 3):
        wire.got(ml.at[k - 1], ms_level + k - 1)
        total = total + ml[k - 1].astype(F32)
    ps[...] = total.astype(LOW)
    for k, chip in enumerate(plane_chips):
        wire.send(
            ps.at[block_rows(lax.rem(chip, 4), rows), :], mb.at[:, my_part], ms_plane + k, chip
        )
    mb[:, my_part] = ps[block_rows(place.plane, rows), :]
    sums = bucket_sums(ids, diag, table.shape[1])
    t1[...] = jnp.concatenate(
        (sums, jnp.zeros((sums.shape[0], t1.shape[1] - sums.shape[1]), F32)), axis=1
    )
    so_.pass_level()
    sw.pass_near((1, 2))
    sx.pass_level()
    sw.pass_near((3, 0))
    sum_o.finish()
    se.finish()
    x_slot, e_slot = wire.slots(1), wire.slots(1)
    wire.swap(NE.at[:, mine], NE.at[:, mine], e_slot)
    sx.finish()
    wire.swap(NG.at[:, mine], NG.at[:, mine], x_slot)
    sw.pass_level()
    wire.got(NG.at[:, away], x_slot)
    extra, gain_one = rms_backward(layer_in[...], gains[0:1], NG[...])
    input_grad[...] = self_grad[...] + extra
    s1[...] = jnp.concatenate(
        (gain_one, gain_two, gain_three, jnp.zeros((5, model), F32)), axis=0
    )
    small = wire.slots(10)
    wire.send(s1, sr.at[0], small, place.fx)
    wire.send(t1, tr.at[0], small + 5, place.fx)
    sum_o.finish_core()
    layer_out[...] = after_cross[...] + po_whole[...].astype(F32)
    wire.got(NE.at[:, away], e_slot)
    enc_grad[...] = NE[...]
    wire.got(sr.at[0], small)
    wire.got(tr.at[0], small + 5)
    s2[...] = s1[...] + sr[0]
    t2[...] = t1[...] + tr[0]
    wire.send(s2, sr.at[1], small + 1, place.fy)
    wire.send(t2, tr.at[1], small + 6, place.fy)
    sp.finish()
    sc.finish()
    so_.finish()
    wire.got(sr.at[1], small + 1)
    wire.got(tr.at[1], small + 6)
    sl[pl.ds(place.level, 1)] = (s2[...] + sr[1])[None]
    tl[pl.ds(place.level, 1)] = (t2[...] + tr[1])[None]
    for k in (1, 2, 3):
        wire.send(sl.at[place.level], sl.at[place.level], small + 1 + k, place.above[k])
        wire.send(tl.at[place.level], tl.at[place.level], small + 6 + k, place.above[k])
    sw.finish()
    for k, chip in enumerate(plane_chips):
        cols = pl.ds(aligned(lax.rem(chip, 4) * size.part, 128), size.part)
        wire.got(mb.at[:, cols], ms_plane + k)
    for k in (1, 2, 3):
        level = place.below[k] // 4
        wire.got(sl.at[level], small + 1 + k)
        wire.got(tl.at[level], small + 6 + k)
    totals[...] = (sl[0] + sl[1]) + (sl[2] + sl[3])
    bias_totals[...] = (tl[0] + tl[1]) + (tl[2] + tl[3])
    for made in (gx, ge, gs, gc_, go, gp):
        made.drain()
    wire.drain()


def emit_kernel(size, layer_out, input_grad, enc_grad, WG, mb, totals, bias_totals, *outs):
    for ref, out in zip((layer_out, input_grad, enc_grad), outs):
        out[...] = ref[...]
    for name, out in zip(size.names, outs[3:]):
        out[...] = WG[:, size.col[name]]
    for i, out in enumerate(outs[11:14]):
        for p in range(4):
            base = p * size.part + i * size.quarter
            out[:, p * size.quarter : (p + 1) * size.quarter] = mb[
                :, base : base + size.quarter
            ].astype(F32)
    outs[14][...] = totals[:3]
    heads, buckets = outs[15].shape
    outs[15][...] = bias_totals[:heads, :buckets]


def quick_device(
    layer_in, encoded, self_query, self_key, self_value, self_out, cross_query, cross_key,
    cross_value, cross_out, gate_proj, up_proj, down_proj, norm_gains, position_bias,
    bucket_ids, block_order, out_grad,
):
    tok, model = layer_in.shape
    enc = encoded.shape[0]
    wide, units = self_query.shape[1], gate_proj.shape[1]
    ctx = block_order.shape[0]
    buckets, heads = position_bias.shape
    size = Sizes(ctx, tok, enc, model, wide, units)
    rows, quarter, pairs = size.rows, size.quarter, size.pairs
    tok_all, enc_all, tok4 = ctx * tok, ctx * enc, 4 * tok

    def vmem(*shape, dtype=LOW):
        return pltpu.VMEM(shape, dtype)

    def full(*shape):
        return pltpu.VMEM(shape, F32)

    def streams(name):
        return [vmem(15, rows, last - first) for first, last in size.cuts[name]]

    ins = {
        "layer_in": layer_in, "encoded": encoded, "sq": self_query, "sk": self_key,
        "sv": self_value, "so": self_out.T, "cq": cross_query, "ck": cross_key,
        "cv": cross_value, "co": cross_out.T, "gate_w": gate_proj, "up_w": up_proj,
        "down_w": down_proj.T, "gains": norm_gains, "table": position_bias.T,
        "buckets": bucket_ids.reshape(ctx, tok), "order": block_order, "out_grad": out_grad,
    }
    outs = {
        "layer_out": ((tok, model), F32), "input_grad": ((tok, model), F32),
        "enc_grad": ((enc, model), F32), "WG": ((rows, size.attn_cols), F32),
        "mb": ((rows, size.mlp_cols), LOW), "totals": ((8, model), F32),
        "bias_totals": ((8, 128), F32),
    }
    (bs0, bs1), (bc0, bc1) = streams("s"), streams("c")
    (bo0, bo1), (bp0, bp1) = streams("o"), streams("co")
    scratch = {
        "WA": vmem(model, size.attn_cols), "WM": vmem(model, size.part),
        "wm": vmem(rows, size.mlp_cols), "X": vmem(tok_all, model), "E": vmem(enc_all, model),
        "GR": vmem(tok4, model), "PW": vmem(model, size.attn_cols),
        "PM": vmem(model, size.part),
        "q": vmem(tok, wide), "kv": vmem(tok_all, 2 * wide), "mkv": vmem(enc_all, 2 * wide),
        "probes": vmem(tok, wide), "s": full(2 * tok, tok_all),
        "e1": vmem(pairs, 2 * tok, tok_all), "e2": vmem(pairs, 2 * tok, enc_all),
        "rl1": full(pairs, 2 * tok, 1), "rl2": full(pairs, 2 * tok, 1),
        "mixed1": vmem(tok, wide), "mixed2": vmem(tok, wide), "table_rows": full(2 * ctx, tok),
        "ids": full(1, 2 * tok_all), "bias": full(8, 2 * tok_all), "diag": full(8, 2 * tok_all),
        "after_self": full(tok, model), "after_cross": full(tok, model),
        "cross_grad": full(tok, model), "self_grad": full(tok, model), "n2": vmem(tok, model),
        "N3": vmem(tok4, model), "act": vmem(tok4, quarter), "GU": vmem(tok4, 2 * quarter),
        "PN": vmem(tok4, model), "PO": vmem(tok4, model), "low": vmem(tok, model),
        "mixed_grad": vmem(tok, wide), "q_grad": vmem(tok, wide),
        "kv_grad": vmem(tok_all, 2 * wide), "mkv_grad": vmem(enc_all, 2 * wide),
        "ca": vmem(3, tok, model), "cb": vmem(3, tok, model),
        "pn_core": vmem(tok4, model // 2), "pn_plane": vmem(3, tok, model // 2),
        "pn_whole": vmem(tok, model), "po_core": vmem(tok4, model // 2),
        "po_plane": vmem(3, tok, model // 2), "po_whole": vmem(tok, model),
        "qc": vmem(pairs, 2 * tok, 128), "gc": vmem(pairs, 2 * tok, 128),
        "dl": full(pairs, 2 * tok, 1), "dq": full(pairs, 2 * tok, 128),
        "bs0": bs0, "bs1": bs1, "bc0": bc0, "bc1": bc1, "bo0": bo0, "bo1": bo1,
        "bp0": bp0, "bp1": bp1, "bx": vmem(2, 15, tok // 2, model // 2),
        "be": vmem(2, 15, enc // 2, model // 2), "px": vmem(tok_all, model // 2),
        "pe": vmem(enc_all, model // 2), "NG": full(tok, model), "NE": full(enc, model),
        "ml": vmem(3, 4 * rows, size.part), "ps": vmem(4 * rows, size.part),
        "s1": full(8, model), "s2": full(8, model), "sr": full(2, 8, model),
        "sl": full(4, 8, model), "t1": full(8, 128), "t2": full(8, 128), "tr": full(2, 8, 128), "tl": full(4, 8, 128), **wire_sems(73, 323),
    }
    names = list(ins) + list(outs) + list(scratch)
    made = pl.pallas_call(
        named(functools.partial(layer_kernel, size), names),
        out_shape=tuple(jax.ShapeDtypeStruct(*spec) for spec in outs.values()),
        in_specs=[
            pl.BlockSpec(memory_space=pltpu.SMEM if name == "order" else pltpu.VMEM)
            for name in ins
        ],
        out_specs=tuple(pl.BlockSpec(memory_space=pltpu.VMEM) for _ in outs),
        scratch_shapes=list(scratch.values()),
        compiler_params=pltpu.CompilerParams(
            collective_id=1, has_side_effects=True, vmem_limit_bytes=VMEM_LIMIT
        ),
    )(*ins.values())
    specs = [
        (tok, model), (tok, model), (enc, model), *((rows, wide),) * 8, *((rows, units),) * 3,
        (3, model), (heads, buckets),
    ]
    parts = pl.pallas_call(
        functools.partial(emit_kernel, size),
        out_shape=tuple(jax.ShapeDtypeStruct(spec, F32) for spec in specs),
        in_specs=[pl.BlockSpec(memory_space=pltpu.VMEM)] * len(made),
        out_specs=tuple(pl.BlockSpec(memory_space=pltpu.VMEM) for _ in specs),
    )(*made)
    named_parts = dict(zip(size.names, parts[3:11]))
    gate, upward, down, gains, bias_grad = parts[11:]
    return (
        *parts[:3], named_parts["q"], named_parts["k"], named_parts["v"], named_parts["o"].T,
        named_parts["cq"], named_parts["ck"], named_parts["cv"], named_parts["co"].T,
        gate, upward, down.T, gains, bias_grad.T,
    )


def quick_fits(mesh):
    return mesh.shape["ctx"] == 16 and mesh.shape["head"] == 2


def as_sent(shard):

    def short(part):
        return part.astype(jnp.bfloat16) if part.dtype == jnp.float32 else part

    return jax.tree.map(short, shard)


def rms_scale(rows, gain):
    return rows * lax.rsqrt(jnp.mean(rows * rows, axis=-1, keepdims=True) + EPS) * gain


def geglu(gate, upper):
    return jax.nn.gelu(gate, approximate=True) * upper


def times(left, right):
    return jnp.dot(left, right, preferred_element_type=jnp.float32)


def left_times(left, right):
    return lax.dot_general(
        left, right, (((0,), (0,)), ((), ())), preferred_element_type=jnp.float32
    )


def right_times(left, right):
    return lax.dot_general(
        left, right, (((1,), (1,)), ((), ())), preferred_element_type=jnp.float32
    )


def join_heads(parts):
    return jax.tree.map(lambda part: part.astype(jnp.float32), lax.psum(as_sent(parts), "head"))


def gather_self(keys_own, values_own):
    return (
        lax.all_gather(keys_own, "ctx", axis=0, tiled=True),
        lax.all_gather(values_own, "ctx", axis=0, tiled=True),
    )


def gather_cross(memory_keys, memory_values):
    return (
        lax.all_gather(memory_keys, "ctx", axis=0, tiled=True),
        lax.all_gather(memory_values, "ctx", axis=0, tiled=True),
    )


def bias_scores(steps, bias_table):
    rises = bias_table[1:] - bias_table[:-1]
    return bias_table[0][:, None, None] + jnp.einsum("qkb,bh->hqk", steps, rises, precision=HIGH)


def bias_grads(score_grad, steps):
    above = jnp.einsum("hqk,qkb->bh", score_grad, steps, precision=HIGH)
    total = jnp.sum(score_grad, axis=(1, 2))
    upper_rows = jnp.concatenate((total[None], above), axis=0)
    lower_rows = jnp.concatenate((above, jnp.zeros((1, above.shape[1]), jnp.float32)), axis=0)
    return upper_rows - lower_rows


def delta_of(mixed, mixed_grad, head_count):
    tok_rows, total_width = mixed.shape
    width = total_width // head_count
    product = mixed.astype(jnp.float32).reshape(tok_rows, head_count, width) * mixed_grad.astype(
        jnp.float32
    ).reshape(tok_rows, head_count, width)
    return jnp.transpose(jnp.sum(product, axis=-1))


def attend_fold(queries, head_count, parts_fn, bias_table):
    tok_rows = queries.shape[0]
    width = queries.shape[1] // head_count
    query3 = queries.reshape(tok_rows, head_count, width)

    def fold(state, pieces, start):
        key_piece, value_piece = pieces
        count = key_piece.shape[0]
        block = math.gcd(count, 512)

        def fold_step(index, inner):
            summed, run_max, run_sum = inner
            key3 = lax.dynamic_slice_in_dim(key_piece, index * block, block, 0).reshape(
                block, head_count, width
            )
            value3 = lax.dynamic_slice_in_dim(value_piece, index * block, block, 0).reshape(
                block, head_count, width
            )
            scores = jnp.einsum("qhe,khe->hqk", query3, key3, preferred_element_type=jnp.float32)
            if parts_fn is not None:
                steps, valid = parts_fn(index * block, block)
                scores = jnp.where(valid[None], scores + bias_scores(steps, bias_table), NEG)
            new_max = jnp.maximum(run_max, jnp.max(scores, axis=-1))
            ratio = jnp.exp(run_max - new_max)
            weights = jnp.exp(scores - new_max[..., None])
            run_sum = run_sum * ratio + jnp.sum(weights, axis=-1)
            summed = summed * ratio[..., None] + jnp.einsum(
                "hqk,khe->hqe",
                weights.astype(jnp.bfloat16),
                value3,
                preferred_element_type=jnp.float32,
            )
            return (summed, new_max, run_sum)

        return lax.fori_loop(0, count // block, fold_step, state)

    return fold


def finish(state):
    summed, run_max, run_sum = state
    head_count, tok_rows, width = summed.shape
    mixed = jnp.transpose(summed / run_sum[..., None], (1, 0, 2)).reshape(
        tok_rows, head_count * width
    )
    return (mixed.astype(jnp.bfloat16), run_max + jnp.log(run_sum))


def attend_back(
    queries, mixed_grad, lse, delta, keys_all, values_all, head_count, parts_fn, bias_table
):
    tok_rows, total_width = queries.shape
    width = total_width // head_count
    query3 = queries.reshape(tok_rows, head_count, width)
    grad3 = mixed_grad.reshape(tok_rows, head_count, width)
    count = keys_all.shape[0]
    block = math.gcd(count, 512)

    def attend_step(carry, index):
        query_grad, bias_grad = carry
        key3 = lax.dynamic_slice_in_dim(keys_all, index * block, block, 0).reshape(
            block, head_count, width
        )
        value3 = lax.dynamic_slice_in_dim(values_all, index * block, block, 0).reshape(
            block, head_count, width
        )
        scores = jnp.einsum("qhe,khe->hqk", query3, key3, preferred_element_type=jnp.float32)
        if parts_fn is not None:
            steps, valid = parts_fn(index * block, block)
            scores = jnp.where(valid[None], scores + bias_scores(steps, bias_table), NEG)
        weights = jnp.exp(scores - lse[..., None])
        weight_grad = jnp.einsum("qhe,khe->hqk", grad3, value3, preferred_element_type=jnp.float32)
        score_grad = weights * (weight_grad - delta[..., None])
        if parts_fn is not None:
            bias_grad = bias_grad + bias_grads(score_grad, steps)
        score_low = score_grad.astype(jnp.bfloat16)
        query_grad = query_grad + jnp.einsum(
            "hqk,khe->qhe", score_low, key3, preferred_element_type=jnp.float32
        )
        stacked = None
        value_term = jnp.einsum(
            "hqk,qhe->khe", weights.astype(jnp.bfloat16), grad3, preferred_element_type=jnp.float32
        )
        key_term = jnp.einsum("hqk,qhe->khe", score_low, query3, preferred_element_type=jnp.float32)
        stacked = jnp.concatenate(
            (key_term.reshape(block, total_width), value_term.reshape(block, total_width)), axis=1
        )
        return ((query_grad, bias_grad), stacked)

    start = (
        jnp.zeros((tok_rows, head_count, width), jnp.float32),
        jnp.zeros(bias_table.shape, jnp.float32),
    )
    (query_grad, bias_grad), terms = lax.scan(attend_step, start, jnp.arange(count // block))
    query_grad = query_grad.reshape(tok_rows, total_width).astype(jnp.bfloat16)
    terms = terms.reshape(count, 2 * total_width)
    return (query_grad, bias_grad, terms)


def per_device(
    layer_in,
    encoded,
    self_query,
    self_key,
    self_value,
    self_out,
    cross_query,
    cross_key,
    cross_value,
    cross_out,
    gate_proj,
    up_proj,
    down_proj,
    norm_gains,
    position_bias,
    bucket_ids,
    block_order,
    out_grad,
):
    low = jnp.bfloat16
    tok_rows = layer_in.shape[0]
    bucket_count, head_count = position_bias.shape
    block_count = block_order.shape[0]
    full_weights = (
        lax.all_gather(self_query, "ctx", axis=0, tiled=True),
        lax.all_gather(self_key, "ctx", axis=0, tiled=True),
        lax.all_gather(self_value, "ctx", axis=0, tiled=True),
        lax.all_gather(self_out, "ctx", axis=1, tiled=True),
        lax.all_gather(cross_query, "ctx", axis=0, tiled=True),
        lax.all_gather(cross_key, "ctx", axis=0, tiled=True),
        lax.all_gather(cross_value, "ctx", axis=0, tiled=True),
        lax.all_gather(cross_out, "ctx", axis=1, tiled=True),
        lax.all_gather(gate_proj, "ctx", axis=0, tiled=True),
        lax.all_gather(up_proj, "ctx", axis=0, tiled=True),
        lax.all_gather(down_proj, "ctx", axis=1, tiled=True),
    )
    (
        query_full,
        key_full,
        value_full,
        output_full,
        probe_full,
        lookup_full,
        recall_full,
        merge_full,
        gate_full,
        upward_full,
        down_full,
    ) = full_weights
    boundaries = jnp.arange(1, bucket_count, dtype=jnp.int32)
    starts = jnp.sum((bucket_ids[None, :] < boundaries[:, None]).astype(jnp.int32), axis=1)
    block_ids = jnp.arange(block_count, dtype=jnp.int32)
    here = lax.axis_index("ctx")
    own_block = jnp.sum(jnp.where(block_ids == here, block_order, 0))
    query_pos = own_block * tok_rows + jnp.arange(tok_rows, dtype=jnp.int32)

    def position_of(rows_index):
        slot = rows_index // tok_rows
        owner = jnp.sum(
            jnp.where(slot[:, None] == block_ids[None, :], block_order[None, :], 0), axis=1
        )
        return owner * tok_rows + rows_index % tok_rows

    def pair_parts(first_pos, second_pos):
        dist = first_pos[:, None] - second_pos[None, :]
        steps = (dist[:, :, None] >= starts[None, None, :]).astype(jnp.float32)
        return (steps, dist >= 0)

    def causal_parts(key_start, count):
        return pair_parts(query_pos, position_of(key_start + jnp.arange(count, dtype=jnp.int32)))

    normed_one = rms_scale(layer_in, norm_gains[0]).astype(low)
    queries = times(normed_one, query_full).astype(low)
    keys_own = times(normed_one, key_full).astype(low)
    values_own = times(normed_one, value_full).astype(low)
    memory_keys = times(encoded, lookup_full).astype(low)
    memory_values = times(encoded, recall_full).astype(low)
    total_width = queries.shape[1]
    width = total_width // head_count
    start_state = (
        jnp.zeros((head_count, tok_rows, width), jnp.float32),
        jnp.full((head_count, tok_rows), NEG, jnp.float32),
        jnp.zeros((head_count, tok_rows), jnp.float32),
    )
    self_fold = attend_fold(queries, head_count, causal_parts, position_bias)
    self_state = self_fold(
        start_state,
        (
            lax.all_gather(keys_own, "ctx", axis=0, tiled=True),
            lax.all_gather(values_own, "ctx", axis=0, tiled=True),
        ),
        jnp.int32(0),
    )
    mixed_one, lse_one = finish(self_state)
    after_self = layer_in + join_heads(times(mixed_one, output_full))
    normed_two = rms_scale(after_self, norm_gains[1]).astype(low)
    probes = times(normed_two, probe_full).astype(low)
    cross_fold = attend_fold(probes, head_count, None, position_bias)
    cross_state = cross_fold(
        start_state,
        (
            lax.all_gather(memory_keys, "ctx", axis=0, tiled=True),
            lax.all_gather(memory_values, "ctx", axis=0, tiled=True),
        ),
        jnp.int32(0),
    )
    mixed_two, lse_two = finish(cross_state)
    after_cross = after_self + join_heads(times(mixed_two, merge_full))
    normed_three = rms_scale(after_cross, norm_gains[2]).astype(low)
    gate_pre = times(normed_three, gate_full)
    upper = times(normed_three, upward_full)
    activated = geglu(gate_pre, upper).astype(low)
    layer_out = after_cross + join_heads(times(activated, down_full))
    grad_rows = out_grad.astype(low)
    down_wgrad = left_times(activated, grad_rows)
    act_grad = right_times(grad_rows, down_full)
    geglu_out, geglu_pull = jax.vjp(geglu, gate_pre, upper)
    gate_grad, upper_grad = geglu_pull(act_grad)
    gate_grad = gate_grad.astype(low)
    upper_grad = upper_grad.astype(low)
    gate_wgrad = left_times(normed_three, gate_grad)
    up_wgrad = left_times(normed_three, upper_grad)
    normed_three_grad = join_heads(
        right_times(gate_grad, gate_full) + right_times(upper_grad, upward_full)
    )
    norm_out, norm_pull = jax.vjp(rms_scale, after_cross, norm_gains[2])
    cross_extra, gain_three = norm_pull(normed_three_grad)
    cross_grad = out_grad + cross_extra
    cross_rows = cross_grad.astype(low)
    merge_wgrad = left_times(mixed_two, cross_rows)
    mixed_two_grad = right_times(cross_rows, merge_full).astype(low)
    delta_two = delta_of(mixed_two, mixed_two_grad, head_count)
    memory_all = gather_cross(memory_keys, memory_values)
    probe_grad, unused_bias, cross_terms = attend_back(
        probes,
        mixed_two_grad,
        lse_two,
        delta_two,
        memory_all[0],
        memory_all[1],
        head_count,
        None,
        position_bias,
    )
    cross_terms = lax.psum_scatter(cross_terms, "ctx", scatter_dimension=0, tiled=True)
    memory_key_grad = cross_terms[:, :total_width].astype(low)
    memory_value_grad = cross_terms[:, total_width:].astype(low)
    probe_wgrad = left_times(normed_two, probe_grad)
    lookup_wgrad = left_times(encoded, memory_key_grad)
    recall_wgrad = left_times(encoded, memory_value_grad)
    normed_two_grad, encoded_grad = join_heads(
        (
            right_times(probe_grad, probe_full),
            right_times(memory_key_grad, lookup_full) + right_times(memory_value_grad, recall_full),
        )
    )
    norm_out, norm_pull = jax.vjp(rms_scale, after_self, norm_gains[1])
    self_extra, gain_two = norm_pull(normed_two_grad)
    self_grad = cross_grad + self_extra
    self_rows = self_grad.astype(low)
    output_wgrad = left_times(mixed_one, self_rows)
    mixed_one_grad = right_times(self_rows, output_full).astype(low)
    delta_one = delta_of(mixed_one, mixed_one_grad, head_count)
    sequence_all = gather_self(keys_own, values_own)
    query_grad, bias_grad, self_terms = attend_back(
        queries,
        mixed_one_grad,
        lse_one,
        delta_one,
        sequence_all[0],
        sequence_all[1],
        head_count,
        causal_parts,
        position_bias,
    )
    self_terms = lax.psum_scatter(self_terms, "ctx", scatter_dimension=0, tiled=True)
    key_grad = self_terms[:, :total_width].astype(low)
    value_grad = self_terms[:, total_width:].astype(low)
    query_wgrad = left_times(normed_one, query_grad)
    key_wgrad = left_times(normed_one, key_grad)
    value_wgrad = left_times(normed_one, value_grad)
    normed_one_grad = join_heads(
        right_times(query_grad, query_full)
        + right_times(key_grad, key_full)
        + right_times(value_grad, value_full)
    )
    norm_out, norm_pull = jax.vjp(rms_scale, layer_in, norm_gains[0])
    input_extra, gain_one = norm_pull(normed_one_grad)
    input_grad = self_grad + input_extra
    weight_sums = (
        lax.psum_scatter(query_wgrad, "ctx", scatter_dimension=0, tiled=True),
        lax.psum_scatter(key_wgrad, "ctx", scatter_dimension=0, tiled=True),
        lax.psum_scatter(value_wgrad, "ctx", scatter_dimension=0, tiled=True),
        lax.psum_scatter(output_wgrad, "ctx", scatter_dimension=1, tiled=True),
        lax.psum_scatter(probe_wgrad, "ctx", scatter_dimension=0, tiled=True),
        lax.psum_scatter(lookup_wgrad, "ctx", scatter_dimension=0, tiled=True),
        lax.psum_scatter(recall_wgrad, "ctx", scatter_dimension=0, tiled=True),
        lax.psum_scatter(merge_wgrad, "ctx", scatter_dimension=1, tiled=True),
        lax.psum_scatter(gate_wgrad, "ctx", scatter_dimension=0, tiled=True),
        lax.psum_scatter(up_wgrad, "ctx", scatter_dimension=0, tiled=True),
        lax.psum_scatter(down_wgrad, "ctx", scatter_dimension=1, tiled=True),
    )
    gains_sum, bias_sum = lax.psum((jnp.stack((gain_one, gain_two, gain_three)), bias_grad), "ctx")
    return (layer_out, input_grad, encoded_grad) + tuple(weight_sums) + (gains_sum, bias_sum)


def solution(mesh):
    body = quick_device if quick_fits(mesh) else per_device
    placed = (
        P("ctx", None),
        P("ctx", None),
        P("ctx", "head"),
        P("ctx", "head"),
        P("ctx", "head"),
        P("head", "ctx"),
        P("ctx", "head"),
        P("ctx", "head"),
        P("ctx", "head"),
        P("head", "ctx"),
        P("ctx", "head"),
        P("ctx", "head"),
        P("head", "ctx"),
        P(),
        P(None, "head"),
        P(),
        P(),
        P("ctx", None),
    )
    return jax.shard_map(
        body,
        mesh=mesh,
        in_specs=placed,
        out_specs=(
            P("ctx", None),
            P("ctx", None),
            P("ctx", None),
            P("ctx", "head"),
            P("ctx", "head"),
            P("ctx", "head"),
            P("head", "ctx"),
            P("ctx", "head"),
            P("ctx", "head"),
            P("ctx", "head"),
            P("head", "ctx"),
            P("ctx", "head"),
            P("ctx", "head"),
            P("head", "ctx"),
            P(),
            P(None, "head"),
        ),
        check_vma=False,
    )
```

```python
import functools
import math

import jax
import jax.numpy as jnp
from jax import lax
from jax.experimental import pallas as pl
from jax.experimental.pallas import tpu as pltpu
from jax.sharding import PartitionSpec as P

EPS = 1e-06
NEG = -1e30
HIGH = lax.Precision.HIGHEST
LOW = jnp.bfloat16
F32 = jnp.float32
MESH = pl.DeviceIdType.MESH
VMEM_LIMIT = 66_000_000


def dot(left, right, **kw):
    return jnp.dot(left, right, preferred_element_type=F32, **kw)


def dot_nt(left, right, **kw):
    return lax.dot_general(left, right, (((1,), (1,)), ((), ())), preferred_element_type=F32, **kw)


def dot_tn(left, right, **kw):
    return lax.dot_general(left, right, (((0,), (0,)), ((), ())), preferred_element_type=F32, **kw)


def rms_forward(rows, gain):
    return rows * lax.rsqrt(jnp.mean(rows * rows, axis=-1, keepdims=True) + EPS) * gain


def rms_backward(rows, gain, grad):
    scale = lax.rsqrt(jnp.mean(rows * rows, axis=-1, keepdims=True) + EPS)
    scaled = gain * grad
    inner = jnp.mean(scaled * rows, axis=-1, keepdims=True)
    row_grad = scale * scaled - rows * (scale * scale * scale * inner)
    gain_grad = jnp.sum(grad * rows * scale, axis=0, keepdims=True)
    return row_grad, gain_grad


def aligned(value, step):
    return value if isinstance(value, int) else pl.multiple_of(value, step)


class Place:
    def __init__(self, count):
        self.count = count
        self.here = lax.axis_index("ctx")
        self.core = lax.axis_index("head")
        self.other = 1 - self.core
        self.plane = lax.rem(self.here, 4)
        self.level = self.here // 4
        self.fx = self.flip(self.here, 0)
        self.fy = self.flip(self.here, 1)
        self.fxy = self.flip(self.fx, 1)
        self.above = [lax.rem(self.here + 4 * k, count) for k in range(4)]
        self.below = [lax.rem(self.here + count - 4 * k, count) for k in range(4)]
        self.top = count // 4 - 1
        bottom, head = self.level == 0, self.level == self.top
        self.nearest = (
            jnp.where(bottom, 3, 1),
            jnp.where(bottom, 2, jnp.where(head, 2, 3)),
            jnp.where(bottom, 1, jnp.where(head, 3, 2)),
        )

    def flip(self, index, axis):
        if axis == 0:
            return index + 1 - 2 * lax.rem(index, 2)
        return index + 2 - 4 * lax.rem(index // 2, 2)

    def near(self, half):
        return (self.fx, self.fy) if half == 0 else (self.fy, self.fx)

    def signal(self, chips):
        barrier = pltpu.get_barrier_semaphore()
        for chip in chips:
            pl.semaphore_signal(
                barrier, inc=1, device_id=(chip, self.core), device_id_type=MESH
            )
        pl.semaphore_signal(barrier, inc=1, device_id=(self.here, self.other), device_id_type=MESH)

    def meet(self, count):
        pl.semaphore_wait(pltpu.get_barrier_semaphore(), count)


class Wire:
    def __init__(self, place, send_sem, recv_sem):
        self.place, self.send_sem, self.recv_sem = place, send_sem, recv_sem
        self.used = 0
        self.send_used = 0
        self.pending = []

    def slots(self, count):
        base = self.used
        self.used += count
        assert self.used <= self.recv_sem.shape[0], self.used
        return base

    def sender(self, whole=None):
        slot = self.send_used
        self.send_used += 1
        assert slot < self.send_sem.shape[0], slot
        if whole is not None:
            self.pending.append((slot, whole))
        return slot

    def copy(self, src, dst, out, slot, chip, core):
        return pltpu.make_async_remote_copy(
            src_ref=src,
            dst_ref=dst,
            send_sem=self.send_sem.at[out],
            recv_sem=self.recv_sem.at[slot],
            device_id=(chip, core),
            device_id_type=MESH,
        )

    def send(self, src, dst, slot, chip=None, core=None, out=None):
        chip = self.place.here if chip is None else chip
        core = self.place.core if core is None else core
        if out is None:
            out = self.sender(src)
        self.copy(src, dst, out, slot, chip, core).start()

    def swap(self, src, dst, slot, out=None):
        self.send(src, dst, slot, None, self.place.other, out)

    def got(self, dst, slot):
        place = self.place
        self.copy(dst, dst, 0, slot, place.here, place.other).wait_recv()

    def sent(self, whole, out):
        place = self.place
        self.copy(whole, whole, out, 0, place.here, place.other).wait_send()

    def drain(self):
        for out, whole in self.pending:
            self.sent(whole, out)
        self.pending = []


class Gather:
    def __init__(self, wire, view, share, spare):
        self.wire, self.view, self.share, self.spare = wire, view, share, spare
        self.halves = range(2)
        self.base = [wire.slots(8) for _ in self.halves]
        self.out = [wire.sender(spare(half, 12)) for half in self.halves]
        self.line_out = [wire.sender() for _ in self.halves]
        if share:
            self.side = [wire.slots(1) for _ in self.halves]
            self.side_out = [wire.sender(spare(half, 15)) for half in self.halves]

    def _line(self, half, block, slot, chip):
        ref = self.view(half, block)
        self.wire.send(ref, ref, self.base[half] + slot, chip, out=self.line_out[half])

    def _out(self, half, block, slot, chip):
        ref = self.view(half, block)
        self.wire.send(ref, ref, self.base[half] + slot, chip, out=self.out[half])

    def _give(self, half, block):
        if self.share:
            ref = self.view(half, block)
            self.wire.swap(ref, ref, self.side[half], self.side_out[half])

    def start_level(self):
        place = self.wire.place
        for half in self.halves:

            @pl.when(place.level < place.top)
            def _():
                self._line(half, place.here, 0, place.here + 4)

            @pl.when(place.level > 0)
            def _():
                self._line(half, place.here, 2, place.here - 4)

    def start_plane(self):
        place = self.wire.place
        for half in self.halves:
            near, far = place.near(half)
            self._out(half, place.here, 3, near)
            self._out(half, place.here, 7, far)

    def _level_block(self, step):
        place = self.wire.place
        k = place.nearest[step]
        return k, lax.rem(place.here + place.count - 4 * k, place.count)

    def pass_line(self, step):
        place = self.wire.place
        k, block = self._level_block(step)
        rising = place.level >= k
        onward = jnp.where(rising, place.level < place.top, place.level > 0)
        chip = jnp.where(rising, place.here + 4, place.here - 4)
        slot = jnp.where(rising, k, k - 2)
        for half in self.halves:
            self.wire.got(self.view(half, block), self.base[half] + k - 1)

            @pl.when(onward)
            def _():
                self._line(half, block, slot, chip)

    def pass_plane(self, step):
        place = self.wire.place
        k, block = self._level_block(step)
        for half in self.halves:
            near, far = place.near(half)
            self._out(half, block, 3 + k, near)
            self._out(half, block, 7, far)
            self._give(half, block)

    def pass_near(self, step):
        place = self.wire.place
        k = (0, *place.nearest)[step]
        block = lax.rem(place.here + place.count - 4 * k, place.count)
        for half in self.halves:
            _, far = place.near(half)
            arrived = place.flip(block, half)
            self.wire.got(self.view(half, arrived), self.base[half] + 3 + k)
            self._out(half, arrived, 7, far)
            self._give(half, arrived)

    def finish(self):
        place = self.wire.place
        for half in self.halves:
            self.wire.got(self.spare(half, 8), self.base[half] + 7)
            if self.share:
                for k in range(4):
                    block = place.flip(place.below[k], 1 - half)
                    self._give(half, block)
                    self._give(half, place.flip(block, half))

    def finish_share(self):
        for half in self.halves:
            self.wire.got(self.spare(half, 15), self.side[half])

    def drain(self):
        place = self.wire.place
        for half in self.halves:

            @pl.when(jnp.logical_or(place.level == 0, place.level == place.top))
            def _():
                self.wire.sent(self.spare(half, 1), self.line_out[half])

            @pl.when(jnp.logical_and(place.level > 0, place.level < place.top))
            def _():
                self.wire.sent(self.spare(half, 5), self.line_out[half])


class Scatter:
    def __init__(self, wire, view, buf, out):
        self.wire, self.view, self.buf, self.out = wire, view, buf, out
        self.halves = range(2)
        self.base = [wire.slots(9) for _ in self.halves]
        self.send_slot = [wire.sender(buf(half)) for half in self.halves]

    def _send(self, half, block, place_in, slot, chip):
        self.wire.send(
            self.view(half, block),
            self.buf(half).at[place_in],
            self.base[half] + slot,
            chip,
            out=self.send_slot[half],
        )

    def start(self, k):
        place = self.wire.place
        for half in self.halves:
            _, far = place.near(half)
            away = place.flip(place.below[k], 1 - half)
            for pair, block in ((1, place.flip(away, half)), (0, away)):
                self._send(half, block, 2 * k + pair, k, far)

    def pass_near(self, k):
        place = self.wire.place
        for half in self.halves:
            near, _ = place.near(half)
            block = place.flip(place.below[k], half)
            pair = self.buf(half).at[2 * k : 2 * k + 2]
            self.wire.got(pair, self.base[half] + k)
            ref = self.view(half, block)
            ref[...] = (ref[...].astype(F32) + pair[1].astype(F32)).astype(LOW)
            self._send(half, block, 8 + k, 4 + k, near)

    def pass_level(self, k):
        place = self.wire.place
        for half in self.halves:
            ref = self.view(half, place.below[k])
            ref[...] = self._sum(half, k).astype(LOW)
            self._send(half, place.below[k], 11 + k, 8, place.below[k])

    def _sum(self, half, k):
        place, buf = self.wire.place, self.buf(half)
        self.wire.got(buf.at[8 + k], self.base[half] + 4 + k)
        total = self.view(half, place.below[k])[...].astype(F32)
        return total + buf[2 * k].astype(F32) + buf[8 + k].astype(F32)

    def finish(self):
        for half in self.halves:
            buf = self.buf(half)
            total = self._sum(half, 0)
            self.wire.got(buf.at[12:15], self.base[half] + 8)
            for k in (1, 2, 3):
                total = total + buf[11 + k].astype(F32)
            self.out(half, total)


def lane_split(rows):
    lane = lax.broadcasted_iota(jnp.int32, rows.shape, 1)
    low = lane < rows.shape[1] // 2
    zero = jnp.zeros_like(rows)
    return jnp.concatenate((jnp.where(low, rows, zero), jnp.where(low, zero, rows)), axis=0)


def lane_join(rows):
    count, width = rows.shape[0] // 2, rows.shape[1]
    lane = lax.broadcasted_iota(jnp.int32, (count, width), 1)
    return jnp.where(lane < width // 2, rows[:count], rows[count:])


def pair_attend(tok, pairs, chunk, q_ref, kv_ref, s_ref, e_ref, rl_ref, mixed_ref, bias_ref, between):
    keys = kv_ref.shape[0]
    total = pairs * 128

    for j in range(pairs):
        cols = slice(j * 128, (j + 1) * 128)
        vcols = slice(total + j * 128, total + (j + 1) * 128)
        q_cat = lane_split(q_ref[:, cols])

        def score(c, top):
            rows = pl.ds(aligned(c * chunk, chunk), chunk)
            s = dot_nt(q_cat, kv_ref[rows, cols])
            if bias_ref is not None:
                tiles = []
                for half in range(2):
                    row = []
                    for b in range(chunk // tok):
                        lanes = pl.ds(aligned((c * (chunk // tok) + b) * 2 * tok, 128), 2 * tok)
                        vec = bias_ref[2 * j + half : 2 * j + half + 1, lanes]
                        wide = jnp.broadcast_to(vec, (tok, 2 * tok))
                        row.append(pltpu.roll(wide, 0, 1, stride=1, stride_axis=0)[:, :tok])
                    tiles.append(jnp.concatenate(row, axis=1))
                s = s + jnp.concatenate(tiles, axis=0)
            s_ref[:, rows] = s
            for b in range(chunk // 128):
                top = jnp.maximum(top, s[:, b * 128 : (b + 1) * 128])
            return top

        top = lax.fori_loop(0, keys // chunk, score, jnp.full((2 * tok, 128), NEG, F32))
        peak = jnp.max(top, axis=1, keepdims=True)

        def weigh(c, state):
            acc, run = state
            rows = pl.ds(aligned(c * chunk, chunk), chunk)
            e = jnp.exp(s_ref[:, rows] - peak)
            for b in range(chunk // 128):
                run = run + e[:, b * 128 : (b + 1) * 128]
            low = e.astype(LOW)
            e_ref[j, :, rows] = low
            return (acc + dot(low, kv_ref[rows, vcols]), run)

        zero = jnp.zeros((2 * tok, 128), F32)
        acc, run = lax.fori_loop(0, keys // chunk, weigh, (zero, zero))
        rl = 1.0 / jnp.sum(run, axis=1, keepdims=True)
        rl_ref[j] = rl
        mixed_ref[:, cols] = lane_join(acc * rl).astype(LOW)
        between(j)


class PairBack:
    def __init__(self, tok, pairs, q, kv, e, rl, mixed, grad, kv_grad, diag, qc, gc, dl, dq):
        self.tok, self.pairs, self.kv, self.e = tok, pairs, kv, e
        self.kv_grad, self.diag, self.qc, self.gc, self.dl, self.dq = kv_grad, diag, qc, gc, dl, dq
        self.total = pairs * 128
        for j in range(pairs):
            cols = slice(j * 128, (j + 1) * 128)
            rl_j = rl[j]
            grads = lane_split(grad[:, cols].astype(F32))
            qc[j] = lane_split(q[:, cols])
            gc[j] = (grads * rl_j).astype(LOW)
            values = lane_split(mixed[:, cols].astype(F32))
            dl[j] = jnp.sum(grads * values, axis=1, keepdims=True) * rl_j
            dq[j] = jnp.zeros(dq.shape[1:], F32)

    def chunk(self, start, count):
        tok, kv, qc, gc = self.tok, self.kv, self.qc, self.gc
        rows = pl.ds(aligned(start, count), count)
        flip = (
            lax.broadcasted_iota(jnp.int32, (tok, tok), 0)
            + lax.broadcasted_iota(jnp.int32, (tok, tok), 1)
            == tok - 1
        ).astype(LOW)

        def one_pair(j, carry):
            cols = pl.ds(aligned(j * 128, 128), 128)
            vcols = pl.ds(aligned(self.total + j * 128, 128), 128)
            low_e = self.e[j, :, rows]
            dp = dot_nt(gc[j], kv[rows, vcols])
            ds = (low_e.astype(F32) * (dp - self.dl[j])).astype(LOW)
            if self.diag is not None:
                for half in range(2):
                    turned = dot(flip, ds[half * tok : (half + 1) * tok])
                    for b in range(count // tok):
                        tile = turned[:, b * tok : (b + 1) * tok]
                        wide = jnp.concatenate((tile, jnp.zeros_like(tile)), axis=1)
                        wide = pltpu.roll(wide, tok + 1, 1, stride=1, stride_axis=0)
                        lanes = pl.ds(aligned(2 * start + b * 2 * tok, 128), 2 * tok)
                        self.diag[pl.ds(2 * j + half, 1), lanes] = jnp.sum(
                            wide, axis=0, keepdims=True
                        )
            self.kv_grad[rows, cols] = dot_tn(ds, qc[j]).astype(LOW)
            self.kv_grad[rows, vcols] = dot_tn(low_e, gc[j]).astype(LOW)
            self.dq[j] = self.dq[j] + dot(ds, kv[rows, cols])
            return carry

        lax.fori_loop(0, self.pairs, one_pair, 0)

    def finish(self, q_grad):
        for j in range(self.pairs):
            q_grad[:, j * 128 : (j + 1) * 128] = lane_join(self.dq[j]).astype(LOW)


def bucket_rows(buckets_ref, order_ref, here, table_rows, ids_ref):
    count, tok = buckets_ref.shape
    turn = (
        lax.broadcasted_iota(jnp.int32, (tok, tok), 0)
        + lax.broadcasted_iota(jnp.int32, (tok, tok), 1)
        == tok - 1
    ).astype(LOW)
    table_rows[:count, :] = jnp.full((count, tok), -1.0, F32)
    table_rows[count:, :] = dot(buckets_ref[...].astype(LOW), turn)
    own = order_ref[here]
    for block in range(count):
        at = own - order_ref[block] + count
        wide = jnp.concatenate(
            (table_rows[pl.ds(at - 1, 1), :], table_rows[pl.ds(at, 1), :]), axis=1
        )
        ids_ref[:, block * 2 * tok : (block + 1) * 2 * tok] = pltpu.roll(wide, 1, 1)


def bucket_masks(ids_ref, buckets):
    ids = ids_ref[...]
    row = lax.broadcasted_iota(jnp.int32, (buckets, ids.shape[1]), 0).astype(F32)
    return ids, (row == ids).astype(F32)


def bias_vectors(ids_ref, table_ref, bias_ref):
    heads, buckets = table_ref.shape
    ids, mask = bucket_masks(ids_ref, buckets)
    vec = dot(table_ref[...], mask, precision=HIGH)
    bias_ref[:heads, :] = jnp.where(ids >= 0, vec, NEG)


def bucket_sums(ids_ref, diag_ref, buckets):
    _, mask = bucket_masks(ids_ref, buckets)
    return dot_nt(diag_ref[...], mask, precision=HIGH)


def rows_loop(count, step, body):
    def one(index, carry):
        body(pl.ds(aligned(index * step, step), step))
        return carry

    lax.fori_loop(0, count // step, one, 0)


GELU_A = 0.7978845608028654
GELU_B = 0.044715


def gelu_parts(value):
    square = value * value
    wave = jnp.tanh(GELU_A * (value + GELU_B * value * square))
    half = 0.5 * (1.0 + wave)
    slope = half + 0.5 * value * (1.0 - wave * wave) * (GELU_A * (1.0 + 3.0 * GELU_B * square))
    return value * half, slope


def core_sum(wire, part, out_buf, in_buf):
    slot = wire.slots(1)
    out_buf[...] = part.astype(LOW)
    wire.swap(out_buf, in_buf, slot)
    wire.got(in_buf, slot)
    return out_buf[...].astype(F32) + in_buf[...].astype(F32)


class PlaneSum:
    def __init__(self, wire, tok, part, core_buf, plane_buf, whole):
        self.wire, self.tok = wire, tok
        self.out = wire.sender(part)
        self.part, self.core_buf, self.plane_buf, self.whole = part, core_buf, plane_buf, whole
        self.base = wire.slots(8)
        self.half = whole.shape[1] // 2
        place = wire.place
        self.chips = (place.here, place.fx, place.fy, place.fxy)

    def cols(self, core):
        return pl.ds(aligned(core * self.half, 128), self.half)

    def rows(self, k):
        return pl.ds(aligned(lax.rem(self.chips[k], 4) * self.tok, self.tok), self.tok)

    def start(self, k):
        away = self.cols(self.wire.place.other)
        rows = self.rows(k)
        self.wire.swap(self.part.at[rows, away], self.core_buf.at[rows, :], self.base + k, self.out)

    def middle(self, k):
        wire, rows = self.wire, self.rows(k)
        wire.got(self.core_buf.at[rows, :], self.base + k)
        total = self.part[rows, self.cols(wire.place.core)].astype(F32)
        total = total + self.core_buf[rows, :].astype(F32)
        self.core_buf[rows, :] = total.astype(LOW)
        if k:
            wire.send(
                self.core_buf.at[rows, :],
                self.plane_buf.at[k - 1],
                self.base + 3 + k,
                self.chips[k],
                out=self.out,
            )

    def finish(self):
        place, wire = self.wire.place, self.wire
        total = self.core_buf[self.rows(0), :].astype(F32)
        for k in (1, 2, 3):
            wire.got(self.plane_buf.at[k - 1], self.base + 3 + k)
            total = total + self.plane_buf[k - 1].astype(F32)
        mine = self.cols(place.core)
        self.whole[:, mine] = total.astype(LOW)
        wire.swap(self.whole.at[:, mine], self.whole.at[:, mine], self.base + 7, self.out)

    def finish_core(self):
        self.wire.got(self.whole.at[:, self.cols(self.wire.place.other)], self.base + 7)


class PlaneGather:
    def __init__(self, wire, tok, ref):
        self.wire, self.tok, self.ref = wire, tok, ref
        self.half = ref.shape[1] // 2
        self.base = wire.slots(8)
        self.out = wire.sender(ref.at[: 3 * tok, :])
        place = wire.place
        self.chips = (place.here, place.fx, place.fy, place.fxy)

    def view(self, k, core):
        rows = pl.ds(aligned(lax.rem(self.chips[k], 4) * self.tok, self.tok), self.tok)
        return self.ref.at[rows, pl.ds(aligned(core * self.half, 128), self.half)]

    def start(self):
        own = self.view(0, self.wire.place.core)
        for k in (3, 1, 2):
            self.wire.send(own, own, self.base + k, self.chips[k], out=self.out)

    def share(self, k):
        ref = self.view(k, self.wire.place.core)
        self.wire.got(ref, self.base + k)
        self.wire.swap(ref, ref, self.base + 4 + k, self.out)

    def finish(self, k):
        self.wire.got(self.view(k, self.wire.place.other), self.base + 4 + k)


class Sizes:
    def __init__(self, ctx, tok, enc, model, wide, units):
        self.ctx, self.tok, self.enc, self.model, self.wide = ctx, tok, enc, model, wide
        self.rows = model // ctx
        self.units = units
        self.quarter = units // 4
        self.pairs = wide // 128
        self.levels = ctx // 4
        self.attn_cols = 8 * wide
        self.mlp_cols = 3 * units
        self.part = 3 * self.quarter
        self.names = ("q", "k", "v", "cq", "ck", "cv", "o", "co")
        self.col = {n: slice(i * wide, (i + 1) * wide) for i, n in enumerate(self.names)}
        self.col["kv"] = slice(wide, 3 * wide)
        self.col["ckv"] = slice(4 * wide, 6 * wide)
        self.cuts = {
            "s": self.halves(0, 3 * wide, 0),
            "c": self.halves(3 * wide, 6 * wide, 1),
            "o": self.halves(6 * wide, 7 * wide, 0),
            "co": self.halves(7 * wide, 8 * wide, 1),
        }

    def halves(self, first, last, up):
        tiles = (last - first) // 128
        middle = first + (tiles + up) // 2 * 128
        return ((first, middle), (middle, last))


def named(kernel, names):
    def body(*refs):
        kernel(**dict(zip(names, refs, strict=True)))

    return body


def wire_sems(send, recv):
    return {
        "send_sem": pltpu.SemaphoreType.DMA((send,)),
        "recv_sem": pltpu.SemaphoreType.DMA((recv,)),
    }


def layer_kernel(
    size, layer_in, encoded, sq, sk, sv, so, cq, ck, cv, co, gate_w, up_w, down_w, gains,
    table, buckets, order, out_grad,
    layer_out, input_grad, enc_grad, WG, mb, totals, bias_totals,
    WA, WM, wm, X, E, GR, PW, PM,
    q, kv, mkv, probes, s, e1, e2, rl1, rl2, mixed1, mixed2, table_rows, ids, bias, diag,
    after_self, after_cross, cross_grad, self_grad, n2, N3, act, GU, PN, PO, low, mixed_grad,
    q_grad, kv_grad, mkv_grad, ca, cb, pn_core, pn_plane, pn_whole, po_core, po_plane, po_whole,
    qc, gc, dl, dq, bs0, bs1, bc0, bc1, bo0, bo1, bp0, bp1, bx, be, px, pe, NG, NE, ml, ps,
    s1, s2, sr, sl, t1, t2, tr, tl, send_sem, recv_sem,
):
    place = Place(size.ctx)
    wire = Wire(place, send_sem, recv_sem)
    tok, enc, rows, half_d = size.tok, size.enc, size.rows, size.model // 2
    col, model, quarter = size.col, size.model, size.quarter
    ctx_tok, ctx_enc = X.shape[0], E.shape[0]
    plane_chips = (place.fx, place.fy, place.fxy)
    XG, EG = kv, mkv

    def block_rows(block, count):
        return pl.ds(aligned(block * count, 16), count)

    here_rows = block_rows(place.here, tok)
    own_weights = block_rows(place.here, rows)
    my_part = pl.ds(aligned(place.plane * size.part, 128), size.part)
    mine = pl.ds(aligned(place.core * half_d, 128), half_d)
    away = pl.ds(aligned(place.other * half_d, 128), half_d)

    def token_view(ref, count, core):
        def view(half, block):
            return ref.at[
                pl.ds(aligned(block * count + half * (count // 2), 16), count // 2),
                pl.ds(aligned(core * half_d, 128), half_d),
            ]

        return view

    def weight_view(ref, name):
        def view(half, block):
            first, last = size.cuts[name][half]
            return ref.at[block_rows(block, rows), first:last]

        return view

    def token_spare(buf):
        return lambda half, count: buf.at[half, 0:count]

    def weight_spare(*bufs):
        return lambda half, count: bufs[half].at[0:count]

    def token_gather(ref, count, buf):
        return Gather(
            wire,
            token_view(ref, count, place.core),
            True,
            token_spare(buf),
        )

    gx, ge = token_gather(X, tok, bx), token_gather(E, enc, be)
    gs, gc_, go, gp = (
        Gather(wire, weight_view(WA, name), False, weight_spare(*bufs))
        for name, bufs in (("s", (bs0, bs1)), ("c", (bc0, bc1)), ("o", (bo0, bo1)), ("co", (bp0, bp1)))
    )
    gg = PlaneGather(wire, tok, GR)
    spread = PlaneGather(wire, tok, N3)
    sum_n = PlaneSum(wire, tok, PN, pn_core, pn_plane, pn_whole)
    sum_o = PlaneSum(wire, tok, PO, po_core, po_plane, po_whole)
    mg_plane, mg_level, ms_level, ms_plane = (wire.slots(3) for _ in range(4))

    def units_out():
        for k, chip in enumerate(plane_chips):
            wire.send(
                wm.at[:, pl.ds(aligned(lax.rem(chip, 4) * size.part, 128), size.part)],
                WM.at[own_weights, :],
                mg_plane + k,
                chip,
            )

    def units_up():
        for k, chip in enumerate(plane_chips):
            wire.got(WM.at[block_rows(chip, rows), :], mg_plane + k)
        own = WM.at[block_rows(place.level, 4 * rows), :]
        for k in (1, 2, 3):
            wire.send(own, own, mg_level + k - 1, place.above[k])

    place.signal(place.above[1:] + list(plane_chips))
    X[here_rows, :] = rms_forward(layer_in[...], gains[0:1]).astype(LOW)
    for name, ref in zip(("q", "k", "v", "cq", "ck", "cv", "o", "co"), (sq, sk, sv, cq, ck, cv, so, co)):
        WA[own_weights, col[name]] = ref[...]
    E[block_rows(place.here, enc), :] = encoded[...]
    plane_rows = block_rows(place.plane, tok)
    GR[plane_rows, :] = out_grad[...].astype(LOW)
    for p in range(4):
        cols = slice(p * quarter, (p + 1) * quarter)
        for i, ref in enumerate((gate_w, up_w, down_w)):
            base = p * size.part + i * quarter
            wm[:, base : base + quarter] = ref[:, cols]
    WM[own_weights, :] = wm[:, my_part]
    place.meet(7)
    gx.start_level()
    gs.start_level()
    gx.start_plane()
    gs.start_plane()
    gx.pass_near(0)
    gx.pass_line(0)
    gx.pass_plane(0)
    gs.pass_near(0)
    gs.pass_line(0)
    gs.pass_plane(0)
    gx.pass_line(1)
    gx.pass_plane(1)
    gs.pass_line(1)
    gs.pass_plane(1)
    go.start_level()
    ge.start_level()
    gx.pass_near(1)
    gs.pass_near(1)
    gx.pass_line(2)
    gx.pass_plane(2)
    gs.pass_line(2)
    gs.pass_plane(2)
    gc_.start_level()
    gp.start_level()
    gx.pass_near(2)
    gs.pass_near(2)
    gx.pass_near(3)
    gs.pass_near(3)
    go.start_plane()
    ge.start_plane()
    gc_.start_plane()
    units_out()
    bucket_rows(buckets, order, place.here, table_rows, ids)
    bias_vectors(ids, table, bias)
    diag[...] = jnp.zeros_like(diag)
    go.pass_line(0)
    go.pass_plane(0)
    ge.pass_line(0)
    ge.pass_plane(0)
    gc_.pass_line(0)
    gp.pass_line(0)
    go.pass_line(1)
    go.pass_plane(1)
    ge.pass_line(1)
    ge.pass_plane(1)
    gc_.pass_line(1)
    gp.pass_line(1)
    go.pass_line(2)
    go.pass_plane(2)
    ge.pass_line(2)
    ge.pass_plane(2)
    gc_.pass_line(2)
    gp.pass_line(2)
    gc_.pass_plane(0)
    gc_.pass_plane(1)
    gc_.pass_plane(2)
    gx.finish()
    go.pass_near(0)
    ge.pass_near(0)
    gx.finish_share()
    gs.finish()
    units_up()

    def project(rows_):
        kv[rows_, :] = dot(X[rows_, :], WA[:, col["kv"]]).astype(LOW)

    def project_enc(rows_):
        mkv[rows_, :] = dot(E[rows_, :], WA[:, col["ckv"]]).astype(LOW)

    def project_level(level):
        for part_ in range(2):
            project(slice((2 * level + part_) * 2 * tok, (2 * level + part_ + 1) * 2 * tok))

    q[...] = dot(X[here_rows, :], WA[:, col["q"]]).astype(LOW)
    project_level(0)
    project_level(1)
    project_level(2)
    project_level(3)
    go.pass_near(1)
    go.pass_near(2)
    go.pass_near(3)
    ge.pass_near(1)
    ge.pass_near(2)
    ge.pass_near(3)

    def during_self(j):
        if j == 0:
            gc_.pass_near(0)
            gc_.pass_near(1)
        elif j == 1:
            gc_.pass_near(2)
            gc_.pass_near(3)
            gp.start_plane()
            gp.pass_plane(0)
            gp.pass_plane(1)
            gp.pass_plane(2)
        elif j == 2:
            gg.start()
            go.finish()

    pair_attend(tok, size.pairs, 512, q, kv, s, e1, rl1, mixed1, bias, during_self)
    part = dot_nt(mixed1[...], WA[:, col["o"]])
    after_self[...] = layer_in[...] + core_sum(wire, part, ca.at[0], cb.at[0])
    n2[...] = rms_forward(after_self[...], gains[1:2]).astype(LOW)
    ge.finish()
    ge.finish_share()
    gc_.finish()

    rows_loop(ctx_enc, 256, project_enc)
    probes[...] = dot(n2[...], WA[:, col["cq"]]).astype(LOW)

    def during_cross(j):
        if j == 0:
            gp.pass_near(0)
            gp.pass_near(1)
            gp.pass_near(2)
            gp.pass_near(3)
        elif j == 1:
            for k in (1, 2, 3):
                gg.share(k)

    pair_attend(tok, size.pairs, 512, probes, mkv, s, e2, rl2, mixed2, None, during_cross)
    gp.finish()
    part = dot_nt(mixed2[...], WA[:, col["co"]])
    after_cross[...] = after_self[...] + core_sum(wire, part, ca.at[1], cb.at[1])

    N3[plane_rows, :] = rms_forward(after_cross[...], gains[2:3]).astype(LOW)
    spread.start()
    for k in (1, 2, 3):
        level = place.below[k] // 4
        wire.got(WM.at[block_rows(level, 4 * rows), :], mg_level + k - 1)

    def units(k):
        rows_ = spread_rows(k)
        pre = dot(N3[rows_, :], WM[:, : 2 * quarter])
        gate, upper = pre[:, :quarter], pre[:, quarter:]
        value, slope = gelu_parts(gate)
        act[rows_, :] = (value * upper).astype(LOW)
        grad = dot(GR[rows_, :], WM[:, 2 * quarter :])
        GU[rows_, :quarter] = (grad * upper * slope).astype(LOW)
        GU[rows_, quarter:] = (grad * value).astype(LOW)
        PN[rows_, :] = dot_nt(GU[rows_, :], WM[:, : 2 * quarter]).astype(LOW)

    def spread_rows(k):
        return sum_n.rows(k)

    units(0)
    sum_n.start(0)
    spread.share(1)
    spread.share(3)
    spread.share(2)
    gg.finish(3)
    spread.finish(3)
    units(3)
    sum_n.start(3)
    gg.finish(1)
    spread.finish(1)
    units(1)
    sum_n.start(1)
    sum_n.middle(3)
    gg.finish(2)
    spread.finish(2)
    units(2)
    sum_n.start(2)
    sum_n.middle(1)

    def back_out(k):
        rows_ = spread_rows(k)
        PO[rows_, :] = dot_nt(act[rows_, :], WM[:, 2 * quarter :]).astype(LOW)

    def unit_grads(cols):
        PM[cols, : 2 * quarter] = dot_tn(N3[:, cols], GU[...]).astype(LOW)
        PM[cols, 2 * quarter :] = dot_tn(GR[:, cols], act[...]).astype(LOW)

    back_out(0)
    sum_n.middle(2)
    sum_n.middle(0)
    rows_loop(model, 128, unit_grads)
    for k in (1, 2, 3):
        wire.send(
            PM.at[block_rows(place.above[k] // 4, 4 * rows), :],
            ml.at[k - 1],
            ms_level + k - 1,
            place.above[k],
        )
    sum_n.finish()
    for k in (1, 2, 3):
        back_out(k)
    for k in range(4):
        sum_o.start(k)
    sum_n.finish_core()
    extra, gain_three = rms_backward(after_cross[...], gains[2:3], pn_whole[...].astype(F32))
    cross_grad[...] = out_grad[...] + extra
    low[...] = cross_grad[...].astype(LOW)
    mixed_grad[...] = dot(low[...], WA[:, col["co"]]).astype(LOW)
    def out_grads(left, right, target):
        def body(cols):
            PW[cols, target] = dot_tn(left[:, cols], right[...]).astype(LOW)

        rows_loop(model, 128, body)

    def weight_stream(name, *bufs):
        def out(half, total):
            first, last = size.cuts[name][half]
            WG[:, first:last] = total

        return Scatter(wire, weight_view(PW, name), lambda half: bufs[half], out)

    def token_out(ref, count):
        def out(half, total):
            ref[half * (count // 2) : (half + 1) * (count // 2), mine] = total

        return out

    sp = weight_stream("co", bp0, bp1)
    so_ = weight_stream("o", bo0, bo1)
    sc = weight_stream("c", bc0, bc1)
    sw = weight_stream("s", bs0, bs1)
    sx = Scatter(wire, token_view(XG, tok, place.core), lambda half: bx.at[half], token_out(NG, tok))
    se = Scatter(wire, token_view(EG, enc, place.core), lambda half: be.at[half], token_out(NE, enc))
    x_base, e_base = wire.slots(4), wire.slots(4)
    x_out, e_out = wire.sender(px), wire.sender(pe)

    def pair_start(ref, recv, count, base, k, out):
        at = block_rows(place.below[k] // 4, 4 * count)
        wire.swap(ref.at[at, away], recv.at[at, :], base + k, out)

    def pair_ready(ref, recv, count, base, k):
        at = block_rows(place.below[k] // 4, 4 * count)
        wire.got(recv.at[at, :], base + k)
        ref[at, mine] = (ref[at, mine].astype(F32) + recv[at, :].astype(F32)).astype(LOW)

    x_slot, e_slot, cross_slot, small = (wire.slots(n) for n in (1, 1, 1, 10))

    def units_down():
        total = PM[block_rows(place.level, 4 * rows), :].astype(F32)
        for k in (1, 2, 3):
            wire.got(ml.at[k - 1], ms_level + k - 1)
            total = total + ml[k - 1].astype(F32)
        ps[...] = total.astype(LOW)
        for k, chip in enumerate(plane_chips):
            wire.send(
                ps.at[block_rows(lax.rem(chip, 4), rows), :], mb.at[:, my_part], ms_plane + k, chip
            )
        mb[:, my_part] = ps[block_rows(place.plane, rows), :]

    def units_back():
        for k, chip in enumerate(plane_chips):
            cols = pl.ds(aligned(lax.rem(chip, 4) * size.part, 128), size.part)
            wire.got(mb.at[:, cols], ms_plane + k)

    def result_out():
        for k in (3, 1, 2, 0):
            sum_o.middle(k)

    def result_back():
        sum_o.finish_core()
        layer_out[...] = after_cross[...] + po_whole[...].astype(F32)

    def tokens_back():
        sx.finish()
        wire.swap(NG.at[:, mine], NG.at[:, mine], x_slot)

    def encoder_back():
        se.finish()
        wire.swap(NE.at[:, mine], NE.at[:, mine], e_slot)

    def input_back():
        wire.got(NG.at[:, away], x_slot)
        extra, gain_one = rms_backward(layer_in[...], gains[0:1], NG[...])
        input_grad[...] = self_grad[...] + extra
        s1[...] = jnp.concatenate(
            (gain_one, gain_two, gain_three, jnp.zeros((5, model), F32)), axis=0
        )

    def small_first():
        wire.send(s1, sr.at[0], small, place.fx)
        wire.send(t1, tr.at[0], small + 5, place.fx)

    def small_second():
        wire.got(sr.at[0], small)
        wire.got(tr.at[0], small + 5)
        s2[...] = s1[...] + sr[0]
        t2[...] = t1[...] + tr[0]
        wire.send(s2, sr.at[1], small + 1, place.fy)
        wire.send(t2, tr.at[1], small + 6, place.fy)

    def small_third():
        wire.got(sr.at[1], small + 1)
        wire.got(tr.at[1], small + 6)
        sl[pl.ds(place.level, 1)] = (s2[...] + sr[1])[None]
        tl[pl.ds(place.level, 1)] = (t2[...] + tr[1])[None]
        for k in (1, 2, 3):
            wire.send(sl.at[place.level], sl.at[place.level], small + 1 + k, place.above[k])
            wire.send(tl.at[place.level], tl.at[place.level], small + 6 + k, place.above[k])

    def small_last():
        for k in (1, 2, 3):
            level = place.below[k] // 4
            wire.got(sl.at[level], small + 1 + k)
            wire.got(tl.at[level], small + 6 + k)
        totals[...] = (sl[0] + sl[1]) + (sl[2] + sl[3])
        bias_totals[...] = (tl[0] + tl[1]) + (tl[2] + tl[3])

    result_out()
    out_grads(low, mixed2, col["co"])
    sp.start(1)
    sp.start(2)
    back = PairBack(
        tok, size.pairs, probes, mkv, e2, rl2, mixed2, mixed_grad, mkv_grad, None, qc, gc, dl, dq
    )
    for c in range(ctx_enc // 1024):
        back.chunk(c * 512, 512)
    sp.start(0)
    for c in range(ctx_enc // 1024, ctx_enc // 512):
        back.chunk(c * 512, 512)
    back.finish(q_grad)
    sp.start(3)
    part = dot_nt(q_grad[...], WA[:, col["cq"]])
    ca[2] = part.astype(LOW)
    wire.swap(ca.at[2], cb.at[2], cross_slot)
    sp.pass_near(1)
    sp.pass_near(2)
    out_grads(E, mkv_grad, col["ckv"])
    sp.pass_near(0)
    sp.pass_near(3)
    out_grads(n2, q_grad, col["cq"])
    sc.start(3)
    sc.start(2)
    sp.pass_level(2)
    sc.start(1)

    def enc_rows(rows_):
        EG[rows_, :] = dot_nt(mkv_grad[rows_, :], WA[:, col["ckv"]]).astype(LOW)

    rows_loop(ctx_enc, 256, enc_rows)
    for k in (1, 2, 3, 0):
        pair_start(EG, pe, enc, e_base, k, e_out)
    wire.got(cb.at[2], cross_slot)
    n_grad = ca[2].astype(F32) + cb[2].astype(F32)
    extra, gain_two = rms_backward(after_self[...], gains[1:2], n_grad)
    self_grad[...] = cross_grad[...] + extra
    low[...] = self_grad[...].astype(LOW)
    mixed_grad[...] = dot(low[...], WA[:, col["o"]]).astype(LOW)
    for k in (1, 2, 3, 0):
        pair_ready(EG, pe, enc, e_base, k)
    se.start(3)
    out_grads(low, mixed1, col["o"])
    se.start(1)
    se.start(2)
    so_.start(1)
    sum_o.finish()
    sc.pass_near(3)

    back = PairBack(
        tok, size.pairs, q, kv, e1, rl1, mixed1, mixed_grad, kv_grad, diag, qc, gc, dl, dq
    )

    def tok_rows(k):
        for part_ in range(2):
            at = pl.ds(aligned(place.below[k] // 4 * 4 * tok + part_ * 2 * tok, 16), 2 * tok)
            XG[at, :] = dot_nt(kv_grad[at, :], WA[:, col["kv"]]).astype(LOW)

    n2[...] = X[here_rows, :]
    back.chunk(place.below[1] // 4 * 4 * tok, 4 * tok)
    tok_rows(1)
    pair_start(XG, px, tok, x_base, 1, x_out)
    back.chunk(place.below[2] // 4 * 4 * tok, 4 * tok)
    tok_rows(2)
    pair_start(XG, px, tok, x_base, 2, x_out)
    pair_ready(XG, px, tok, x_base, 1)
    sc.pass_near(2)
    so_.start(2)
    back.chunk(place.below[3] // 4 * 4 * tok, 4 * tok)
    tok_rows(3)
    pair_start(XG, px, tok, x_base, 3, x_out)
    pair_ready(XG, px, tok, x_base, 2)
    so_.start(3)
    sc.pass_near(1)
    so_.start(0)
    back.chunk(place.level * 4 * tok, 4 * tok)
    back.finish(q_grad)
    tok_rows(0)
    own = dot_nt(q_grad[...], WA[:, col["q"]]) + XG[here_rows, :].astype(F32)
    XG[here_rows, :] = own.astype(LOW)
    pair_start(XG, px, tok, x_base, 0, x_out)
    pair_ready(XG, px, tok, x_base, 3)
    sp.pass_level(1)
    so_.pass_near(2)
    sx.start(2)
    out_grads(n2, q_grad, col["q"])
    pair_ready(XG, px, tok, x_base, 0)
    so_.pass_near(1)
    sc.pass_level(2)
    out_grads(X, kv_grad.at[:, : size.wide], col["k"])
    sx.start(3)
    out_grads(X, kv_grad.at[:, size.wide :], col["v"])
    so_.pass_level(2)
    sx.pass_near(2)
    sw.start(1)
    sx.pass_level(2)
    se.pass_near(1)
    sx.start(1)
    sw.pass_near(1)
    sw.start(2)
    se.pass_near(2)
    sc.pass_level(1)
    se.start(0)
    sx.pass_near(3)
    se.pass_level(1)
    sp.pass_level(3)
    se.pass_near(3)
    sw.pass_level(1)
    sx.pass_near(1)
    se.pass_level(2)
    sums = bucket_sums(ids, diag, table.shape[1])
    t1[...] = jnp.concatenate(
        (sums, jnp.zeros((sums.shape[0], t1.shape[1] - sums.shape[1]), F32)), axis=1
    )

    se.pass_near(0)
    sx.pass_level(3)
    sw.pass_near(2)
    sx.pass_level(1)
    sx.start(0)
    sp.finish()
    so_.pass_near(3)
    so_.pass_level(1)
    sw.start(3)
    so_.pass_near(0)
    sx.pass_near(0)
    sc.pass_level(3)
    sc.start(0)
    se.pass_level(3)
    sw.start(0)
    sw.pass_level(2)
    tokens_back()
    input_back()
    small_first()
    result_back()
    sw.pass_near(3)
    sw.pass_near(0)
    small_second()
    so_.pass_level(3)
    units_down()
    sw.pass_level(3)
    so_.finish()
    small_third()
    sc.pass_near(0)
    encoder_back()
    units_back()
    sw.finish()
    small_last()
    sc.finish()
    wire.got(NE.at[:, away], e_slot)
    enc_grad[...] = NE[...]
    for made in (gx, ge, gs, gc_, go, gp):
        made.drain()
    wire.drain()


def emit_kernel(size, layer_out, input_grad, enc_grad, WG, mb, totals, bias_totals, *outs):
    for ref, out in zip((layer_out, input_grad, enc_grad), outs):
        out[...] = ref[...]
    for name, out in zip(size.names, outs[3:]):
        out[...] = WG[:, size.col[name]]
    for i, out in enumerate(outs[11:14]):
        for p in range(4):
            base = p * size.part + i * size.quarter
            out[:, p * size.quarter : (p + 1) * size.quarter] = mb[
                :, base : base + size.quarter
            ].astype(F32)
    outs[14][...] = totals[:3]
    heads, buckets = outs[15].shape
    outs[15][...] = bias_totals[:heads, :buckets]


def quick_device(
    layer_in, encoded, self_query, self_key, self_value, self_out, cross_query, cross_key,
    cross_value, cross_out, gate_proj, up_proj, down_proj, norm_gains, position_bias,
    bucket_ids, block_order, out_grad,
):
    tok, model = layer_in.shape
    enc = encoded.shape[0]
    wide, units = self_query.shape[1], gate_proj.shape[1]
    ctx = block_order.shape[0]
    buckets, heads = position_bias.shape
    size = Sizes(ctx, tok, enc, model, wide, units)
    rows, quarter, pairs = size.rows, size.quarter, size.pairs
    tok_all, enc_all, tok4 = ctx * tok, ctx * enc, 4 * tok

    def vmem(*shape, dtype=LOW):
        return pltpu.VMEM(shape, dtype)

    def full(*shape):
        return pltpu.VMEM(shape, F32)

    def streams(name):
        return [vmem(15, rows, last - first) for first, last in size.cuts[name]]

    ins = {
        "layer_in": layer_in, "encoded": encoded, "sq": self_query, "sk": self_key,
        "sv": self_value, "so": self_out.T, "cq": cross_query, "ck": cross_key,
        "cv": cross_value, "co": cross_out.T, "gate_w": gate_proj, "up_w": up_proj,
        "down_w": down_proj.T, "gains": norm_gains, "table": position_bias.T,
        "buckets": bucket_ids.reshape(ctx, tok), "order": block_order, "out_grad": out_grad,
    }
    outs = {
        "layer_out": ((tok, model), F32), "input_grad": ((tok, model), F32),
        "enc_grad": ((enc, model), F32), "WG": ((rows, size.attn_cols), F32),
        "mb": ((rows, size.mlp_cols), LOW), "totals": ((8, model), F32),
        "bias_totals": ((8, 128), F32),
    }
    (bs0, bs1), (bc0, bc1) = streams("s"), streams("c")
    (bo0, bo1), (bp0, bp1) = streams("o"), streams("co")
    scratch = {
        "WA": vmem(model, size.attn_cols), "WM": vmem(model, size.part),
        "wm": vmem(rows, size.mlp_cols), "X": vmem(tok_all, model), "E": vmem(enc_all, model),
        "GR": vmem(tok4, model), "PW": vmem(model, size.attn_cols),
        "PM": vmem(model, size.part),
        "q": vmem(tok, wide), "kv": vmem(tok_all, 2 * wide), "mkv": vmem(enc_all, 2 * wide),
        "probes": vmem(tok, wide), "s": full(2 * tok, tok_all),
        "e1": vmem(pairs, 2 * tok, tok_all), "e2": vmem(pairs, 2 * tok, enc_all),
        "rl1": full(pairs, 2 * tok, 1), "rl2": full(pairs, 2 * tok, 1),
        "mixed1": vmem(tok, wide), "mixed2": vmem(tok, wide), "table_rows": full(2 * ctx, tok),
        "ids": full(1, 2 * tok_all), "bias": full(8, 2 * tok_all), "diag": full(8, 2 * tok_all),
        "after_self": full(tok, model), "after_cross": full(tok, model),
        "cross_grad": full(tok, model), "self_grad": full(tok, model), "n2": vmem(tok, model),
        "N3": vmem(tok4, model), "act": vmem(tok4, quarter), "GU": vmem(tok4, 2 * quarter),
        "PN": vmem(tok4, model), "PO": vmem(tok4, model), "low": vmem(tok, model),
        "mixed_grad": vmem(tok, wide), "q_grad": vmem(tok, wide),
        "kv_grad": vmem(tok_all, 2 * wide), "mkv_grad": vmem(enc_all, 2 * wide),
        "ca": vmem(3, tok, model), "cb": vmem(3, tok, model),
        "pn_core": vmem(tok4, model // 2), "pn_plane": vmem(3, tok, model // 2),
        "pn_whole": vmem(tok, model), "po_core": vmem(tok4, model // 2),
        "po_plane": vmem(3, tok, model // 2), "po_whole": vmem(tok, model),
        "qc": vmem(pairs, 2 * tok, 128), "gc": vmem(pairs, 2 * tok, 128),
        "dl": full(pairs, 2 * tok, 1), "dq": full(pairs, 2 * tok, 128),
        "bs0": bs0, "bs1": bs1, "bc0": bc0, "bc1": bc1, "bo0": bo0, "bo1": bo1,
        "bp0": bp0, "bp1": bp1, "bx": vmem(2, 15, tok // 2, model // 2),
        "be": vmem(2, 15, enc // 2, model // 2), "px": vmem(tok_all, model // 2),
        "pe": vmem(enc_all, model // 2), "NG": full(tok, model), "NE": full(enc, model),
        "ml": vmem(3, 4 * rows, size.part), "ps": vmem(4 * rows, size.part),
        "s1": full(8, model), "s2": full(8, model), "sr": full(2, 8, model),
        "sl": full(4, 8, model), "t1": full(8, 128), "t2": full(8, 128), "tr": full(2, 8, 128), "tl": full(4, 8, 128), **wire_sems(73, 275),
    }
    names = list(ins) + list(outs) + list(scratch)
    made = pl.pallas_call(
        named(functools.partial(layer_kernel, size), names),
        out_shape=tuple(jax.ShapeDtypeStruct(*spec) for spec in outs.values()),
        in_specs=[
            pl.BlockSpec(memory_space=pltpu.SMEM if name == "order" else pltpu.VMEM)
            for name in ins
        ],
        out_specs=tuple(pl.BlockSpec(memory_space=pltpu.VMEM) for _ in outs),
        scratch_shapes=list(scratch.values()),
        compiler_params=pltpu.CompilerParams(
            collective_id=1, has_side_effects=True, vmem_limit_bytes=VMEM_LIMIT
        ),
    )(*ins.values())
    specs = [
        (tok, model), (tok, model), (enc, model), *((rows, wide),) * 8, *((rows, units),) * 3,
        (3, model), (heads, buckets),
    ]
    parts = pl.pallas_call(
        functools.partial(emit_kernel, size),
        out_shape=tuple(jax.ShapeDtypeStruct(spec, F32) for spec in specs),
        in_specs=[pl.BlockSpec(memory_space=pltpu.VMEM)] * len(made),
        out_specs=tuple(pl.BlockSpec(memory_space=pltpu.VMEM) for _ in specs),
    )(*made)
    named_parts = dict(zip(size.names, parts[3:11]))
    gate, upward, down, gains, bias_grad = parts[11:]
    return (
        *parts[:3], named_parts["q"], named_parts["k"], named_parts["v"], named_parts["o"].T,
        named_parts["cq"], named_parts["ck"], named_parts["cv"], named_parts["co"].T,
        gate, upward, down.T, gains, bias_grad.T,
    )


def quick_fits(mesh):
    return mesh.shape["ctx"] == 16 and mesh.shape["head"] == 2


def as_sent(shard):

    def short(part):
        return part.astype(jnp.bfloat16) if part.dtype == jnp.float32 else part

    return jax.tree.map(short, shard)


def rms_scale(rows, gain):
    return rows * lax.rsqrt(jnp.mean(rows * rows, axis=-1, keepdims=True) + EPS) * gain


def geglu(gate, upper):
    return jax.nn.gelu(gate, approximate=True) * upper


def times(left, right):
    return jnp.dot(left, right, preferred_element_type=jnp.float32)


def left_times(left, right):
    return lax.dot_general(
        left, right, (((0,), (0,)), ((), ())), preferred_element_type=jnp.float32
    )


def right_times(left, right):
    return lax.dot_general(
        left, right, (((1,), (1,)), ((), ())), preferred_element_type=jnp.float32
    )


def join_heads(parts):
    return jax.tree.map(lambda part: part.astype(jnp.float32), lax.psum(as_sent(parts), "head"))


def gather_self(keys_own, values_own):
    return (
        lax.all_gather(keys_own, "ctx", axis=0, tiled=True),
        lax.all_gather(values_own, "ctx", axis=0, tiled=True),
    )


def gather_cross(memory_keys, memory_values):
    return (
        lax.all_gather(memory_keys, "ctx", axis=0, tiled=True),
        lax.all_gather(memory_values, "ctx", axis=0, tiled=True),
    )


def bias_scores(steps, bias_table):
    rises = bias_table[1:] - bias_table[:-1]
    return bias_table[0][:, None, None] + jnp.einsum("qkb,bh->hqk", steps, rises, precision=HIGH)


def bias_grads(score_grad, steps):
    above = jnp.einsum("hqk,qkb->bh", score_grad, steps, precision=HIGH)
    total = jnp.sum(score_grad, axis=(1, 2))
    upper_rows = jnp.concatenate((total[None], above), axis=0)
    lower_rows = jnp.concatenate((above, jnp.zeros((1, above.shape[1]), jnp.float32)), axis=0)
    return upper_rows - lower_rows


def delta_of(mixed, mixed_grad, head_count):
    tok_rows, total_width = mixed.shape
    width = total_width // head_count
    product = mixed.astype(jnp.float32).reshape(tok_rows, head_count, width) * mixed_grad.astype(
        jnp.float32
    ).reshape(tok_rows, head_count, width)
    return jnp.transpose(jnp.sum(product, axis=-1))


def attend_fold(queries, head_count, parts_fn, bias_table):
    tok_rows = queries.shape[0]
    width = queries.shape[1] // head_count
    query3 = queries.reshape(tok_rows, head_count, width)

    def fold(state, pieces, start):
        key_piece, value_piece = pieces
        count = key_piece.shape[0]
        block = math.gcd(count, 512)

        def fold_step(index, inner):
            summed, run_max, run_sum = inner
            key3 = lax.dynamic_slice_in_dim(key_piece, index * block, block, 0).reshape(
                block, head_count, width
            )
            value3 = lax.dynamic_slice_in_dim(value_piece, index * block, block, 0).reshape(
                block, head_count, width
            )
            scores = jnp.einsum("qhe,khe->hqk", query3, key3, preferred_element_type=jnp.float32)
            if parts_fn is not None:
                steps, valid = parts_fn(index * block, block)
                scores = jnp.where(valid[None], scores + bias_scores(steps, bias_table), NEG)
            new_max = jnp.maximum(run_max, jnp.max(scores, axis=-1))
            ratio = jnp.exp(run_max - new_max)
            weights = jnp.exp(scores - new_max[..., None])
            run_sum = run_sum * ratio + jnp.sum(weights, axis=-1)
            summed = summed * ratio[..., None] + jnp.einsum(
                "hqk,khe->hqe",
                weights.astype(jnp.bfloat16),
                value3,
                preferred_element_type=jnp.float32,
            )
            return (summed, new_max, run_sum)

        return lax.fori_loop(0, count // block, fold_step, state)

    return fold


def finish(state):
    summed, run_max, run_sum = state
    head_count, tok_rows, width = summed.shape
    mixed = jnp.transpose(summed / run_sum[..., None], (1, 0, 2)).reshape(
        tok_rows, head_count * width
    )
    return (mixed.astype(jnp.bfloat16), run_max + jnp.log(run_sum))


def attend_back(
    queries, mixed_grad, lse, delta, keys_all, values_all, head_count, parts_fn, bias_table
):
    tok_rows, total_width = queries.shape
    width = total_width // head_count
    query3 = queries.reshape(tok_rows, head_count, width)
    grad3 = mixed_grad.reshape(tok_rows, head_count, width)
    count = keys_all.shape[0]
    block = math.gcd(count, 512)

    def attend_step(carry, index):
        query_grad, bias_grad = carry
        key3 = lax.dynamic_slice_in_dim(keys_all, index * block, block, 0).reshape(
            block, head_count, width
        )
        value3 = lax.dynamic_slice_in_dim(values_all, index * block, block, 0).reshape(
            block, head_count, width
        )
        scores = jnp.einsum("qhe,khe->hqk", query3, key3, preferred_element_type=jnp.float32)
        if parts_fn is not None:
            steps, valid = parts_fn(index * block, block)
            scores = jnp.where(valid[None], scores + bias_scores(steps, bias_table), NEG)
        weights = jnp.exp(scores - lse[..., None])
        weight_grad = jnp.einsum("qhe,khe->hqk", grad3, value3, preferred_element_type=jnp.float32)
        score_grad = weights * (weight_grad - delta[..., None])
        if parts_fn is not None:
            bias_grad = bias_grad + bias_grads(score_grad, steps)
        score_low = score_grad.astype(jnp.bfloat16)
        query_grad = query_grad + jnp.einsum(
            "hqk,khe->qhe", score_low, key3, preferred_element_type=jnp.float32
        )
        stacked = None
        value_term = jnp.einsum(
            "hqk,qhe->khe", weights.astype(jnp.bfloat16), grad3, preferred_element_type=jnp.float32
        )
        key_term = jnp.einsum("hqk,qhe->khe", score_low, query3, preferred_element_type=jnp.float32)
        stacked = jnp.concatenate(
            (key_term.reshape(block, total_width), value_term.reshape(block, total_width)), axis=1
        )
        return ((query_grad, bias_grad), stacked)

    start = (
        jnp.zeros((tok_rows, head_count, width), jnp.float32),
        jnp.zeros(bias_table.shape, jnp.float32),
    )
    (query_grad, bias_grad), terms = lax.scan(attend_step, start, jnp.arange(count // block))
    query_grad = query_grad.reshape(tok_rows, total_width).astype(jnp.bfloat16)
    terms = terms.reshape(count, 2 * total_width)
    return (query_grad, bias_grad, terms)


def per_device(
    layer_in,
    encoded,
    self_query,
    self_key,
    self_value,
    self_out,
    cross_query,
    cross_key,
    cross_value,
    cross_out,
    gate_proj,
    up_proj,
    down_proj,
    norm_gains,
    position_bias,
    bucket_ids,
    block_order,
    out_grad,
):
    low = jnp.bfloat16
    tok_rows = layer_in.shape[0]
    bucket_count, head_count = position_bias.shape
    block_count = block_order.shape[0]
    full_weights = (
        lax.all_gather(self_query, "ctx", axis=0, tiled=True),
        lax.all_gather(self_key, "ctx", axis=0, tiled=True),
        lax.all_gather(self_value, "ctx", axis=0, tiled=True),
        lax.all_gather(self_out, "ctx", axis=1, tiled=True),
        lax.all_gather(cross_query, "ctx", axis=0, tiled=True),
        lax.all_gather(cross_key, "ctx", axis=0, tiled=True),
        lax.all_gather(cross_value, "ctx", axis=0, tiled=True),
        lax.all_gather(cross_out, "ctx", axis=1, tiled=True),
        lax.all_gather(gate_proj, "ctx", axis=0, tiled=True),
        lax.all_gather(up_proj, "ctx", axis=0, tiled=True),
        lax.all_gather(down_proj, "ctx", axis=1, tiled=True),
    )
    (
        query_full,
        key_full,
        value_full,
        output_full,
        probe_full,
        lookup_full,
        recall_full,
        merge_full,
        gate_full,
        upward_full,
        down_full,
    ) = full_weights
    boundaries = jnp.arange(1, bucket_count, dtype=jnp.int32)
    starts = jnp.sum((bucket_ids[None, :] < boundaries[:, None]).astype(jnp.int32), axis=1)
    block_ids = jnp.arange(block_count, dtype=jnp.int32)
    here = lax.axis_index("ctx")
    own_block = jnp.sum(jnp.where(block_ids == here, block_order, 0))
    query_pos = own_block * tok_rows + jnp.arange(tok_rows, dtype=jnp.int32)

    def position_of(rows_index):
        slot = rows_index // tok_rows
        owner = jnp.sum(
            jnp.where(slot[:, None] == block_ids[None, :], block_order[None, :], 0), axis=1
        )
        return owner * tok_rows + rows_index % tok_rows

    def pair_parts(first_pos, second_pos):
        dist = first_pos[:, None] - second_pos[None, :]
        steps = (dist[:, :, None] >= starts[None, None, :]).astype(jnp.float32)
        return (steps, dist >= 0)

    def causal_parts(key_start, count):
        return pair_parts(query_pos, position_of(key_start + jnp.arange(count, dtype=jnp.int32)))

    normed_one = rms_scale(layer_in, norm_gains[0]).astype(low)
    queries = times(normed_one, query_full).astype(low)
    keys_own = times(normed_one, key_full).astype(low)
    values_own = times(normed_one, value_full).astype(low)
    memory_keys = times(encoded, lookup_full).astype(low)
    memory_values = times(encoded, recall_full).astype(low)
    total_width = queries.shape[1]
    width = total_width // head_count
    start_state = (
        jnp.zeros((head_count, tok_rows, width), jnp.float32),
        jnp.full((head_count, tok_rows), NEG, jnp.float32),
        jnp.zeros((head_count, tok_rows), jnp.float32),
    )
    self_fold = attend_fold(queries, head_count, causal_parts, position_bias)
    self_state = self_fold(
        start_state,
        (
            lax.all_gather(keys_own, "ctx", axis=0, tiled=True),
            lax.all_gather(values_own, "ctx", axis=0, tiled=True),
        ),
        jnp.int32(0),
    )
    mixed_one, lse_one = finish(self_state)
    after_self = layer_in + join_heads(times(mixed_one, output_full))
    normed_two = rms_scale(after_self, norm_gains[1]).astype(low)
    probes = times(normed_two, probe_full).astype(low)
    cross_fold = attend_fold(probes, head_count, None, position_bias)
    cross_state = cross_fold(
        start_state,
        (
            lax.all_gather(memory_keys, "ctx", axis=0, tiled=True),
            lax.all_gather(memory_values, "ctx", axis=0, tiled=True),
        ),
        jnp.int32(0),
    )
    mixed_two, lse_two = finish(cross_state)
    after_cross = after_self + join_heads(times(mixed_two, merge_full))
    normed_three = rms_scale(after_cross, norm_gains[2]).astype(low)
    gate_pre = times(normed_three, gate_full)
    upper = times(normed_three, upward_full)
    activated = geglu(gate_pre, upper).astype(low)
    layer_out = after_cross + join_heads(times(activated, down_full))
    grad_rows = out_grad.astype(low)
    down_wgrad = left_times(activated, grad_rows)
    act_grad = right_times(grad_rows, down_full)
    geglu_out, geglu_pull = jax.vjp(geglu, gate_pre, upper)
    gate_grad, upper_grad = geglu_pull(act_grad)
    gate_grad = gate_grad.astype(low)
    upper_grad = upper_grad.astype(low)
    gate_wgrad = left_times(normed_three, gate_grad)
    up_wgrad = left_times(normed_three, upper_grad)
    normed_three_grad = join_heads(
        right_times(gate_grad, gate_full) + right_times(upper_grad, upward_full)
    )
    norm_out, norm_pull = jax.vjp(rms_scale, after_cross, norm_gains[2])
    cross_extra, gain_three = norm_pull(normed_three_grad)
    cross_grad = out_grad + cross_extra
    cross_rows = cross_grad.astype(low)
    merge_wgrad = left_times(mixed_two, cross_rows)
    mixed_two_grad = right_times(cross_rows, merge_full).astype(low)
    delta_two = delta_of(mixed_two, mixed_two_grad, head_count)
    memory_all = gather_cross(memory_keys, memory_values)
    probe_grad, unused_bias, cross_terms = attend_back(
        probes,
        mixed_two_grad,
        lse_two,
        delta_two,
        memory_all[0],
        memory_all[1],
        head_count,
        None,
        position_bias,
    )
    cross_terms = lax.psum_scatter(cross_terms, "ctx", scatter_dimension=0, tiled=True)
    memory_key_grad = cross_terms[:, :total_width].astype(low)
    memory_value_grad = cross_terms[:, total_width:].astype(low)
    probe_wgrad = left_times(normed_two, probe_grad)
    lookup_wgrad = left_times(encoded, memory_key_grad)
    recall_wgrad = left_times(encoded, memory_value_grad)
    normed_two_grad, encoded_grad = join_heads(
        (
            right_times(probe_grad, probe_full),
            right_times(memory_key_grad, lookup_full) + right_times(memory_value_grad, recall_full),
        )
    )
    norm_out, norm_pull = jax.vjp(rms_scale, after_self, norm_gains[1])
    self_extra, gain_two = norm_pull(normed_two_grad)
    self_grad = cross_grad + self_extra
    self_rows = self_grad.astype(low)
    output_wgrad = left_times(mixed_one, self_rows)
    mixed_one_grad = right_times(self_rows, output_full).astype(low)
    delta_one = delta_of(mixed_one, mixed_one_grad, head_count)
    sequence_all = gather_self(keys_own, values_own)
    query_grad, bias_grad, self_terms = attend_back(
        queries,
        mixed_one_grad,
        lse_one,
        delta_one,
        sequence_all[0],
        sequence_all[1],
        head_count,
        causal_parts,
        position_bias,
    )
    self_terms = lax.psum_scatter(self_terms, "ctx", scatter_dimension=0, tiled=True)
    key_grad = self_terms[:, :total_width].astype(low)
    value_grad = self_terms[:, total_width:].astype(low)
    query_wgrad = left_times(normed_one, query_grad)
    key_wgrad = left_times(normed_one, key_grad)
    value_wgrad = left_times(normed_one, value_grad)
    normed_one_grad = join_heads(
        right_times(query_grad, query_full)
        + right_times(key_grad, key_full)
        + right_times(value_grad, value_full)
    )
    norm_out, norm_pull = jax.vjp(rms_scale, layer_in, norm_gains[0])
    input_extra, gain_one = norm_pull(normed_one_grad)
    input_grad = self_grad + input_extra
    weight_sums = (
        lax.psum_scatter(query_wgrad, "ctx", scatter_dimension=0, tiled=True),
        lax.psum_scatter(key_wgrad, "ctx", scatter_dimension=0, tiled=True),
        lax.psum_scatter(value_wgrad, "ctx", scatter_dimension=0, tiled=True),
        lax.psum_scatter(output_wgrad, "ctx", scatter_dimension=1, tiled=True),
        lax.psum_scatter(probe_wgrad, "ctx", scatter_dimension=0, tiled=True),
        lax.psum_scatter(lookup_wgrad, "ctx", scatter_dimension=0, tiled=True),
        lax.psum_scatter(recall_wgrad, "ctx", scatter_dimension=0, tiled=True),
        lax.psum_scatter(merge_wgrad, "ctx", scatter_dimension=1, tiled=True),
        lax.psum_scatter(gate_wgrad, "ctx", scatter_dimension=0, tiled=True),
        lax.psum_scatter(up_wgrad, "ctx", scatter_dimension=0, tiled=True),
        lax.psum_scatter(down_wgrad, "ctx", scatter_dimension=1, tiled=True),
    )
    gains_sum, bias_sum = lax.psum((jnp.stack((gain_one, gain_two, gain_three)), bias_grad), "ctx")
    return (layer_out, input_grad, encoded_grad) + tuple(weight_sums) + (gains_sum, bias_sum)


def solution(mesh):
    body = quick_device if quick_fits(mesh) else per_device
    placed = (
        P("ctx", None),
        P("ctx", None),
        P("ctx", "head"),
        P("ctx", "head"),
        P("ctx", "head"),
        P("head", "ctx"),
        P("ctx", "head"),
        P("ctx", "head"),
        P("ctx", "head"),
        P("head", "ctx"),
        P("ctx", "head"),
        P("ctx", "head"),
        P("head", "ctx"),
        P(),
        P(None, "head"),
        P(),
        P(),
        P("ctx", None),
    )
    return jax.shard_map(
        body,
        mesh=mesh,
        in_specs=placed,
        out_specs=(
            P("ctx", None),
            P("ctx", None),
            P("ctx", None),
            P("ctx", "head"),
            P("ctx", "head"),
            P("ctx", "head"),
            P("head", "ctx"),
            P("ctx", "head"),
            P("ctx", "head"),
            P("ctx", "head"),
            P("head", "ctx"),
            P("ctx", "head"),
            P("ctx", "head"),
            P("head", "ctx"),
            P(),
            P(None, "head"),
        ),
        check_vma=False,
    )
```

```python
import functools
import math

import jax
import jax.numpy as jnp
from jax import lax
from jax.experimental import pallas as pl
from jax.experimental.pallas import tpu as pltpu
from jax.sharding import PartitionSpec as P

EPS = 1e-06
NEG = -1e30
HIGH = lax.Precision.HIGHEST
LOW = jnp.bfloat16
F32 = jnp.float32
MESH = pl.DeviceIdType.MESH
VMEM_LIMIT = 66_000_000


def dot(left, right, **kw):
    return jnp.dot(left, right, preferred_element_type=F32, **kw)


def dot_nt(left, right, **kw):
    return lax.dot_general(left, right, (((1,), (1,)), ((), ())), preferred_element_type=F32, **kw)


def dot_tn(left, right, **kw):
    return lax.dot_general(left, right, (((0,), (0,)), ((), ())), preferred_element_type=F32, **kw)


def rms_forward(rows, gain):
    return rows * lax.rsqrt(jnp.mean(rows * rows, axis=-1, keepdims=True) + EPS) * gain


def rms_backward(rows, gain, grad):
    scale = lax.rsqrt(jnp.mean(rows * rows, axis=-1, keepdims=True) + EPS)
    scaled = gain * grad
    inner = jnp.mean(scaled * rows, axis=-1, keepdims=True)
    row_grad = scale * scaled - rows * (scale * scale * scale * inner)
    gain_grad = jnp.sum(grad * rows * scale, axis=0, keepdims=True)
    return row_grad, gain_grad


def aligned(value, step):
    return value if isinstance(value, int) else pl.multiple_of(value, step)


class Place:
    def __init__(self, count):
        self.count = count
        self.here = lax.axis_index("ctx")
        self.core = lax.axis_index("head")
        self.other = 1 - self.core
        self.plane = lax.rem(self.here, 4)
        self.level = self.here // 4
        self.fx = self.flip(self.here, 0)
        self.fy = self.flip(self.here, 1)
        self.fxy = self.flip(self.fx, 1)
        self.above = [lax.rem(self.here + 4 * k, count) for k in range(4)]
        self.below = [lax.rem(self.here + count - 4 * k, count) for k in range(4)]
        self.top = count // 4 - 1
        bottom, head = self.level == 0, self.level == self.top
        self.nearest = (
            jnp.where(bottom, 3, 1),
            jnp.where(bottom, 2, jnp.where(head, 2, 3)),
            jnp.where(bottom, 1, jnp.where(head, 3, 2)),
        )

    def flip(self, index, axis):
        if axis == 0:
            return index + 1 - 2 * lax.rem(index, 2)
        return index + 2 - 4 * lax.rem(index // 2, 2)

    def near(self, half):
        return (self.fx, self.fy) if half == 0 else (self.fy, self.fx)

    def signal(self, chips):
        barrier = pltpu.get_barrier_semaphore()
        for chip in chips:
            pl.semaphore_signal(
                barrier, inc=1, device_id=(chip, self.core), device_id_type=MESH
            )
        pl.semaphore_signal(barrier, inc=1, device_id=(self.here, self.other), device_id_type=MESH)

    def meet(self, count):
        pl.semaphore_wait(pltpu.get_barrier_semaphore(), count)


class Wire:
    def __init__(self, place, send_sem, recv_sem):
        self.place, self.send_sem, self.recv_sem = place, send_sem, recv_sem
        self.used = 0
        self.send_used = 0
        self.pending = []

    def slots(self, count):
        base = self.used
        self.used += count
        assert self.used <= self.recv_sem.shape[0], self.used
        return base

    def sender(self, whole=None):
        slot = self.send_used
        self.send_used += 1
        assert slot < self.send_sem.shape[0], slot
        if whole is not None:
            self.pending.append((slot, whole))
        return slot

    def copy(self, src, dst, out, slot, chip, core):
        return pltpu.make_async_remote_copy(
            src_ref=src,
            dst_ref=dst,
            send_sem=self.send_sem.at[out],
            recv_sem=self.recv_sem.at[slot],
            device_id=(chip, core),
            device_id_type=MESH,
        )

    def send(self, src, dst, slot, chip=None, core=None, out=None):
        chip = self.place.here if chip is None else chip
        core = self.place.core if core is None else core
        if out is None:
            out = self.sender(src)
        self.copy(src, dst, out, slot, chip, core).start()

    def swap(self, src, dst, slot, out=None):
        self.send(src, dst, slot, None, self.place.other, out)

    def got(self, dst, slot):
        place = self.place
        self.copy(dst, dst, 0, slot, place.here, place.other).wait_recv()

    def sent(self, whole, out):
        place = self.place
        self.copy(whole, whole, out, 0, place.here, place.other).wait_send()

    def drain(self):
        for out, whole in self.pending:
            self.sent(whole, out)
        self.pending = []


class Gather:
    def __init__(self, wire, view, share, spare):
        self.wire, self.view, self.share, self.spare = wire, view, share, spare
        self.halves = range(2)
        self.base = wire.slots(8)
        self.out = wire.sender(spare(12))
        self.line_out = wire.sender()
        if share:
            self.side = wire.slots(1)
            self.side_out = wire.sender(spare(15))

    def _line(self, half, block, slot, chip):
        ref = self.view(half, block)
        self.wire.send(ref, ref, self.base + slot, chip, out=self.line_out)

    def _out(self, half, block, slot, chip):
        ref = self.view(half, block)
        self.wire.send(ref, ref, self.base + slot, chip, out=self.out)

    def _give(self, half, block):
        if self.share:
            ref = self.view(half, block)
            self.wire.swap(ref, ref, self.side, self.side_out)

    def start_level(self):
        place = self.wire.place
        for half in self.halves:

            @pl.when(place.level < place.top)
            def _():
                self._line(half, place.here, 0, place.here + 4)

            @pl.when(place.level > 0)
            def _():
                self._line(half, place.here, 2, place.here - 4)

    def start_plane(self):
        place = self.wire.place
        for half in self.halves:
            near, far = place.near(half)
            self._out(half, place.here, 3, near)
            self._out(half, place.here, 7, far)

    def _level_block(self, step):
        place = self.wire.place
        k = place.nearest[step]
        return k, lax.rem(place.here + place.count - 4 * k, place.count)

    def pass_line(self, step):
        place = self.wire.place
        k, block = self._level_block(step)
        rising = place.level >= k
        onward = jnp.where(rising, place.level < place.top, place.level > 0)
        chip = jnp.where(rising, place.here + 4, place.here - 4)
        slot = jnp.where(rising, k, k - 2)
        self.wire.got(self.spare(1), self.base + k - 1)
        for half in self.halves:

            @pl.when(onward)
            def _():
                self._line(half, block, slot, chip)

    def pass_plane(self, step):
        place = self.wire.place
        k, block = self._level_block(step)
        for half in self.halves:
            near, far = place.near(half)
            self._out(half, block, 3 + k, near)
            self._out(half, block, 7, far)
            self._give(half, block)

    def pass_near(self, step):
        place = self.wire.place
        k = (0, *place.nearest)[step]
        block = lax.rem(place.here + place.count - 4 * k, place.count)
        self.wire.got(self.spare(1), self.base + 3 + k)
        for half in self.halves:
            _, far = place.near(half)
            arrived = place.flip(block, half)
            self._out(half, arrived, 7, far)
            self._give(half, arrived)

    def finish(self):
        place = self.wire.place
        self.wire.got(self.spare(8), self.base + 7)
        for half in self.halves:
            if self.share:
                for k in range(4):
                    block = place.flip(place.below[k], 1 - half)
                    self._give(half, block)
                    self._give(half, place.flip(block, half))

    def finish_share(self):
        self.wire.got(self.spare(15), self.side)

    def drain(self):
        place = self.wire.place

        @pl.when(jnp.logical_or(place.level == 0, place.level == place.top))
        def _():
            self.wire.sent(self.spare(1), self.line_out)

        @pl.when(jnp.logical_and(place.level > 0, place.level < place.top))
        def _():
            self.wire.sent(self.spare(5), self.line_out)


class Scatter:
    def __init__(self, wire, view, buf, out, spare):
        self.wire, self.view, self.buf, self.out, self.spare = wire, view, buf, out, spare
        self.halves = range(2)
        self.base = wire.slots(9)
        self.send_slot = wire.sender(spare(15))

    def _send(self, half, block, place_in, slot, chip):
        self.wire.send(
            self.view(half, block),
            self.buf(half).at[place_in],
            self.base + slot,
            chip,
            out=self.send_slot,
        )

    def start(self, k):
        place = self.wire.place
        for half in self.halves:
            _, far = place.near(half)
            away = place.flip(place.below[k], 1 - half)
            for pair, block in ((1, place.flip(away, half)), (0, away)):
                self._send(half, block, 2 * k + pair, k, far)

    def pass_near(self, k):
        place = self.wire.place
        self.wire.got(self.spare(2), self.base + k)
        for half in self.halves:
            near, _ = place.near(half)
            block = place.flip(place.below[k], half)
            ref = self.view(half, block)
            ref[...] = (ref[...].astype(F32) + self.buf(half)[2 * k + 1].astype(F32)).astype(LOW)
            self._send(half, block, 8 + k, 4 + k, near)

    def pass_level(self, k):
        place = self.wire.place
        self.wire.got(self.spare(1), self.base + 4 + k)
        for half in self.halves:
            ref = self.view(half, place.below[k])
            ref[...] = self._sum(half, k).astype(LOW)
            self._send(half, place.below[k], 11 + k, 8, place.below[k])

    def _sum(self, half, k):
        buf = self.buf(half)
        total = self.view(half, self.wire.place.below[k])[...].astype(F32)
        return total + buf[2 * k].astype(F32) + buf[8 + k].astype(F32)

    def finish(self):
        self.wire.got(self.spare(1), self.base + 4)
        self.wire.got(self.spare(3), self.base + 8)
        for half in self.halves:
            total = self._sum(half, 0)
            for k in (1, 2, 3):
                total = total + self.buf(half)[11 + k].astype(F32)
            self.out(half, total)


def lane_split(rows):
    lane = lax.broadcasted_iota(jnp.int32, rows.shape, 1)
    low = lane < rows.shape[1] // 2
    zero = jnp.zeros_like(rows)
    return jnp.concatenate((jnp.where(low, rows, zero), jnp.where(low, zero, rows)), axis=0)


def lane_join(rows):
    count, width = rows.shape[0] // 2, rows.shape[1]
    lane = lax.broadcasted_iota(jnp.int32, (count, width), 1)
    return jnp.where(lane < width // 2, rows[:count], rows[count:])


def pair_attend(tok, pairs, chunk, q_ref, kv_ref, s_ref, e_ref, rl_ref, mixed_ref, bias_ref, between):
    keys = kv_ref.shape[0]
    total = pairs * 128

    for j in range(pairs):
        cols = slice(j * 128, (j + 1) * 128)
        vcols = slice(total + j * 128, total + (j + 1) * 128)
        q_cat = lane_split(q_ref[:, cols])

        def score(c, top):
            rows = pl.ds(aligned(c * chunk, chunk), chunk)
            s = dot_nt(q_cat, kv_ref[rows, cols])
            if bias_ref is not None:
                tiles = []
                for half in range(2):
                    row = []
                    for b in range(chunk // tok):
                        lanes = pl.ds(aligned((c * (chunk // tok) + b) * 2 * tok, 128), 2 * tok)
                        vec = bias_ref[2 * j + half : 2 * j + half + 1, lanes]
                        wide = jnp.broadcast_to(vec, (tok, 2 * tok))
                        row.append(pltpu.roll(wide, 0, 1, stride=1, stride_axis=0)[:, :tok])
                    tiles.append(jnp.concatenate(row, axis=1))
                s = s + jnp.concatenate(tiles, axis=0)
            s_ref[:, rows] = s
            for b in range(chunk // 128):
                top = jnp.maximum(top, s[:, b * 128 : (b + 1) * 128])
            return top

        top = lax.fori_loop(0, keys // chunk, score, jnp.full((2 * tok, 128), NEG, F32))
        peak = jnp.max(top, axis=1, keepdims=True)

        def weigh(c, state):
            acc, run = state
            rows = pl.ds(aligned(c * chunk, chunk), chunk)
            e = jnp.exp(s_ref[:, rows] - peak)
            for b in range(chunk // 128):
                run = run + e[:, b * 128 : (b + 1) * 128]
            low = e.astype(LOW)
            e_ref[j, :, rows] = low
            return (acc + dot(low, kv_ref[rows, vcols]), run)

        zero = jnp.zeros((2 * tok, 128), F32)
        acc, run = lax.fori_loop(0, keys // chunk, weigh, (zero, zero))
        rl = 1.0 / jnp.sum(run, axis=1, keepdims=True)
        rl_ref[j] = rl
        mixed_ref[:, cols] = lane_join(acc * rl).astype(LOW)
        between(j)


class PairBack:
    def __init__(self, tok, pairs, q, kv, e, rl, mixed, grad, kv_grad, diag, qc, gc, dl, dq):
        self.tok, self.pairs, self.kv, self.e = tok, pairs, kv, e
        self.kv_grad, self.diag, self.qc, self.gc, self.dl, self.dq = kv_grad, diag, qc, gc, dl, dq
        self.total = pairs * 128
        for j in range(pairs):
            cols = slice(j * 128, (j + 1) * 128)
            rl_j = rl[j]
            grads = lane_split(grad[:, cols].astype(F32))
            qc[j] = lane_split(q[:, cols])
            gc[j] = (grads * rl_j).astype(LOW)
            values = lane_split(mixed[:, cols].astype(F32))
            dl[j] = jnp.sum(grads * values, axis=1, keepdims=True) * rl_j
            dq[j] = jnp.zeros(dq.shape[1:], F32)

    def chunk(self, start, count):
        tok, kv, qc, gc = self.tok, self.kv, self.qc, self.gc
        rows = pl.ds(aligned(start, count), count)
        flip = (
            lax.broadcasted_iota(jnp.int32, (tok, tok), 0)
            + lax.broadcasted_iota(jnp.int32, (tok, tok), 1)
            == tok - 1
        ).astype(LOW)

        def one_pair(j, carry):
            cols = pl.ds(aligned(j * 128, 128), 128)
            vcols = pl.ds(aligned(self.total + j * 128, 128), 128)
            low_e = self.e[j, :, rows]
            dp = dot_nt(gc[j], kv[rows, vcols])
            ds = (low_e.astype(F32) * (dp - self.dl[j])).astype(LOW)
            if self.diag is not None:
                for half in range(2):
                    turned = dot(flip, ds[half * tok : (half + 1) * tok])
                    for b in range(count // tok):
                        tile = turned[:, b * tok : (b + 1) * tok]
                        wide = jnp.concatenate((tile, jnp.zeros_like(tile)), axis=1)
                        wide = pltpu.roll(wide, tok + 1, 1, stride=1, stride_axis=0)
                        lanes = pl.ds(aligned(2 * start + b * 2 * tok, 128), 2 * tok)
                        self.diag[pl.ds(2 * j + half, 1), lanes] = jnp.sum(
                            wide, axis=0, keepdims=True
                        )
            self.kv_grad[rows, cols] = dot_tn(ds, qc[j]).astype(LOW)
            self.kv_grad[rows, vcols] = dot_tn(low_e, gc[j]).astype(LOW)
            self.dq[j] = self.dq[j] + dot(ds, kv[rows, cols])
            return carry

        lax.fori_loop(0, self.pairs, one_pair, 0)

    def finish(self, q_grad):
        for j in range(self.pairs):
            q_grad[:, j * 128 : (j + 1) * 128] = lane_join(self.dq[j]).astype(LOW)


def bucket_rows(buckets_ref, order_ref, here, table_rows, ids_ref):
    count, tok = buckets_ref.shape
    turn = (
        lax.broadcasted_iota(jnp.int32, (tok, tok), 0)
        + lax.broadcasted_iota(jnp.int32, (tok, tok), 1)
        == tok - 1
    ).astype(LOW)
    table_rows[:count, :] = jnp.full((count, tok), -1.0, F32)
    table_rows[count:, :] = dot(buckets_ref[...].astype(LOW), turn)
    own = order_ref[here]
    for block in range(count):
        at = own - order_ref[block] + count
        wide = jnp.concatenate(
            (table_rows[pl.ds(at - 1, 1), :], table_rows[pl.ds(at, 1), :]), axis=1
        )
        ids_ref[:, block * 2 * tok : (block + 1) * 2 * tok] = pltpu.roll(wide, 1, 1)


def bucket_masks(ids_ref, buckets):
    ids = ids_ref[...]
    row = lax.broadcasted_iota(jnp.int32, (buckets, ids.shape[1]), 0).astype(F32)
    return ids, (row == ids).astype(F32)


def bias_vectors(ids_ref, table_ref, bias_ref):
    heads, buckets = table_ref.shape
    ids, mask = bucket_masks(ids_ref, buckets)
    vec = dot(table_ref[...], mask, precision=HIGH)
    bias_ref[:heads, :] = jnp.where(ids >= 0, vec, NEG)


def bucket_sums(ids_ref, diag_ref, buckets):
    _, mask = bucket_masks(ids_ref, buckets)
    return dot_nt(diag_ref[...], mask, precision=HIGH)


def rows_loop(count, step, body):
    def one(index, carry):
        body(pl.ds(aligned(index * step, step), step))
        return carry

    lax.fori_loop(0, count // step, one, 0)


GELU_A = 0.7978845608028654
GELU_B = 0.044715


def gelu_parts(value):
    square = value * value
    wave = jnp.tanh(GELU_A * (value + GELU_B * value * square))
    half = 0.5 * (1.0 + wave)
    slope = half + 0.5 * value * (1.0 - wave * wave) * (GELU_A * (1.0 + 3.0 * GELU_B * square))
    return value * half, slope


def core_sum(wire, part, out_buf, in_buf):
    slot = wire.slots(1)
    out_buf[...] = part.astype(LOW)
    wire.swap(out_buf, in_buf, slot)
    wire.got(in_buf, slot)
    return out_buf[...].astype(F32) + in_buf[...].astype(F32)


class PlaneSum:
    def __init__(self, wire, tok, part, core_buf, plane_buf, whole):
        self.wire, self.tok = wire, tok
        self.out = wire.sender(part)
        self.part, self.core_buf, self.plane_buf, self.whole = part, core_buf, plane_buf, whole
        self.base = wire.slots(8)
        self.half = whole.shape[1] // 2
        place = wire.place
        self.chips = (place.here, place.fx, place.fy, place.fxy)

    def cols(self, core):
        return pl.ds(aligned(core * self.half, 128), self.half)

    def rows(self, k):
        return pl.ds(aligned(lax.rem(self.chips[k], 4) * self.tok, self.tok), self.tok)

    def start(self, k):
        away = self.cols(self.wire.place.other)
        rows = self.rows(k)
        self.wire.swap(self.part.at[rows, away], self.core_buf.at[rows, :], self.base + k, self.out)

    def middle(self, k):
        wire, rows = self.wire, self.rows(k)
        wire.got(self.core_buf.at[rows, :], self.base + k)
        total = self.part[rows, self.cols(wire.place.core)].astype(F32)
        total = total + self.core_buf[rows, :].astype(F32)
        self.core_buf[rows, :] = total.astype(LOW)
        if k:
            wire.send(
                self.core_buf.at[rows, :],
                self.plane_buf.at[k - 1],
                self.base + 3 + k,
                self.chips[k],
                out=self.out,
            )

    def finish(self):
        place, wire = self.wire.place, self.wire
        total = self.core_buf[self.rows(0), :].astype(F32)
        for k in (1, 2, 3):
            wire.got(self.plane_buf.at[k - 1], self.base + 3 + k)
            total = total + self.plane_buf[k - 1].astype(F32)
        mine = self.cols(place.core)
        self.whole[:, mine] = total.astype(LOW)
        wire.swap(self.whole.at[:, mine], self.whole.at[:, mine], self.base + 7, self.out)

    def finish_core(self):
        self.wire.got(self.whole.at[:, self.cols(self.wire.place.other)], self.base + 7)


class PlaneGather:
    def __init__(self, wire, tok, ref):
        self.wire, self.tok, self.ref = wire, tok, ref
        self.half = ref.shape[1] // 2
        self.base = wire.slots(8)
        self.out = wire.sender(ref.at[: 3 * tok, :])
        place = wire.place
        self.chips = (place.here, place.fx, place.fy, place.fxy)

    def view(self, k, core):
        rows = pl.ds(aligned(lax.rem(self.chips[k], 4) * self.tok, self.tok), self.tok)
        return self.ref.at[rows, pl.ds(aligned(core * self.half, 128), self.half)]

    def start(self):
        own = self.view(0, self.wire.place.core)
        for k in (1, 2, 3):
            self.wire.send(own, own, self.base + k, self.chips[k], out=self.out)

    def share(self, k):
        ref = self.view(k, self.wire.place.core)
        self.wire.got(ref, self.base + k)
        self.wire.swap(ref, ref, self.base + 4 + k, self.out)

    def finish(self, k):
        self.wire.got(self.view(k, self.wire.place.other), self.base + 4 + k)


class Sizes:
    def __init__(self, ctx, tok, enc, model, wide, units):
        self.ctx, self.tok, self.enc, self.model, self.wide = ctx, tok, enc, model, wide
        self.rows = model // ctx
        self.units = units
        self.quarter = units // 4
        self.pairs = wide // 128
        self.levels = ctx // 4
        self.attn_cols = 8 * wide
        self.mlp_cols = 3 * units
        self.part = 3 * self.quarter
        self.names = ("q", "k", "v", "cq", "ck", "cv", "o", "co")
        self.col = {n: slice(i * wide, (i + 1) * wide) for i, n in enumerate(self.names)}
        self.col["kv"] = slice(wide, 3 * wide)
        self.col["ckv"] = slice(4 * wide, 6 * wide)
        self.cuts = {
            "s": self.halves(0, 3 * wide, 0),
            "c": self.halves(3 * wide, 6 * wide, 1),
            "o": self.halves(6 * wide, 7 * wide, 0),
            "co": self.halves(7 * wide, 8 * wide, 1),
        }

    def halves(self, first, last, up):
        tiles = (last - first) // 128
        middle = first + (tiles + up) // 2 * 128
        return ((first, middle), (middle, last))


def named(kernel, names):
    def body(*refs):
        kernel(**dict(zip(names, refs, strict=True)))

    return body


def wire_sems(send, recv):
    return {
        "send_sem": pltpu.SemaphoreType.DMA((send,)),
        "recv_sem": pltpu.SemaphoreType.DMA((recv,)),
    }


def layer_kernel(
    size, layer_in, encoded, sq, sk, sv, so, cq, ck, cv, co, gate_w, up_w, down_w, gains,
    table, buckets, order, out_grad,
    layer_out, input_grad, enc_grad, WG, mb, totals, bias_totals,
    WA, WM, wm, X, E, GR, PW, PM,
    q, kv, mkv, probes, s, e1, e2, rl1, rl2, mixed1, mixed2, table_rows, ids, bias, diag,
    after_self, after_cross, cross_grad, self_grad, n2, N3, act, GU, PN, PO, low, mixed_grad,
    q_grad, kv_grad, mkv_grad, ca, cb, pn_core, pn_plane, pn_whole, po_core, po_plane, po_whole,
    qc, gc, dl, dq, bs0, bs1, bc0, bc1, bo0, bo1, bp0, bp1, bx, be, px, pe, NG, NE, ml, ps,
    s1, s2, sr, sl, t1, t2, tr, tl, send_sem, recv_sem,
):
    place = Place(size.ctx)
    wire = Wire(place, send_sem, recv_sem)
    tok, enc, rows, half_d = size.tok, size.enc, size.rows, size.model // 2
    col, model, quarter = size.col, size.model, size.quarter
    ctx_tok, ctx_enc = X.shape[0], E.shape[0]
    plane_chips = (place.fx, place.fy, place.fxy)
    XG, EG = kv, mkv

    def block_rows(block, count):
        return pl.ds(aligned(block * count, 16), count)

    here_rows = block_rows(place.here, tok)
    own_weights = block_rows(place.here, rows)
    my_part = pl.ds(aligned(place.plane * size.part, 128), size.part)
    mine = pl.ds(aligned(place.core * half_d, 128), half_d)
    away = pl.ds(aligned(place.other * half_d, 128), half_d)

    def token_view(ref, count, core):
        def view(half, block):
            return ref.at[
                pl.ds(aligned(block * count + half * (count // 2), 16), count // 2),
                pl.ds(aligned(core * half_d, 128), half_d),
            ]

        return view

    def weight_view(ref, name):
        def view(half, block):
            first, last = size.cuts[name][half]
            return ref.at[block_rows(block, rows), first:last]

        return view

    def token_spare(buf):
        return lambda count: buf.at[:, 0:count]

    def weight_spare(name):
        (first, _), (_, last) = size.cuts[name]
        return lambda count: WA.at[0 : count * rows, first:last]

    gx = Gather(wire, token_view(X, tok, place.core), True, token_spare(bx))
    ge = Gather(wire, token_view(E, enc, place.core), True, token_spare(be))
    gs, gc_, go, gp = (
        Gather(wire, weight_view(WA, name), False, weight_spare(name))
        for name in ("s", "c", "o", "co")
    )
    gg = PlaneGather(wire, tok, GR)
    spread = PlaneGather(wire, tok, N3)
    sum_n = PlaneSum(wire, tok, PN, pn_core, pn_plane, pn_whole)
    sum_o = PlaneSum(wire, tok, PO, po_core, po_plane, po_whole)
    mg_plane, mg_level, ms_level, ms_plane = (wire.slots(3) for _ in range(4))

    def units_out():
        for k, chip in enumerate(plane_chips):
            wire.send(
                wm.at[:, pl.ds(aligned(lax.rem(chip, 4) * size.part, 128), size.part)],
                WM.at[own_weights, :],
                mg_plane + k,
                chip,
            )

    def units_up():
        for k, chip in enumerate(plane_chips):
            wire.got(WM.at[block_rows(chip, rows), :], mg_plane + k)
        own = WM.at[block_rows(place.level, 4 * rows), :]
        for k in (1, 2, 3):
            wire.send(own, own, mg_level + k - 1, place.above[k])

    place.signal(place.above[1:] + list(plane_chips))
    X[here_rows, :] = rms_forward(layer_in[...], gains[0:1]).astype(LOW)
    for name, ref in zip(("q", "k", "v", "cq", "ck", "cv", "o", "co"), (sq, sk, sv, cq, ck, cv, so, co)):
        WA[own_weights, col[name]] = ref[...]
    E[block_rows(place.here, enc), :] = encoded[...]
    plane_rows = block_rows(place.plane, tok)
    GR[plane_rows, :] = out_grad[...].astype(LOW)
    for p in range(4):
        cols = slice(p * quarter, (p + 1) * quarter)
        for i, ref in enumerate((gate_w, up_w, down_w)):
            base = p * size.part + i * quarter
            wm[:, base : base + quarter] = ref[:, cols]
    WM[own_weights, :] = wm[:, my_part]
    place.meet(7)
    gx.start_level()
    gs.start_level()
    gx.start_plane()
    gs.start_plane()
    gx.pass_near(0)
    gx.pass_line(0)
    gx.pass_plane(0)
    gs.pass_near(0)
    gs.pass_line(0)
    gs.pass_plane(0)
    gx.pass_line(1)
    gx.pass_plane(1)
    gs.pass_line(1)
    gs.pass_plane(1)
    go.start_level()
    ge.start_level()
    gx.pass_near(1)
    gs.pass_near(1)
    gx.pass_line(2)
    gx.pass_plane(2)
    gs.pass_line(2)
    gs.pass_plane(2)
    gc_.start_level()
    gp.start_level()
    gx.pass_near(2)
    gs.pass_near(2)
    gx.pass_near(3)
    gs.pass_near(3)
    go.start_plane()
    ge.start_plane()
    gc_.start_plane()
    units_out()
    bucket_rows(buckets, order, place.here, table_rows, ids)
    bias_vectors(ids, table, bias)
    diag[...] = jnp.zeros_like(diag)
    go.pass_line(0)
    go.pass_plane(0)
    ge.pass_line(0)
    ge.pass_plane(0)
    gc_.pass_line(0)
    gp.pass_line(0)
    go.pass_line(1)
    go.pass_plane(1)
    ge.pass_line(1)
    ge.pass_plane(1)
    gc_.pass_line(1)
    gp.pass_line(1)
    go.pass_line(2)
    go.pass_plane(2)
    ge.pass_line(2)
    ge.pass_plane(2)
    gc_.pass_line(2)
    gp.pass_line(2)
    gc_.pass_plane(0)
    gc_.pass_plane(1)
    gc_.pass_plane(2)
    gx.finish()
    go.pass_near(0)
    ge.pass_near(0)
    gx.finish_share()
    gs.finish()
    units_up()

    def project(rows_):
        kv[rows_, :] = dot(X[rows_, :], WA[:, col["kv"]]).astype(LOW)

    def project_enc(rows_):
        mkv[rows_, :] = dot(E[rows_, :], WA[:, col["ckv"]]).astype(LOW)

    def project_level(level):
        for part_ in range(2):
            project(slice((2 * level + part_) * 2 * tok, (2 * level + part_ + 1) * 2 * tok))

    q[...] = dot(X[here_rows, :], WA[:, col["q"]]).astype(LOW)
    project_level(0)
    project_level(1)
    project_level(2)
    project_level(3)
    go.pass_near(1)
    go.pass_near(2)
    go.pass_near(3)
    ge.pass_near(1)
    ge.pass_near(2)
    ge.pass_near(3)

    def during_self(j):
        if j == 0:
            gc_.pass_near(0)
            gc_.pass_near(1)
        elif j == 1:
            gc_.pass_near(2)
            gc_.pass_near(3)
            gp.start_plane()
            gp.pass_plane(0)
            gp.pass_plane(1)
            gp.pass_plane(2)
        elif j == 2:
            gg.start()
            go.finish()

    pair_attend(tok, size.pairs, 512, q, kv, s, e1, rl1, mixed1, bias, during_self)
    part = dot_nt(mixed1[...], WA[:, col["o"]])
    after_self[...] = layer_in[...] + core_sum(wire, part, ca.at[0], cb.at[0])
    n2[...] = rms_forward(after_self[...], gains[1:2]).astype(LOW)
    ge.finish()
    ge.finish_share()
    gc_.finish()

    rows_loop(ctx_enc, 256, project_enc)
    probes[...] = dot(n2[...], WA[:, col["cq"]]).astype(LOW)

    def during_cross(j):
        if j == 0:
            gp.pass_near(0)
            gp.pass_near(1)
            gp.pass_near(2)
            gp.pass_near(3)
    pair_attend(tok, size.pairs, 512, probes, mkv, s, e2, rl2, mixed2, None, during_cross)
    gp.finish()
    part = dot_nt(mixed2[...], WA[:, col["co"]])
    after_cross[...] = after_self[...] + core_sum(wire, part, ca.at[1], cb.at[1])

    N3[plane_rows, :] = rms_forward(after_cross[...], gains[2:3]).astype(LOW)
    spread.start()
    for k in (1, 2, 3):
        level = place.below[k] // 4
        wire.got(WM.at[block_rows(level, 4 * rows), :], mg_level + k - 1)

    def units(k):
        rows_ = spread_rows(k)
        pre = dot(N3[rows_, :], WM[:, : 2 * quarter])
        gate, upper = pre[:, :quarter], pre[:, quarter:]
        value, slope = gelu_parts(gate)
        act[rows_, :] = (value * upper).astype(LOW)
        grad = dot(GR[rows_, :], WM[:, 2 * quarter :])
        GU[rows_, :quarter] = (grad * upper * slope).astype(LOW)
        GU[rows_, quarter:] = (grad * value).astype(LOW)
        PN[rows_, :] = dot_nt(GU[rows_, :], WM[:, : 2 * quarter]).astype(LOW)

    def spread_rows(k):
        return sum_n.rows(k)

    units(0)
    sum_n.start(0)
    for k in (1, 2, 3):
        gg.share(k)
    spread.share(1)
    spread.share(2)
    gg.finish(1)
    spread.finish(1)
    units(1)
    sum_n.start(1)
    gg.finish(2)
    spread.finish(2)
    units(2)
    sum_n.start(2)
    sum_n.middle(1)
    spread.share(3)
    gg.finish(3)
    spread.finish(3)
    units(3)
    sum_n.start(3)
    sum_n.middle(2)

    def back_out(k):
        rows_ = spread_rows(k)
        PO[rows_, :] = dot_nt(act[rows_, :], WM[:, 2 * quarter :]).astype(LOW)

    def unit_grads(cols):
        PM[cols, : 2 * quarter] = dot_tn(N3[:, cols], GU[...]).astype(LOW)
        PM[cols, 2 * quarter :] = dot_tn(GR[:, cols], act[...]).astype(LOW)

    back_out(0)
    sum_n.middle(3)
    sum_n.middle(0)
    for k in (1, 2, 3):
        back_out(k)
    for k in range(4):
        sum_o.start(k)
    rows_loop(model, 128, unit_grads)
    for k in (1, 2, 3):
        wire.send(
            PM.at[block_rows(place.above[k] // 4, 4 * rows), :],
            ml.at[k - 1],
            ms_level + k - 1,
            place.above[k],
        )
    for k in (3, 1, 2, 0):
        sum_o.middle(k)
    sum_n.finish()
    sum_n.finish_core()
    extra, gain_three = rms_backward(after_cross[...], gains[2:3], pn_whole[...].astype(F32))
    cross_grad[...] = out_grad[...] + extra
    low[...] = cross_grad[...].astype(LOW)
    mixed_grad[...] = dot(low[...], WA[:, col["co"]]).astype(LOW)
    def out_grads(left, right, target):
        def body(cols):
            PW[cols, target] = dot_tn(left[:, cols], right[...]).astype(LOW)

        rows_loop(model, 128, body)

    def weight_stream(name, *bufs):
        def out(half, total):
            first, last = size.cuts[name][half]
            WG[:, first:last] = total

        return Scatter(
            wire, weight_view(PW, name), lambda half: bufs[half], out, weight_spare(name)
        )

    def token_out(ref, count):
        def out(half, total):
            ref[half * (count // 2) : (half + 1) * (count // 2), mine] = total

        return out

    sp = weight_stream("co", bp0, bp1)
    so_ = weight_stream("o", bo0, bo1)
    sc = weight_stream("c", bc0, bc1)
    sw = weight_stream("s", bs0, bs1)
    sx = Scatter(
        wire, token_view(XG, tok, place.core), lambda half: bx.at[half], token_out(NG, tok),
        token_spare(bx),
    )
    se = Scatter(
        wire, token_view(EG, enc, place.core), lambda half: be.at[half], token_out(NE, enc),
        token_spare(be),
    )
    x_base, e_base = wire.slots(4), wire.slots(4)
    x_out, e_out = wire.sender(px), wire.sender(pe)

    def pair_start(ref, recv, count, base, k, out):
        at = block_rows(place.below[k] // 4, 4 * count)
        wire.swap(ref.at[at, away], recv.at[at, :], base + k, out)

    def pair_ready(ref, recv, count, base, k):
        at = block_rows(place.below[k] // 4, 4 * count)
        wire.got(recv.at[at, :], base + k)
        ref[at, mine] = (ref[at, mine].astype(F32) + recv[at, :].astype(F32)).astype(LOW)

    x_slot, e_slot, cross_slot, small = (wire.slots(n) for n in (1, 1, 1, 10))

    def units_down():
        total = PM[block_rows(place.level, 4 * rows), :].astype(F32)
        for k in (1, 2, 3):
            wire.got(ml.at[k - 1], ms_level + k - 1)
            total = total + ml[k - 1].astype(F32)
        ps[...] = total.astype(LOW)
        for k, chip in enumerate(plane_chips):
            wire.send(
                ps.at[block_rows(lax.rem(chip, 4), rows), :], mb.at[:, my_part], ms_plane + k, chip
            )
        mb[:, my_part] = ps[block_rows(place.plane, rows), :]

    def units_back():
        for k, chip in enumerate(plane_chips):
            cols = pl.ds(aligned(lax.rem(chip, 4) * size.part, 128), size.part)
            wire.got(mb.at[:, cols], ms_plane + k)

    def result_back():
        sum_o.finish_core()
        layer_out[...] = after_cross[...] + po_whole[...].astype(F32)

    def tokens_back():
        sx.finish()
        wire.swap(NG.at[:, mine], NG.at[:, mine], x_slot)

    def encoder_back():
        se.finish()
        wire.swap(NE.at[:, mine], NE.at[:, mine], e_slot)

    def input_back():
        wire.got(NG.at[:, away], x_slot)
        extra, gain_one = rms_backward(layer_in[...], gains[0:1], NG[...])
        input_grad[...] = self_grad[...] + extra
        s1[...] = jnp.concatenate(
            (gain_one, gain_two, gain_three, jnp.zeros((5, model), F32)), axis=0
        )

    def small_first():
        wire.send(s1, sr.at[0], small, place.fx)
        wire.send(t1, tr.at[0], small + 5, place.fx)

    def small_second():
        wire.got(sr.at[0], small)
        wire.got(tr.at[0], small + 5)
        s2[...] = s1[...] + sr[0]
        t2[...] = t1[...] + tr[0]
        wire.send(s2, sr.at[1], small + 1, place.fy)
        wire.send(t2, tr.at[1], small + 6, place.fy)

    def small_third():
        wire.got(sr.at[1], small + 1)
        wire.got(tr.at[1], small + 6)
        sl[pl.ds(place.level, 1)] = (s2[...] + sr[1])[None]
        tl[pl.ds(place.level, 1)] = (t2[...] + tr[1])[None]
        for k in (1, 2, 3):
            wire.send(sl.at[place.level], sl.at[place.level], small + 1 + k, place.above[k])
            wire.send(tl.at[place.level], tl.at[place.level], small + 6 + k, place.above[k])

    def small_last():
        for k in (1, 2, 3):
            level = place.below[k] // 4
            wire.got(sl.at[level], small + 1 + k)
            wire.got(tl.at[level], small + 6 + k)
        totals[...] = (sl[0] + sl[1]) + (sl[2] + sl[3])
        bias_totals[...] = (tl[0] + tl[1]) + (tl[2] + tl[3])

    out_grads(low, mixed2, col["co"])
    sp.start(1)
    sp.start(2)
    back = PairBack(
        tok, size.pairs, probes, mkv, e2, rl2, mixed2, mixed_grad, mkv_grad, None, qc, gc, dl, dq
    )
    for c in range(ctx_enc // 1024):
        back.chunk(c * 512, 512)
    sp.start(3)
    for c in range(ctx_enc // 1024, ctx_enc // 512):
        back.chunk(c * 512, 512)
    back.finish(q_grad)
    sp.pass_near(1)
    part = dot_nt(q_grad[...], WA[:, col["cq"]])
    ca[2] = part.astype(LOW)
    wire.swap(ca.at[2], cb.at[2], cross_slot)
    out_grads(E, mkv_grad, col["ckv"])
    sp.pass_near(3)
    out_grads(n2, q_grad, col["cq"])
    sc.start(2)

    def enc_rows(rows_):
        EG[rows_, :] = dot_nt(mkv_grad[rows_, :], WA[:, col["ckv"]]).astype(LOW)

    rows_loop(ctx_enc, 256, enc_rows)
    for k in (1, 2, 3, 0):
        pair_start(EG, pe, enc, e_base, k, e_out)
    sc.start(1)
    wire.got(cb.at[2], cross_slot)
    n_grad = ca[2].astype(F32) + cb[2].astype(F32)
    extra, gain_two = rms_backward(after_self[...], gains[1:2], n_grad)
    self_grad[...] = cross_grad[...] + extra
    low[...] = self_grad[...].astype(LOW)
    mixed_grad[...] = dot(low[...], WA[:, col["o"]]).astype(LOW)
    for k in (1, 2, 3, 0):
        pair_ready(EG, pe, enc, e_base, k)
    sc.start(3)
    out_grads(low, mixed1, col["o"])
    se.start(2)
    sp.pass_near(2)
    so_.start(0)
    sp.pass_level(1)
    sc.pass_near(2)
    so_.start(3)
    sc.pass_near(1)
    so_.start(1)

    back = PairBack(
        tok, size.pairs, q, kv, e1, rl1, mixed1, mixed_grad, kv_grad, diag, qc, gc, dl, dq
    )

    def tok_rows(k):
        for part_ in range(2):
            at = pl.ds(aligned(place.below[k] // 4 * 4 * tok + part_ * 2 * tok, 16), 2 * tok)
            XG[at, :] = dot_nt(kv_grad[at, :], WA[:, col["kv"]]).astype(LOW)

    n2[...] = X[here_rows, :]
    back.chunk(place.below[1] // 4 * 4 * tok, 4 * tok)
    tok_rows(1)
    pair_start(XG, px, tok, x_base, 1, x_out)
    back.chunk(place.below[2] // 4 * 4 * tok, 4 * tok)
    tok_rows(2)
    pair_start(XG, px, tok, x_base, 2, x_out)
    pair_ready(XG, px, tok, x_base, 1)
    sc.pass_near(3)
    se.start(0)
    se.start(1)
    back.chunk(place.below[3] // 4 * 4 * tok, 4 * tok)
    tok_rows(3)
    pair_start(XG, px, tok, x_base, 3, x_out)
    pair_ready(XG, px, tok, x_base, 2)
    sc.pass_level(1)
    sx.start(2)
    se.pass_near(2)
    sx.start(1)
    so_.start(2)
    sc.pass_level(2)
    back.chunk(place.level * 4 * tok, 4 * tok)
    back.finish(q_grad)
    tok_rows(0)
    own = dot_nt(q_grad[...], WA[:, col["q"]]) + XG[here_rows, :].astype(F32)
    XG[here_rows, :] = own.astype(LOW)
    pair_start(XG, px, tok, x_base, 0, x_out)
    pair_ready(XG, px, tok, x_base, 3)
    out_grads(n2, q_grad, col["q"])
    pair_ready(XG, px, tok, x_base, 0)
    sx.pass_near(2)
    se.pass_near(1)
    sx.start(3)
    sp.pass_level(2)
    out_grads(X, kv_grad, col["kv"])
    so_.pass_near(1)
    so_.pass_near(2)
    se.start(3)
    sw.start(3)
    sw.start(1)
    sx.pass_level(2)
    so_.pass_near(3)
    se.pass_near(3)
    sx.pass_near(1)
    sx.pass_near(3)
    se.pass_level(1)
    sc.pass_level(3)
    se.pass_level(2)
    so_.pass_level(1)
    so_.pass_level(3)
    sw.start(2)
    sx.pass_level(1)
    sx.start(0)
    sx.pass_level(3)
    so_.pass_near(0)
    sum_o.finish()
    sw.pass_near(1)
    sw.pass_near(2)
    sp.pass_level(3)
    so_.pass_level(2)
    sx.pass_near(0)
    sp.start(0)
    sw.pass_level(1)
    sw.start(0)
    se.pass_level(3)
    se.pass_near(0)
    sums = bucket_sums(ids, diag, table.shape[1])
    t1[...] = jnp.concatenate(
        (sums, jnp.zeros((sums.shape[0], t1.shape[1] - sums.shape[1]), F32)), axis=1
    )

    tokens_back()
    sw.pass_level(2)
    sw.pass_near(3)
    input_back()
    small_first()
    sc.start(0)
    small_second()
    sw.pass_near(0)
    so_.finish()
    sw.pass_level(3)
    units_down()
    sp.pass_near(0)
    sc.pass_near(0)
    small_third()
    sw.finish()
    sp.finish()
    result_back()
    encoder_back()
    small_last()
    units_back()
    sc.finish()
    wire.got(NE.at[:, away], e_slot)
    enc_grad[...] = NE[...]
    for made in (gx, ge, gs, gc_, go, gp):
        made.drain()
    wire.drain()


def emit_kernel(size, layer_out, input_grad, enc_grad, WG, mb, totals, bias_totals, *outs):
    for ref, out in zip((layer_out, input_grad, enc_grad), outs):
        out[...] = ref[...]
    for name, out in zip(size.names, outs[3:]):
        out[...] = WG[:, size.col[name]]
    for i, out in enumerate(outs[11:14]):
        for p in range(4):
            base = p * size.part + i * size.quarter
            out[:, p * size.quarter : (p + 1) * size.quarter] = mb[
                :, base : base + size.quarter
            ].astype(F32)
    outs[14][...] = totals[:3]
    heads, buckets = outs[15].shape
    outs[15][...] = bias_totals[:heads, :buckets]


def quick_device(
    layer_in, encoded, self_query, self_key, self_value, self_out, cross_query, cross_key,
    cross_value, cross_out, gate_proj, up_proj, down_proj, norm_gains, position_bias,
    bucket_ids, block_order, out_grad,
):
    tok, model = layer_in.shape
    enc = encoded.shape[0]
    wide, units = self_query.shape[1], gate_proj.shape[1]
    ctx = block_order.shape[0]
    buckets, heads = position_bias.shape
    size = Sizes(ctx, tok, enc, model, wide, units)
    rows, quarter, pairs = size.rows, size.quarter, size.pairs
    tok_all, enc_all, tok4 = ctx * tok, ctx * enc, 4 * tok

    def vmem(*shape, dtype=LOW):
        return pltpu.VMEM(shape, dtype)

    def full(*shape):
        return pltpu.VMEM(shape, F32)

    def streams(name):
        return [vmem(15, rows, last - first) for first, last in size.cuts[name]]

    ins = {
        "layer_in": layer_in, "encoded": encoded, "sq": self_query, "sk": self_key,
        "sv": self_value, "so": self_out.T, "cq": cross_query, "ck": cross_key,
        "cv": cross_value, "co": cross_out.T, "gate_w": gate_proj, "up_w": up_proj,
        "down_w": down_proj.T, "gains": norm_gains, "table": position_bias.T,
        "buckets": bucket_ids.reshape(ctx, tok), "order": block_order, "out_grad": out_grad,
    }
    outs = {
        "layer_out": ((tok, model), F32), "input_grad": ((tok, model), F32),
        "enc_grad": ((enc, model), F32), "WG": ((rows, size.attn_cols), F32),
        "mb": ((rows, size.mlp_cols), LOW), "totals": ((8, model), F32),
        "bias_totals": ((8, 128), F32),
    }
    (bs0, bs1), (bc0, bc1) = streams("s"), streams("c")
    (bo0, bo1), (bp0, bp1) = streams("o"), streams("co")
    scratch = {
        "WA": vmem(model, size.attn_cols), "WM": vmem(model, size.part),
        "wm": vmem(rows, size.mlp_cols), "X": vmem(tok_all, model), "E": vmem(enc_all, model),
        "GR": vmem(tok4, model), "PW": vmem(model, size.attn_cols),
        "PM": vmem(model, size.part),
        "q": vmem(tok, wide), "kv": vmem(tok_all, 2 * wide), "mkv": vmem(enc_all, 2 * wide),
        "probes": vmem(tok, wide), "s": full(2 * tok, tok_all),
        "e1": vmem(pairs, 2 * tok, tok_all), "e2": vmem(pairs, 2 * tok, enc_all),
        "rl1": full(pairs, 2 * tok, 1), "rl2": full(pairs, 2 * tok, 1),
        "mixed1": vmem(tok, wide), "mixed2": vmem(tok, wide), "table_rows": full(2 * ctx, tok),
        "ids": full(1, 2 * tok_all), "bias": full(8, 2 * tok_all), "diag": full(8, 2 * tok_all),
        "after_self": full(tok, model), "after_cross": full(tok, model),
        "cross_grad": full(tok, model), "self_grad": full(tok, model), "n2": vmem(tok, model),
        "N3": vmem(tok4, model), "act": vmem(tok4, quarter), "GU": vmem(tok4, 2 * quarter),
        "PN": vmem(tok4, model), "PO": vmem(tok4, model), "low": vmem(tok, model),
        "mixed_grad": vmem(tok, wide), "q_grad": vmem(tok, wide),
        "kv_grad": vmem(tok_all, 2 * wide), "mkv_grad": vmem(enc_all, 2 * wide),
        "ca": vmem(3, tok, model), "cb": vmem(3, tok, model),
        "pn_core": vmem(tok4, model // 2), "pn_plane": vmem(3, tok, model // 2),
        "pn_whole": vmem(tok, model), "po_core": vmem(tok4, model // 2),
        "po_plane": vmem(3, tok, model // 2), "po_whole": vmem(tok, model),
        "qc": vmem(pairs, 2 * tok, 128), "gc": vmem(pairs, 2 * tok, 128),
        "dl": full(pairs, 2 * tok, 1), "dq": full(pairs, 2 * tok, 128),
        "bs0": bs0, "bs1": bs1, "bc0": bc0, "bc1": bc1, "bo0": bo0, "bo1": bo1,
        "bp0": bp0, "bp1": bp1, "bx": vmem(2, 15, tok // 2, model // 2),
        "be": vmem(2, 15, enc // 2, model // 2), "px": vmem(tok_all, model // 2),
        "pe": vmem(enc_all, model // 2), "NG": full(tok, model), "NE": full(enc, model),
        "ml": vmem(3, 4 * rows, size.part), "ps": vmem(4 * rows, size.part),
        "s1": full(8, model), "s2": full(8, model), "sr": full(2, 8, model),
        "sl": full(4, 8, model), "t1": full(8, 128), "t2": full(8, 128), "tr": full(2, 8, 128), "tl": full(4, 8, 128), **wire_sems(53, 171),
    }
    names = list(ins) + list(outs) + list(scratch)
    made = pl.pallas_call(
        named(functools.partial(layer_kernel, size), names),
        out_shape=tuple(jax.ShapeDtypeStruct(*spec) for spec in outs.values()),
        in_specs=[
            pl.BlockSpec(memory_space=pltpu.SMEM if name == "order" else pltpu.VMEM)
            for name in ins
        ],
        out_specs=tuple(pl.BlockSpec(memory_space=pltpu.VMEM) for _ in outs),
        scratch_shapes=list(scratch.values()),
        compiler_params=pltpu.CompilerParams(
            collective_id=1, has_side_effects=True, vmem_limit_bytes=VMEM_LIMIT
        ),
    )(*ins.values())
    specs = [
        (tok, model), (tok, model), (enc, model), *((rows, wide),) * 8, *((rows, units),) * 3,
        (3, model), (heads, buckets),
    ]
    parts = pl.pallas_call(
        functools.partial(emit_kernel, size),
        out_shape=tuple(jax.ShapeDtypeStruct(spec, F32) for spec in specs),
        in_specs=[pl.BlockSpec(memory_space=pltpu.VMEM)] * len(made),
        out_specs=tuple(pl.BlockSpec(memory_space=pltpu.VMEM) for _ in specs),
    )(*made)
    named_parts = dict(zip(size.names, parts[3:11]))
    gate, upward, down, gains, bias_grad = parts[11:]
    return (
        *parts[:3], named_parts["q"], named_parts["k"], named_parts["v"], named_parts["o"].T,
        named_parts["cq"], named_parts["ck"], named_parts["cv"], named_parts["co"].T,
        gate, upward, down.T, gains, bias_grad.T,
    )


def quick_fits(mesh):
    return mesh.shape["ctx"] == 16 and mesh.shape["head"] == 2


def as_sent(shard):

    def short(part):
        return part.astype(jnp.bfloat16) if part.dtype == jnp.float32 else part

    return jax.tree.map(short, shard)


def rms_scale(rows, gain):
    return rows * lax.rsqrt(jnp.mean(rows * rows, axis=-1, keepdims=True) + EPS) * gain


def geglu(gate, upper):
    return jax.nn.gelu(gate, approximate=True) * upper


def times(left, right):
    return jnp.dot(left, right, preferred_element_type=jnp.float32)


def left_times(left, right):
    return lax.dot_general(
        left, right, (((0,), (0,)), ((), ())), preferred_element_type=jnp.float32
    )


def right_times(left, right):
    return lax.dot_general(
        left, right, (((1,), (1,)), ((), ())), preferred_element_type=jnp.float32
    )


def join_heads(parts):
    return jax.tree.map(lambda part: part.astype(jnp.float32), lax.psum(as_sent(parts), "head"))


def gather_self(keys_own, values_own):
    return (
        lax.all_gather(keys_own, "ctx", axis=0, tiled=True),
        lax.all_gather(values_own, "ctx", axis=0, tiled=True),
    )


def gather_cross(memory_keys, memory_values):
    return (
        lax.all_gather(memory_keys, "ctx", axis=0, tiled=True),
        lax.all_gather(memory_values, "ctx", axis=0, tiled=True),
    )


def bias_scores(steps, bias_table):
    rises = bias_table[1:] - bias_table[:-1]
    return bias_table[0][:, None, None] + jnp.einsum("qkb,bh->hqk", steps, rises, precision=HIGH)


def bias_grads(score_grad, steps):
    above = jnp.einsum("hqk,qkb->bh", score_grad, steps, precision=HIGH)
    total = jnp.sum(score_grad, axis=(1, 2))
    upper_rows = jnp.concatenate((total[None], above), axis=0)
    lower_rows = jnp.concatenate((above, jnp.zeros((1, above.shape[1]), jnp.float32)), axis=0)
    return upper_rows - lower_rows


def delta_of(mixed, mixed_grad, head_count):
    tok_rows, total_width = mixed.shape
    width = total_width // head_count
    product = mixed.astype(jnp.float32).reshape(tok_rows, head_count, width) * mixed_grad.astype(
        jnp.float32
    ).reshape(tok_rows, head_count, width)
    return jnp.transpose(jnp.sum(product, axis=-1))


def attend_fold(queries, head_count, parts_fn, bias_table):
    tok_rows = queries.shape[0]
    width = queries.shape[1] // head_count
    query3 = queries.reshape(tok_rows, head_count, width)

    def fold(state, pieces, start):
        key_piece, value_piece = pieces
        count = key_piece.shape[0]
        block = math.gcd(count, 512)

        def fold_step(index, inner):
            summed, run_max, run_sum = inner
            key3 = lax.dynamic_slice_in_dim(key_piece, index * block, block, 0).reshape(
                block, head_count, width
            )
            value3 = lax.dynamic_slice_in_dim(value_piece, index * block, block, 0).reshape(
                block, head_count, width
            )
            scores = jnp.einsum("qhe,khe->hqk", query3, key3, preferred_element_type=jnp.float32)
            if parts_fn is not None:
                steps, valid = parts_fn(index * block, block)
                scores = jnp.where(valid[None], scores + bias_scores(steps, bias_table), NEG)
            new_max = jnp.maximum(run_max, jnp.max(scores, axis=-1))
            ratio = jnp.exp(run_max - new_max)
            weights = jnp.exp(scores - new_max[..., None])
            run_sum = run_sum * ratio + jnp.sum(weights, axis=-1)
            summed = summed * ratio[..., None] + jnp.einsum(
                "hqk,khe->hqe",
                weights.astype(jnp.bfloat16),
                value3,
                preferred_element_type=jnp.float32,
            )
            return (summed, new_max, run_sum)

        return lax.fori_loop(0, count // block, fold_step, state)

    return fold


def finish(state):
    summed, run_max, run_sum = state
    head_count, tok_rows, width = summed.shape
    mixed = jnp.transpose(summed / run_sum[..., None], (1, 0, 2)).reshape(
        tok_rows, head_count * width
    )
    return (mixed.astype(jnp.bfloat16), run_max + jnp.log(run_sum))


def attend_back(
    queries, mixed_grad, lse, delta, keys_all, values_all, head_count, parts_fn, bias_table
):
    tok_rows, total_width = queries.shape
    width = total_width // head_count
    query3 = queries.reshape(tok_rows, head_count, width)
    grad3 = mixed_grad.reshape(tok_rows, head_count, width)
    count = keys_all.shape[0]
    block = math.gcd(count, 512)

    def attend_step(carry, index):
        query_grad, bias_grad = carry
        key3 = lax.dynamic_slice_in_dim(keys_all, index * block, block, 0).reshape(
            block, head_count, width
        )
        value3 = lax.dynamic_slice_in_dim(values_all, index * block, block, 0).reshape(
            block, head_count, width
        )
        scores = jnp.einsum("qhe,khe->hqk", query3, key3, preferred_element_type=jnp.float32)
        if parts_fn is not None:
            steps, valid = parts_fn(index * block, block)
            scores = jnp.where(valid[None], scores + bias_scores(steps, bias_table), NEG)
        weights = jnp.exp(scores - lse[..., None])
        weight_grad = jnp.einsum("qhe,khe->hqk", grad3, value3, preferred_element_type=jnp.float32)
        score_grad = weights * (weight_grad - delta[..., None])
        if parts_fn is not None:
            bias_grad = bias_grad + bias_grads(score_grad, steps)
        score_low = score_grad.astype(jnp.bfloat16)
        query_grad = query_grad + jnp.einsum(
            "hqk,khe->qhe", score_low, key3, preferred_element_type=jnp.float32
        )
        stacked = None
        value_term = jnp.einsum(
            "hqk,qhe->khe", weights.astype(jnp.bfloat16), grad3, preferred_element_type=jnp.float32
        )
        key_term = jnp.einsum("hqk,qhe->khe", score_low, query3, preferred_element_type=jnp.float32)
        stacked = jnp.concatenate(
            (key_term.reshape(block, total_width), value_term.reshape(block, total_width)), axis=1
        )
        return ((query_grad, bias_grad), stacked)

    start = (
        jnp.zeros((tok_rows, head_count, width), jnp.float32),
        jnp.zeros(bias_table.shape, jnp.float32),
    )
    (query_grad, bias_grad), terms = lax.scan(attend_step, start, jnp.arange(count // block))
    query_grad = query_grad.reshape(tok_rows, total_width).astype(jnp.bfloat16)
    terms = terms.reshape(count, 2 * total_width)
    return (query_grad, bias_grad, terms)


def per_device(
    layer_in,
    encoded,
    self_query,
    self_key,
    self_value,
    self_out,
    cross_query,
    cross_key,
    cross_value,
    cross_out,
    gate_proj,
    up_proj,
    down_proj,
    norm_gains,
    position_bias,
    bucket_ids,
    block_order,
    out_grad,
):
    low = jnp.bfloat16
    tok_rows = layer_in.shape[0]
    bucket_count, head_count = position_bias.shape
    block_count = block_order.shape[0]
    full_weights = (
        lax.all_gather(self_query, "ctx", axis=0, tiled=True),
        lax.all_gather(self_key, "ctx", axis=0, tiled=True),
        lax.all_gather(self_value, "ctx", axis=0, tiled=True),
        lax.all_gather(self_out, "ctx", axis=1, tiled=True),
        lax.all_gather(cross_query, "ctx", axis=0, tiled=True),
        lax.all_gather(cross_key, "ctx", axis=0, tiled=True),
        lax.all_gather(cross_value, "ctx", axis=0, tiled=True),
        lax.all_gather(cross_out, "ctx", axis=1, tiled=True),
        lax.all_gather(gate_proj, "ctx", axis=0, tiled=True),
        lax.all_gather(up_proj, "ctx", axis=0, tiled=True),
        lax.all_gather(down_proj, "ctx", axis=1, tiled=True),
    )
    (
        query_full,
        key_full,
        value_full,
        output_full,
        probe_full,
        lookup_full,
        recall_full,
        merge_full,
        gate_full,
        upward_full,
        down_full,
    ) = full_weights
    boundaries = jnp.arange(1, bucket_count, dtype=jnp.int32)
    starts = jnp.sum((bucket_ids[None, :] < boundaries[:, None]).astype(jnp.int32), axis=1)
    block_ids = jnp.arange(block_count, dtype=jnp.int32)
    here = lax.axis_index("ctx")
    own_block = jnp.sum(jnp.where(block_ids == here, block_order, 0))
    query_pos = own_block * tok_rows + jnp.arange(tok_rows, dtype=jnp.int32)

    def position_of(rows_index):
        slot = rows_index // tok_rows
        owner = jnp.sum(
            jnp.where(slot[:, None] == block_ids[None, :], block_order[None, :], 0), axis=1
        )
        return owner * tok_rows + rows_index % tok_rows

    def pair_parts(first_pos, second_pos):
        dist = first_pos[:, None] - second_pos[None, :]
        steps = (dist[:, :, None] >= starts[None, None, :]).astype(jnp.float32)
        return (steps, dist >= 0)

    def causal_parts(key_start, count):
        return pair_parts(query_pos, position_of(key_start + jnp.arange(count, dtype=jnp.int32)))

    normed_one = rms_scale(layer_in, norm_gains[0]).astype(low)
    queries = times(normed_one, query_full).astype(low)
    keys_own = times(normed_one, key_full).astype(low)
    values_own = times(normed_one, value_full).astype(low)
    memory_keys = times(encoded, lookup_full).astype(low)
    memory_values = times(encoded, recall_full).astype(low)
    total_width = queries.shape[1]
    width = total_width // head_count
    start_state = (
        jnp.zeros((head_count, tok_rows, width), jnp.float32),
        jnp.full((head_count, tok_rows), NEG, jnp.float32),
        jnp.zeros((head_count, tok_rows), jnp.float32),
    )
    self_fold = attend_fold(queries, head_count, causal_parts, position_bias)
    self_state = self_fold(
        start_state,
        (
            lax.all_gather(keys_own, "ctx", axis=0, tiled=True),
            lax.all_gather(values_own, "ctx", axis=0, tiled=True),
        ),
        jnp.int32(0),
    )
    mixed_one, lse_one = finish(self_state)
    after_self = layer_in + join_heads(times(mixed_one, output_full))
    normed_two = rms_scale(after_self, norm_gains[1]).astype(low)
    probes = times(normed_two, probe_full).astype(low)
    cross_fold = attend_fold(probes, head_count, None, position_bias)
    cross_state = cross_fold(
        start_state,
        (
            lax.all_gather(memory_keys, "ctx", axis=0, tiled=True),
            lax.all_gather(memory_values, "ctx", axis=0, tiled=True),
        ),
        jnp.int32(0),
    )
    mixed_two, lse_two = finish(cross_state)
    after_cross = after_self + join_heads(times(mixed_two, merge_full))
    normed_three = rms_scale(after_cross, norm_gains[2]).astype(low)
    gate_pre = times(normed_three, gate_full)
    upper = times(normed_three, upward_full)
    activated = geglu(gate_pre, upper).astype(low)
    layer_out = after_cross + join_heads(times(activated, down_full))
    grad_rows = out_grad.astype(low)
    down_wgrad = left_times(activated, grad_rows)
    act_grad = right_times(grad_rows, down_full)
    geglu_out, geglu_pull = jax.vjp(geglu, gate_pre, upper)
    gate_grad, upper_grad = geglu_pull(act_grad)
    gate_grad = gate_grad.astype(low)
    upper_grad = upper_grad.astype(low)
    gate_wgrad = left_times(normed_three, gate_grad)
    up_wgrad = left_times(normed_three, upper_grad)
    normed_three_grad = join_heads(
        right_times(gate_grad, gate_full) + right_times(upper_grad, upward_full)
    )
    norm_out, norm_pull = jax.vjp(rms_scale, after_cross, norm_gains[2])
    cross_extra, gain_three = norm_pull(normed_three_grad)
    cross_grad = out_grad + cross_extra
    cross_rows = cross_grad.astype(low)
    merge_wgrad = left_times(mixed_two, cross_rows)
    mixed_two_grad = right_times(cross_rows, merge_full).astype(low)
    delta_two = delta_of(mixed_two, mixed_two_grad, head_count)
    memory_all = gather_cross(memory_keys, memory_values)
    probe_grad, unused_bias, cross_terms = attend_back(
        probes,
        mixed_two_grad,
        lse_two,
        delta_two,
        memory_all[0],
        memory_all[1],
        head_count,
        None,
        position_bias,
    )
    cross_terms = lax.psum_scatter(cross_terms, "ctx", scatter_dimension=0, tiled=True)
    memory_key_grad = cross_terms[:, :total_width].astype(low)
    memory_value_grad = cross_terms[:, total_width:].astype(low)
    probe_wgrad = left_times(normed_two, probe_grad)
    lookup_wgrad = left_times(encoded, memory_key_grad)
    recall_wgrad = left_times(encoded, memory_value_grad)
    normed_two_grad, encoded_grad = join_heads(
        (
            right_times(probe_grad, probe_full),
            right_times(memory_key_grad, lookup_full) + right_times(memory_value_grad, recall_full),
        )
    )
    norm_out, norm_pull = jax.vjp(rms_scale, after_self, norm_gains[1])
    self_extra, gain_two = norm_pull(normed_two_grad)
    self_grad = cross_grad + self_extra
    self_rows = self_grad.astype(low)
    output_wgrad = left_times(mixed_one, self_rows)
    mixed_one_grad = right_times(self_rows, output_full).astype(low)
    delta_one = delta_of(mixed_one, mixed_one_grad, head_count)
    sequence_all = gather_self(keys_own, values_own)
    query_grad, bias_grad, self_terms = attend_back(
        queries,
        mixed_one_grad,
        lse_one,
        delta_one,
        sequence_all[0],
        sequence_all[1],
        head_count,
        causal_parts,
        position_bias,
    )
    self_terms = lax.psum_scatter(self_terms, "ctx", scatter_dimension=0, tiled=True)
    key_grad = self_terms[:, :total_width].astype(low)
    value_grad = self_terms[:, total_width:].astype(low)
    query_wgrad = left_times(normed_one, query_grad)
    key_wgrad = left_times(normed_one, key_grad)
    value_wgrad = left_times(normed_one, value_grad)
    normed_one_grad = join_heads(
        right_times(query_grad, query_full)
        + right_times(key_grad, key_full)
        + right_times(value_grad, value_full)
    )
    norm_out, norm_pull = jax.vjp(rms_scale, layer_in, norm_gains[0])
    input_extra, gain_one = norm_pull(normed_one_grad)
    input_grad = self_grad + input_extra
    weight_sums = (
        lax.psum_scatter(query_wgrad, "ctx", scatter_dimension=0, tiled=True),
        lax.psum_scatter(key_wgrad, "ctx", scatter_dimension=0, tiled=True),
        lax.psum_scatter(value_wgrad, "ctx", scatter_dimension=0, tiled=True),
        lax.psum_scatter(output_wgrad, "ctx", scatter_dimension=1, tiled=True),
        lax.psum_scatter(probe_wgrad, "ctx", scatter_dimension=0, tiled=True),
        lax.psum_scatter(lookup_wgrad, "ctx", scatter_dimension=0, tiled=True),
        lax.psum_scatter(recall_wgrad, "ctx", scatter_dimension=0, tiled=True),
        lax.psum_scatter(merge_wgrad, "ctx", scatter_dimension=1, tiled=True),
        lax.psum_scatter(gate_wgrad, "ctx", scatter_dimension=0, tiled=True),
        lax.psum_scatter(up_wgrad, "ctx", scatter_dimension=0, tiled=True),
        lax.psum_scatter(down_wgrad, "ctx", scatter_dimension=1, tiled=True),
    )
    gains_sum, bias_sum = lax.psum((jnp.stack((gain_one, gain_two, gain_three)), bias_grad), "ctx")
    return (layer_out, input_grad, encoded_grad) + tuple(weight_sums) + (gains_sum, bias_sum)


def solution(mesh):
    body = quick_device if quick_fits(mesh) else per_device
    placed = (
        P("ctx", None),
        P("ctx", None),
        P("ctx", "head"),
        P("ctx", "head"),
        P("ctx", "head"),
        P("head", "ctx"),
        P("ctx", "head"),
        P("ctx", "head"),
        P("ctx", "head"),
        P("head", "ctx"),
        P("ctx", "head"),
        P("ctx", "head"),
        P("head", "ctx"),
        P(),
        P(None, "head"),
        P(),
        P(),
        P("ctx", None),
    )
    return jax.shard_map(
        body,
        mesh=mesh,
        in_specs=placed,
        out_specs=(
            P("ctx", None),
            P("ctx", None),
            P("ctx", None),
            P("ctx", "head"),
            P("ctx", "head"),
            P("ctx", "head"),
            P("head", "ctx"),
            P("ctx", "head"),
            P("ctx", "head"),
            P("ctx", "head"),
            P("head", "ctx"),
            P("ctx", "head"),
            P("ctx", "head"),
            P("head", "ctx"),
            P(),
            P(None, "head"),
        ),
        check_vma=False,
    )
```

```python
import functools
import math

import jax
import jax.numpy as jnp
from jax import lax
from jax.experimental import pallas as pl
from jax.experimental.pallas import tpu as pltpu
from jax.sharding import PartitionSpec as P

EPS = 1e-06
NEG = -1e30
HIGH = lax.Precision.HIGHEST
LOW = jnp.bfloat16
F32 = jnp.float32
MESH = pl.DeviceIdType.MESH
VMEM_LIMIT = 66_000_000


def dot(left, right, **kw):
    return jnp.dot(left, right, preferred_element_type=F32, **kw)


def dot_nt(left, right, **kw):
    return lax.dot_general(left, right, (((1,), (1,)), ((), ())), preferred_element_type=F32, **kw)


def dot_tn(left, right, **kw):
    return lax.dot_general(left, right, (((0,), (0,)), ((), ())), preferred_element_type=F32, **kw)


def rms_forward(rows, gain):
    return rows * lax.rsqrt(jnp.mean(rows * rows, axis=-1, keepdims=True) + EPS) * gain


def rms_backward(rows, gain, grad):
    scale = lax.rsqrt(jnp.mean(rows * rows, axis=-1, keepdims=True) + EPS)
    scaled = gain * grad
    inner = jnp.mean(scaled * rows, axis=-1, keepdims=True)
    row_grad = scale * scaled - rows * (scale * scale * scale * inner)
    gain_grad = jnp.sum(grad * rows * scale, axis=0, keepdims=True)
    return row_grad, gain_grad


def aligned(value, step):
    return value if isinstance(value, int) else pl.multiple_of(value, step)


class Place:
    def __init__(self, count):
        self.count = count
        self.here = lax.axis_index("ctx")
        self.core = lax.axis_index("head")
        self.other = 1 - self.core
        self.plane = lax.rem(self.here, 4)
        self.level = self.here // 4
        self.fx = self.flip(self.here, 0)
        self.fy = self.flip(self.here, 1)
        self.fxy = self.flip(self.fx, 1)
        self.above = [lax.rem(self.here + 4 * k, count) for k in range(4)]
        self.below = [lax.rem(self.here + count - 4 * k, count) for k in range(4)]
        self.top = count // 4 - 1
        bottom, head = self.level == 0, self.level == self.top
        self.nearest = (
            jnp.where(bottom, 3, 1),
            jnp.where(bottom, 2, jnp.where(head, 2, 3)),
            jnp.where(bottom, 1, jnp.where(head, 3, 2)),
        )

    def flip(self, index, axis):
        if axis == 0:
            return index + 1 - 2 * lax.rem(index, 2)
        return index + 2 - 4 * lax.rem(index // 2, 2)

    def near(self, half):
        return (self.fx, self.fy) if half == 0 else (self.fy, self.fx)

    def signal(self, chips):
        barrier = pltpu.get_barrier_semaphore()
        for chip in chips:
            pl.semaphore_signal(
                barrier, inc=1, device_id=(chip, self.core), device_id_type=MESH
            )
        pl.semaphore_signal(barrier, inc=1, device_id=(self.here, self.other), device_id_type=MESH)

    def meet(self, count):
        pl.semaphore_wait(pltpu.get_barrier_semaphore(), count)


class Wire:
    def __init__(self, place, send_sem, recv_sem):
        self.place, self.send_sem, self.recv_sem = place, send_sem, recv_sem
        self.used = 0
        self.send_used = 0
        self.pending = []

    def slots(self, count):
        base = self.used
        self.used += count
        assert self.used <= self.recv_sem.shape[0], self.used
        return base

    def sender(self, whole=None):
        slot = self.send_used
        self.send_used += 1
        assert slot < self.send_sem.shape[0], slot
        if whole is not None:
            self.pending.append((slot, whole))
        return slot

    def copy(self, src, dst, out, slot, chip, core):
        return pltpu.make_async_remote_copy(
            src_ref=src,
            dst_ref=dst,
            send_sem=self.send_sem.at[out],
            recv_sem=self.recv_sem.at[slot],
            device_id=(chip, core),
            device_id_type=MESH,
        )

    def send(self, src, dst, slot, chip=None, core=None, out=None):
        chip = self.place.here if chip is None else chip
        core = self.place.core if core is None else core
        if out is None:
            out = self.sender(src)
        self.copy(src, dst, out, slot, chip, core).start()

    def swap(self, src, dst, slot, out=None):
        self.send(src, dst, slot, None, self.place.other, out)

    def got(self, dst, slot):
        place = self.place
        self.copy(dst, dst, 0, slot, place.here, place.other).wait_recv()

    def sent(self, whole, out):
        place = self.place
        self.copy(whole, whole, out, 0, place.here, place.other).wait_send()

    def drain(self):
        for out, whole in self.pending:
            self.sent(whole, out)
        self.pending = []


class Gather:
    def __init__(self, wire, view, share, spare):
        self.wire, self.view, self.share, self.spare = wire, view, share, spare
        self.halves = range(2)
        self.base = wire.slots(8)
        self.out = wire.sender(spare(12))
        self.line_out = wire.sender()
        if share:
            self.side = wire.slots(1)
            self.side_out = wire.sender(spare(15))

    def _line(self, half, block, slot, chip):
        ref = self.view(half, block)
        self.wire.send(ref, ref, self.base + slot, chip, out=self.line_out)

    def _out(self, half, block, slot, chip):
        ref = self.view(half, block)
        self.wire.send(ref, ref, self.base + slot, chip, out=self.out)

    def _give(self, half, block):
        if self.share:
            ref = self.view(half, block)
            self.wire.swap(ref, ref, self.side, self.side_out)

    def start_level(self):
        place = self.wire.place
        for half in self.halves:

            @pl.when(place.level < place.top)
            def _():
                self._line(half, place.here, 0, place.here + 4)

            @pl.when(place.level > 0)
            def _():
                self._line(half, place.here, 2, place.here - 4)

    def start_plane(self):
        place = self.wire.place
        for half in self.halves:
            near, far = place.near(half)
            self._out(half, place.here, 3, near)
            self._out(half, place.here, 7, far)

    def _level_block(self, step):
        place = self.wire.place
        k = place.nearest[step]
        return k, lax.rem(place.here + place.count - 4 * k, place.count)

    def pass_line(self, step):
        place = self.wire.place
        k, block = self._level_block(step)
        rising = place.level >= k
        onward = jnp.where(rising, place.level < place.top, place.level > 0)
        chip = jnp.where(rising, place.here + 4, place.here - 4)
        slot = jnp.where(rising, k, k - 2)
        self.wire.got(self.spare(1), self.base + k - 1)
        for half in self.halves:

            @pl.when(onward)
            def _():
                self._line(half, block, slot, chip)

    def pass_plane(self, step):
        place = self.wire.place
        k, block = self._level_block(step)
        for half in self.halves:
            near, far = place.near(half)
            self._out(half, block, 3 + k, near)
            self._out(half, block, 7, far)
            self._give(half, block)

    def pass_near(self, step):
        place = self.wire.place
        k = (0, *place.nearest)[step]
        block = lax.rem(place.here + place.count - 4 * k, place.count)
        self.wire.got(self.spare(1), self.base + 3 + k)
        for half in self.halves:
            _, far = place.near(half)
            arrived = place.flip(block, half)
            self._out(half, arrived, 7, far)
            self._give(half, arrived)

    def finish(self):
        place = self.wire.place
        self.wire.got(self.spare(8), self.base + 7)
        for half in self.halves:
            if self.share:
                for k in range(4):
                    block = place.flip(place.below[k], 1 - half)
                    self._give(half, block)
                    self._give(half, place.flip(block, half))

    def finish_share(self):
        self.wire.got(self.spare(15), self.side)

    def drain(self):
        place = self.wire.place

        @pl.when(jnp.logical_or(place.level == 0, place.level == place.top))
        def _():
            self.wire.sent(self.spare(1), self.line_out)

        @pl.when(jnp.logical_and(place.level > 0, place.level < place.top))
        def _():
            self.wire.sent(self.spare(5), self.line_out)


class Scatter:
    def __init__(self, wire, view, buf, out, spare):
        self.wire, self.view, self.buf, self.out, self.spare = wire, view, buf, out, spare
        self.halves = range(2)
        self.base = wire.slots(9)
        self.send_slot = wire.sender(spare(15))

    def _send(self, half, block, place_in, slot, chip):
        self.wire.send(
            self.view(half, block),
            self.buf(half).at[place_in],
            self.base + slot,
            chip,
            out=self.send_slot,
        )

    def start(self, k):
        place = self.wire.place
        for half in self.halves:
            _, far = place.near(half)
            away = place.flip(place.below[k], 1 - half)
            for pair, block in ((1, place.flip(away, half)), (0, away)):
                self._send(half, block, 2 * k + pair, k, far)

    def pass_near(self, k):
        place = self.wire.place
        self.wire.got(self.spare(2), self.base + k)
        for half in self.halves:
            near, _ = place.near(half)
            block = place.flip(place.below[k], half)
            ref = self.view(half, block)
            ref[...] = (ref[...].astype(F32) + self.buf(half)[2 * k + 1].astype(F32)).astype(LOW)
            self._send(half, block, 8 + k, 4 + k, near)

    def pass_level(self, k):
        place = self.wire.place
        self.wire.got(self.spare(1), self.base + 4 + k)
        for half in self.halves:
            ref = self.view(half, place.below[k])
            ref[...] = self._sum(half, k).astype(LOW)
            self._send(half, place.below[k], 11 + k, 8, place.below[k])

    def _sum(self, half, k):
        buf = self.buf(half)
        total = self.view(half, self.wire.place.below[k])[...].astype(F32)
        return total + buf[2 * k].astype(F32) + buf[8 + k].astype(F32)

    def finish(self):
        self.wire.got(self.spare(1), self.base + 4)
        self.wire.got(self.spare(3), self.base + 8)
        for half in self.halves:
            total = self._sum(half, 0)
            for k in (1, 2, 3):
                total = total + self.buf(half)[11 + k].astype(F32)
            self.out(half, total)


def lane_split(rows):
    lane = lax.broadcasted_iota(jnp.int32, rows.shape, 1)
    low = lane < rows.shape[1] // 2
    zero = jnp.zeros_like(rows)
    return jnp.concatenate((jnp.where(low, rows, zero), jnp.where(low, zero, rows)), axis=0)


def lane_join(rows):
    count, width = rows.shape[0] // 2, rows.shape[1]
    lane = lax.broadcasted_iota(jnp.int32, (count, width), 1)
    return jnp.where(lane < width // 2, rows[:count], rows[count:])


def pair_attend(tok, pairs, chunk, q_ref, kv_ref, s_ref, e_ref, rl_ref, mixed_ref, bias_ref, between):
    keys = kv_ref.shape[0]
    total = pairs * 128

    for j in range(pairs):
        cols = slice(j * 128, (j + 1) * 128)
        vcols = slice(total + j * 128, total + (j + 1) * 128)
        q_cat = lane_split(q_ref[:, cols])

        def score(c, top):
            rows = pl.ds(aligned(c * chunk, chunk), chunk)
            s = dot_nt(q_cat, kv_ref[rows, cols])
            if bias_ref is not None:
                tiles = []
                for half in range(2):
                    row = []
                    for b in range(chunk // tok):
                        lanes = pl.ds(aligned((c * (chunk // tok) + b) * 2 * tok, 128), 2 * tok)
                        vec = bias_ref[2 * j + half : 2 * j + half + 1, lanes]
                        wide = jnp.broadcast_to(vec, (tok, 2 * tok))
                        row.append(pltpu.roll(wide, 0, 1, stride=1, stride_axis=0)[:, :tok])
                    tiles.append(jnp.concatenate(row, axis=1))
                s = s + jnp.concatenate(tiles, axis=0)
            s_ref[:, rows] = s
            for b in range(chunk // 128):
                top = jnp.maximum(top, s[:, b * 128 : (b + 1) * 128])
            return top

        top = lax.fori_loop(0, keys // chunk, score, jnp.full((2 * tok, 128), NEG, F32))
        peak = jnp.max(top, axis=1, keepdims=True)

        def weigh(c, state):
            acc, run = state
            rows = pl.ds(aligned(c * chunk, chunk), chunk)
            e = jnp.exp(s_ref[:, rows] - peak)
            for b in range(chunk // 128):
                run = run + e[:, b * 128 : (b + 1) * 128]
            low = e.astype(LOW)
            e_ref[j, :, rows] = low
            return (acc + dot(low, kv_ref[rows, vcols]), run)

        zero = jnp.zeros((2 * tok, 128), F32)
        acc, run = lax.fori_loop(0, keys // chunk, weigh, (zero, zero))
        rl = 1.0 / jnp.sum(run, axis=1, keepdims=True)
        rl_ref[j] = rl
        mixed_ref[:, cols] = lane_join(acc * rl).astype(LOW)
        between(j)


class PairBack:
    def __init__(self, tok, pairs, q, kv, e, rl, mixed, grad, kv_grad, diag, qc, gc, dl, dq):
        self.tok, self.pairs, self.kv, self.e = tok, pairs, kv, e
        self.kv_grad, self.diag, self.qc, self.gc, self.dl, self.dq = kv_grad, diag, qc, gc, dl, dq
        self.total = pairs * 128
        for j in range(pairs):
            cols = slice(j * 128, (j + 1) * 128)
            rl_j = rl[j]
            grads = lane_split(grad[:, cols].astype(F32))
            qc[j] = lane_split(q[:, cols])
            gc[j] = (grads * rl_j).astype(LOW)
            values = lane_split(mixed[:, cols].astype(F32))
            dl[j] = jnp.sum(grads * values, axis=1, keepdims=True) * rl_j
            dq[j] = jnp.zeros(dq.shape[1:], F32)

    def chunk(self, start, count):
        tok, kv, qc, gc = self.tok, self.kv, self.qc, self.gc
        rows = pl.ds(aligned(start, count), count)
        flip = (
            lax.broadcasted_iota(jnp.int32, (tok, tok), 0)
            + lax.broadcasted_iota(jnp.int32, (tok, tok), 1)
            == tok - 1
        ).astype(LOW)

        def one_pair(j, carry):
            cols = pl.ds(aligned(j * 128, 128), 128)
            vcols = pl.ds(aligned(self.total + j * 128, 128), 128)
            low_e = self.e[j, :, rows]
            dp = dot_nt(gc[j], kv[rows, vcols])
            ds = (low_e.astype(F32) * (dp - self.dl[j])).astype(LOW)
            if self.diag is not None:
                for half in range(2):
                    turned = dot(flip, ds[half * tok : (half + 1) * tok])
                    for b in range(count // tok):
                        tile = turned[:, b * tok : (b + 1) * tok]
                        wide = jnp.concatenate((tile, jnp.zeros_like(tile)), axis=1)
                        wide = pltpu.roll(wide, tok + 1, 1, stride=1, stride_axis=0)
                        lanes = pl.ds(aligned(2 * start + b * 2 * tok, 128), 2 * tok)
                        self.diag[pl.ds(2 * j + half, 1), lanes] = jnp.sum(
                            wide, axis=0, keepdims=True
                        )
            self.kv_grad[rows, cols] = dot_tn(ds, qc[j]).astype(LOW)
            self.kv_grad[rows, vcols] = dot_tn(low_e, gc[j]).astype(LOW)
            self.dq[j] = self.dq[j] + dot(ds, kv[rows, cols])
            return carry

        lax.fori_loop(0, self.pairs, one_pair, 0)

    def finish(self, q_grad):
        for j in range(self.pairs):
            q_grad[:, j * 128 : (j + 1) * 128] = lane_join(self.dq[j]).astype(LOW)


def bucket_rows(buckets_ref, order_ref, here, table_rows, ids_ref):
    count, tok = buckets_ref.shape
    turn = (
        lax.broadcasted_iota(jnp.int32, (tok, tok), 0)
        + lax.broadcasted_iota(jnp.int32, (tok, tok), 1)
        == tok - 1
    ).astype(LOW)
    table_rows[:count, :] = jnp.full((count, tok), -1.0, F32)
    table_rows[count:, :] = dot(buckets_ref[...].astype(LOW), turn)
    own = order_ref[here]
    for block in range(count):
        at = own - order_ref[block] + count
        wide = jnp.concatenate(
            (table_rows[pl.ds(at - 1, 1), :], table_rows[pl.ds(at, 1), :]), axis=1
        )
        ids_ref[:, block * 2 * tok : (block + 1) * 2 * tok] = pltpu.roll(wide, 1, 1)


def bucket_masks(ids_ref, buckets):
    ids = ids_ref[...]
    row = lax.broadcasted_iota(jnp.int32, (buckets, ids.shape[1]), 0).astype(F32)
    return ids, (row == ids).astype(F32)


def bias_vectors(ids_ref, table_ref, bias_ref):
    heads, buckets = table_ref.shape
    ids, mask = bucket_masks(ids_ref, buckets)
    vec = dot(table_ref[...], mask, precision=HIGH)
    bias_ref[:heads, :] = jnp.where(ids >= 0, vec, NEG)


def bucket_sums(ids_ref, diag_ref, buckets):
    _, mask = bucket_masks(ids_ref, buckets)
    return dot_nt(diag_ref[...], mask, precision=HIGH)


def rows_loop(count, step, body):
    def one(index, carry):
        body(pl.ds(aligned(index * step, step), step))
        return carry

    lax.fori_loop(0, count // step, one, 0)


GELU_A = 0.7978845608028654
GELU_B = 0.044715


def gelu_parts(value):
    square = value * value
    wave = jnp.tanh(GELU_A * (value + GELU_B * value * square))
    half = 0.5 * (1.0 + wave)
    slope = half + 0.5 * value * (1.0 - wave * wave) * (GELU_A * (1.0 + 3.0 * GELU_B * square))
    return value * half, slope


def core_sum(wire, part, out_buf, in_buf):
    slot = wire.slots(1)
    out_buf[...] = part.astype(LOW)
    wire.swap(out_buf, in_buf, slot)
    wire.got(in_buf, slot)
    return out_buf[...].astype(F32) + in_buf[...].astype(F32)


class PlaneSum:
    def __init__(self, wire, tok, part, core_buf, plane_buf, whole):
        self.wire, self.tok = wire, tok
        self.out = wire.sender(part)
        self.part, self.core_buf, self.plane_buf, self.whole = part, core_buf, plane_buf, whole
        self.base = wire.slots(8)
        self.half = whole.shape[1] // 2
        place = wire.place
        self.chips = (place.here, place.fx, place.fy, place.fxy)

    def cols(self, core):
        return pl.ds(aligned(core * self.half, 128), self.half)

    def rows(self, k):
        return pl.ds(aligned(lax.rem(self.chips[k], 4) * self.tok, self.tok), self.tok)

    def start(self, k):
        away = self.cols(self.wire.place.other)
        rows = self.rows(k)
        self.wire.swap(self.part.at[rows, away], self.core_buf.at[rows, :], self.base + k, self.out)

    def middle(self, k):
        wire, rows = self.wire, self.rows(k)
        wire.got(self.core_buf.at[rows, :], self.base + k)
        total = self.part[rows, self.cols(wire.place.core)].astype(F32)
        total = total + self.core_buf[rows, :].astype(F32)
        self.core_buf[rows, :] = total.astype(LOW)
        if k:
            wire.send(
                self.core_buf.at[rows, :],
                self.plane_buf.at[k - 1],
                self.base + 3 + k,
                self.chips[k],
                out=self.out,
            )

    def finish(self):
        place, wire = self.wire.place, self.wire
        total = self.core_buf[self.rows(0), :].astype(F32)
        for k in (1, 2, 3):
            wire.got(self.plane_buf.at[k - 1], self.base + 3 + k)
            total = total + self.plane_buf[k - 1].astype(F32)
        mine = self.cols(place.core)
        self.whole[:, mine] = total.astype(LOW)
        wire.swap(self.whole.at[:, mine], self.whole.at[:, mine], self.base + 7, self.out)

    def finish_core(self):
        self.wire.got(self.whole.at[:, self.cols(self.wire.place.other)], self.base + 7)


class PlaneGather:
    def __init__(self, wire, tok, ref):
        self.wire, self.tok, self.ref = wire, tok, ref
        self.half = ref.shape[1] // 2
        self.base = wire.slots(8)
        self.out = wire.sender(ref.at[: 3 * tok, :])
        place = wire.place
        self.chips = (place.here, place.fx, place.fy, place.fxy)

    def view(self, k, core):
        rows = pl.ds(aligned(lax.rem(self.chips[k], 4) * self.tok, self.tok), self.tok)
        return self.ref.at[rows, pl.ds(aligned(core * self.half, 128), self.half)]

    def start(self):
        own = self.view(0, self.wire.place.core)
        for k in (1, 2, 3):
            self.wire.send(own, own, self.base + k, self.chips[k], out=self.out)

    def share(self, k):
        ref = self.view(k, self.wire.place.core)
        self.wire.got(ref, self.base + k)
        self.wire.swap(ref, ref, self.base + 4 + k, self.out)

    def finish(self, k):
        self.wire.got(self.view(k, self.wire.place.other), self.base + 4 + k)


class Sizes:
    def __init__(self, ctx, tok, enc, model, wide, units):
        self.ctx, self.tok, self.enc, self.model, self.wide = ctx, tok, enc, model, wide
        self.rows = model // ctx
        self.units = units
        self.quarter = units // 4
        self.pairs = wide // 128
        self.levels = ctx // 4
        self.attn_cols = 8 * wide
        self.mlp_cols = 3 * units
        self.part = 3 * self.quarter
        self.names = ("q", "k", "v", "cq", "ck", "cv", "o", "co")
        self.col = {n: slice(i * wide, (i + 1) * wide) for i, n in enumerate(self.names)}
        self.col["kv"] = slice(wide, 3 * wide)
        self.col["ckv"] = slice(4 * wide, 6 * wide)
        self.cuts = {
            "s": self.halves(0, 3 * wide, 0),
            "c": self.halves(3 * wide, 6 * wide, 1),
            "o": self.halves(6 * wide, 7 * wide, 0),
            "co": self.halves(7 * wide, 8 * wide, 1),
        }

    def halves(self, first, last, up):
        tiles = (last - first) // 128
        middle = first + (tiles + up) // 2 * 128
        return ((first, middle), (middle, last))


def named(kernel, names):
    def body(*refs):
        kernel(**dict(zip(names, refs, strict=True)))

    return body


def wire_sems(send, recv):
    return {
        "send_sem": pltpu.SemaphoreType.DMA((send,)),
        "recv_sem": pltpu.SemaphoreType.DMA((recv,)),
    }


def layer_kernel(
    size, layer_src, encoded, sq, sk, sv, so, cq, ck, cv, co, gate_w, up_w, down_w, gains_src,
    table_src, buckets_src, order_src, out_grad_src,
    layer_out, input_grad, enc_grad, WG, mb, totals, bias_totals,
    layer_in, gains, table, buckets, order, out_grad, WA, WM, wm, X, E, GR, PW, PM,
    q, kv, mkv, probes, s, e1, e2, rl1, rl2, mixed1, mixed2, table_rows, ids, bias, diag,
    after_self, after_cross, cross_grad, self_grad, n2, N3, act, GU, PN, PO, low, mixed_grad,
    q_grad, kv_grad, mkv_grad, ca, cb, pn_core, pn_plane, pn_whole, po_core, po_plane, po_whole,
    qc, gc, dl, dq, bs0, bs1, bc0, bc1, bo0, bo1, bp0, bp1, bx, be, px, pe, NG, NE, ml, ps,
    s1, s2, sr, sl, t1, t2, tr, tl, local, send_sem, recv_sem,
):
    place = Place(size.ctx)
    wire = Wire(place, send_sem, recv_sem)
    tok, enc, rows, half_d = size.tok, size.enc, size.rows, size.model // 2
    col, model, quarter = size.col, size.model, size.quarter
    ctx_tok, ctx_enc = X.shape[0], E.shape[0]
    plane_chips = (place.fx, place.fy, place.fxy)
    XG, EG = kv, mkv

    def block_rows(block, count):
        return pl.ds(aligned(block * count, 16), count)

    here_rows = block_rows(place.here, tok)
    own_weights = block_rows(place.here, rows)
    my_part = pl.ds(aligned(place.plane * size.part, 128), size.part)
    mine = pl.ds(aligned(place.core * half_d, 128), half_d)
    away = pl.ds(aligned(place.other * half_d, 128), half_d)

    def token_view(ref, count, core):
        def view(half, block):
            return ref.at[
                pl.ds(aligned(block * count + half * (count // 2), 16), count // 2),
                pl.ds(aligned(core * half_d, 128), half_d),
            ]

        return view

    def weight_view(ref, name):
        def view(half, block):
            first, last = size.cuts[name][half]
            return ref.at[block_rows(block, rows), first:last]

        return view

    def token_spare(buf):
        return lambda count: buf.at[:, 0:count]

    def weight_spare(name):
        (first, _), (_, last) = size.cuts[name]
        return lambda count: WA.at[0 : count * rows, first:last]

    gx = Gather(wire, token_view(X, tok, place.core), True, token_spare(bx))
    ge = Gather(wire, token_view(E, enc, place.core), True, token_spare(be))
    gs, gc_, go, gp = (
        Gather(wire, weight_view(WA, name), False, weight_spare(name))
        for name in ("s", "c", "o", "co")
    )
    gg = PlaneGather(wire, tok, GR)
    spread = PlaneGather(wire, tok, N3)
    sum_n = PlaneSum(wire, tok, PN, pn_core, pn_plane, pn_whole)
    sum_o = PlaneSum(wire, tok, PO, po_core, po_plane, po_whole)
    mg_plane, mg_level, ms_level, ms_plane = (wire.slots(3) for _ in range(4))

    def units_out():
        for k, chip in enumerate(plane_chips):
            wire.send(
                wm.at[:, pl.ds(aligned(lax.rem(chip, 4) * size.part, 128), size.part)],
                WM.at[own_weights, :],
                mg_plane + k,
                chip,
            )

    def units_up():
        for k, chip in enumerate(plane_chips):
            wire.got(WM.at[block_rows(chip, rows), :], mg_plane + k)
        own = WM.at[block_rows(place.level, 4 * rows), :]
        for k in (1, 2, 3):
            wire.send(own, own, mg_level + k - 1, place.above[k])

    place.signal(place.above[1:] + list(plane_chips))
    attention = size.attn_cols
    first = 3 * size.wide

    def load(slot, *pairs):
        for src, dst in pairs:
            pltpu.make_async_copy(src, dst, local.at[slot]).start()

    def loaded(slot, whole):
        pltpu.make_async_copy(whole, whole, local.at[slot]).wait()

    def own_columns(name):
        return WA.at[own_weights, col[name]]

    load(0, (layer_src, layer_in))
    load(1, (gains_src, gains))
    load(2, *((ref, own_columns(n)) for n, ref in (("q", sq), ("k", sk), ("v", sv))))
    load(3, *((ref, own_columns(n)) for n, ref in (("cq", cq), ("ck", ck), ("cv", cv), ("o", so), ("co", co))))
    load(4, (encoded, E.at[block_rows(place.here, enc), :]))
    load(
        5,
        *(
            (ref.at[:, p * quarter : (p + 1) * quarter], wm.at[:, base : base + quarter])
            for p in range(4)
            for i, ref in enumerate((gate_w, up_w, down_w))
            for base in (p * size.part + i * quarter,)
        ),
    )
    load(6, (out_grad_src, out_grad))
    load(7, (table_src, table))
    load(8, (buckets_src, buckets))
    load(9, (order_src, order))
    loaded(0, layer_in)
    loaded(1, gains)
    X[here_rows, :] = rms_forward(layer_in[...], gains[0:1]).astype(LOW)
    loaded(2, WA.at[own_weights, 0:first])
    place.meet(7)
    gx.start_level()
    gs.start_level()
    gx.start_plane()
    gs.start_plane()
    loaded(3, WA.at[own_weights, first:attention])
    loaded(4, E.at[block_rows(place.here, enc), :])
    loaded(5, wm)
    WM[own_weights, :] = wm[:, my_part]
    loaded(6, out_grad)
    plane_rows = block_rows(place.plane, tok)
    GR[plane_rows, :] = out_grad[...].astype(LOW)
    loaded(7, table)
    loaded(8, buckets)
    loaded(9, order)
    gx.pass_near(0)
    gx.pass_line(0)
    gx.pass_plane(0)
    gs.pass_near(0)
    gs.pass_line(0)
    gs.pass_plane(0)
    gx.pass_line(1)
    gx.pass_plane(1)
    gs.pass_line(1)
    gs.pass_plane(1)
    go.start_level()
    ge.start_level()
    gx.pass_near(1)
    gs.pass_near(1)
    gx.pass_line(2)
    gx.pass_plane(2)
    gs.pass_line(2)
    gs.pass_plane(2)
    gc_.start_level()
    gp.start_level()
    gx.pass_near(2)
    gs.pass_near(2)
    gx.pass_near(3)
    gs.pass_near(3)
    go.start_plane()
    ge.start_plane()
    gc_.start_plane()
    units_out()
    bucket_rows(buckets, order, place.here, table_rows, ids)
    bias_vectors(ids, table, bias)
    diag[...] = jnp.zeros_like(diag)
    go.pass_line(0)
    go.pass_plane(0)
    ge.pass_line(0)
    ge.pass_plane(0)
    gc_.pass_line(0)
    gp.pass_line(0)
    go.pass_line(1)
    go.pass_plane(1)
    ge.pass_line(1)
    ge.pass_plane(1)
    gc_.pass_line(1)
    gp.pass_line(1)
    go.pass_line(2)
    go.pass_plane(2)
    ge.pass_line(2)
    ge.pass_plane(2)
    gc_.pass_line(2)
    gp.pass_line(2)
    gc_.pass_plane(0)
    gc_.pass_plane(1)
    gc_.pass_plane(2)
    gx.finish()
    go.pass_near(0)
    ge.pass_near(0)
    gx.finish_share()
    gs.finish()
    units_up()

    def project(rows_):
        kv[rows_, :] = dot(X[rows_, :], WA[:, col["kv"]]).astype(LOW)

    def project_enc(rows_):
        mkv[rows_, :] = dot(E[rows_, :], WA[:, col["ckv"]]).astype(LOW)

    def project_level(level):
        for part_ in range(2):
            project(slice((2 * level + part_) * 2 * tok, (2 * level + part_ + 1) * 2 * tok))

    q[...] = dot(X[here_rows, :], WA[:, col["q"]]).astype(LOW)
    project_level(0)
    project_level(1)
    project_level(2)
    project_level(3)
    go.pass_near(1)
    go.pass_near(2)
    go.pass_near(3)
    ge.pass_near(1)
    ge.pass_near(2)
    ge.pass_near(3)

    def during_self(j):
        if j == 0:
            gc_.pass_near(0)
            gc_.pass_near(1)
        elif j == 1:
            gc_.pass_near(2)
            gc_.pass_near(3)
            gp.start_plane()
            gp.pass_plane(0)
            gp.pass_plane(1)
            gp.pass_plane(2)
        elif j == 2:
            go.finish()

    pair_attend(tok, size.pairs, 512, q, kv, s, e1, rl1, mixed1, bias, during_self)
    part = dot_nt(mixed1[...], WA[:, col["o"]])
    after_self[...] = layer_in[...] + core_sum(wire, part, ca.at[0], cb.at[0])
    n2[...] = rms_forward(after_self[...], gains[1:2]).astype(LOW)
    ge.finish()
    ge.finish_share()
    gc_.finish()

    rows_loop(ctx_enc, 256, project_enc)
    probes[...] = dot(n2[...], WA[:, col["cq"]]).astype(LOW)

    def during_cross(j):
        if j == 0:
            gp.pass_near(0)
            gp.pass_near(1)
            gp.pass_near(2)
            gp.pass_near(3)
            gg.start()
    pair_attend(tok, size.pairs, 512, probes, mkv, s, e2, rl2, mixed2, None, during_cross)
    gp.finish()
    part = dot_nt(mixed2[...], WA[:, col["co"]])
    after_cross[...] = after_self[...] + core_sum(wire, part, ca.at[1], cb.at[1])

    N3[plane_rows, :] = rms_forward(after_cross[...], gains[2:3]).astype(LOW)
    spread.start()
    for k in (1, 2, 3):
        level = place.below[k] // 4
        wire.got(WM.at[block_rows(level, 4 * rows), :], mg_level + k - 1)

    def units(k):
        rows_ = spread_rows(k)
        pre = dot(N3[rows_, :], WM[:, : 2 * quarter])
        gate, upper = pre[:, :quarter], pre[:, quarter:]
        value, slope = gelu_parts(gate)
        act[rows_, :] = (value * upper).astype(LOW)
        grad = dot(GR[rows_, :], WM[:, 2 * quarter :])
        GU[rows_, :quarter] = (grad * upper * slope).astype(LOW)
        GU[rows_, quarter:] = (grad * value).astype(LOW)
        PN[rows_, :] = dot_nt(GU[rows_, :], WM[:, : 2 * quarter]).astype(LOW)

    def spread_rows(k):
        return sum_n.rows(k)

    units(0)
    sum_n.start(0)
    for k in (1, 2, 3):
        gg.share(k)
    spread.share(1)
    spread.share(2)
    gg.finish(1)
    spread.finish(1)
    units(1)
    sum_n.start(1)
    gg.finish(2)
    spread.finish(2)
    units(2)
    sum_n.start(2)
    sum_n.middle(1)
    spread.share(3)
    gg.finish(3)
    spread.finish(3)
    units(3)
    sum_n.start(3)
    sum_n.middle(2)

    def back_out(k):
        rows_ = spread_rows(k)
        PO[rows_, :] = dot_nt(act[rows_, :], WM[:, 2 * quarter :]).astype(LOW)

    def unit_grads(cols):
        PM[cols, : 2 * quarter] = dot_tn(N3[:, cols], GU[...]).astype(LOW)
        PM[cols, 2 * quarter :] = dot_tn(GR[:, cols], act[...]).astype(LOW)

    back_out(0)
    sum_n.middle(3)
    sum_n.middle(0)
    for k in (1, 2, 3):
        back_out(k)
    for k in range(4):
        sum_o.start(k)
    rows_loop(model, 128, unit_grads)
    for k in (1, 2, 3):
        wire.send(
            PM.at[block_rows(place.above[k] // 4, 4 * rows), :],
            ml.at[k - 1],
            ms_level + k - 1,
            place.above[k],
        )
    for k in (3, 1, 2, 0):
        sum_o.middle(k)
    sum_n.finish()
    sum_n.finish_core()
    extra, gain_three = rms_backward(after_cross[...], gains[2:3], pn_whole[...].astype(F32))
    cross_grad[...] = out_grad[...] + extra
    low[...] = cross_grad[...].astype(LOW)
    mixed_grad[...] = dot(low[...], WA[:, col["co"]]).astype(LOW)
    def out_grads(left, right, target):
        def body(cols):
            PW[cols, target] = dot_tn(left[:, cols], right[...]).astype(LOW)

        rows_loop(model, 128, body)

    def weight_stream(name, *bufs):
        def out(half, total):
            first, last = size.cuts[name][half]
            WG[:, first:last] = total

        return Scatter(
            wire, weight_view(PW, name), lambda half: bufs[half], out, weight_spare(name)
        )

    def token_out(ref, count):
        def out(half, total):
            ref[half * (count // 2) : (half + 1) * (count // 2), mine] = total

        return out

    sp = weight_stream("co", bp0, bp1)
    so_ = weight_stream("o", bo0, bo1)
    sc = weight_stream("c", bc0, bc1)
    sw = weight_stream("s", bs0, bs1)
    sx = Scatter(
        wire, token_view(XG, tok, place.core), lambda half: bx.at[half], token_out(NG, tok),
        token_spare(bx),
    )
    se = Scatter(
        wire, token_view(EG, enc, place.core), lambda half: be.at[half], token_out(NE, enc),
        token_spare(be),
    )
    x_base, e_base = wire.slots(4), wire.slots(4)
    x_out, e_out = wire.sender(px), wire.sender(pe)

    def pair_start(ref, recv, count, base, k, out):
        at = block_rows(place.below[k] // 4, 4 * count)
        wire.swap(ref.at[at, away], recv.at[at, :], base + k, out)

    def pair_ready(ref, recv, count, base, k):
        at = block_rows(place.below[k] // 4, 4 * count)
        wire.got(recv.at[at, :], base + k)
        ref[at, mine] = (ref[at, mine].astype(F32) + recv[at, :].astype(F32)).astype(LOW)

    x_slot, e_slot, cross_slot, small = (wire.slots(n) for n in (1, 1, 1, 10))

    def units_down():
        total = PM[block_rows(place.level, 4 * rows), :].astype(F32)
        for k in (1, 2, 3):
            wire.got(ml.at[k - 1], ms_level + k - 1)
            total = total + ml[k - 1].astype(F32)
        ps[...] = total.astype(LOW)
        for k, chip in enumerate(plane_chips):
            wire.send(
                ps.at[block_rows(lax.rem(chip, 4), rows), :], mb.at[:, my_part], ms_plane + k, chip
            )
        mb[:, my_part] = ps[block_rows(place.plane, rows), :]

    def units_back():
        for k, chip in enumerate(plane_chips):
            cols = pl.ds(aligned(lax.rem(chip, 4) * size.part, 128), size.part)
            wire.got(mb.at[:, cols], ms_plane + k)

    def result_back():
        sum_o.finish_core()
        layer_out[...] = after_cross[...] + po_whole[...].astype(F32)

    def tokens_back():
        sx.finish()
        wire.swap(NG.at[:, mine], NG.at[:, mine], x_slot)

    def encoder_back():
        se.finish()
        wire.swap(NE.at[:, mine], NE.at[:, mine], e_slot)

    def input_back():
        wire.got(NG.at[:, away], x_slot)
        extra, gain_one = rms_backward(layer_in[...], gains[0:1], NG[...])
        input_grad[...] = self_grad[...] + extra
        s1[...] = jnp.concatenate(
            (gain_one, gain_two, gain_three, jnp.zeros((5, model), F32)), axis=0
        )

    def small_first():
        wire.send(s1, sr.at[0], small, place.fx)
        wire.send(t1, tr.at[0], small + 5, place.fx)

    def small_second():
        wire.got(sr.at[0], small)
        wire.got(tr.at[0], small + 5)
        s2[...] = s1[...] + sr[0]
        t2[...] = t1[...] + tr[0]
        wire.send(s2, sr.at[1], small + 1, place.fy)
        wire.send(t2, tr.at[1], small + 6, place.fy)

    def small_third():
        wire.got(sr.at[1], small + 1)
        wire.got(tr.at[1], small + 6)
        sl[pl.ds(place.level, 1)] = (s2[...] + sr[1])[None]
        tl[pl.ds(place.level, 1)] = (t2[...] + tr[1])[None]
        for k in (1, 2, 3):
            wire.send(sl.at[place.level], sl.at[place.level], small + 1 + k, place.above[k])
            wire.send(tl.at[place.level], tl.at[place.level], small + 6 + k, place.above[k])

    def small_last():
        for k in (1, 2, 3):
            level = place.below[k] // 4
            wire.got(sl.at[level], small + 1 + k)
            wire.got(tl.at[level], small + 6 + k)
        totals[...] = (sl[0] + sl[1]) + (sl[2] + sl[3])
        bias_totals[...] = (tl[0] + tl[1]) + (tl[2] + tl[3])

    out_grads(low, mixed2, col["co"])
    sp.start(1)
    sp.start(2)
    back = PairBack(
        tok, size.pairs, probes, mkv, e2, rl2, mixed2, mixed_grad, mkv_grad, None, qc, gc, dl, dq
    )
    for c in range(ctx_enc // 1024):
        back.chunk(c * 512, 512)
    sp.start(3)
    for c in range(ctx_enc // 1024, ctx_enc // 512):
        back.chunk(c * 512, 512)
    back.finish(q_grad)
    sp.pass_near(1)
    part = dot_nt(q_grad[...], WA[:, col["cq"]])
    ca[2] = part.astype(LOW)
    wire.swap(ca.at[2], cb.at[2], cross_slot)
    out_grads(E, mkv_grad, col["ckv"])
    sp.pass_near(3)
    out_grads(n2, q_grad, col["cq"])
    sc.start(2)

    def enc_rows(rows_):
        EG[rows_, :] = dot_nt(mkv_grad[rows_, :], WA[:, col["ckv"]]).astype(LOW)

    rows_loop(ctx_enc, 256, enc_rows)
    for k in (1, 2, 3, 0):
        pair_start(EG, pe, enc, e_base, k, e_out)
    sc.start(1)
    wire.got(cb.at[2], cross_slot)
    n_grad = ca[2].astype(F32) + cb[2].astype(F32)
    extra, gain_two = rms_backward(after_self[...], gains[1:2], n_grad)
    self_grad[...] = cross_grad[...] + extra
    low[...] = self_grad[...].astype(LOW)
    mixed_grad[...] = dot(low[...], WA[:, col["o"]]).astype(LOW)
    for k in (1, 2, 3, 0):
        pair_ready(EG, pe, enc, e_base, k)
    sc.start(3)
    out_grads(low, mixed1, col["o"])
    se.start(2)
    sp.pass_near(2)
    so_.start(0)
    sp.pass_level(1)
    sc.pass_near(2)
    so_.start(3)
    sc.pass_near(1)
    so_.start(1)

    back = PairBack(
        tok, size.pairs, q, kv, e1, rl1, mixed1, mixed_grad, kv_grad, diag, qc, gc, dl, dq
    )

    def tok_rows(k):
        for part_ in range(2):
            at = pl.ds(aligned(place.below[k] // 4 * 4 * tok + part_ * 2 * tok, 16), 2 * tok)
            XG[at, :] = dot_nt(kv_grad[at, :], WA[:, col["kv"]]).astype(LOW)

    n2[...] = X[here_rows, :]
    back.chunk(place.below[1] // 4 * 4 * tok, 4 * tok)
    tok_rows(1)
    pair_start(XG, px, tok, x_base, 1, x_out)
    back.chunk(place.below[2] // 4 * 4 * tok, 4 * tok)
    tok_rows(2)
    pair_start(XG, px, tok, x_base, 2, x_out)
    pair_ready(XG, px, tok, x_base, 1)
    sc.pass_near(3)
    se.start(0)
    se.start(1)
    back.chunk(place.below[3] // 4 * 4 * tok, 4 * tok)
    tok_rows(3)
    pair_start(XG, px, tok, x_base, 3, x_out)
    pair_ready(XG, px, tok, x_base, 2)
    sc.pass_level(1)
    sx.start(2)
    se.pass_near(2)
    sx.start(1)
    so_.start(2)
    sc.pass_level(2)
    back.chunk(place.level * 4 * tok, 4 * tok)
    back.finish(q_grad)
    tok_rows(0)
    own = dot_nt(q_grad[...], WA[:, col["q"]]) + XG[here_rows, :].astype(F32)
    XG[here_rows, :] = own.astype(LOW)
    pair_start(XG, px, tok, x_base, 0, x_out)
    pair_ready(XG, px, tok, x_base, 3)
    out_grads(n2, q_grad, col["q"])
    pair_ready(XG, px, tok, x_base, 0)
    sx.pass_near(2)
    se.pass_near(1)
    sx.start(3)
    sp.pass_level(2)
    out_grads(X, kv_grad, col["kv"])
    so_.pass_near(1)
    so_.pass_near(2)
    se.start(3)
    sw.start(3)
    sw.start(1)
    sx.pass_level(2)
    so_.pass_near(3)
    se.pass_near(3)
    sx.pass_near(1)
    sx.pass_near(3)
    se.pass_level(1)
    sc.pass_level(3)
    se.pass_level(2)
    so_.pass_level(1)
    so_.pass_level(3)
    sw.start(2)
    sx.pass_level(1)
    sx.start(0)
    sx.pass_level(3)
    so_.pass_near(0)
    sum_o.finish()
    sw.pass_near(1)
    sw.pass_near(2)
    sp.pass_level(3)
    so_.pass_level(2)
    sx.pass_near(0)
    sp.start(0)
    sw.pass_level(1)
    sw.start(0)
    se.pass_level(3)
    se.pass_near(0)
    sums = bucket_sums(ids, diag, table.shape[1])
    t1[...] = jnp.concatenate(
        (sums, jnp.zeros((sums.shape[0], t1.shape[1] - sums.shape[1]), F32)), axis=1
    )

    tokens_back()
    sw.pass_level(2)
    sw.pass_near(3)
    input_back()
    small_first()
    sc.start(0)
    small_second()
    sw.pass_near(0)
    so_.finish()
    sw.pass_level(3)
    units_down()
    sp.pass_near(0)
    sc.pass_near(0)
    small_third()
    sw.finish()
    sp.finish()
    result_back()
    encoder_back()
    small_last()
    units_back()
    sc.finish()
    wire.got(NE.at[:, away], e_slot)
    enc_grad[...] = NE[...]
    for made in (gx, ge, gs, gc_, go, gp):
        made.drain()
    wire.drain()


def emit_kernel(size, layer_out, input_grad, enc_grad, WG, mb, totals, bias_totals, *outs):
    for ref, out in zip((layer_out, input_grad, enc_grad), outs):
        out[...] = ref[...]
    for name, out in zip(size.names, outs[3:]):
        out[...] = WG[:, size.col[name]]
    for i, out in enumerate(outs[11:14]):
        for p in range(4):
            base = p * size.part + i * size.quarter
            out[:, p * size.quarter : (p + 1) * size.quarter] = mb[
                :, base : base + size.quarter
            ].astype(F32)
    outs[14][...] = totals[:3]
    heads, buckets = outs[15].shape
    outs[15][...] = bias_totals[:heads, :buckets]


def quick_device(
    layer_in, encoded, self_query, self_key, self_value, self_out, cross_query, cross_key,
    cross_value, cross_out, gate_proj, up_proj, down_proj, norm_gains, position_bias,
    bucket_ids, block_order, out_grad,
):
    tok, model = layer_in.shape
    enc = encoded.shape[0]
    wide, units = self_query.shape[1], gate_proj.shape[1]
    ctx = block_order.shape[0]
    buckets, heads = position_bias.shape
    size = Sizes(ctx, tok, enc, model, wide, units)
    rows, quarter, pairs = size.rows, size.quarter, size.pairs
    tok_all, enc_all, tok4 = ctx * tok, ctx * enc, 4 * tok

    def vmem(*shape, dtype=LOW):
        return pltpu.VMEM(shape, dtype)

    def full(*shape):
        return pltpu.VMEM(shape, F32)

    def streams(name):
        return [vmem(15, rows, last - first) for first, last in size.cuts[name]]

    ins = {
        "layer_src": layer_in, "encoded": encoded, "sq": self_query, "sk": self_key,
        "sv": self_value, "so": self_out.T, "cq": cross_query, "ck": cross_key,
        "cv": cross_value, "co": cross_out.T, "gate_w": gate_proj, "up_w": up_proj,
        "down_w": down_proj.T, "gains_src": norm_gains, "table_src": position_bias.T,
        "buckets_src": bucket_ids.reshape(ctx, tok), "order_src": block_order,
        "out_grad_src": out_grad,
    }
    outs = {
        "layer_out": ((tok, model), F32), "input_grad": ((tok, model), F32),
        "enc_grad": ((enc, model), F32), "WG": ((rows, size.attn_cols), F32),
        "mb": ((rows, size.mlp_cols), LOW), "totals": ((8, model), F32),
        "bias_totals": ((8, 128), F32),
    }
    (bs0, bs1), (bc0, bc1) = streams("s"), streams("c")
    (bo0, bo1), (bp0, bp1) = streams("o"), streams("co")
    scratch = {
        "layer_in": full(tok, model), "gains": full(*norm_gains.shape),
        "table": full(heads, buckets), "buckets": pltpu.VMEM((ctx, tok), jnp.int32),
        "order": pltpu.SMEM((ctx,), jnp.int32), "out_grad": full(tok, model),
        "WA": vmem(model, size.attn_cols), "WM": vmem(model, size.part),
        "wm": vmem(rows, size.mlp_cols), "X": vmem(tok_all, model), "E": vmem(enc_all, model),
        "GR": vmem(tok4, model), "PW": vmem(model, size.attn_cols),
        "PM": vmem(model, size.part),
        "q": vmem(tok, wide), "kv": vmem(tok_all, 2 * wide), "mkv": vmem(enc_all, 2 * wide),
        "probes": vmem(tok, wide), "s": full(2 * tok, tok_all),
        "e1": vmem(pairs, 2 * tok, tok_all), "e2": vmem(pairs, 2 * tok, enc_all),
        "rl1": full(pairs, 2 * tok, 1), "rl2": full(pairs, 2 * tok, 1),
        "mixed1": vmem(tok, wide), "mixed2": vmem(tok, wide), "table_rows": full(2 * ctx, tok),
        "ids": full(1, 2 * tok_all), "bias": full(8, 2 * tok_all), "diag": full(8, 2 * tok_all),
        "after_self": full(tok, model), "after_cross": full(tok, model),
        "cross_grad": full(tok, model), "self_grad": full(tok, model), "n2": vmem(tok, model),
        "N3": vmem(tok4, model), "act": vmem(tok4, quarter), "GU": vmem(tok4, 2 * quarter),
        "PN": vmem(tok4, model), "PO": vmem(tok4, model), "low": vmem(tok, model),
        "mixed_grad": vmem(tok, wide), "q_grad": vmem(tok, wide),
        "kv_grad": vmem(tok_all, 2 * wide), "mkv_grad": vmem(enc_all, 2 * wide),
        "ca": vmem(3, tok, model), "cb": vmem(3, tok, model),
        "pn_core": vmem(tok4, model // 2), "pn_plane": vmem(3, tok, model // 2),
        "pn_whole": vmem(tok, model), "po_core": vmem(tok4, model // 2),
        "po_plane": vmem(3, tok, model // 2), "po_whole": vmem(tok, model),
        "qc": vmem(pairs, 2 * tok, 128), "gc": vmem(pairs, 2 * tok, 128),
        "dl": full(pairs, 2 * tok, 1), "dq": full(pairs, 2 * tok, 128),
        "bs0": bs0, "bs1": bs1, "bc0": bc0, "bc1": bc1, "bo0": bo0, "bo1": bo1,
        "bp0": bp0, "bp1": bp1, "bx": vmem(2, 15, tok // 2, model // 2),
        "be": vmem(2, 15, enc // 2, model // 2), "px": vmem(tok_all, model // 2),
        "pe": vmem(enc_all, model // 2), "NG": full(tok, model), "NE": full(enc, model),
        "ml": vmem(3, 4 * rows, size.part), "ps": vmem(4 * rows, size.part),
        "s1": full(8, model), "s2": full(8, model), "sr": full(2, 8, model),
        "sl": full(4, 8, model), "t1": full(8, 128), "t2": full(8, 128), "tr": full(2, 8, 128), "tl": full(4, 8, 128),
        "local": pltpu.SemaphoreType.DMA((10,)), **wire_sems(53, 171),
    }
    names = list(ins) + list(outs) + list(scratch)
    made = pl.pallas_call(
        named(functools.partial(layer_kernel, size), names),
        out_shape=tuple(jax.ShapeDtypeStruct(*spec) for spec in outs.values()),
        in_specs=[
            pl.BlockSpec(memory_space=pl.ANY)
            for name in ins
        ],
        out_specs=tuple(pl.BlockSpec(memory_space=pltpu.VMEM) for _ in outs),
        scratch_shapes=list(scratch.values()),
        compiler_params=pltpu.CompilerParams(
            collective_id=1, has_side_effects=True, vmem_limit_bytes=VMEM_LIMIT
        ),
    )(*ins.values())
    specs = [
        (tok, model), (tok, model), (enc, model), *((rows, wide),) * 8, *((rows, units),) * 3,
        (3, model), (heads, buckets),
    ]
    parts = pl.pallas_call(
        functools.partial(emit_kernel, size),
        out_shape=tuple(jax.ShapeDtypeStruct(spec, F32) for spec in specs),
        in_specs=[pl.BlockSpec(memory_space=pltpu.VMEM)] * len(made),
        out_specs=tuple(pl.BlockSpec(memory_space=pltpu.VMEM) for _ in specs),
    )(*made)
    named_parts = dict(zip(size.names, parts[3:11]))
    gate, upward, down, gains, bias_grad = parts[11:]
    return (
        *parts[:3], named_parts["q"], named_parts["k"], named_parts["v"], named_parts["o"].T,
        named_parts["cq"], named_parts["ck"], named_parts["cv"], named_parts["co"].T,
        gate, upward, down.T, gains, bias_grad.T,
    )


def quick_fits(mesh):
    return mesh.shape["ctx"] == 16 and mesh.shape["head"] == 2


def as_sent(shard):

    def short(part):
        return part.astype(jnp.bfloat16) if part.dtype == jnp.float32 else part

    return jax.tree.map(short, shard)


def rms_scale(rows, gain):
    return rows * lax.rsqrt(jnp.mean(rows * rows, axis=-1, keepdims=True) + EPS) * gain


def geglu(gate, upper):
    return jax.nn.gelu(gate, approximate=True) * upper


def times(left, right):
    return jnp.dot(left, right, preferred_element_type=jnp.float32)


def left_times(left, right):
    return lax.dot_general(
        left, right, (((0,), (0,)), ((), ())), preferred_element_type=jnp.float32
    )


def right_times(left, right):
    return lax.dot_general(
        left, right, (((1,), (1,)), ((), ())), preferred_element_type=jnp.float32
    )


def join_heads(parts):
    return jax.tree.map(lambda part: part.astype(jnp.float32), lax.psum(as_sent(parts), "head"))


def gather_self(keys_own, values_own):
    return (
        lax.all_gather(keys_own, "ctx", axis=0, tiled=True),
        lax.all_gather(values_own, "ctx", axis=0, tiled=True),
    )


def gather_cross(memory_keys, memory_values):
    return (
        lax.all_gather(memory_keys, "ctx", axis=0, tiled=True),
        lax.all_gather(memory_values, "ctx", axis=0, tiled=True),
    )


def bias_scores(steps, bias_table):
    rises = bias_table[1:] - bias_table[:-1]
    return bias_table[0][:, None, None] + jnp.einsum("qkb,bh->hqk", steps, rises, precision=HIGH)


def bias_grads(score_grad, steps):
    above = jnp.einsum("hqk,qkb->bh", score_grad, steps, precision=HIGH)
    total = jnp.sum(score_grad, axis=(1, 2))
    upper_rows = jnp.concatenate((total[None], above), axis=0)
    lower_rows = jnp.concatenate((above, jnp.zeros((1, above.shape[1]), jnp.float32)), axis=0)
    return upper_rows - lower_rows


def delta_of(mixed, mixed_grad, head_count):
    tok_rows, total_width = mixed.shape
    width = total_width // head_count
    product = mixed.astype(jnp.float32).reshape(tok_rows, head_count, width) * mixed_grad.astype(
        jnp.float32
    ).reshape(tok_rows, head_count, width)
    return jnp.transpose(jnp.sum(product, axis=-1))


def attend_fold(queries, head_count, parts_fn, bias_table):
    tok_rows = queries.shape[0]
    width = queries.shape[1] // head_count
    query3 = queries.reshape(tok_rows, head_count, width)

    def fold(state, pieces, start):
        key_piece, value_piece = pieces
        count = key_piece.shape[0]
        block = math.gcd(count, 512)

        def fold_step(index, inner):
            summed, run_max, run_sum = inner
            key3 = lax.dynamic_slice_in_dim(key_piece, index * block, block, 0).reshape(
                block, head_count, width
            )
            value3 = lax.dynamic_slice_in_dim(value_piece, index * block, block, 0).reshape(
                block, head_count, width
            )
            scores = jnp.einsum("qhe,khe->hqk", query3, key3, preferred_element_type=jnp.float32)
            if parts_fn is not None:
                steps, valid = parts_fn(index * block, block)
                scores = jnp.where(valid[None], scores + bias_scores(steps, bias_table), NEG)
            new_max = jnp.maximum(run_max, jnp.max(scores, axis=-1))
            ratio = jnp.exp(run_max - new_max)
            weights = jnp.exp(scores - new_max[..., None])
            run_sum = run_sum * ratio + jnp.sum(weights, axis=-1)
            summed = summed * ratio[..., None] + jnp.einsum(
                "hqk,khe->hqe",
                weights.astype(jnp.bfloat16),
                value3,
                preferred_element_type=jnp.float32,
            )
            return (summed, new_max, run_sum)

        return lax.fori_loop(0, count // block, fold_step, state)

    return fold


def finish(state):
    summed, run_max, run_sum = state
    head_count, tok_rows, width = summed.shape
    mixed = jnp.transpose(summed / run_sum[..., None], (1, 0, 2)).reshape(
        tok_rows, head_count * width
    )
    return (mixed.astype(jnp.bfloat16), run_max + jnp.log(run_sum))


def attend_back(
    queries, mixed_grad, lse, delta, keys_all, values_all, head_count, parts_fn, bias_table
):
    tok_rows, total_width = queries.shape
    width = total_width // head_count
    query3 = queries.reshape(tok_rows, head_count, width)
    grad3 = mixed_grad.reshape(tok_rows, head_count, width)
    count = keys_all.shape[0]
    block = math.gcd(count, 512)

    def attend_step(carry, index):
        query_grad, bias_grad = carry
        key3 = lax.dynamic_slice_in_dim(keys_all, index * block, block, 0).reshape(
            block, head_count, width
        )
        value3 = lax.dynamic_slice_in_dim(values_all, index * block, block, 0).reshape(
            block, head_count, width
        )
        scores = jnp.einsum("qhe,khe->hqk", query3, key3, preferred_element_type=jnp.float32)
        if parts_fn is not None:
            steps, valid = parts_fn(index * block, block)
            scores = jnp.where(valid[None], scores + bias_scores(steps, bias_table), NEG)
        weights = jnp.exp(scores - lse[..., None])
        weight_grad = jnp.einsum("qhe,khe->hqk", grad3, value3, preferred_element_type=jnp.float32)
        score_grad = weights * (weight_grad - delta[..., None])
        if parts_fn is not None:
            bias_grad = bias_grad + bias_grads(score_grad, steps)
        score_low = score_grad.astype(jnp.bfloat16)
        query_grad = query_grad + jnp.einsum(
            "hqk,khe->qhe", score_low, key3, preferred_element_type=jnp.float32
        )
        stacked = None
        value_term = jnp.einsum(
            "hqk,qhe->khe", weights.astype(jnp.bfloat16), grad3, preferred_element_type=jnp.float32
        )
        key_term = jnp.einsum("hqk,qhe->khe", score_low, query3, preferred_element_type=jnp.float32)
        stacked = jnp.concatenate(
            (key_term.reshape(block, total_width), value_term.reshape(block, total_width)), axis=1
        )
        return ((query_grad, bias_grad), stacked)

    start = (
        jnp.zeros((tok_rows, head_count, width), jnp.float32),
        jnp.zeros(bias_table.shape, jnp.float32),
    )
    (query_grad, bias_grad), terms = lax.scan(attend_step, start, jnp.arange(count // block))
    query_grad = query_grad.reshape(tok_rows, total_width).astype(jnp.bfloat16)
    terms = terms.reshape(count, 2 * total_width)
    return (query_grad, bias_grad, terms)


def per_device(
    layer_in,
    encoded,
    self_query,
    self_key,
    self_value,
    self_out,
    cross_query,
    cross_key,
    cross_value,
    cross_out,
    gate_proj,
    up_proj,
    down_proj,
    norm_gains,
    position_bias,
    bucket_ids,
    block_order,
    out_grad,
):
    low = jnp.bfloat16
    tok_rows = layer_in.shape[0]
    bucket_count, head_count = position_bias.shape
    block_count = block_order.shape[0]
    full_weights = (
        lax.all_gather(self_query, "ctx", axis=0, tiled=True),
        lax.all_gather(self_key, "ctx", axis=0, tiled=True),
        lax.all_gather(self_value, "ctx", axis=0, tiled=True),
        lax.all_gather(self_out, "ctx", axis=1, tiled=True),
        lax.all_gather(cross_query, "ctx", axis=0, tiled=True),
        lax.all_gather(cross_key, "ctx", axis=0, tiled=True),
        lax.all_gather(cross_value, "ctx", axis=0, tiled=True),
        lax.all_gather(cross_out, "ctx", axis=1, tiled=True),
        lax.all_gather(gate_proj, "ctx", axis=0, tiled=True),
        lax.all_gather(up_proj, "ctx", axis=0, tiled=True),
        lax.all_gather(down_proj, "ctx", axis=1, tiled=True),
    )
    (
        query_full,
        key_full,
        value_full,
        output_full,
        probe_full,
        lookup_full,
        recall_full,
        merge_full,
        gate_full,
        upward_full,
        down_full,
    ) = full_weights
    boundaries = jnp.arange(1, bucket_count, dtype=jnp.int32)
    starts = jnp.sum((bucket_ids[None, :] < boundaries[:, None]).astype(jnp.int32), axis=1)
    block_ids = jnp.arange(block_count, dtype=jnp.int32)
    here = lax.axis_index("ctx")
    own_block = jnp.sum(jnp.where(block_ids == here, block_order, 0))
    query_pos = own_block * tok_rows + jnp.arange(tok_rows, dtype=jnp.int32)

    def position_of(rows_index):
        slot = rows_index // tok_rows
        owner = jnp.sum(
            jnp.where(slot[:, None] == block_ids[None, :], block_order[None, :], 0), axis=1
        )
        return owner * tok_rows + rows_index % tok_rows

    def pair_parts(first_pos, second_pos):
        dist = first_pos[:, None] - second_pos[None, :]
        steps = (dist[:, :, None] >= starts[None, None, :]).astype(jnp.float32)
        return (steps, dist >= 0)

    def causal_parts(key_start, count):
        return pair_parts(query_pos, position_of(key_start + jnp.arange(count, dtype=jnp.int32)))

    normed_one = rms_scale(layer_in, norm_gains[0]).astype(low)
    queries = times(normed_one, query_full).astype(low)
    keys_own = times(normed_one, key_full).astype(low)
    values_own = times(normed_one, value_full).astype(low)
    memory_keys = times(encoded, lookup_full).astype(low)
    memory_values = times(encoded, recall_full).astype(low)
    total_width = queries.shape[1]
    width = total_width // head_count
    start_state = (
        jnp.zeros((head_count, tok_rows, width), jnp.float32),
        jnp.full((head_count, tok_rows), NEG, jnp.float32),
        jnp.zeros((head_count, tok_rows), jnp.float32),
    )
    self_fold = attend_fold(queries, head_count, causal_parts, position_bias)
    self_state = self_fold(
        start_state,
        (
            lax.all_gather(keys_own, "ctx", axis=0, tiled=True),
            lax.all_gather(values_own, "ctx", axis=0, tiled=True),
        ),
        jnp.int32(0),
    )
    mixed_one, lse_one = finish(self_state)
    after_self = layer_in + join_heads(times(mixed_one, output_full))
    normed_two = rms_scale(after_self, norm_gains[1]).astype(low)
    probes = times(normed_two, probe_full).astype(low)
    cross_fold = attend_fold(probes, head_count, None, position_bias)
    cross_state = cross_fold(
        start_state,
        (
            lax.all_gather(memory_keys, "ctx", axis=0, tiled=True),
            lax.all_gather(memory_values, "ctx", axis=0, tiled=True),
        ),
        jnp.int32(0),
    )
    mixed_two, lse_two = finish(cross_state)
    after_cross = after_self + join_heads(times(mixed_two, merge_full))
    normed_three = rms_scale(after_cross, norm_gains[2]).astype(low)
    gate_pre = times(normed_three, gate_full)
    upper = times(normed_three, upward_full)
    activated = geglu(gate_pre, upper).astype(low)
    layer_out = after_cross + join_heads(times(activated, down_full))
    grad_rows = out_grad.astype(low)
    down_wgrad = left_times(activated, grad_rows)
    act_grad = right_times(grad_rows, down_full)
    geglu_out, geglu_pull = jax.vjp(geglu, gate_pre, upper)
    gate_grad, upper_grad = geglu_pull(act_grad)
    gate_grad = gate_grad.astype(low)
    upper_grad = upper_grad.astype(low)
    gate_wgrad = left_times(normed_three, gate_grad)
    up_wgrad = left_times(normed_three, upper_grad)
    normed_three_grad = join_heads(
        right_times(gate_grad, gate_full) + right_times(upper_grad, upward_full)
    )
    norm_out, norm_pull = jax.vjp(rms_scale, after_cross, norm_gains[2])
    cross_extra, gain_three = norm_pull(normed_three_grad)
    cross_grad = out_grad + cross_extra
    cross_rows = cross_grad.astype(low)
    merge_wgrad = left_times(mixed_two, cross_rows)
    mixed_two_grad = right_times(cross_rows, merge_full).astype(low)
    delta_two = delta_of(mixed_two, mixed_two_grad, head_count)
    memory_all = gather_cross(memory_keys, memory_values)
    probe_grad, unused_bias, cross_terms = attend_back(
        probes,
        mixed_two_grad,
        lse_two,
        delta_two,
        memory_all[0],
        memory_all[1],
        head_count,
        None,
        position_bias,
    )
    cross_terms = lax.psum_scatter(cross_terms, "ctx", scatter_dimension=0, tiled=True)
    memory_key_grad = cross_terms[:, :total_width].astype(low)
    memory_value_grad = cross_terms[:, total_width:].astype(low)
    probe_wgrad = left_times(normed_two, probe_grad)
    lookup_wgrad = left_times(encoded, memory_key_grad)
    recall_wgrad = left_times(encoded, memory_value_grad)
    normed_two_grad, encoded_grad = join_heads(
        (
            right_times(probe_grad, probe_full),
            right_times(memory_key_grad, lookup_full) + right_times(memory_value_grad, recall_full),
        )
    )
    norm_out, norm_pull = jax.vjp(rms_scale, after_self, norm_gains[1])
    self_extra, gain_two = norm_pull(normed_two_grad)
    self_grad = cross_grad + self_extra
    self_rows = self_grad.astype(low)
    output_wgrad = left_times(mixed_one, self_rows)
    mixed_one_grad = right_times(self_rows, output_full).astype(low)
    delta_one = delta_of(mixed_one, mixed_one_grad, head_count)
    sequence_all = gather_self(keys_own, values_own)
    query_grad, bias_grad, self_terms = attend_back(
        queries,
        mixed_one_grad,
        lse_one,
        delta_one,
        sequence_all[0],
        sequence_all[1],
        head_count,
        causal_parts,
        position_bias,
    )
    self_terms = lax.psum_scatter(self_terms, "ctx", scatter_dimension=0, tiled=True)
    key_grad = self_terms[:, :total_width].astype(low)
    value_grad = self_terms[:, total_width:].astype(low)
    query_wgrad = left_times(normed_one, query_grad)
    key_wgrad = left_times(normed_one, key_grad)
    value_wgrad = left_times(normed_one, value_grad)
    normed_one_grad = join_heads(
        right_times(query_grad, query_full)
        + right_times(key_grad, key_full)
        + right_times(value_grad, value_full)
    )
    norm_out, norm_pull = jax.vjp(rms_scale, layer_in, norm_gains[0])
    input_extra, gain_one = norm_pull(normed_one_grad)
    input_grad = self_grad + input_extra
    weight_sums = (
        lax.psum_scatter(query_wgrad, "ctx", scatter_dimension=0, tiled=True),
        lax.psum_scatter(key_wgrad, "ctx", scatter_dimension=0, tiled=True),
        lax.psum_scatter(value_wgrad, "ctx", scatter_dimension=0, tiled=True),
        lax.psum_scatter(output_wgrad, "ctx", scatter_dimension=1, tiled=True),
        lax.psum_scatter(probe_wgrad, "ctx", scatter_dimension=0, tiled=True),
        lax.psum_scatter(lookup_wgrad, "ctx", scatter_dimension=0, tiled=True),
        lax.psum_scatter(recall_wgrad, "ctx", scatter_dimension=0, tiled=True),
        lax.psum_scatter(merge_wgrad, "ctx", scatter_dimension=1, tiled=True),
        lax.psum_scatter(gate_wgrad, "ctx", scatter_dimension=0, tiled=True),
        lax.psum_scatter(up_wgrad, "ctx", scatter_dimension=0, tiled=True),
        lax.psum_scatter(down_wgrad, "ctx", scatter_dimension=1, tiled=True),
    )
    gains_sum, bias_sum = lax.psum((jnp.stack((gain_one, gain_two, gain_three)), bias_grad), "ctx")
    return (layer_out, input_grad, encoded_grad) + tuple(weight_sums) + (gains_sum, bias_sum)


def solution(mesh):
    body = quick_device if quick_fits(mesh) else per_device
    placed = (
        P("ctx", None),
        P("ctx", None),
        P("ctx", "head"),
        P("ctx", "head"),
        P("ctx", "head"),
        P("head", "ctx"),
        P("ctx", "head"),
        P("ctx", "head"),
        P("ctx", "head"),
        P("head", "ctx"),
        P("ctx", "head"),
        P("ctx", "head"),
        P("head", "ctx"),
        P(),
        P(None, "head"),
        P(),
        P(),
        P("ctx", None),
    )
    return jax.shard_map(
        body,
        mesh=mesh,
        in_specs=placed,
        out_specs=(
            P("ctx", None),
            P("ctx", None),
            P("ctx", None),
            P("ctx", "head"),
            P("ctx", "head"),
            P("ctx", "head"),
            P("head", "ctx"),
            P("ctx", "head"),
            P("ctx", "head"),
            P("ctx", "head"),
            P("head", "ctx"),
            P("ctx", "head"),
            P("ctx", "head"),
            P("head", "ctx"),
            P(),
            P(None, "head"),
        ),
        check_vma=False,
    )
```

```python
import functools
import math

import jax
import jax.numpy as jnp
from jax import lax
from jax.experimental import pallas as pl
from jax.experimental.pallas import tpu as pltpu
from jax.sharding import PartitionSpec as P

EPS = 1e-06
NEG = -1e30
HIGH = lax.Precision.HIGHEST
LOW = jnp.bfloat16
F32 = jnp.float32
MESH = pl.DeviceIdType.MESH
VMEM_LIMIT = 66_000_000


def dot(left, right, **kw):
    return jnp.dot(left, right, preferred_element_type=F32, **kw)


def dot_nt(left, right, **kw):
    return lax.dot_general(left, right, (((1,), (1,)), ((), ())), preferred_element_type=F32, **kw)


def dot_tn(left, right, **kw):
    return lax.dot_general(left, right, (((0,), (0,)), ((), ())), preferred_element_type=F32, **kw)


def rms_forward(rows, gain):
    return rows * lax.rsqrt(jnp.mean(rows * rows, axis=-1, keepdims=True) + EPS) * gain


def rms_backward(rows, gain, grad):
    scale = lax.rsqrt(jnp.mean(rows * rows, axis=-1, keepdims=True) + EPS)
    scaled = gain * grad
    inner = jnp.mean(scaled * rows, axis=-1, keepdims=True)
    row_grad = scale * scaled - rows * (scale * scale * scale * inner)
    gain_grad = jnp.sum(grad * rows * scale, axis=0, keepdims=True)
    return row_grad, gain_grad


def aligned(value, step):
    return value if isinstance(value, int) else pl.multiple_of(value, step)


class Place:
    def __init__(self, count):
        self.count = count
        self.here = lax.axis_index("ctx")
        self.core = lax.axis_index("head")
        self.other = 1 - self.core
        self.plane = lax.rem(self.here, 4)
        self.level = self.here // 4
        self.fx = self.flip(self.here, 0)
        self.fy = self.flip(self.here, 1)
        self.fxy = self.flip(self.fx, 1)
        self.above = [lax.rem(self.here + 4 * k, count) for k in range(4)]
        self.below = [lax.rem(self.here + count - 4 * k, count) for k in range(4)]
        self.top = count // 4 - 1
        bottom, head = self.level == 0, self.level == self.top
        self.nearest = (
            jnp.where(bottom, 3, 1),
            jnp.where(bottom, 2, jnp.where(head, 2, 3)),
            jnp.where(bottom, 1, jnp.where(head, 3, 2)),
        )

    def flip(self, index, axis):
        if axis == 0:
            return index + 1 - 2 * lax.rem(index, 2)
        return index + 2 - 4 * lax.rem(index // 2, 2)

    def near(self, half):
        return (self.fx, self.fy) if half == 0 else (self.fy, self.fx)

    def signal(self, chips):
        barrier = pltpu.get_barrier_semaphore()
        for chip in chips:
            pl.semaphore_signal(
                barrier, inc=1, device_id=(chip, self.core), device_id_type=MESH
            )
        pl.semaphore_signal(barrier, inc=1, device_id=(self.here, self.other), device_id_type=MESH)

    def meet(self, count):
        pl.semaphore_wait(pltpu.get_barrier_semaphore(), count)


class Wire:
    def __init__(self, place, send_sem, recv_sem):
        self.place, self.send_sem, self.recv_sem = place, send_sem, recv_sem
        self.used = 0
        self.send_used = 0
        self.pending = []

    def slots(self, count):
        base = self.used
        self.used += count
        assert self.used <= self.recv_sem.shape[0], self.used
        return base

    def sender(self, whole=None):
        slot = self.send_used
        self.send_used += 1
        assert slot < self.send_sem.shape[0], slot
        if whole is not None:
            self.pending.append((slot, whole))
        return slot

    def copy(self, src, dst, out, slot, chip, core):
        return pltpu.make_async_remote_copy(
            src_ref=src,
            dst_ref=dst,
            send_sem=self.send_sem.at[out],
            recv_sem=self.recv_sem.at[slot],
            device_id=(chip, core),
            device_id_type=MESH,
        )

    def send(self, src, dst, slot, chip=None, core=None, out=None):
        chip = self.place.here if chip is None else chip
        core = self.place.core if core is None else core
        if out is None:
            out = self.sender(src)
        self.copy(src, dst, out, slot, chip, core).start()

    def swap(self, src, dst, slot, out=None):
        self.send(src, dst, slot, None, self.place.other, out)

    def got(self, dst, slot):
        place = self.place
        self.copy(dst, dst, 0, slot, place.here, place.other).wait_recv()

    def sent(self, whole, out):
        place = self.place
        self.copy(whole, whole, out, 0, place.here, place.other).wait_send()

    def drain(self):
        for out, whole in self.pending:
            self.sent(whole, out)
        self.pending = []


class Gather:
    def __init__(self, wire, view, share, spare):
        self.wire, self.view, self.share, self.spare = wire, view, share, spare
        self.halves = range(2)
        self.base = wire.slots(8)
        self.out = wire.sender(spare(12))
        self.line_out = wire.sender()
        if share:
            self.side = wire.slots(1)
            self.side_out = wire.sender(spare(15))

    def _line(self, half, block, slot, chip):
        ref = self.view(half, block)
        self.wire.send(ref, ref, self.base + slot, chip, out=self.line_out)

    def _out(self, half, block, slot, chip):
        ref = self.view(half, block)
        self.wire.send(ref, ref, self.base + slot, chip, out=self.out)

    def _give(self, half, block):
        if self.share:
            ref = self.view(half, block)
            self.wire.swap(ref, ref, self.side, self.side_out)

    def start_level(self):
        place = self.wire.place
        for half in self.halves:

            @pl.when(place.level < place.top)
            def _():
                self._line(half, place.here, 0, place.here + 4)

            @pl.when(place.level > 0)
            def _():
                self._line(half, place.here, 2, place.here - 4)

    def start_plane(self):
        place = self.wire.place
        for half in self.halves:
            near, far = place.near(half)
            self._out(half, place.here, 3, near)
            self._out(half, place.here, 7, far)

    def _level_block(self, step):
        place = self.wire.place
        k = place.nearest[step]
        return k, lax.rem(place.here + place.count - 4 * k, place.count)

    def pass_line(self, step):
        place = self.wire.place
        k, block = self._level_block(step)
        rising = place.level >= k
        onward = jnp.where(rising, place.level < place.top, place.level > 0)
        chip = jnp.where(rising, place.here + 4, place.here - 4)
        slot = jnp.where(rising, k, k - 2)
        self.wire.got(self.spare(1), self.base + k - 1)
        for half in self.halves:

            @pl.when(onward)
            def _():
                self._line(half, block, slot, chip)

    def pass_plane(self, step):
        place = self.wire.place
        k, block = self._level_block(step)
        for half in self.halves:
            near, far = place.near(half)
            self._out(half, block, 3 + k, near)
            self._out(half, block, 7, far)
            self._give(half, block)

    def pass_near(self, step):
        place = self.wire.place
        k = (0, *place.nearest)[step]
        block = lax.rem(place.here + place.count - 4 * k, place.count)
        self.wire.got(self.spare(1), self.base + 3 + k)
        for half in self.halves:
            _, far = place.near(half)
            arrived = place.flip(block, half)
            self._out(half, arrived, 7, far)
            self._give(half, arrived)

    def finish(self):
        place = self.wire.place
        self.wire.got(self.spare(8), self.base + 7)
        for half in self.halves:
            if self.share:
                for k in range(4):
                    block = place.flip(place.below[k], 1 - half)
                    self._give(half, block)
                    self._give(half, place.flip(block, half))

    def finish_share(self):
        self.wire.got(self.spare(15), self.side)

    def drain(self):
        place = self.wire.place

        @pl.when(jnp.logical_or(place.level == 0, place.level == place.top))
        def _():
            self.wire.sent(self.spare(1), self.line_out)

        @pl.when(jnp.logical_and(place.level > 0, place.level < place.top))
        def _():
            self.wire.sent(self.spare(5), self.line_out)


class Scatter:
    def __init__(self, wire, view, buf, out, spare):
        self.wire, self.view, self.buf, self.out, self.spare = wire, view, buf, out, spare
        self.halves = range(2)
        self.base = wire.slots(9)
        self.send_slot = wire.sender(spare(15))

    def _send(self, half, block, place_in, slot, chip):
        self.wire.send(
            self.view(half, block),
            self.buf(half).at[place_in],
            self.base + slot,
            chip,
            out=self.send_slot,
        )

    def start(self, k):
        place = self.wire.place
        for half in self.halves:
            _, far = place.near(half)
            away = place.flip(place.below[k], 1 - half)
            for pair, block in ((1, place.flip(away, half)), (0, away)):
                self._send(half, block, 2 * k + pair, k, far)

    def pass_near(self, k):
        place = self.wire.place
        self.wire.got(self.spare(2), self.base + k)
        for half in self.halves:
            near, _ = place.near(half)
            block = place.flip(place.below[k], half)
            ref = self.view(half, block)
            ref[...] = (ref[...].astype(F32) + self.buf(half)[2 * k + 1].astype(F32)).astype(LOW)
            self._send(half, block, 8 + k, 4 + k, near)

    def pass_level(self, k):
        place = self.wire.place
        self.wire.got(self.spare(1), self.base + 4 + k)
        for half in self.halves:
            ref = self.view(half, place.below[k])
            ref[...] = self._sum(half, k).astype(LOW)
            self._send(half, place.below[k], 11 + k, 8, place.below[k])

    def _sum(self, half, k):
        buf = self.buf(half)
        total = self.view(half, self.wire.place.below[k])[...].astype(F32)
        return total + buf[2 * k].astype(F32) + buf[8 + k].astype(F32)

    def finish(self):
        self.wire.got(self.spare(1), self.base + 4)
        self.wire.got(self.spare(3), self.base + 8)
        for half in self.halves:
            total = self._sum(half, 0)
            for k in (1, 2, 3):
                total = total + self.buf(half)[11 + k].astype(F32)
            self.out(half, total)


def lane_split(rows):
    lane = lax.broadcasted_iota(jnp.int32, rows.shape, 1)
    low = lane < rows.shape[1] // 2
    zero = jnp.zeros_like(rows)
    return jnp.concatenate((jnp.where(low, rows, zero), jnp.where(low, zero, rows)), axis=0)


def lane_join(rows):
    count, width = rows.shape[0] // 2, rows.shape[1]
    lane = lax.broadcasted_iota(jnp.int32, (count, width), 1)
    return jnp.where(lane < width // 2, rows[:count], rows[count:])


def pair_attend(tok, pairs, chunk, q_ref, kv_ref, s_ref, e_ref, rl_ref, mixed_ref, bias_ref, between):
    keys = kv_ref.shape[0]
    total = pairs * 128

    for j in range(pairs):
        cols = slice(j * 128, (j + 1) * 128)
        vcols = slice(total + j * 128, total + (j + 1) * 128)
        q_cat = lane_split(q_ref[:, cols])

        def score(c, top):
            rows = pl.ds(aligned(c * chunk, chunk), chunk)
            s = dot_nt(q_cat, kv_ref[rows, cols])
            if bias_ref is not None:
                tiles = []
                for half in range(2):
                    row = []
                    for b in range(chunk // tok):
                        lanes = pl.ds(aligned((c * (chunk // tok) + b) * 2 * tok, 128), 2 * tok)
                        vec = bias_ref[2 * j + half : 2 * j + half + 1, lanes]
                        wide = jnp.broadcast_to(vec, (tok, 2 * tok))
                        row.append(pltpu.roll(wide, 0, 1, stride=1, stride_axis=0)[:, :tok])
                    tiles.append(jnp.concatenate(row, axis=1))
                s = s + jnp.concatenate(tiles, axis=0)
            s_ref[:, rows] = s
            for b in range(chunk // 128):
                top = jnp.maximum(top, s[:, b * 128 : (b + 1) * 128])
            return top

        top = lax.fori_loop(0, keys // chunk, score, jnp.full((2 * tok, 128), NEG, F32))
        peak = jnp.max(top, axis=1, keepdims=True)

        def weigh(c, state):
            acc, run = state
            rows = pl.ds(aligned(c * chunk, chunk), chunk)
            e = jnp.exp(s_ref[:, rows] - peak)
            for b in range(chunk // 128):
                run = run + e[:, b * 128 : (b + 1) * 128]
            low = e.astype(LOW)
            e_ref[j, :, rows] = low
            return (acc + dot(low, kv_ref[rows, vcols]), run)

        zero = jnp.zeros((2 * tok, 128), F32)
        acc, run = lax.fori_loop(0, keys // chunk, weigh, (zero, zero))
        rl = 1.0 / jnp.sum(run, axis=1, keepdims=True)
        rl_ref[j] = rl
        mixed_ref[:, cols] = lane_join(acc * rl).astype(LOW)
        between(j)


class PairBack:
    def __init__(self, tok, pairs, q, kv, e, rl, mixed, grad, kv_grad, diag, qc, gc, dl, dq):
        self.tok, self.pairs, self.kv, self.e = tok, pairs, kv, e
        self.kv_grad, self.diag, self.qc, self.gc, self.dl, self.dq = kv_grad, diag, qc, gc, dl, dq
        self.total = pairs * 128
        for j in range(pairs):
            cols = slice(j * 128, (j + 1) * 128)
            rl_j = rl[j]
            grads = lane_split(grad[:, cols].astype(F32))
            qc[j] = lane_split(q[:, cols])
            gc[j] = (grads * rl_j).astype(LOW)
            values = lane_split(mixed[:, cols].astype(F32))
            dl[j] = jnp.sum(grads * values, axis=1, keepdims=True) * rl_j
            dq[j] = jnp.zeros(dq.shape[1:], F32)

    def chunk(self, start, count):
        tok, kv, qc, gc = self.tok, self.kv, self.qc, self.gc
        rows = pl.ds(aligned(start, count), count)
        flip = (
            lax.broadcasted_iota(jnp.int32, (tok, tok), 0)
            + lax.broadcasted_iota(jnp.int32, (tok, tok), 1)
            == tok - 1
        ).astype(LOW)

        def one_pair(j, carry):
            cols = pl.ds(aligned(j * 128, 128), 128)
            vcols = pl.ds(aligned(self.total + j * 128, 128), 128)
            low_e = self.e[j, :, rows]
            dp = dot_nt(gc[j], kv[rows, vcols])
            ds = (low_e.astype(F32) * (dp - self.dl[j])).astype(LOW)
            if self.diag is not None:
                for half in range(2):
                    turned = dot(flip, ds[half * tok : (half + 1) * tok])
                    for b in range(count // tok):
                        tile = turned[:, b * tok : (b + 1) * tok]
                        wide = jnp.concatenate((tile, jnp.zeros_like(tile)), axis=1)
                        wide = pltpu.roll(wide, tok + 1, 1, stride=1, stride_axis=0)
                        lanes = pl.ds(aligned(2 * start + b * 2 * tok, 128), 2 * tok)
                        self.diag[pl.ds(2 * j + half, 1), lanes] = jnp.sum(
                            wide, axis=0, keepdims=True
                        )
            self.kv_grad[rows, cols] = dot_tn(ds, qc[j]).astype(LOW)
            self.kv_grad[rows, vcols] = dot_tn(low_e, gc[j]).astype(LOW)
            self.dq[j] = self.dq[j] + dot(ds, kv[rows, cols])
            return carry

        lax.fori_loop(0, self.pairs, one_pair, 0)

    def finish(self, q_grad):
        for j in range(self.pairs):
            q_grad[:, j * 128 : (j + 1) * 128] = lane_join(self.dq[j]).astype(LOW)


def bucket_rows(buckets_ref, order_ref, here, table_rows, ids_ref):
    count, tok = buckets_ref.shape
    turn = (
        lax.broadcasted_iota(jnp.int32, (tok, tok), 0)
        + lax.broadcasted_iota(jnp.int32, (tok, tok), 1)
        == tok - 1
    ).astype(LOW)
    table_rows[:count, :] = jnp.full((count, tok), -1.0, F32)
    table_rows[count:, :] = dot(buckets_ref[...].astype(LOW), turn)
    own = order_ref[here]
    for block in range(count):
        at = own - order_ref[block] + count
        wide = jnp.concatenate(
            (table_rows[pl.ds(at - 1, 1), :], table_rows[pl.ds(at, 1), :]), axis=1
        )
        ids_ref[:, block * 2 * tok : (block + 1) * 2 * tok] = pltpu.roll(wide, 1, 1)


def bucket_masks(ids_ref, buckets):
    ids = ids_ref[...]
    row = lax.broadcasted_iota(jnp.int32, (buckets, ids.shape[1]), 0).astype(F32)
    return ids, (row == ids).astype(F32)


def bias_vectors(ids_ref, table_ref, bias_ref):
    heads, buckets = table_ref.shape
    ids, mask = bucket_masks(ids_ref, buckets)
    vec = dot(table_ref[...], mask, precision=HIGH)
    bias_ref[:heads, :] = jnp.where(ids >= 0, vec, NEG)


def bucket_sums(ids_ref, diag_ref, buckets):
    _, mask = bucket_masks(ids_ref, buckets)
    return dot_nt(diag_ref[...], mask, precision=HIGH)


def rows_loop(count, step, body):
    def one(index, carry):
        body(pl.ds(aligned(index * step, step), step))
        return carry

    lax.fori_loop(0, count // step, one, 0)


GELU_A = 0.7978845608028654
GELU_B = 0.044715


def gelu_parts(value):
    square = value * value
    wave = jnp.tanh(GELU_A * (value + GELU_B * value * square))
    half = 0.5 * (1.0 + wave)
    slope = half + 0.5 * value * (1.0 - wave * wave) * (GELU_A * (1.0 + 3.0 * GELU_B * square))
    return value * half, slope


def core_sum(wire, part, out_buf, in_buf):
    slot = wire.slots(1)
    out_buf[...] = part.astype(LOW)
    wire.swap(out_buf, in_buf, slot)
    wire.got(in_buf, slot)
    return out_buf[...].astype(F32) + in_buf[...].astype(F32)


class PlaneSum:
    def __init__(self, wire, tok, part, core_buf, plane_buf, whole):
        self.wire, self.tok = wire, tok
        self.out = wire.sender(part)
        self.part, self.core_buf, self.plane_buf, self.whole = part, core_buf, plane_buf, whole
        self.base = wire.slots(8)
        self.half = whole.shape[1] // 2
        place = wire.place
        self.chips = (place.here, place.fx, place.fy, place.fxy)

    def cols(self, core):
        return pl.ds(aligned(core * self.half, 128), self.half)

    def rows(self, k):
        return pl.ds(aligned(lax.rem(self.chips[k], 4) * self.tok, self.tok), self.tok)

    def start(self, k):
        away = self.cols(self.wire.place.other)
        rows = self.rows(k)
        self.wire.swap(self.part.at[rows, away], self.core_buf.at[rows, :], self.base + k, self.out)

    def middle(self, k):
        wire, rows = self.wire, self.rows(k)
        wire.got(self.core_buf.at[rows, :], self.base + k)
        total = self.part[rows, self.cols(wire.place.core)].astype(F32)
        total = total + self.core_buf[rows, :].astype(F32)
        self.core_buf[rows, :] = total.astype(LOW)
        if k:
            wire.send(
                self.core_buf.at[rows, :],
                self.plane_buf.at[k - 1],
                self.base + 3 + k,
                self.chips[k],
                out=self.out,
            )

    def finish(self):
        place, wire = self.wire.place, self.wire
        total = self.core_buf[self.rows(0), :].astype(F32)
        for k in (1, 2, 3):
            wire.got(self.plane_buf.at[k - 1], self.base + 3 + k)
            total = total + self.plane_buf[k - 1].astype(F32)
        mine = self.cols(place.core)
        self.whole[:, mine] = total.astype(LOW)
        wire.swap(self.whole.at[:, mine], self.whole.at[:, mine], self.base + 7, self.out)

    def finish_core(self):
        self.wire.got(self.whole.at[:, self.cols(self.wire.place.other)], self.base + 7)


class PlaneGather:
    def __init__(self, wire, tok, ref):
        self.wire, self.tok, self.ref = wire, tok, ref
        self.half = ref.shape[1] // 2
        self.base = wire.slots(8)
        self.out = wire.sender(ref.at[: 3 * tok, :])
        place = wire.place
        self.chips = (place.here, place.fx, place.fy, place.fxy)

    def view(self, k, core):
        rows = pl.ds(aligned(lax.rem(self.chips[k], 4) * self.tok, self.tok), self.tok)
        return self.ref.at[rows, pl.ds(aligned(core * self.half, 128), self.half)]

    def start(self):
        own = self.view(0, self.wire.place.core)
        for k in (1, 2, 3):
            self.wire.send(own, own, self.base + k, self.chips[k], out=self.out)

    def share(self, k):
        ref = self.view(k, self.wire.place.core)
        self.wire.got(ref, self.base + k)
        self.wire.swap(ref, ref, self.base + 4 + k, self.out)

    def finish(self, k):
        self.wire.got(self.view(k, self.wire.place.other), self.base + 4 + k)


class Sizes:
    def __init__(self, ctx, tok, enc, model, wide, units):
        self.ctx, self.tok, self.enc, self.model, self.wide = ctx, tok, enc, model, wide
        self.rows = model // ctx
        self.units = units
        self.quarter = units // 4
        self.pairs = wide // 128
        self.levels = ctx // 4
        self.attn_cols = 8 * wide
        self.mlp_cols = 3 * units
        self.part = 3 * self.quarter
        self.names = ("q", "k", "v", "cq", "ck", "cv", "o", "co")
        self.col = {n: slice(i * wide, (i + 1) * wide) for i, n in enumerate(self.names)}
        self.col["kv"] = slice(wide, 3 * wide)
        self.col["ckv"] = slice(4 * wide, 6 * wide)
        self.cuts = {
            "s": self.halves(0, 3 * wide, 0),
            "c": self.halves(3 * wide, 6 * wide, 1),
            "o": self.halves(6 * wide, 7 * wide, 0),
            "co": self.halves(7 * wide, 8 * wide, 1),
        }

    def halves(self, first, last, up):
        tiles = (last - first) // 128
        middle = first + (tiles + up) // 2 * 128
        return ((first, middle), (middle, last))


def named(kernel, names):
    def body(*refs):
        kernel(**dict(zip(names, refs, strict=True)))

    return body


def wire_sems(send, recv):
    return {
        "send_sem": pltpu.SemaphoreType.DMA((send,)),
        "recv_sem": pltpu.SemaphoreType.DMA((recv,)),
    }


def layer_kernel(
    size, layer_src, encoded, sq, sk, sv, so, cq, ck, cv, co, gate_w, up_w, down_w, gains_src,
    table_src, buckets_src, order_src, out_grad_src,
    layer_out, input_grad, enc_grad, WG, mb, totals, bias_totals,
    layer_in, gains, table, buckets, order, out_grad, WA, WM, wm, X, E, GR, PW, PM,
    q, kv, mkv, probes, s, e1, e2, rl1, rl2, mixed1, mixed2, table_rows, ids, bias, diag,
    after_self, after_cross, cross_grad, self_grad, n2, N3, act, GU, PN, PO, low, mixed_grad,
    q_grad, kv_grad, mkv_grad, ca, cb, pn_core, pn_plane, pn_whole, po_core, po_plane, po_whole,
    qc, gc, dl, dq, bs0, bs1, bc0, bc1, bo0, bo1, bp0, bp1, bx, be, px, pe, NG, NE, ml, ps,
    s1, s2, sr, sl, t1, t2, tr, tl, local, send_sem, recv_sem,
):
    place = Place(size.ctx)
    wire = Wire(place, send_sem, recv_sem)
    tok, enc, rows, half_d = size.tok, size.enc, size.rows, size.model // 2
    col, model, quarter = size.col, size.model, size.quarter
    ctx_tok, ctx_enc = X.shape[0], E.shape[0]
    plane_chips = (place.fx, place.fy, place.fxy)
    XG, EG = kv, mkv

    def block_rows(block, count):
        return pl.ds(aligned(block * count, 16), count)

    here_rows = block_rows(place.here, tok)
    own_weights = block_rows(place.here, rows)
    my_part = pl.ds(aligned(place.plane * size.part, 128), size.part)
    mine = pl.ds(aligned(place.core * half_d, 128), half_d)
    away = pl.ds(aligned(place.other * half_d, 128), half_d)

    def token_view(ref, count, core):
        def view(half, block):
            return ref.at[
                pl.ds(aligned(block * count + half * (count // 2), 16), count // 2),
                pl.ds(aligned(core * half_d, 128), half_d),
            ]

        return view

    def weight_view(ref, name):
        def view(half, block):
            first, last = size.cuts[name][half]
            return ref.at[block_rows(block, rows), first:last]

        return view

    def token_spare(buf):
        return lambda count: buf.at[:, 0:count]

    def weight_spare(name):
        (first, _), (_, last) = size.cuts[name]
        return lambda count: WA.at[0 : count * rows, first:last]

    gx = Gather(wire, token_view(X, tok, place.core), True, token_spare(bx))
    ge = Gather(wire, token_view(E, enc, place.core), True, token_spare(be))
    gs, gc_, go, gp = (
        Gather(wire, weight_view(WA, name), False, weight_spare(name))
        for name in ("s", "c", "o", "co")
    )
    gg = PlaneGather(wire, tok, GR)
    spread = PlaneGather(wire, tok, N3)
    sum_n = PlaneSum(wire, tok, PN, pn_core, pn_plane, pn_whole)
    sum_o = PlaneSum(wire, tok, PO, po_core, po_plane, po_whole)
    mg_plane, mg_level, ms_level, ms_plane = (wire.slots(3) for _ in range(4))

    def units_out():
        for k, chip in enumerate(plane_chips):
            wire.send(
                wm.at[:, pl.ds(aligned(lax.rem(chip, 4) * size.part, 128), size.part)],
                WM.at[own_weights, :],
                mg_plane + k,
                chip,
            )

    def units_up():
        for k, chip in enumerate(plane_chips):
            wire.got(WM.at[block_rows(chip, rows), :], mg_plane + k)
        own = WM.at[block_rows(place.level, 4 * rows), :]
        for k in (1, 2, 3):
            wire.send(own, own, mg_level + k - 1, place.above[k])

    place.signal(place.above[1:] + list(plane_chips))
    attention = size.attn_cols
    first = 3 * size.wide

    def load(slot, *pairs):
        for src, dst in pairs:
            pltpu.make_async_copy(src, dst, local.at[slot]).start()

    def loaded(slot, whole):
        pltpu.make_async_copy(whole, whole, local.at[slot]).wait()

    def own_columns(name):
        return WA.at[own_weights, col[name]]

    load(0, (layer_src, layer_in))
    load(1, (gains_src, gains))
    load(2, *((ref, own_columns(n)) for n, ref in (("q", sq), ("k", sk), ("v", sv))))
    load(3, *((ref, own_columns(n)) for n, ref in (("cq", cq), ("ck", ck), ("cv", cv), ("o", so), ("co", co))))
    load(4, (encoded, E.at[block_rows(place.here, enc), :]))
    load(
        5,
        *(
            (ref.at[:, p * quarter : (p + 1) * quarter], wm.at[:, base : base + quarter])
            for p in range(4)
            for i, ref in enumerate((gate_w, up_w, down_w))
            for base in (p * size.part + i * quarter,)
        ),
    )
    load(6, (out_grad_src, out_grad))
    load(7, (table_src, table))
    load(8, (buckets_src, buckets))
    load(9, (order_src, order))
    loaded(0, layer_in)
    loaded(1, gains)
    X[here_rows, :] = rms_forward(layer_in[...], gains[0:1]).astype(LOW)
    loaded(2, WA.at[own_weights, 0:first])
    place.meet(7)
    gx.start_level()
    gs.start_level()
    gx.start_plane()
    gs.start_plane()
    loaded(3, WA.at[own_weights, first:attention])
    loaded(4, E.at[block_rows(place.here, enc), :])
    loaded(5, wm)
    WM[own_weights, :] = wm[:, my_part]
    loaded(6, out_grad)
    plane_rows = block_rows(place.plane, tok)
    GR[plane_rows, :] = out_grad[...].astype(LOW)
    loaded(7, table)
    loaded(8, buckets)
    loaded(9, order)
    gx.pass_near(0)
    gx.pass_line(0)
    gx.pass_plane(0)
    gs.pass_near(0)
    gs.pass_line(0)
    gs.pass_plane(0)
    gx.pass_line(1)
    gx.pass_plane(1)
    gs.pass_line(1)
    gs.pass_plane(1)
    go.start_level()
    ge.start_level()
    gx.pass_near(1)
    gs.pass_near(1)
    gx.pass_line(2)
    gx.pass_plane(2)
    gs.pass_line(2)
    gs.pass_plane(2)
    gc_.start_level()
    gp.start_level()
    gx.pass_near(2)
    gs.pass_near(2)
    gx.pass_near(3)
    gs.pass_near(3)
    go.start_plane()
    ge.start_plane()
    gc_.start_plane()
    units_out()
    bucket_rows(buckets, order, place.here, table_rows, ids)
    bias_vectors(ids, table, bias)
    diag[...] = jnp.zeros_like(diag)
    go.pass_line(0)
    go.pass_plane(0)
    ge.pass_line(0)
    ge.pass_plane(0)
    gc_.pass_line(0)
    gp.pass_line(0)
    go.pass_line(1)
    go.pass_plane(1)
    ge.pass_line(1)
    ge.pass_plane(1)
    gc_.pass_line(1)
    gp.pass_line(1)
    go.pass_line(2)
    go.pass_plane(2)
    ge.pass_line(2)
    ge.pass_plane(2)
    gc_.pass_line(2)
    gp.pass_line(2)
    gc_.pass_plane(0)
    gc_.pass_plane(1)
    gc_.pass_plane(2)
    gx.finish()
    go.pass_near(0)
    ge.pass_near(0)
    gx.finish_share()
    gs.finish()
    units_up()

    def project(rows_):
        kv[rows_, :] = dot(X[rows_, :], WA[:, col["kv"]]).astype(LOW)

    def project_enc(rows_):
        mkv[rows_, :] = dot(E[rows_, :], WA[:, col["ckv"]]).astype(LOW)

    def project_level(level):
        for part_ in range(2):
            project(slice((2 * level + part_) * 2 * tok, (2 * level + part_ + 1) * 2 * tok))

    q[...] = dot(X[here_rows, :], WA[:, col["q"]]).astype(LOW)
    project_level(0)
    project_level(1)
    project_level(2)
    project_level(3)
    go.pass_near(1)
    go.pass_near(2)
    go.pass_near(3)
    ge.pass_near(1)
    ge.pass_near(2)
    ge.pass_near(3)

    def during_self(j):
        if j == 0:
            gc_.pass_near(0)
            gc_.pass_near(1)
        elif j == 1:
            gc_.pass_near(2)
            gc_.pass_near(3)
            gp.start_plane()
            gp.pass_plane(0)
            gp.pass_plane(1)
            gp.pass_plane(2)
        elif j == 2:
            go.finish()

    pair_attend(tok, size.pairs, 512, q, kv, s, e1, rl1, mixed1, bias, during_self)
    part = dot_nt(mixed1[...], WA[:, col["o"]])
    after_self[...] = layer_in[...] + core_sum(wire, part, ca.at[0], cb.at[0])
    n2[...] = rms_forward(after_self[...], gains[1:2]).astype(LOW)
    ge.finish()
    ge.finish_share()
    gc_.finish()

    rows_loop(ctx_enc, 256, project_enc)
    probes[...] = dot(n2[...], WA[:, col["cq"]]).astype(LOW)

    def during_cross(j):
        if j == 0:
            gp.pass_near(0)
            gp.pass_near(1)
            gp.pass_near(2)
            gp.pass_near(3)
            gg.start()
    pair_attend(tok, size.pairs, 512, probes, mkv, s, e2, rl2, mixed2, None, during_cross)
    gp.finish()
    part = dot_nt(mixed2[...], WA[:, col["co"]])
    after_cross[...] = after_self[...] + core_sum(wire, part, ca.at[1], cb.at[1])

    N3[plane_rows, :] = rms_forward(after_cross[...], gains[2:3]).astype(LOW)
    spread.start()
    for k in (1, 2, 3):
        level = place.below[k] // 4
        wire.got(WM.at[block_rows(level, 4 * rows), :], mg_level + k - 1)

    def units(k):
        rows_ = spread_rows(k)
        pre = dot(N3[rows_, :], WM[:, : 2 * quarter])
        gate, upper = pre[:, :quarter], pre[:, quarter:]
        value, slope = gelu_parts(gate)
        act[rows_, :] = (value * upper).astype(LOW)
        grad = dot(GR[rows_, :], WM[:, 2 * quarter :])
        GU[rows_, :quarter] = (grad * upper * slope).astype(LOW)
        GU[rows_, quarter:] = (grad * value).astype(LOW)
        PN[rows_, :] = dot_nt(GU[rows_, :], WM[:, : 2 * quarter]).astype(LOW)

    def spread_rows(k):
        return sum_n.rows(k)

    units(0)
    sum_n.start(0)
    for k in (1, 2, 3):
        gg.share(k)
    spread.share(1)
    spread.share(2)
    gg.finish(1)
    spread.finish(1)
    units(1)
    sum_n.start(1)
    gg.finish(2)
    spread.finish(2)
    units(2)
    sum_n.start(2)
    sum_n.middle(1)
    spread.share(3)
    gg.finish(3)
    spread.finish(3)
    units(3)
    sum_n.start(3)
    sum_n.middle(2)

    def back_out(k):
        rows_ = spread_rows(k)
        PO[rows_, :] = dot_nt(act[rows_, :], WM[:, 2 * quarter :]).astype(LOW)

    def unit_grads(cols):
        PM[cols, : 2 * quarter] = dot_tn(N3[:, cols], GU[...]).astype(LOW)
        PM[cols, 2 * quarter :] = dot_tn(GR[:, cols], act[...]).astype(LOW)

    back_out(0)
    sum_n.middle(3)
    sum_n.middle(0)
    for k in (1, 2, 3):
        back_out(k)
    for k in range(4):
        sum_o.start(k)
    rows_loop(model, 128, unit_grads)
    for k in (1, 2, 3):
        wire.send(
            PM.at[block_rows(place.above[k] // 4, 4 * rows), :],
            ml.at[k - 1],
            ms_level + k - 1,
            place.above[k],
        )
    sum_n.finish()
    sum_n.finish_core()
    extra, gain_three = rms_backward(after_cross[...], gains[2:3], pn_whole[...].astype(F32))
    cross_grad[...] = out_grad[...] + extra
    low[...] = cross_grad[...].astype(LOW)
    mixed_grad[...] = dot(low[...], WA[:, col["co"]]).astype(LOW)
    def out_grads(left, right, target):
        def body(cols):
            PW[cols, target] = dot_tn(left[:, cols], right[...]).astype(LOW)

        rows_loop(model, 128, body)

    def weight_stream(name, *bufs):
        def out(half, total):
            first, last = size.cuts[name][half]
            WG[:, first:last] = total

        return Scatter(
            wire, weight_view(PW, name), lambda half: bufs[half], out, weight_spare(name)
        )

    def token_out(ref, count):
        def out(half, total):
            ref[half * (count // 2) : (half + 1) * (count // 2), mine] = total

        return out

    sp = weight_stream("co", bp0, bp1)
    so_ = weight_stream("o", bo0, bo1)
    sc = weight_stream("c", bc0, bc1)
    sw = weight_stream("s", bs0, bs1)
    sx = Scatter(
        wire, token_view(XG, tok, place.core), lambda half: bx.at[half], token_out(NG, tok),
        token_spare(bx),
    )
    se = Scatter(
        wire, token_view(EG, enc, place.core), lambda half: be.at[half], token_out(NE, enc),
        token_spare(be),
    )
    x_base, e_base = wire.slots(4), wire.slots(4)
    x_out, e_out = wire.sender(px), wire.sender(pe)

    def pair_start(ref, recv, count, base, k, out):
        at = block_rows(place.below[k] // 4, 4 * count)
        wire.swap(ref.at[at, away], recv.at[at, :], base + k, out)

    def pair_ready(ref, recv, count, base, k):
        at = block_rows(place.below[k] // 4, 4 * count)
        wire.got(recv.at[at, :], base + k)
        ref[at, mine] = (ref[at, mine].astype(F32) + recv[at, :].astype(F32)).astype(LOW)

    x_slot, e_slot, cross_slot, small = (wire.slots(n) for n in (1, 1, 1, 10))

    def units_down():
        total = PM[block_rows(place.level, 4 * rows), :].astype(F32)
        for k in (1, 2, 3):
            wire.got(ml.at[k - 1], ms_level + k - 1)
            total = total + ml[k - 1].astype(F32)
        ps[...] = total.astype(LOW)
        for k, chip in enumerate(plane_chips):
            wire.send(
                ps.at[block_rows(lax.rem(chip, 4), rows), :], mb.at[:, my_part], ms_plane + k, chip
            )
        mb[:, my_part] = ps[block_rows(place.plane, rows), :]

    def units_back():
        for k, chip in enumerate(plane_chips):
            cols = pl.ds(aligned(lax.rem(chip, 4) * size.part, 128), size.part)
            wire.got(mb.at[:, cols], ms_plane + k)

    def result_back():
        sum_o.finish_core()
        layer_out[...] = after_cross[...] + po_whole[...].astype(F32)

    def tokens_back():
        sx.finish()
        wire.swap(NG.at[:, mine], NG.at[:, mine], x_slot)

    def encoder_back():
        se.finish()
        wire.swap(NE.at[:, mine], NE.at[:, mine], e_slot)

    def input_back():
        wire.got(NG.at[:, away], x_slot)
        extra, gain_one = rms_backward(layer_in[...], gains[0:1], NG[...])
        input_grad[...] = self_grad[...] + extra
        s1[...] = jnp.concatenate(
            (gain_one, gain_two, gain_three, jnp.zeros((5, model), F32)), axis=0
        )

    def small_first():
        wire.send(s1, sr.at[0], small, place.fx)
        wire.send(t1, tr.at[0], small + 5, place.fx)

    def small_second():
        wire.got(sr.at[0], small)
        wire.got(tr.at[0], small + 5)
        s2[...] = s1[...] + sr[0]
        t2[...] = t1[...] + tr[0]
        wire.send(s2, sr.at[1], small + 1, place.fy)
        wire.send(t2, tr.at[1], small + 6, place.fy)

    def small_third():
        wire.got(sr.at[1], small + 1)
        wire.got(tr.at[1], small + 6)
        sl[pl.ds(place.level, 1)] = (s2[...] + sr[1])[None]
        tl[pl.ds(place.level, 1)] = (t2[...] + tr[1])[None]
        for k in (1, 2, 3):
            wire.send(sl.at[place.level], sl.at[place.level], small + 1 + k, place.above[k])
            wire.send(tl.at[place.level], tl.at[place.level], small + 6 + k, place.above[k])

    def small_last():
        for k in (1, 2, 3):
            level = place.below[k] // 4
            wire.got(sl.at[level], small + 1 + k)
            wire.got(tl.at[level], small + 6 + k)
        totals[...] = (sl[0] + sl[1]) + (sl[2] + sl[3])
        bias_totals[...] = (tl[0] + tl[1]) + (tl[2] + tl[3])

    out_grads(low, mixed2, col["co"])
    sp.start(1)
    sp.start(2)
    back = PairBack(
        tok, size.pairs, probes, mkv, e2, rl2, mixed2, mixed_grad, mkv_grad, None, qc, gc, dl, dq
    )
    for c in range(ctx_enc // 1024):
        back.chunk(c * 512, 512)
    sp.start(3)
    for c in range(ctx_enc // 1024, ctx_enc // 512):
        back.chunk(c * 512, 512)
    back.finish(q_grad)
    for k in (3, 1, 2, 0):
        sum_o.middle(k)
    sp.pass_near(1)
    part = dot_nt(q_grad[...], WA[:, col["cq"]])
    ca[2] = part.astype(LOW)
    wire.swap(ca.at[2], cb.at[2], cross_slot)
    out_grads(E, mkv_grad, col["ckv"])
    sp.pass_near(3)
    out_grads(n2, q_grad, col["cq"])
    sc.start(2)

    def enc_rows(rows_):
        EG[rows_, :] = dot_nt(mkv_grad[rows_, :], WA[:, col["ckv"]]).astype(LOW)

    rows_loop(ctx_enc, 256, enc_rows)
    for k in (1, 2, 3, 0):
        pair_start(EG, pe, enc, e_base, k, e_out)
    sc.start(1)
    wire.got(cb.at[2], cross_slot)
    n_grad = ca[2].astype(F32) + cb[2].astype(F32)
    extra, gain_two = rms_backward(after_self[...], gains[1:2], n_grad)
    self_grad[...] = cross_grad[...] + extra
    low[...] = self_grad[...].astype(LOW)
    mixed_grad[...] = dot(low[...], WA[:, col["o"]]).astype(LOW)
    for k in (1, 2, 3, 0):
        pair_ready(EG, pe, enc, e_base, k)
    sc.start(3)
    out_grads(low, mixed1, col["o"])
    se.start(2)
    sp.pass_near(2)
    so_.start(0)
    sp.pass_level(1)
    sc.pass_near(2)
    so_.start(3)
    sc.pass_near(1)
    so_.start(1)

    back = PairBack(
        tok, size.pairs, q, kv, e1, rl1, mixed1, mixed_grad, kv_grad, diag, qc, gc, dl, dq
    )

    def tok_rows(k):
        for part_ in range(2):
            at = pl.ds(aligned(place.below[k] // 4 * 4 * tok + part_ * 2 * tok, 16), 2 * tok)
            XG[at, :] = dot_nt(kv_grad[at, :], WA[:, col["kv"]]).astype(LOW)

    n2[...] = X[here_rows, :]
    back.chunk(place.below[1] // 4 * 4 * tok, 4 * tok)
    tok_rows(1)
    pair_start(XG, px, tok, x_base, 1, x_out)
    back.chunk(place.below[2] // 4 * 4 * tok, 4 * tok)
    tok_rows(2)
    pair_start(XG, px, tok, x_base, 2, x_out)
    pair_ready(XG, px, tok, x_base, 1)
    sc.pass_near(3)
    se.start(0)
    se.start(1)
    back.chunk(place.below[3] // 4 * 4 * tok, 4 * tok)
    tok_rows(3)
    pair_start(XG, px, tok, x_base, 3, x_out)
    pair_ready(XG, px, tok, x_base, 2)
    sc.pass_level(1)
    sx.start(2)
    se.pass_near(2)
    sx.start(1)
    so_.start(2)
    sc.pass_level(2)
    back.chunk(place.level * 4 * tok, 4 * tok)
    back.finish(q_grad)
    tok_rows(0)
    own = dot_nt(q_grad[...], WA[:, col["q"]]) + XG[here_rows, :].astype(F32)
    XG[here_rows, :] = own.astype(LOW)
    pair_start(XG, px, tok, x_base, 0, x_out)
    pair_ready(XG, px, tok, x_base, 3)
    out_grads(n2, q_grad, col["q"])
    pair_ready(XG, px, tok, x_base, 0)
    sx.pass_near(2)
    se.pass_near(1)
    sx.start(3)
    sp.pass_level(2)
    out_grads(X, kv_grad, col["kv"])
    so_.pass_near(1)
    so_.pass_near(2)
    se.start(3)
    sw.start(3)
    sw.start(1)
    sx.pass_level(2)
    so_.pass_near(3)
    se.pass_near(3)
    sx.pass_near(1)
    sx.pass_near(3)
    se.pass_level(1)
    sc.pass_level(3)
    se.pass_level(2)
    so_.pass_level(1)
    so_.pass_level(3)
    sw.start(2)
    sx.pass_level(1)
    sx.start(0)
    sx.pass_level(3)
    so_.pass_near(0)
    sum_o.finish()
    sw.pass_near(1)
    sw.pass_near(2)
    sp.pass_level(3)
    so_.pass_level(2)
    sx.pass_near(0)
    sp.start(0)
    sw.pass_level(1)
    sw.start(0)
    se.pass_level(3)
    se.pass_near(0)
    sums = bucket_sums(ids, diag, table.shape[1])
    t1[...] = jnp.concatenate(
        (sums, jnp.zeros((sums.shape[0], t1.shape[1] - sums.shape[1]), F32)), axis=1
    )

    tokens_back()
    sw.pass_level(2)
    sw.pass_near(3)
    input_back()
    small_first()
    sc.start(0)
    small_second()
    sw.pass_near(0)
    so_.finish()
    sw.pass_level(3)
    units_down()
    sp.pass_near(0)
    sc.pass_near(0)
    small_third()
    sw.finish()
    sp.finish()
    result_back()
    encoder_back()
    small_last()
    units_back()
    sc.finish()
    wire.got(NE.at[:, away], e_slot)
    enc_grad[...] = NE[...]
    for made in (gx, ge, gs, gc_, go, gp):
        made.drain()
    wire.drain()


def emit_kernel(size, layer_out, input_grad, enc_grad, WG, mb, totals, bias_totals, *outs):
    for ref, out in zip((layer_out, input_grad, enc_grad), outs):
        out[...] = ref[...]
    for name, out in zip(size.names, outs[3:]):
        out[...] = WG[:, size.col[name]]
    for i, out in enumerate(outs[11:14]):
        for p in range(4):
            base = p * size.part + i * size.quarter
            out[:, p * size.quarter : (p + 1) * size.quarter] = mb[
                :, base : base + size.quarter
            ].astype(F32)
    outs[14][...] = totals[:3]
    heads, buckets = outs[15].shape
    outs[15][...] = bias_totals[:heads, :buckets]


def quick_device(
    layer_in, encoded, self_query, self_key, self_value, self_out, cross_query, cross_key,
    cross_value, cross_out, gate_proj, up_proj, down_proj, norm_gains, position_bias,
    bucket_ids, block_order, out_grad,
):
    tok, model = layer_in.shape
    enc = encoded.shape[0]
    wide, units = self_query.shape[1], gate_proj.shape[1]
    ctx = block_order.shape[0]
    buckets, heads = position_bias.shape
    size = Sizes(ctx, tok, enc, model, wide, units)
    rows, quarter, pairs = size.rows, size.quarter, size.pairs
    tok_all, enc_all, tok4 = ctx * tok, ctx * enc, 4 * tok

    def vmem(*shape, dtype=LOW):
        return pltpu.VMEM(shape, dtype)

    def full(*shape):
        return pltpu.VMEM(shape, F32)

    def streams(name):
        return [vmem(15, rows, last - first) for first, last in size.cuts[name]]

    ins = {
        "layer_src": layer_in, "encoded": encoded, "sq": self_query, "sk": self_key,
        "sv": self_value, "so": self_out.T, "cq": cross_query, "ck": cross_key,
        "cv": cross_value, "co": cross_out.T, "gate_w": gate_proj, "up_w": up_proj,
        "down_w": down_proj.T, "gains_src": norm_gains, "table_src": position_bias.T,
        "buckets_src": bucket_ids.reshape(ctx, tok), "order_src": block_order,
        "out_grad_src": out_grad,
    }
    outs = {
        "layer_out": ((tok, model), F32), "input_grad": ((tok, model), F32),
        "enc_grad": ((enc, model), F32), "WG": ((rows, size.attn_cols), F32),
        "mb": ((rows, size.mlp_cols), LOW), "totals": ((8, model), F32),
        "bias_totals": ((8, 128), F32),
    }
    (bs0, bs1), (bc0, bc1) = streams("s"), streams("c")
    (bo0, bo1), (bp0, bp1) = streams("o"), streams("co")
    scratch = {
        "layer_in": full(tok, model), "gains": full(*norm_gains.shape),
        "table": full(heads, buckets), "buckets": pltpu.VMEM((ctx, tok), jnp.int32),
        "order": pltpu.SMEM((ctx,), jnp.int32), "out_grad": full(tok, model),
        "WA": vmem(model, size.attn_cols), "WM": vmem(model, size.part),
        "wm": vmem(rows, size.mlp_cols), "X": vmem(tok_all, model), "E": vmem(enc_all, model),
        "GR": vmem(tok4, model), "PW": vmem(model, size.attn_cols),
        "PM": vmem(model, size.part),
        "q": vmem(tok, wide), "kv": vmem(tok_all, 2 * wide), "mkv": vmem(enc_all, 2 * wide),
        "probes": vmem(tok, wide), "s": full(2 * tok, tok_all),
        "e1": vmem(pairs, 2 * tok, tok_all), "e2": vmem(pairs, 2 * tok, enc_all),
        "rl1": full(pairs, 2 * tok, 1), "rl2": full(pairs, 2 * tok, 1),
        "mixed1": vmem(tok, wide), "mixed2": vmem(tok, wide), "table_rows": full(2 * ctx, tok),
        "ids": full(1, 2 * tok_all), "bias": full(8, 2 * tok_all), "diag": full(8, 2 * tok_all),
        "after_self": full(tok, model), "after_cross": full(tok, model),
        "cross_grad": full(tok, model), "self_grad": full(tok, model), "n2": vmem(tok, model),
        "N3": vmem(tok4, model), "act": vmem(tok4, quarter), "GU": vmem(tok4, 2 * quarter),
        "PN": vmem(tok4, model), "PO": vmem(tok4, model), "low": vmem(tok, model),
        "mixed_grad": vmem(tok, wide), "q_grad": vmem(tok, wide),
        "kv_grad": vmem(tok_all, 2 * wide), "mkv_grad": vmem(enc_all, 2 * wide),
        "ca": vmem(3, tok, model), "cb": vmem(3, tok, model),
        "pn_core": vmem(tok4, model // 2), "pn_plane": vmem(3, tok, model // 2),
        "pn_whole": vmem(tok, model), "po_core": vmem(tok4, model // 2),
        "po_plane": vmem(3, tok, model // 2), "po_whole": vmem(tok, model),
        "qc": vmem(pairs, 2 * tok, 128), "gc": vmem(pairs, 2 * tok, 128),
        "dl": full(pairs, 2 * tok, 1), "dq": full(pairs, 2 * tok, 128),
        "bs0": bs0, "bs1": bs1, "bc0": bc0, "bc1": bc1, "bo0": bo0, "bo1": bo1,
        "bp0": bp0, "bp1": bp1, "bx": vmem(2, 15, tok // 2, model // 2),
        "be": vmem(2, 15, enc // 2, model // 2), "px": vmem(tok_all, model // 2),
        "pe": vmem(enc_all, model // 2), "NG": full(tok, model), "NE": full(enc, model),
        "ml": vmem(3, 4 * rows, size.part), "ps": vmem(4 * rows, size.part),
        "s1": full(8, model), "s2": full(8, model), "sr": full(2, 8, model),
        "sl": full(4, 8, model), "t1": full(8, 128), "t2": full(8, 128), "tr": full(2, 8, 128), "tl": full(4, 8, 128),
        "local": pltpu.SemaphoreType.DMA((10,)), **wire_sems(53, 171),
    }
    names = list(ins) + list(outs) + list(scratch)
    made = pl.pallas_call(
        named(functools.partial(layer_kernel, size), names),
        out_shape=tuple(jax.ShapeDtypeStruct(*spec) for spec in outs.values()),
        in_specs=[
            pl.BlockSpec(memory_space=pl.ANY)
            for name in ins
        ],
        out_specs=tuple(pl.BlockSpec(memory_space=pltpu.VMEM) for _ in outs),
        scratch_shapes=list(scratch.values()),
        compiler_params=pltpu.CompilerParams(
            collective_id=1, has_side_effects=True, vmem_limit_bytes=VMEM_LIMIT
        ),
    )(*ins.values())
    specs = [
        (tok, model), (tok, model), (enc, model), *((rows, wide),) * 8, *((rows, units),) * 3,
        (3, model), (heads, buckets),
    ]
    parts = pl.pallas_call(
        functools.partial(emit_kernel, size),
        out_shape=tuple(jax.ShapeDtypeStruct(spec, F32) for spec in specs),
        in_specs=[pl.BlockSpec(memory_space=pltpu.VMEM)] * len(made),
        out_specs=tuple(pl.BlockSpec(memory_space=pltpu.VMEM) for _ in specs),
    )(*made)
    named_parts = dict(zip(size.names, parts[3:11]))
    gate, upward, down, gains, bias_grad = parts[11:]
    return (
        *parts[:3], named_parts["q"], named_parts["k"], named_parts["v"], named_parts["o"].T,
        named_parts["cq"], named_parts["ck"], named_parts["cv"], named_parts["co"].T,
        gate, upward, down.T, gains, bias_grad.T,
    )


def quick_fits(mesh):
    return mesh.shape["ctx"] == 16 and mesh.shape["head"] == 2


def as_sent(shard):

    def short(part):
        return part.astype(jnp.bfloat16) if part.dtype == jnp.float32 else part

    return jax.tree.map(short, shard)


def rms_scale(rows, gain):
    return rows * lax.rsqrt(jnp.mean(rows * rows, axis=-1, keepdims=True) + EPS) * gain


def geglu(gate, upper):
    return jax.nn.gelu(gate, approximate=True) * upper


def times(left, right):
    return jnp.dot(left, right, preferred_element_type=jnp.float32)


def left_times(left, right):
    return lax.dot_general(
        left, right, (((0,), (0,)), ((), ())), preferred_element_type=jnp.float32
    )


def right_times(left, right):
    return lax.dot_general(
        left, right, (((1,), (1,)), ((), ())), preferred_element_type=jnp.float32
    )


def join_heads(parts):
    return jax.tree.map(lambda part: part.astype(jnp.float32), lax.psum(as_sent(parts), "head"))


def gather_self(keys_own, values_own):
    return (
        lax.all_gather(keys_own, "ctx", axis=0, tiled=True),
        lax.all_gather(values_own, "ctx", axis=0, tiled=True),
    )


def gather_cross(memory_keys, memory_values):
    return (
        lax.all_gather(memory_keys, "ctx", axis=0, tiled=True),
        lax.all_gather(memory_values, "ctx", axis=0, tiled=True),
    )


def bias_scores(steps, bias_table):
    rises = bias_table[1:] - bias_table[:-1]
    return bias_table[0][:, None, None] + jnp.einsum("qkb,bh->hqk", steps, rises, precision=HIGH)


def bias_grads(score_grad, steps):
    above = jnp.einsum("hqk,qkb->bh", score_grad, steps, precision=HIGH)
    total = jnp.sum(score_grad, axis=(1, 2))
    upper_rows = jnp.concatenate((total[None], above), axis=0)
    lower_rows = jnp.concatenate((above, jnp.zeros((1, above.shape[1]), jnp.float32)), axis=0)
    return upper_rows - lower_rows


def delta_of(mixed, mixed_grad, head_count):
    tok_rows, total_width = mixed.shape
    width = total_width // head_count
    product = mixed.astype(jnp.float32).reshape(tok_rows, head_count, width) * mixed_grad.astype(
        jnp.float32
    ).reshape(tok_rows, head_count, width)
    return jnp.transpose(jnp.sum(product, axis=-1))


def attend_fold(queries, head_count, parts_fn, bias_table):
    tok_rows = queries.shape[0]
    width = queries.shape[1] // head_count
    query3 = queries.reshape(tok_rows, head_count, width)

    def fold(state, pieces, start):
        key_piece, value_piece = pieces
        count = key_piece.shape[0]
        block = math.gcd(count, 512)

        def fold_step(index, inner):
            summed, run_max, run_sum = inner
            key3 = lax.dynamic_slice_in_dim(key_piece, index * block, block, 0).reshape(
                block, head_count, width
            )
            value3 = lax.dynamic_slice_in_dim(value_piece, index * block, block, 0).reshape(
                block, head_count, width
            )
            scores = jnp.einsum("qhe,khe->hqk", query3, key3, preferred_element_type=jnp.float32)
            if parts_fn is not None:
                steps, valid = parts_fn(index * block, block)
                scores = jnp.where(valid[None], scores + bias_scores(steps, bias_table), NEG)
            new_max = jnp.maximum(run_max, jnp.max(scores, axis=-1))
            ratio = jnp.exp(run_max - new_max)
            weights = jnp.exp(scores - new_max[..., None])
            run_sum = run_sum * ratio + jnp.sum(weights, axis=-1)
            summed = summed * ratio[..., None] + jnp.einsum(
                "hqk,khe->hqe",
                weights.astype(jnp.bfloat16),
                value3,
                preferred_element_type=jnp.float32,
            )
            return (summed, new_max, run_sum)

        return lax.fori_loop(0, count // block, fold_step, state)

    return fold


def finish(state):
    summed, run_max, run_sum = state
    head_count, tok_rows, width = summed.shape
    mixed = jnp.transpose(summed / run_sum[..., None], (1, 0, 2)).reshape(
        tok_rows, head_count * width
    )
    return (mixed.astype(jnp.bfloat16), run_max + jnp.log(run_sum))


def attend_back(
    queries, mixed_grad, lse, delta, keys_all, values_all, head_count, parts_fn, bias_table
):
    tok_rows, total_width = queries.shape
    width = total_width // head_count
    query3 = queries.reshape(tok_rows, head_count, width)
    grad3 = mixed_grad.reshape(tok_rows, head_count, width)
    count = keys_all.shape[0]
    block = math.gcd(count, 512)

    def attend_step(carry, index):
        query_grad, bias_grad = carry
        key3 = lax.dynamic_slice_in_dim(keys_all, index * block, block, 0).reshape(
            block, head_count, width
        )
        value3 = lax.dynamic_slice_in_dim(values_all, index * block, block, 0).reshape(
            block, head_count, width
        )
        scores = jnp.einsum("qhe,khe->hqk", query3, key3, preferred_element_type=jnp.float32)
        if parts_fn is not None:
            steps, valid = parts_fn(index * block, block)
            scores = jnp.where(valid[None], scores + bias_scores(steps, bias_table), NEG)
        weights = jnp.exp(scores - lse[..., None])
        weight_grad = jnp.einsum("qhe,khe->hqk", grad3, value3, preferred_element_type=jnp.float32)
        score_grad = weights * (weight_grad - delta[..., None])
        if parts_fn is not None:
            bias_grad = bias_grad + bias_grads(score_grad, steps)
        score_low = score_grad.astype(jnp.bfloat16)
        query_grad = query_grad + jnp.einsum(
            "hqk,khe->qhe", score_low, key3, preferred_element_type=jnp.float32
        )
        stacked = None
        value_term = jnp.einsum(
            "hqk,qhe->khe", weights.astype(jnp.bfloat16), grad3, preferred_element_type=jnp.float32
        )
        key_term = jnp.einsum("hqk,qhe->khe", score_low, query3, preferred_element_type=jnp.float32)
        stacked = jnp.concatenate(
            (key_term.reshape(block, total_width), value_term.reshape(block, total_width)), axis=1
        )
        return ((query_grad, bias_grad), stacked)

    start = (
        jnp.zeros((tok_rows, head_count, width), jnp.float32),
        jnp.zeros(bias_table.shape, jnp.float32),
    )
    (query_grad, bias_grad), terms = lax.scan(attend_step, start, jnp.arange(count // block))
    query_grad = query_grad.reshape(tok_rows, total_width).astype(jnp.bfloat16)
    terms = terms.reshape(count, 2 * total_width)
    return (query_grad, bias_grad, terms)


def per_device(
    layer_in,
    encoded,
    self_query,
    self_key,
    self_value,
    self_out,
    cross_query,
    cross_key,
    cross_value,
    cross_out,
    gate_proj,
    up_proj,
    down_proj,
    norm_gains,
    position_bias,
    bucket_ids,
    block_order,
    out_grad,
):
    low = jnp.bfloat16
    tok_rows = layer_in.shape[0]
    bucket_count, head_count = position_bias.shape
    block_count = block_order.shape[0]
    full_weights = (
        lax.all_gather(self_query, "ctx", axis=0, tiled=True),
        lax.all_gather(self_key, "ctx", axis=0, tiled=True),
        lax.all_gather(self_value, "ctx", axis=0, tiled=True),
        lax.all_gather(self_out, "ctx", axis=1, tiled=True),
        lax.all_gather(cross_query, "ctx", axis=0, tiled=True),
        lax.all_gather(cross_key, "ctx", axis=0, tiled=True),
        lax.all_gather(cross_value, "ctx", axis=0, tiled=True),
        lax.all_gather(cross_out, "ctx", axis=1, tiled=True),
        lax.all_gather(gate_proj, "ctx", axis=0, tiled=True),
        lax.all_gather(up_proj, "ctx", axis=0, tiled=True),
        lax.all_gather(down_proj, "ctx", axis=1, tiled=True),
    )
    (
        query_full,
        key_full,
        value_full,
        output_full,
        probe_full,
        lookup_full,
        recall_full,
        merge_full,
        gate_full,
        upward_full,
        down_full,
    ) = full_weights
    boundaries = jnp.arange(1, bucket_count, dtype=jnp.int32)
    starts = jnp.sum((bucket_ids[None, :] < boundaries[:, None]).astype(jnp.int32), axis=1)
    block_ids = jnp.arange(block_count, dtype=jnp.int32)
    here = lax.axis_index("ctx")
    own_block = jnp.sum(jnp.where(block_ids == here, block_order, 0))
    query_pos = own_block * tok_rows + jnp.arange(tok_rows, dtype=jnp.int32)

    def position_of(rows_index):
        slot = rows_index // tok_rows
        owner = jnp.sum(
            jnp.where(slot[:, None] == block_ids[None, :], block_order[None, :], 0), axis=1
        )
        return owner * tok_rows + rows_index % tok_rows

    def pair_parts(first_pos, second_pos):
        dist = first_pos[:, None] - second_pos[None, :]
        steps = (dist[:, :, None] >= starts[None, None, :]).astype(jnp.float32)
        return (steps, dist >= 0)

    def causal_parts(key_start, count):
        return pair_parts(query_pos, position_of(key_start + jnp.arange(count, dtype=jnp.int32)))

    normed_one = rms_scale(layer_in, norm_gains[0]).astype(low)
    queries = times(normed_one, query_full).astype(low)
    keys_own = times(normed_one, key_full).astype(low)
    values_own = times(normed_one, value_full).astype(low)
    memory_keys = times(encoded, lookup_full).astype(low)
    memory_values = times(encoded, recall_full).astype(low)
    total_width = queries.shape[1]
    width = total_width // head_count
    start_state = (
        jnp.zeros((head_count, tok_rows, width), jnp.float32),
        jnp.full((head_count, tok_rows), NEG, jnp.float32),
        jnp.zeros((head_count, tok_rows), jnp.float32),
    )
    self_fold = attend_fold(queries, head_count, causal_parts, position_bias)
    self_state = self_fold(
        start_state,
        (
            lax.all_gather(keys_own, "ctx", axis=0, tiled=True),
            lax.all_gather(values_own, "ctx", axis=0, tiled=True),
        ),
        jnp.int32(0),
    )
    mixed_one, lse_one = finish(self_state)
    after_self = layer_in + join_heads(times(mixed_one, output_full))
    normed_two = rms_scale(after_self, norm_gains[1]).astype(low)
    probes = times(normed_two, probe_full).astype(low)
    cross_fold = attend_fold(probes, head_count, None, position_bias)
    cross_state = cross_fold(
        start_state,
        (
            lax.all_gather(memory_keys, "ctx", axis=0, tiled=True),
            lax.all_gather(memory_values, "ctx", axis=0, tiled=True),
        ),
        jnp.int32(0),
    )
    mixed_two, lse_two = finish(cross_state)
    after_cross = after_self + join_heads(times(mixed_two, merge_full))
    normed_three = rms_scale(after_cross, norm_gains[2]).astype(low)
    gate_pre = times(normed_three, gate_full)
    upper = times(normed_three, upward_full)
    activated = geglu(gate_pre, upper).astype(low)
    layer_out = after_cross + join_heads(times(activated, down_full))
    grad_rows = out_grad.astype(low)
    down_wgrad = left_times(activated, grad_rows)
    act_grad = right_times(grad_rows, down_full)
    geglu_out, geglu_pull = jax.vjp(geglu, gate_pre, upper)
    gate_grad, upper_grad = geglu_pull(act_grad)
    gate_grad = gate_grad.astype(low)
    upper_grad = upper_grad.astype(low)
    gate_wgrad = left_times(normed_three, gate_grad)
    up_wgrad = left_times(normed_three, upper_grad)
    normed_three_grad = join_heads(
        right_times(gate_grad, gate_full) + right_times(upper_grad, upward_full)
    )
    norm_out, norm_pull = jax.vjp(rms_scale, after_cross, norm_gains[2])
    cross_extra, gain_three = norm_pull(normed_three_grad)
    cross_grad = out_grad + cross_extra
    cross_rows = cross_grad.astype(low)
    merge_wgrad = left_times(mixed_two, cross_rows)
    mixed_two_grad = right_times(cross_rows, merge_full).astype(low)
    delta_two = delta_of(mixed_two, mixed_two_grad, head_count)
    memory_all = gather_cross(memory_keys, memory_values)
    probe_grad, unused_bias, cross_terms = attend_back(
        probes,
        mixed_two_grad,
        lse_two,
        delta_two,
        memory_all[0],
        memory_all[1],
        head_count,
        None,
        position_bias,
    )
    cross_terms = lax.psum_scatter(cross_terms, "ctx", scatter_dimension=0, tiled=True)
    memory_key_grad = cross_terms[:, :total_width].astype(low)
    memory_value_grad = cross_terms[:, total_width:].astype(low)
    probe_wgrad = left_times(normed_two, probe_grad)
    lookup_wgrad = left_times(encoded, memory_key_grad)
    recall_wgrad = left_times(encoded, memory_value_grad)
    normed_two_grad, encoded_grad = join_heads(
        (
            right_times(probe_grad, probe_full),
            right_times(memory_key_grad, lookup_full) + right_times(memory_value_grad, recall_full),
        )
    )
    norm_out, norm_pull = jax.vjp(rms_scale, after_self, norm_gains[1])
    self_extra, gain_two = norm_pull(normed_two_grad)
    self_grad = cross_grad + self_extra
    self_rows = self_grad.astype(low)
    output_wgrad = left_times(mixed_one, self_rows)
    mixed_one_grad = right_times(self_rows, output_full).astype(low)
    delta_one = delta_of(mixed_one, mixed_one_grad, head_count)
    sequence_all = gather_self(keys_own, values_own)
    query_grad, bias_grad, self_terms = attend_back(
        queries,
        mixed_one_grad,
        lse_one,
        delta_one,
        sequence_all[0],
        sequence_all[1],
        head_count,
        causal_parts,
        position_bias,
    )
    self_terms = lax.psum_scatter(self_terms, "ctx", scatter_dimension=0, tiled=True)
    key_grad = self_terms[:, :total_width].astype(low)
    value_grad = self_terms[:, total_width:].astype(low)
    query_wgrad = left_times(normed_one, query_grad)
    key_wgrad = left_times(normed_one, key_grad)
    value_wgrad = left_times(normed_one, value_grad)
    normed_one_grad = join_heads(
        right_times(query_grad, query_full)
        + right_times(key_grad, key_full)
        + right_times(value_grad, value_full)
    )
    norm_out, norm_pull = jax.vjp(rms_scale, layer_in, norm_gains[0])
    input_extra, gain_one = norm_pull(normed_one_grad)
    input_grad = self_grad + input_extra
    weight_sums = (
        lax.psum_scatter(query_wgrad, "ctx", scatter_dimension=0, tiled=True),
        lax.psum_scatter(key_wgrad, "ctx", scatter_dimension=0, tiled=True),
        lax.psum_scatter(value_wgrad, "ctx", scatter_dimension=0, tiled=True),
        lax.psum_scatter(output_wgrad, "ctx", scatter_dimension=1, tiled=True),
        lax.psum_scatter(probe_wgrad, "ctx", scatter_dimension=0, tiled=True),
        lax.psum_scatter(lookup_wgrad, "ctx", scatter_dimension=0, tiled=True),
        lax.psum_scatter(recall_wgrad, "ctx", scatter_dimension=0, tiled=True),
        lax.psum_scatter(merge_wgrad, "ctx", scatter_dimension=1, tiled=True),
        lax.psum_scatter(gate_wgrad, "ctx", scatter_dimension=0, tiled=True),
        lax.psum_scatter(up_wgrad, "ctx", scatter_dimension=0, tiled=True),
        lax.psum_scatter(down_wgrad, "ctx", scatter_dimension=1, tiled=True),
    )
    gains_sum, bias_sum = lax.psum((jnp.stack((gain_one, gain_two, gain_three)), bias_grad), "ctx")
    return (layer_out, input_grad, encoded_grad) + tuple(weight_sums) + (gains_sum, bias_sum)


def solution(mesh):
    body = quick_device if quick_fits(mesh) else per_device
    placed = (
        P("ctx", None),
        P("ctx", None),
        P("ctx", "head"),
        P("ctx", "head"),
        P("ctx", "head"),
        P("head", "ctx"),
        P("ctx", "head"),
        P("ctx", "head"),
        P("ctx", "head"),
        P("head", "ctx"),
        P("ctx", "head"),
        P("ctx", "head"),
        P("head", "ctx"),
        P(),
        P(None, "head"),
        P(),
        P(),
        P("ctx", None),
    )
    return jax.shard_map(
        body,
        mesh=mesh,
        in_specs=placed,
        out_specs=(
            P("ctx", None),
            P("ctx", None),
            P("ctx", None),
            P("ctx", "head"),
            P("ctx", "head"),
            P("ctx", "head"),
            P("head", "ctx"),
            P("ctx", "head"),
            P("ctx", "head"),
            P("ctx", "head"),
            P("head", "ctx"),
            P("ctx", "head"),
            P("ctx", "head"),
            P("head", "ctx"),
            P(),
            P(None, "head"),
        ),
        check_vma=False,
    )
```
